32 devices in a mesh: data: 32 (over z, y, x, core).
Axes of the slice: x: 2, y: 2, z: 4, core: 2. Of those that a mesh axis runs over, the one named last changes fastest.
Arguments:
- x_init: bfloat16 [128, 256, 1024], P('data')
- cot_out: bfloat16 [128, 256, 1024], P('data')
- w_query: bfloat16 [2, 1024, 1024], replicated
- w_key: bfloat16 [2, 1024, 1024], replicated
- w_value: bfloat16 [2, 1024, 1024], replicated
- w_proj: bfloat16 [2, 1024, 1024], replicated
- w_up: bfloat16 [1024, 4096], replicated
- w_down: bfloat16 [4096, 1024], replicated
Outputs:
- output 1: float32 [2, 1024, 1024], replicated
- output 2: float32 [2, 1024, 1024], replicated
- output 3: float32 [2, 1024, 1024], replicated
- output 4: float32 [2, 1024, 1024], replicated
- output 5: float32 [1024, 4096], replicated
- output 6: float32 [4096, 1024], replicated
- output 7: bfloat16 [128, 256, 1024], P('data')
All inputs are finite; a program needn't handle non-finite values.
Results may differ from the reference program's by a relative error of at most 0.0195979.
Values are sent between devices in bfloat16 or wider.
A program may use at most 1 GiB of HBM per device.

```python
import jax
import jax.numpy as jnp
from jax import lax

D = 1024
HEADS = 16
LAYERS = 2
BATCH = 128
SEQ = 256
FF = 4 * D
HEAD_DIM = D // HEADS
EPS = 1e-6


def setup_inputs(seed: int = 0) -> dict:
    keys = jax.random.split(jax.random.key(seed), 8)
    res_scale = (2.0 * LAYERS) ** -0.5
    x_init = jax.random.normal(keys[0], (BATCH, SEQ, D), jnp.float32)
    cot_out = jax.random.normal(keys[1], (BATCH, SEQ, D), jnp.float32)
    w_query = jax.random.normal(keys[2], (LAYERS, D, D), jnp.float32) * D ** -0.5
    w_key = jax.random.normal(keys[3], (LAYERS, D, D), jnp.float32) * D ** -0.5
    w_value = jax.random.normal(keys[4], (LAYERS, D, D), jnp.float32) * D ** -0.5
    w_proj = jax.random.normal(keys[5], (LAYERS, D, D), jnp.float32) * (D ** -0.5 * res_scale)
    w_up = jax.random.normal(keys[6], (D, FF), jnp.float32) * D ** -0.5
    w_down = jax.random.normal(keys[7], (FF, D), jnp.float32) * (FF ** -0.5 * res_scale)
    return {
        "x_init": x_init.astype(jnp.bfloat16),
        "cot_out": cot_out.astype(jnp.bfloat16),
        "w_query": w_query.astype(jnp.bfloat16),
        "w_key": w_key.astype(jnp.bfloat16),
        "w_value": w_value.astype(jnp.bfloat16),
        "w_proj": w_proj.astype(jnp.bfloat16),
        "w_up": w_up.astype(jnp.bfloat16),
        "w_down": w_down.astype(jnp.bfloat16),
    }


def rms_norm(x_f32):
    return x_f32 * lax.rsqrt(jnp.mean(x_f32 * x_f32, axis=-1, keepdims=True) + EPS)


def as_bf16(val_f32):
    return val_f32.astype(jnp.bfloat16).astype(jnp.float32)


def layer_fwd(x_seq, w_query, w_key, w_value, w_proj, w_up, w_down):
    x_f32 = x_seq.astype(jnp.float32)
    normed = as_bf16(rms_norm(x_f32))
    query = as_bf16(jnp.dot(normed, w_query, preferred_element_type=jnp.float32)).reshape(SEQ, HEADS, HEAD_DIM)
    key_act = as_bf16(jnp.dot(normed, w_key, preferred_element_type=jnp.float32)).reshape(SEQ, HEADS, HEAD_DIM)
    value = as_bf16(jnp.dot(normed, w_value, preferred_element_type=jnp.float32)).reshape(SEQ, HEADS, HEAD_DIM)
    scores = jnp.einsum("qhd,khd->hqk", query, key_act) * HEAD_DIM ** -0.5
    probs = as_bf16(jax.nn.softmax(scores, axis=-1))
    mixed = as_bf16(jnp.einsum("hqk,khd->qhd", probs, value)).reshape(SEQ, D)
    hidden = as_bf16(x_f32 + as_bf16(jnp.dot(mixed, w_proj, preferred_element_type=jnp.float32)))
    normed2 = as_bf16(rms_norm(hidden))
    pre_act = as_bf16(jnp.dot(normed2, w_up, preferred_element_type=jnp.float32))
    activated = as_bf16(jax.nn.gelu(pre_act, approximate=True))
    mlp_out = as_bf16(jnp.dot(activated, w_down, preferred_element_type=jnp.float32))
    return (hidden + mlp_out).astype(jnp.bfloat16)


layer_ckpt = jax.checkpoint(layer_fwd)


def stack_fwd(x_seq, w_query, w_key, w_value, w_proj, w_up, w_down):
    def layer_step(x_carry, layer_w):
        x_new = layer_ckpt(x_carry, layer_w[0], layer_w[1], layer_w[2], layer_w[3], w_up, w_down)
        return x_new, None

    return lax.scan(layer_step, x_seq, (w_query, w_key, w_value, w_proj))[0]


def reference(x_init, cot_out, w_query, w_key, w_value, w_proj, w_up, w_down):
    weights = (
        w_query.astype(jnp.float32),
        w_key.astype(jnp.float32),
        w_value.astype(jnp.float32),
        w_proj.astype(jnp.float32),
        w_up.astype(jnp.float32),
        w_down.astype(jnp.float32),
    )
    zero_sums = tuple(jnp.zeros_like(weight) for weight in weights)

    def per_sequence(grad_sums, seq_pair):
        pull_back = jax.vjp(stack_fwd, seq_pair[0], *weights)[1]
        seq_grads = pull_back(seq_pair[1])
        new_sums = tuple(total + part for total, part in zip(grad_sums, seq_grads[1:]))
        return new_sums, seq_grads[0]

    grad_sums, dx_init = lax.scan(per_sequence, zero_sums, (x_init, cot_out))
    return (grad_sums[0], grad_sums[1], grad_sums[2], grad_sums[3], grad_sums[4], grad_sums[5], dx_init)
```

```python
import functools

import jax
import jax.numpy as jnp
from jax import lax
from jax.experimental import pallas as pl
from jax.experimental.pallas import tpu as pltpu
from jax.sharding import PartitionSpec as P

EPS = 1e-6
HEAD_DIM = 64


def rms_norm(x_f32):
    return x_f32 * lax.rsqrt(jnp.mean(x_f32 * x_f32, axis=-1, keepdims=True) + EPS)


def gelu_tanh(pre_f32):
    return jax.nn.gelu(pre_f32, approximate=True)


def product(subscripts, lhs, rhs):
    return jnp.einsum(subscripts, lhs, rhs, preferred_element_type=jnp.float32)


def layer_forward(x_act, w_query, w_key, w_value, w_proj, w_up, w_down, heads):
    batch, seq_len, width = x_act.shape
    head_dim = width // heads
    x_f32 = x_act.astype(jnp.float32)
    normed = rms_norm(x_f32).astype(jnp.bfloat16)
    query = product("bsd,de->bse", normed, w_query).astype(jnp.bfloat16).reshape(batch, seq_len, heads, head_dim)
    key_act = product("bsd,de->bse", normed, w_key).astype(jnp.bfloat16).reshape(batch, seq_len, heads, head_dim)
    value = product("bsd,de->bse", normed, w_value).astype(jnp.bfloat16).reshape(batch, seq_len, heads, head_dim)
    scores = product("bqhd,bkhd->bhqk", query, key_act) * head_dim ** -0.5
    probs = jax.nn.softmax(scores, axis=-1).astype(jnp.bfloat16)
    mixed = product("bhqk,bkhd->bqhd", probs, value).astype(jnp.bfloat16).reshape(batch, seq_len, width)
    attn_out = product("bsd,de->bse", mixed, w_proj).astype(jnp.bfloat16)
    hidden = (x_f32 + attn_out.astype(jnp.float32)).astype(jnp.bfloat16)
    normed2 = rms_norm(hidden.astype(jnp.float32)).astype(jnp.bfloat16)
    pre_act = product("bsd,df->bsf", normed2, w_up).astype(jnp.bfloat16)
    activated = gelu_tanh(pre_act.astype(jnp.float32)).astype(jnp.bfloat16)
    mlp_out = product("bsf,fd->bsd", activated, w_down).astype(jnp.bfloat16)
    x_next = (hidden.astype(jnp.float32) + mlp_out.astype(jnp.float32)).astype(jnp.bfloat16)
    kept = (x_act, normed, query, key_act, value, probs, mixed, hidden, normed2, pre_act, activated)
    return x_next, kept


def layer_backward(d_next, kept, w_query, w_key, w_value, w_proj, w_up, w_down):
    x_act, normed, query, key_act, value, probs, mixed, hidden, normed2, pre_act, activated = kept
    batch, seq_len, heads, head_dim = query.shape
    width = heads * head_dim
    d_activated = product("bsd,fd->bsf", d_next, w_down).astype(jnp.bfloat16)
    gelu_pull = jax.vjp(gelu_tanh, pre_act.astype(jnp.float32))[1]
    d_pre = gelu_pull(d_activated.astype(jnp.float32))[0].astype(jnp.bfloat16)
    d_normed2 = product("bsf,df->bsd", d_pre, w_up).astype(jnp.bfloat16)
    hidden_pull = jax.vjp(rms_norm, hidden.astype(jnp.float32))[1]
    d_hidden = (d_next.astype(jnp.float32) + hidden_pull(d_normed2.astype(jnp.float32))[0]).astype(jnp.bfloat16)
    d_mixed = product("bse,de->bsd", d_hidden, w_proj).astype(jnp.bfloat16).reshape(batch, seq_len, heads, head_dim)
    d_probs = product("bqhd,bkhd->bhqk", d_mixed, value).astype(jnp.bfloat16).astype(jnp.float32)
    d_value = product("bhqk,bqhd->bkhd", probs, d_mixed).astype(jnp.bfloat16).reshape(batch, seq_len, width)
    probs_f32 = probs.astype(jnp.float32)
    row_dot = jnp.sum(d_probs * probs_f32, axis=-1, keepdims=True)
    d_scores = (probs_f32 * (d_probs - row_dot) * head_dim ** -0.5).astype(jnp.bfloat16)
    d_query = product("bhqk,bkhd->bqhd", d_scores, key_act).astype(jnp.bfloat16).reshape(batch, seq_len, width)
    d_key = product("bhqk,bqhd->bkhd", d_scores, query).astype(jnp.bfloat16).reshape(batch, seq_len, width)
    d_normed = (product("bse,de->bsd", d_query, w_query) + product("bse,de->bsd", d_key, w_key)
                + product("bse,de->bsd", d_value, w_value)).astype(jnp.bfloat16)
    input_pull = jax.vjp(rms_norm, x_act.astype(jnp.float32))[1]
    d_input = (d_hidden.astype(jnp.float32) + input_pull(d_normed.astype(jnp.float32))[0]).astype(jnp.bfloat16)
    attn = (normed, d_query, d_key, d_value, mixed, d_hidden)
    mlp = (normed2, d_pre, activated, d_next)
    flat = lambda arr: arr.reshape(batch * seq_len, -1)
    return d_input, tuple(map(flat, attn)), tuple(map(flat, mlp))


MESH = pl.DeviceIdType.MESH
LANES = 1024
SET_ROWS = 128
CORE_ROWS = 2 * SET_ROWS
TILE_ROWS = 2 * CORE_ROWS
OWN_SLOTS = 8
AG_SLOTS = 10
TYPES = {
    "p1": (0, 0, 80, "xyz"),
    "q1": (0, 80, 48, "zxy"),
    "p2": (1, 128, 80, "yxz"),
    "q2": (1, 208, 48, "zyx"),
}
WRITE_AT = 11


def stage_list():
    stages = []
    for name, (_, _, _, order) in TYPES.items():
        if order[2] == "z":
            plan = [("rs1", 1), ("rs2", 2), ("rsz", 3), ("agz", 6), ("ag2", 9), ("ag1", 10)]
        else:
            plan = [("rsz", 1), ("rs1", 4), ("rs2", 5), ("ag2", 6), ("ag1", 7), ("agz", 8)]
        for kind, at in plan:
            if kind in ("rsz", "agz"):
                for step in range(3):
                    for way in (0, 1):
                        stages.append((name, kind, step, way, at + step))
            else:
                stages.append((name, kind, 0, 0, at))
    return stages


STAGES = stage_list()


def piece_shape(name, kind):
    rows, order = TYPES[name][2], TYPES[name][3]
    if order[2] == "z":
        return {"rs1": (rows, 512), "rs2": (rows, 256), "rsz": (rows // 2, 128)}[kind]
    return {"rsz": (rows // 2, 512), "rs1": (rows // 2, 256), "rs2": (rows // 2, 128)}[kind]


def reduce_kernel(groups, chunks, n_in, n_out, *refs):
    ins, outs, scratch = refs[:n_in], refs[n_in:n_in + n_out], refs[n_in + n_out:]
    (lhs_buf, rhs_buf, own, part, part_in, gath), scratch = scratch[:6], scratch[6:]
    land_keys = [key for key, st in enumerate(STAGES) if st[1].startswith("rs")]
    landing = dict(zip(land_keys, scratch[:len(land_keys)]))
    load_sem, send_sem, recv_sem, pair_send, pair_recv, out_sem, out_send, out_recv, credit = scratch[len(land_keys):]

    me = lax.axis_index("data")
    core = lax.rem(me, 2)
    coord = {"x": lax.rem(lax.div(me, 2), 2), "y": lax.rem(lax.div(me, 4), 2)}
    z = lax.div(me, 8)
    partner = me + 1 - 2 * core
    near = {"x": me + 2 - 4 * coord["x"], "y": me + 4 - 8 * coord["y"]}
    up_ok, down_ok = z < 3, z > 0
    peers = [(partner, 0, None), (near["x"], 1, None), (near["y"], 2, None), (me + 8, 3, up_ok), (me - 8, 4, down_ok)]

    def guarded(cond, fn):
        if cond is None:
            fn()
        else:
            pl.when(cond)(fn)

    barrier = pltpu.get_barrier_semaphore()
    for dev, _, cond in peers:
        guarded(cond, lambda dev=dev: pl.semaphore_signal(barrier, inc=1, device_id=(dev,), device_id_type=MESH))
    inner = jnp.logical_and(up_ok, down_ok)
    guarded(inner, lambda: pl.semaphore_wait(barrier, 5))
    guarded(jnp.logical_not(inner), lambda: pl.semaphore_wait(barrier, 4))

    def region(name, kind, which):
        _, row, rows, order = TYPES[name]
        if order[2] == "z":
            h1, h2 = coord[order[0]], coord[order[1]]
            if kind == "1":
                return pl.ds(row, rows), pl.ds(pl.multiple_of(512 * which, 128), 512)
            if kind == "2":
                return pl.ds(row, rows), pl.ds(pl.multiple_of(512 * h1 + 256 * which, 128), 256)
            first = pl.multiple_of(row + (rows // 2) * lax.div(which, 2), 8)
            lane = pl.multiple_of(512 * h1 + 256 * h2 + 128 * lax.rem(which, 2), 128)
            return pl.ds(first, rows // 2), pl.ds(lane, 128)
        h1 = coord[order[1]]
        if kind == "z":
            first = pl.multiple_of(row + (rows // 2) * lax.div(which, 2), 8)
            return pl.ds(first, rows // 2), pl.ds(pl.multiple_of(512 * lax.rem(which, 2), 128), 512)
        first = pl.multiple_of(row + (rows // 2) * lax.div(z, 2), 8)
        if kind == "1":
            return pl.ds(first, rows // 2), pl.ds(pl.multiple_of(512 * lax.rem(z, 2) + 256 * which, 128), 256)
        lane = pl.multiple_of(512 * lax.rem(z, 2) + 256 * h1 + 128 * which, 128)
        return pl.ds(first, rows // 2), pl.ds(lane, 128)

    def exchange_axis(name, kind):
        order = TYPES[name][3]
        dims = order[:2] if order[2] == "z" else order[1:]
        return dims[int(kind) - 1]

    def plan(key, chunk, parity):
        name, kind, step, way, _ = STAGES[key]
        mine, slot = lax.rem(chunk, OWN_SLOTS), lax.rem(chunk, AG_SLOTS)
        if kind in ("rs1", "rs2"):
            axis = exchange_axis(name, kind[2])
            src, keep = region(name, kind[2], 1 - coord[axis]), region(name, kind[2], coord[axis])
            dev, send_ok, recv_ok = near[axis], None, None
            sent = own.at[mine, src[0], src[1]]
        elif kind in ("ag1", "ag2"):
            axis = exchange_axis(name, kind[2])
            src = keep = region(name, kind[2], coord[axis])
            dev, send_ok, recv_ok = near[axis], None, None
            sent = gath.at[slot, src[0], src[1]]
        elif kind == "rsz":
            if way:
                dev, k_send, k_keep = me + 8, z + 3 - step, z + 2 - step
                send_ok, recv_ok = k_send <= 3, jnp.logical_and(k_keep <= 3, down_ok)
            else:
                dev, k_send, k_keep = me - 8, z - 3 + step, z - 2 + step
                send_ok, recv_ok = k_send >= 0, jnp.logical_and(k_keep >= 0, up_ok)
            src, keep = region(name, "z", k_send), region(name, "z", k_keep)
            sent = own.at[mine, src[0], src[1]]
        else:
            if way:
                dev, k_send, k_keep = me + 8, z - step, z - 1 - step
                send_ok, recv_ok = jnp.logical_and(k_send >= 0, up_ok), k_keep >= 0
            else:
                dev, k_send, k_keep = me - 8, z + step, z + 1 + step
                send_ok, recv_ok = jnp.logical_and(k_send <= 3, down_ok), k_keep <= 3
            src, keep = region(name, "z", k_send), region(name, "z", k_keep)
            sent = gath.at[slot, src[0], src[1]]
        sems = dict(send_sem=send_sem.at[key], recv_sem=recv_sem.at[key, parity], device_id=(dev,), device_id_type=MESH)
        if kind.startswith("rs"):
            target = landing[key].at[parity]
            send = lambda: pltpu.make_async_remote_copy(src_ref=sent, dst_ref=target, **sems)
            recv = lambda: pltpu.make_async_remote_copy(
                src_ref=own.at[mine, keep[0], keep[1]], dst_ref=target, **sems)

            def arrive():
                own[mine, keep[0], keep[1]] += landing[key][parity]
        else:
            send = lambda: pltpu.make_async_remote_copy(src_ref=sent, dst_ref=sent, **sems)
            recv = lambda: pltpu.make_async_remote_copy(
                src_ref=gath.at[slot, keep[0], keep[1]], dst_ref=gath.at[slot, keep[0], keep[1]], **sems)
            arrive = None
        return send, recv, send_ok, recv_ok, arrive

    def finish(name, chunk):
        order = TYPES[name][3]
        reg = region(name, "z", z) if order[2] == "z" else region(name, "2", coord[order[2]])
        gath[lax.rem(chunk, AG_SLOTS), reg[0], reg[1]] = own[lax.rem(chunk, OWN_SLOTS), reg[0], reg[1]]

    def valid(chunk):
        return jnp.logical_and(chunk >= 0, chunk < chunks)

    def set_rows(half):
        return pl.ds(half * SET_ROWS, SET_ROWS)

    def pair_copy(half, parity):
        return pltpu.make_async_remote_copy(
            src_ref=part.at[parity, set_rows(half)], dst_ref=part_in.at[parity, set_rows(half)],
            send_sem=pair_send.at[half], recv_sem=pair_recv.at[half, parity], device_id=(partner,), device_id_type=MESH)

    def out_copies(half, group, local, whose):
        out, layer = group["out"]
        ref = outs[out] if layer is None else outs[out].at[layer]
        rows, cols = group["place"](local)
        first = pl.multiple_of(rows + CORE_ROWS * whose + half * SET_ROWS, SET_ROWS)
        return ref.at[pl.ds(first, SET_ROWS), pl.ds(pl.multiple_of(cols, 128), LANES)]

    def write_copies(half, chunk, dest):
        slot = lax.rem(chunk, AG_SLOTS)
        src = gath.at[slot, set_rows(half)]
        here = pltpu.make_async_copy(src, dest, out_sem.at[half])
        there = pltpu.make_async_remote_copy(
            src_ref=src, dst_ref=dest, send_sem=out_send.at[half], recv_sem=out_recv.at[half, lax.rem(chunk, 2)],
            device_id=(partner,), device_id_type=MESH)
        return here, there

    def load_copies(group, local, slot):
        rows, cols = group["place"](local)
        copies = []
        for app, (lhs, rhs) in enumerate(zip(group["lhs"], group["rhs"])):
            for whose in (0, 1):
                first = rows + CORE_ROWS * (core if whose == 0 else 1 - core)
                copies.append(pltpu.make_async_copy(
                    ins[lhs].at[:, pl.ds(pl.multiple_of(first, CORE_ROWS), CORE_ROWS)],
                    lhs_buf.at[slot, app, whose], load_sem.at[slot, app, whose]))
            copies.append(pltpu.make_async_copy(
                ins[rhs].at[:, pl.ds(pl.multiple_of(cols, 128), LANES)], rhs_buf.at[slot, app], load_sem.at[slot, app, 2]))
        return copies

    def for_group(chunk, fn):
        for group in groups:
            inside = jnp.logical_and(chunk >= group["start"], chunk < group["start"] + group["count"])
            pl.when(inside)(functools.partial(fn, group, chunk - group["start"]))

    def two_apps(chunk):
        flags = [jnp.logical_and(chunk >= g["start"], chunk < g["start"] + g["count"]) for g in groups if len(g["lhs"]) == 2]
        return functools.reduce(jnp.logical_or, flags)

    def start_load(chunk):
        def go(group, local):
            for copy in load_copies(group, local, lax.rem(chunk, 2)):
                copy.start()
        for_group(chunk, go)

    def wait_load(chunk):
        slot = lax.rem(chunk, 2)
        any_two = next(g for g in groups if len(g["lhs"]) == 2)
        copies = load_copies(any_two, 0, slot)
        for copy in copies[:3]:
            copy.wait()

        @pl.when(two_apps(chunk))
        def _():
            for copy in copies[3:]:
                copy.wait()

    def tile(chunk):
        slot, mine, parity = lax.rem(chunk, 2), lax.rem(chunk, OWN_SLOTS), lax.rem(chunk, 2)

        def product(app, whose):
            return lax.dot_general(lhs_buf[slot, app, whose], rhs_buf[slot, app], (((0,), (0,)), ((), ())),
                                   preferred_element_type=jnp.float32)

        own[mine] = product(0, 0)
        part[parity] = product(0, 1)

        @pl.when(two_apps(chunk))
        def _():
            own[mine] += product(1, 0)
            part[parity] += product(1, 1)

    last = chunks + WRITE_AT

    def section(half, step):
        before = lax.rem(step + 1, 2)
        now = lax.rem(step, 2)

        @pl.when(valid(step - 1))
        def _():
            copy = pair_copy(half, before)
            copy.wait_send()
            copy.wait_recv()
            mine = lax.rem(step - 1, OWN_SLOTS)
            own[mine, set_rows(half)] += part_in[before, set_rows(half)]

        names = [name for name in TYPES if TYPES[name][0] == half]
        keys = [key for key, st in enumerate(STAGES) if st[0] in names]
        finals = {name: max(st[4] for st in STAGES if st[0] == name and st[1].startswith("rs")) for name in names}
        for key in keys:
            name, at = STAGES[key][0], STAGES[key][4]
            chunk = step - 1 - at

            @pl.when(valid(chunk))
            def _(key=key, chunk=chunk):
                send, recv, send_ok, recv_ok, arrive = plan(key, chunk, before)

                def arrived():
                    recv().wait_recv()
                    if arrive is not None:
                        arrive()
                guarded(recv_ok, arrived)
                guarded(send_ok, lambda: send().wait_send())
        for name in names:
            chunk = step - 1 - finals[name]
            pl.when(valid(chunk))(functools.partial(finish, name, chunk))

        done = step - 1 - WRITE_AT

        @pl.when(valid(done))
        def _():
            here, there = write_copies(half, done, out_copies(half, groups[0], 0, 0))
            here.wait()
            there.wait_send()
            there.wait_recv()

        @pl.when(step < last)
        def _():
            for dev, way, cond in peers:
                to = way if way < 3 else 7 - way
                guarded(cond, lambda dev=dev, to=to: pl.semaphore_signal(
                    credit.at[half, to], inc=1, device_id=(dev,), device_id_type=MESH))

        @pl.when(step > 0)
        def _():
            for dev, way, cond in peers:
                guarded(cond, lambda way=way: pl.semaphore_wait(credit.at[half, way], 1))

        for key in reversed(keys):
            chunk = step - STAGES[key][4]

            @pl.when(valid(chunk))
            def _(key=key, chunk=chunk):
                send, recv, send_ok, recv_ok, arrive = plan(key, chunk, now)
                guarded(send_ok, lambda: send().start())

        out_chunk = step - WRITE_AT

        @pl.when(valid(out_chunk))
        def _():
            def go(group, local):
                for copy in write_copies(half, out_chunk, out_copies(half, group, local, core)):
                    copy.start()
            for_group(out_chunk, go)

    start_load(jnp.int32(0))

    def round_(step, carry):
        section(0, step)

        @pl.when(valid(step))
        def _():
            pl.when(step + 1 < chunks)(lambda: start_load(step + 1))
            wait_load(step)
            tile(step)
            pair_copy(0, lax.rem(step, 2)).start()

        section(1, step)

        @pl.when(valid(step))
        def _():
            pair_copy(1, lax.rem(step, 2)).start()

        return carry

    lax.fori_loop(0, last + 1, round_, 0)


def reduce_gradients(operands, groups, chunks, out_shapes, tokens, collective_id=0):
    landing = [pltpu.VMEM((2,) + piece_shape(st[0], st[1]), jnp.float32) for st in STAGES if st[1].startswith("rs")]
    apps = max(len(g["lhs"]) for g in groups)
    scratch = [
        pltpu.VMEM((2, apps, 2, tokens, CORE_ROWS), jnp.bfloat16),
        pltpu.VMEM((2, apps, tokens, LANES), jnp.bfloat16),
        pltpu.VMEM((OWN_SLOTS, CORE_ROWS, LANES), jnp.float32),
        pltpu.VMEM((2, CORE_ROWS, LANES), jnp.float32),
        pltpu.VMEM((2, CORE_ROWS, LANES), jnp.float32),
        pltpu.VMEM((AG_SLOTS, CORE_ROWS, LANES), jnp.float32),
        *landing,
        pltpu.SemaphoreType.DMA((2, apps, 3)),
        pltpu.SemaphoreType.DMA((len(STAGES),)),
        pltpu.SemaphoreType.DMA((len(STAGES), 2)),
        pltpu.SemaphoreType.DMA((2,)),
        pltpu.SemaphoreType.DMA((2, 2)),
        pltpu.SemaphoreType.DMA((2,)),
        pltpu.SemaphoreType.DMA((2,)),
        pltpu.SemaphoreType.DMA((2, 2)),
        pltpu.SemaphoreType.REGULAR((2, 5)),
    ]
    flops = sum(2 * g["count"] * len(g["lhs"]) * TILE_ROWS * LANES * tokens for g in groups)
    return pl.pallas_call(
        functools.partial(reduce_kernel, groups, chunks, len(operands), len(out_shapes)),
        out_shape=[jax.ShapeDtypeStruct(shape, jnp.float32) for shape in out_shapes],
        in_specs=[pl.BlockSpec(memory_space=pl.ANY)] * len(operands),
        out_specs=[pl.BlockSpec(memory_space=pl.ANY)] * len(out_shapes),
        scratch_shapes=scratch,
        compiler_params=pltpu.CompilerParams(
            collective_id=collective_id, has_side_effects=True, vmem_limit_bytes=60 * 1024 * 1024),
        cost_estimate=pl.CostEstimate(flops=flops, bytes_accessed=128 * 1024 * 1024, transcendentals=0),
        name="reduce_gradients",
    )(*operands)

def gradient_groups(width, ff):
    groups = []

    def add(count, lhs, rhs, out, place):
        start = groups[-1]["start"] + groups[-1]["count"] if groups else 0
        groups.append(dict(start=start, count=count, lhs=lhs, rhs=rhs, out=out, place=place))

    def tall(local):
        return TILE_ROWS * local, 0

    def wide(local):
        return TILE_ROWS * lax.rem(local, width // TILE_ROWS), LANES * lax.div(local, width // TILE_ROWS)

    def attention(layer):
        base = 6 * layer
        for out in range(3):
            add(width // TILE_ROWS, [base], [base + 1 + out], (out, layer), tall)
        add(width // TILE_ROWS, [base + 4], [base + 5], (3, layer), tall)

    attention(1)
    add(ff // TILE_ROWS, [14, 18], [15, 19], (5, None), tall)
    add(ff // TILE_ROWS, [12, 16], [13, 17], (4, None), wide)
    attention(0)
    return groups, sum(group["count"] for group in groups)


def solution(mesh):
    def local_step(x_init, cot_out, w_query, w_key, w_value, w_proj, w_up, w_down):
        batch, seq_len, width = x_init.shape
        heads = width // HEAD_DIM
        x_act = x_init
        kept_all = []
        for layer in range(2):
            x_act, kept = layer_forward(x_act, w_query[layer], w_key[layer], w_value[layer], w_proj[layer], w_up, w_down, heads)
            kept_all.append(kept)
        d_act = cot_out
        attn, mlp = [None] * 2, [None] * 2
        for layer in (1, 0):
            d_act, attn[layer], mlp[layer] = layer_backward(
                d_act, kept_all[layer], w_query[layer], w_key[layer], w_value[layer], w_proj[layer], w_up, w_down)
        operands = [*attn[0], *attn[1], *mlp[0], *mlp[1]]
        groups, chunks = gradient_groups(width, w_up.shape[1])
        shapes = [w_query.shape, w_key.shape, w_value.shape, w_proj.shape, w_up.shape, w_down.shape]
        grads = reduce_gradients(operands, groups, chunks, shapes, batch * seq_len)
        return (*grads, d_act)

    data_spec = P("data")
    full_spec = P()
    in_specs = (data_spec, data_spec, full_spec, full_spec, full_spec, full_spec, full_spec, full_spec)
    out_specs = (full_spec, full_spec, full_spec, full_spec, full_spec, full_spec, data_spec)
    return jax.shard_map(local_step, mesh=mesh, in_specs=in_specs, out_specs=out_specs, check_vma=False)
```

```python
import functools

import jax
import jax.numpy as jnp
from jax import lax
from jax.experimental import pallas as pl
from jax.experimental.pallas import tpu as pltpu
from jax.sharding import PartitionSpec as P

EPS = 1e-6
HEAD_DIM = 64
PAIR = 2 * HEAD_DIM
FF_BLOCK = 512
OUT_BLOCK = 256
GELU_A = (2.0 / 3.141592653589793) ** 0.5
GELU_B = 0.044715
MIB = 1024 * 1024


def dot(lhs, rhs, lhs_dim, rhs_dim):
    return lax.dot_general(lhs, rhs, (((lhs_dim,), (rhs_dim,)), ((), ())), preferred_element_type=jnp.float32)


def rms_norm(x_f32):
    return x_f32 * lax.rsqrt(jnp.mean(x_f32 * x_f32, axis=-1, keepdims=True) + EPS)


def rms_backward(x_f32, d_out):
    scale = lax.rsqrt(jnp.mean(x_f32 * x_f32, axis=-1, keepdims=True) + EPS)
    inner = jnp.mean(x_f32 * d_out, axis=-1, keepdims=True)
    return scale * d_out - x_f32 * (scale * scale * scale * inner)


def gelu_parts(pre):
    square = pre * pre
    tanh = jnp.tanh(GELU_A * (pre + GELU_B * pre * square))
    half = 0.5 * (1.0 + tanh)
    slope = half + 0.5 * pre * (1.0 - tanh * tanh) * (GELU_A + (3.0 * GELU_A * GELU_B) * square)
    return pre * half, slope


def call(kernel, grid, in_specs, outs, scratch=(), flops=0, moved=0, name=None):
    return pl.pallas_call(
        kernel,
        grid=grid,
        in_specs=in_specs,
        out_specs=[spec for _, spec in outs],
        out_shape=[shape for shape, _ in outs],
        scratch_shapes=list(scratch),
        compiler_params=pltpu.CompilerParams(vmem_limit_bytes=60 * MIB, dimension_semantics=("arbitrary",) * len(grid)),
        cost_estimate=pl.CostEstimate(flops=flops, bytes_accessed=moved, transcendentals=0),
        name=name,
    )


def whole(shape):
    return pl.BlockSpec(shape, lambda *_: (0,) * len(shape), pipeline_mode=pl.Buffered(1))


def bf16(*shape):
    return jax.ShapeDtypeStruct(shape, jnp.bfloat16)


def project_qkv(x_act, w_query, w_key, w_value, layer):
    tokens, width = x_act.shape

    def kernel(x_ref, wq_ref, wk_ref, wv_ref, u_ref, q_ref, k_ref, v_ref):
        @pl.when(pl.program_id(0) == 0)
        def _():
            u_ref[...] = rms_norm(x_ref[...].astype(jnp.float32)).astype(jnp.bfloat16)

        for w_ref, o_ref in ((wq_ref, q_ref), (wk_ref, k_ref), (wv_ref, v_ref)):
            o_ref[...] = dot(u_ref[...], w_ref[...], 1, 0).astype(jnp.bfloat16)

    weight = pl.BlockSpec((None, width, OUT_BLOCK), lambda i: (layer, 0, i))
    block = pl.BlockSpec((tokens, OUT_BLOCK), lambda i: (0, i))
    return call(
        kernel, (width // OUT_BLOCK,), [whole((tokens, width)), weight, weight, weight],
        [(bf16(tokens, width), whole((tokens, width)))] + [(bf16(tokens, width), block)] * 3,
        flops=6 * tokens * width * width, moved=14 * tokens * width, name=f"qkv_{layer}")(x_act, w_query, w_key, w_value)


def attend(x_act, query, key_act, value, w_proj, layer, seq):
    tokens, width = x_act.shape
    heads = width // HEAD_DIM

    def kernel(x_ref, q_ref, k_ref, v_ref, wo_ref, p_ref, mix_ref, h_ref, n_ref):
        low = lax.broadcasted_iota(jnp.int32, (seq, PAIR), 1) < HEAD_DIM

        def pair(j, carry):
            lanes = pl.ds(pl.multiple_of(PAIR * j, PAIR), PAIR)
            q_pair, k_pair, v_pair = q_ref[:, lanes], k_ref[:, lanes], v_ref[:, lanes]
            total = None
            for side in range(2):
                mask = low if side == 0 else jnp.logical_not(low)
                scores = dot(jnp.where(mask, q_pair, 0), k_pair, 1, 1) * HEAD_DIM ** -0.5
                top = jnp.max(scores, axis=-1, keepdims=True)
                raised = jnp.exp(scores - top)
                inverse = 1.0 / jnp.sum(raised, axis=-1, keepdims=True)
                probs = (raised * inverse).astype(jnp.bfloat16)
                p_ref[2 * j + side] = probs
                part = dot(probs, jnp.where(mask, v_pair, 0), 1, 0)
                total = part if total is None else total + part
            mix_ref[:, lanes] = total.astype(jnp.bfloat16)
            return carry

        lax.fori_loop(0, heads // 2, pair, 0)
        attn = dot(mix_ref[...], wo_ref[...], 1, 0).astype(jnp.bfloat16)
        hidden = (x_ref[...].astype(jnp.float32) + attn.astype(jnp.float32)).astype(jnp.bfloat16)
        h_ref[...] = hidden
        n_ref[...] = rms_norm(hidden.astype(jnp.float32)).astype(jnp.bfloat16)

    row = pl.BlockSpec((seq, width), lambda i: (i, 0))
    weight = pl.BlockSpec((None, width, width), lambda i: (layer, 0, 0), pipeline_mode=pl.Buffered(1))
    probs = pl.BlockSpec((None, heads, seq, seq), lambda i: (i, 0, 0, 0))
    act = (bf16(tokens, width), row)
    return call(
        kernel, (tokens // seq,), [row, row, row, row, weight], [(bf16(tokens // seq, heads, seq, seq), probs), act, act, act],
        flops=2 * tokens * width * (width + 2 * seq), moved=20 * tokens * width, name=f"attend_{layer}",
    )(x_act, query, key_act, value, w_proj)


def mlp_forward(hidden, normed2, w_up, w_down):
    tokens, width = hidden.shape
    ff = w_up.shape[1]
    steps = ff // FF_BLOCK

    def kernel(h_ref, n_ref, w1_ref, w2_ref, pre_ref, act_ref, x_ref, acc_ref):
        i = pl.program_id(0)
        pre = dot(n_ref[...], w1_ref[...], 1, 0).astype(jnp.bfloat16)
        pre_ref[...] = pre
        act = gelu_parts(pre.astype(jnp.float32))[0].astype(jnp.bfloat16)
        act_ref[...] = act
        part = dot(act, w2_ref[...], 1, 0)

        @pl.when(i == 0)
        def _():
            acc_ref[...] = part

        @pl.when(i > 0)
        def _():
            acc_ref[...] += part

        @pl.when(i == steps - 1)
        def _():
            out = acc_ref[...].astype(jnp.bfloat16).astype(jnp.float32)
            x_ref[...] = (h_ref[...].astype(jnp.float32) + out).astype(jnp.bfloat16)

    full = whole((tokens, width))
    up = pl.BlockSpec((width, FF_BLOCK), lambda i: (0, i))
    down = pl.BlockSpec((FF_BLOCK, width), lambda i: (i, 0))
    wide = pl.BlockSpec((tokens, FF_BLOCK), lambda i: (0, i))
    return call(
        kernel, (steps,), [full, full, up, down],
        [(bf16(tokens, ff), wide), (bf16(tokens, ff), wide), (bf16(tokens, width), full)],
        [pltpu.VMEM((tokens, width), jnp.float32)], flops=4 * tokens * width * ff, moved=4 * tokens * ff + 4 * width * ff,
        name="mlp_forward")(hidden, normed2, w_up, w_down)


def mlp_backward(d_next, hidden, feed, w_up, w_down, replay, name):
    tokens, width = hidden.shape
    ff = w_up.shape[1]
    steps = ff // FF_BLOCK

    def kernel(d_ref, h_ref, feed_ref, w1_ref, w2_ref, *refs):
        outs, acc_ref = refs[:-1], refs[-1]
        i = pl.program_id(0)
        if replay:
            pre = dot(feed_ref[...], w1_ref[...], 1, 0).astype(jnp.bfloat16)
        else:
            pre = feed_ref[...]
        act, slope = gelu_parts(pre.astype(jnp.float32))
        if replay:
            outs[2][...] = act.astype(jnp.bfloat16)
        d_act = dot(d_ref[...], w2_ref[...], 1, 1).astype(jnp.bfloat16)
        d_pre = (d_act.astype(jnp.float32) * slope).astype(jnp.bfloat16)
        outs[0][...] = d_pre
        part = dot(d_pre, w1_ref[...], 1, 1)

        @pl.when(i == 0)
        def _():
            acc_ref[...] = part

        @pl.when(i > 0)
        def _():
            acc_ref[...] += part

        @pl.when(i == steps - 1)
        def _():
            d_normed = acc_ref[...].astype(jnp.bfloat16).astype(jnp.float32)
            back = rms_backward(h_ref[...].astype(jnp.float32), d_normed)
            outs[1][...] = (d_ref[...].astype(jnp.float32) + back).astype(jnp.bfloat16)

    full = whole((tokens, width))
    up = pl.BlockSpec((width, FF_BLOCK), lambda i: (0, i))
    down = pl.BlockSpec((FF_BLOCK, width), lambda i: (i, 0))
    wide = pl.BlockSpec((tokens, FF_BLOCK), lambda i: (0, i))
    outs = [(bf16(tokens, ff), wide), (bf16(tokens, width), full)] + ([(bf16(tokens, ff), wide)] if replay else [])
    return call(
        kernel, (steps,), [full, full, full if replay else wide, up, down], outs,
        [pltpu.VMEM((tokens, width), jnp.float32)], flops=(6 if replay else 4) * tokens * width * ff,
        moved=4 * tokens * ff + 4 * width * ff, name=name)(d_next, hidden, feed, w_up, w_down)


def attend_backward(d_hidden, query, key_act, value, probs, w_proj, layer, seq):
    tokens, width = d_hidden.shape
    heads = width // HEAD_DIM

    def kernel(d_ref, q_ref, k_ref, v_ref, p_ref, wo_ref, dq_ref, dk_ref, dv_ref, mix_ref):
        mix_ref[...] = dot(d_ref[...], wo_ref[...], 1, 1).astype(jnp.bfloat16)
        low = lax.broadcasted_iota(jnp.int32, (seq, PAIR), 1) < HEAD_DIM

        def pair(j, carry):
            lanes = pl.ds(pl.multiple_of(PAIR * j, PAIR), PAIR)
            q_pair, k_pair, v_pair, d_pair = q_ref[:, lanes], k_ref[:, lanes], v_ref[:, lanes], mix_ref[:, lanes]
            sums = [None] * 3
            for side in range(2):
                mask = low if side == 0 else jnp.logical_not(low)
                d_side = jnp.where(mask, d_pair, 0)
                probs_16 = p_ref[2 * j + side]
                probs_32 = probs_16.astype(jnp.float32)
                d_probs = dot(d_side, v_pair, 1, 1).astype(jnp.bfloat16).astype(jnp.float32)
                row_dot = jnp.sum(d_probs * probs_32, axis=-1, keepdims=True)
                d_scores = (probs_32 * (d_probs - row_dot) * HEAD_DIM ** -0.5).astype(jnp.bfloat16)
                parts = (dot(d_scores, jnp.where(mask, k_pair, 0), 1, 0),
                         dot(d_scores, jnp.where(mask, q_pair, 0), 0, 0),
                         dot(probs_16, d_side, 0, 0))
                sums = [part if total is None else total + part for total, part in zip(sums, parts)]
            for ref, total in zip((dq_ref, dk_ref, dv_ref), sums):
                ref[:, lanes] = total.astype(jnp.bfloat16)
            return carry

        lax.fori_loop(0, heads // 2, pair, 0)

    row = pl.BlockSpec((seq, width), lambda i: (i, 0))
    weight = pl.BlockSpec((None, width, width), lambda i: (layer, 0, 0), pipeline_mode=pl.Buffered(1))
    block = pl.BlockSpec((None, heads, seq, seq), lambda i: (i, 0, 0, 0))
    act = (bf16(tokens, width), row)
    return call(
        kernel, (tokens // seq,), [row, row, row, row, block, weight], [act, act, act],
        [pltpu.VMEM((seq, width), jnp.bfloat16)], flops=2 * tokens * width * (width + 4 * seq), moved=24 * tokens * width,
        name=f"attend_backward_{layer}")(d_hidden, query, key_act, value, probs, w_proj)


def project_backward(x_act, d_hidden, d_query, d_key, d_value, w_query, w_key, w_value, layer):
    tokens, width = x_act.shape
    steps = width // OUT_BLOCK

    def kernel(x_ref, d_ref, dq_ref, dk_ref, dv_ref, wq_ref, wk_ref, wv_ref, o_ref, sum_ref):
        i = pl.program_id(0)
        total = dot(dq_ref[...], wq_ref[...], 1, 1) + dot(dk_ref[...], wk_ref[...], 1, 1) + dot(dv_ref[...], wv_ref[...], 1, 1)
        sum_ref[:, pl.ds(pl.multiple_of(OUT_BLOCK * i, OUT_BLOCK), OUT_BLOCK)] = total.astype(jnp.bfloat16)

        @pl.when(i == steps - 1)
        def _():
            back = rms_backward(x_ref[...].astype(jnp.float32), sum_ref[...].astype(jnp.float32))
            o_ref[...] = (d_ref[...].astype(jnp.float32) + back).astype(jnp.bfloat16)

    full = whole((tokens, width))
    weight = pl.BlockSpec((None, OUT_BLOCK, width), lambda i: (layer, i, 0))
    return call(
        kernel, (steps,), [full] * 5 + [weight] * 3, [(bf16(tokens, width), full)],
        [pltpu.VMEM((tokens, width), jnp.bfloat16)], flops=6 * tokens * width * width, moved=18 * tokens * width,
        name=f"project_backward_{layer}")(x_act, d_hidden, d_query, d_key, d_value, w_query, w_key, w_value)[0]


MESH = pl.DeviceIdType.MESH
LANES = 1024
SET_ROWS = 128
CORE_ROWS = 2 * SET_ROWS
TILE_ROWS = 2 * CORE_ROWS
OWN_SLOTS = 8
AG_SLOTS = 10
TYPES = {
    "p1": (0, 0, 80, "xyz"),
    "q1": (0, 80, 48, "zxy"),
    "p2": (1, 128, 80, "yxz"),
    "q2": (1, 208, 48, "zyx"),
}
WRITE_AT = 11


def stage_list():
    stages = []
    for name, (_, _, _, order) in TYPES.items():
        if order[2] == "z":
            plan = [("rs1", 1), ("rs2", 2), ("rsz", 3), ("agz", 6), ("ag2", 9), ("ag1", 10)]
        else:
            plan = [("rsz", 1), ("rs1", 4), ("rs2", 5), ("ag2", 6), ("ag1", 7), ("agz", 8)]
        for kind, at in plan:
            if kind in ("rsz", "agz"):
                for step in range(3):
                    for way in (0, 1):
                        stages.append((name, kind, step, way, at + step))
            else:
                stages.append((name, kind, 0, 0, at))
    return stages


STAGES = stage_list()


def piece_shape(name, kind):
    rows, order = TYPES[name][2], TYPES[name][3]
    if order[2] == "z":
        return {"rs1": (rows, 512), "rs2": (rows, 256), "rsz": (rows // 2, 128)}[kind]
    return {"rsz": (rows // 2, 512), "rs1": (rows // 2, 256), "rs2": (rows // 2, 128)}[kind]


def reduce_kernel(groups, chunks, n_in, n_out, *refs):
    ins, outs, scratch = refs[:n_in], refs[n_in:n_in + n_out], refs[n_in + n_out:]
    (lhs_buf, rhs_buf, own, part, part_in, gath), scratch = scratch[:6], scratch[6:]
    land_keys = [key for key, st in enumerate(STAGES) if st[1].startswith("rs")]
    landing = dict(zip(land_keys, scratch[:len(land_keys)]))
    load_sem, send_sem, recv_sem, pair_send, pair_recv, out_sem, out_send, out_recv, credit = scratch[len(land_keys):]

    me = lax.axis_index("data")
    core = lax.rem(me, 2)
    coord = {"x": lax.rem(lax.div(me, 2), 2), "y": lax.rem(lax.div(me, 4), 2)}
    z = lax.div(me, 8)
    partner = me + 1 - 2 * core
    near = {"x": me + 2 - 4 * coord["x"], "y": me + 4 - 8 * coord["y"]}
    up_ok, down_ok = z < 3, z > 0
    peers = [(partner, 0, None), (near["x"], 1, None), (near["y"], 2, None), (me + 8, 3, up_ok), (me - 8, 4, down_ok)]

    def guarded(cond, fn):
        if cond is None:
            fn()
        else:
            pl.when(cond)(fn)

    barrier = pltpu.get_barrier_semaphore()
    for dev, _, cond in peers:
        guarded(cond, lambda dev=dev: pl.semaphore_signal(barrier, inc=1, device_id=(dev,), device_id_type=MESH))
    inner = jnp.logical_and(up_ok, down_ok)
    guarded(inner, lambda: pl.semaphore_wait(barrier, 5))
    guarded(jnp.logical_not(inner), lambda: pl.semaphore_wait(barrier, 4))

    def region(name, kind, which):
        _, row, rows, order = TYPES[name]
        if order[2] == "z":
            h1, h2 = coord[order[0]], coord[order[1]]
            if kind == "1":
                return pl.ds(row, rows), pl.ds(pl.multiple_of(512 * which, 128), 512)
            if kind == "2":
                return pl.ds(row, rows), pl.ds(pl.multiple_of(512 * h1 + 256 * which, 128), 256)
            first = pl.multiple_of(row + (rows // 2) * lax.div(which, 2), 8)
            lane = pl.multiple_of(512 * h1 + 256 * h2 + 128 * lax.rem(which, 2), 128)
            return pl.ds(first, rows // 2), pl.ds(lane, 128)
        h1 = coord[order[1]]
        if kind == "z":
            first = pl.multiple_of(row + (rows // 2) * lax.div(which, 2), 8)
            return pl.ds(first, rows // 2), pl.ds(pl.multiple_of(512 * lax.rem(which, 2), 128), 512)
        first = pl.multiple_of(row + (rows // 2) * lax.div(z, 2), 8)
        if kind == "1":
            return pl.ds(first, rows // 2), pl.ds(pl.multiple_of(512 * lax.rem(z, 2) + 256 * which, 128), 256)
        lane = pl.multiple_of(512 * lax.rem(z, 2) + 256 * h1 + 128 * which, 128)
        return pl.ds(first, rows // 2), pl.ds(lane, 128)

    def exchange_axis(name, kind):
        order = TYPES[name][3]
        dims = order[:2] if order[2] == "z" else order[1:]
        return dims[int(kind) - 1]

    def plan(key, chunk, parity):
        name, kind, step, way, _ = STAGES[key]
        mine, slot = lax.rem(chunk, OWN_SLOTS), lax.rem(chunk, AG_SLOTS)
        if kind in ("rs1", "rs2"):
            axis = exchange_axis(name, kind[2])
            src, keep = region(name, kind[2], 1 - coord[axis]), region(name, kind[2], coord[axis])
            dev, send_ok, recv_ok = near[axis], None, None
            sent = own.at[mine, src[0], src[1]]
        elif kind in ("ag1", "ag2"):
            axis = exchange_axis(name, kind[2])
            src = keep = region(name, kind[2], coord[axis])
            dev, send_ok, recv_ok = near[axis], None, None
            sent = gath.at[slot, src[0], src[1]]
        elif kind == "rsz":
            if way:
                dev, k_send, k_keep = me + 8, z + 3 - step, z + 2 - step
                send_ok, recv_ok = k_send <= 3, jnp.logical_and(k_keep <= 3, down_ok)
            else:
                dev, k_send, k_keep = me - 8, z - 3 + step, z - 2 + step
                send_ok, recv_ok = k_send >= 0, jnp.logical_and(k_keep >= 0, up_ok)
            src, keep = region(name, "z", k_send), region(name, "z", k_keep)
            sent = own.at[mine, src[0], src[1]]
        else:
            if way:
                dev, k_send, k_keep = me + 8, z - step, z - 1 - step
                send_ok, recv_ok = jnp.logical_and(k_send >= 0, up_ok), k_keep >= 0
            else:
                dev, k_send, k_keep = me - 8, z + step, z + 1 + step
                send_ok, recv_ok = jnp.logical_and(k_send <= 3, down_ok), k_keep <= 3
            src, keep = region(name, "z", k_send), region(name, "z", k_keep)
            sent = gath.at[slot, src[0], src[1]]
        sems = dict(send_sem=send_sem.at[key], recv_sem=recv_sem.at[key, parity], device_id=(dev,), device_id_type=MESH)
        if kind.startswith("rs"):
            target = landing[key].at[parity]
            send = lambda: pltpu.make_async_remote_copy(src_ref=sent, dst_ref=target, **sems)
            recv = lambda: pltpu.make_async_remote_copy(
                src_ref=own.at[mine, keep[0], keep[1]], dst_ref=target, **sems)

            def arrive():
                own[mine, keep[0], keep[1]] += landing[key][parity]
        else:
            send = lambda: pltpu.make_async_remote_copy(src_ref=sent, dst_ref=sent, **sems)
            recv = lambda: pltpu.make_async_remote_copy(
                src_ref=gath.at[slot, keep[0], keep[1]], dst_ref=gath.at[slot, keep[0], keep[1]], **sems)
            arrive = None
        return send, recv, send_ok, recv_ok, arrive

    def finish(name, chunk):
        order = TYPES[name][3]
        reg = region(name, "z", z) if order[2] == "z" else region(name, "2", coord[order[2]])
        gath[lax.rem(chunk, AG_SLOTS), reg[0], reg[1]] = own[lax.rem(chunk, OWN_SLOTS), reg[0], reg[1]]

    def valid(chunk):
        return jnp.logical_and(chunk >= 0, chunk < chunks)

    def set_rows(half):
        return pl.ds(half * SET_ROWS, SET_ROWS)

    def pair_copy(half, parity):
        return pltpu.make_async_remote_copy(
            src_ref=part.at[parity, set_rows(half)], dst_ref=part_in.at[parity, set_rows(half)],
            send_sem=pair_send.at[half], recv_sem=pair_recv.at[half, parity], device_id=(partner,), device_id_type=MESH)

    def out_copies(half, group, local, whose):
        out, layer = group["out"]
        ref = outs[out] if layer is None else outs[out].at[layer]
        rows, cols = group["place"](local)
        first = pl.multiple_of(rows + CORE_ROWS * whose + half * SET_ROWS, SET_ROWS)
        return ref.at[pl.ds(first, SET_ROWS), pl.ds(pl.multiple_of(cols, 128), LANES)]

    def write_copies(half, chunk, dest):
        slot = lax.rem(chunk, AG_SLOTS)
        src = gath.at[slot, set_rows(half)]
        here = pltpu.make_async_copy(src, dest, out_sem.at[half])
        there = pltpu.make_async_remote_copy(
            src_ref=src, dst_ref=dest, send_sem=out_send.at[half], recv_sem=out_recv.at[half, lax.rem(chunk, 2)],
            device_id=(partner,), device_id_type=MESH)
        return here, there

    def load_copies(group, local, slot):
        rows, cols = group["place"](local)
        copies = []
        for app, (lhs, rhs) in enumerate(zip(group["lhs"], group["rhs"])):
            for whose in (0, 1):
                first = rows + CORE_ROWS * (core if whose == 0 else 1 - core)
                copies.append(pltpu.make_async_copy(
                    ins[lhs].at[:, pl.ds(pl.multiple_of(first, CORE_ROWS), CORE_ROWS)],
                    lhs_buf.at[slot, app, whose], load_sem.at[slot, app, whose]))
            copies.append(pltpu.make_async_copy(
                ins[rhs].at[:, pl.ds(pl.multiple_of(cols, 128), LANES)], rhs_buf.at[slot, app], load_sem.at[slot, app, 2]))
        return copies

    def for_group(chunk, fn):
        for group in groups:
            inside = jnp.logical_and(chunk >= group["start"], chunk < group["start"] + group["count"])
            pl.when(inside)(functools.partial(fn, group, chunk - group["start"]))

    def two_apps(chunk):
        flags = [jnp.logical_and(chunk >= g["start"], chunk < g["start"] + g["count"]) for g in groups if len(g["lhs"]) == 2]
        return functools.reduce(jnp.logical_or, flags)

    def start_load(chunk):
        def go(group, local):
            for copy in load_copies(group, local, lax.rem(chunk, 2)):
                copy.start()
        for_group(chunk, go)

    def wait_load(chunk):
        slot = lax.rem(chunk, 2)
        any_two = next(g for g in groups if len(g["lhs"]) == 2)
        copies = load_copies(any_two, 0, slot)
        for copy in copies[:3]:
            copy.wait()

        @pl.when(two_apps(chunk))
        def _():
            for copy in copies[3:]:
                copy.wait()

    def tile(chunk):
        slot, mine, parity = lax.rem(chunk, 2), lax.rem(chunk, OWN_SLOTS), lax.rem(chunk, 2)

        def product(app, whose):
            return lax.dot_general(lhs_buf[slot, app, whose], rhs_buf[slot, app], (((0,), (0,)), ((), ())),
                                   preferred_element_type=jnp.float32)

        own[mine] = product(0, 0)
        part[parity] = product(0, 1)

        @pl.when(two_apps(chunk))
        def _():
            own[mine] += product(1, 0)
            part[parity] += product(1, 1)

    last = chunks + WRITE_AT

    def section(half, step):
        before = lax.rem(step + 1, 2)
        now = lax.rem(step, 2)

        @pl.when(valid(step - 1))
        def _():
            copy = pair_copy(half, before)
            copy.wait_send()
            copy.wait_recv()
            mine = lax.rem(step - 1, OWN_SLOTS)
            own[mine, set_rows(half)] += part_in[before, set_rows(half)]

        names = [name for name in TYPES if TYPES[name][0] == half]
        keys = [key for key, st in enumerate(STAGES) if st[0] in names]
        finals = {name: max(st[4] for st in STAGES if st[0] == name and st[1].startswith("rs")) for name in names}
        for key in keys:
            name, at = STAGES[key][0], STAGES[key][4]
            chunk = step - 1 - at

            @pl.when(valid(chunk))
            def _(key=key, chunk=chunk):
                send, recv, send_ok, recv_ok, arrive = plan(key, chunk, before)

                def arrived():
                    recv().wait_recv()
                    if arrive is not None:
                        arrive()
                guarded(recv_ok, arrived)
                guarded(send_ok, lambda: send().wait_send())
        for name in names:
            chunk = step - 1 - finals[name]
            pl.when(valid(chunk))(functools.partial(finish, name, chunk))

        done = step - 1 - WRITE_AT

        @pl.when(valid(done))
        def _():
            here, there = write_copies(half, done, out_copies(half, groups[0], 0, 0))
            here.wait()
            there.wait_send()
            there.wait_recv()

        @pl.when(step < last)
        def _():
            for dev, way, cond in peers:
                to = way if way < 3 else 7 - way
                guarded(cond, lambda dev=dev, to=to: pl.semaphore_signal(
                    credit.at[half, to], inc=1, device_id=(dev,), device_id_type=MESH))

        @pl.when(step > 0)
        def _():
            for dev, way, cond in peers:
                guarded(cond, lambda way=way: pl.semaphore_wait(credit.at[half, way], 1))

        for key in reversed(keys):
            chunk = step - STAGES[key][4]

            @pl.when(valid(chunk))
            def _(key=key, chunk=chunk):
                send, recv, send_ok, recv_ok, arrive = plan(key, chunk, now)
                guarded(send_ok, lambda: send().start())

        out_chunk = step - WRITE_AT

        @pl.when(valid(out_chunk))
        def _():
            def go(group, local):
                for copy in write_copies(half, out_chunk, out_copies(half, group, local, core)):
                    copy.start()
            for_group(out_chunk, go)

    start_load(jnp.int32(0))

    def round_(step, carry):
        section(0, step)

        @pl.when(valid(step))
        def _():
            pl.when(step + 1 < chunks)(lambda: start_load(step + 1))
            wait_load(step)
            tile(step)
            pair_copy(0, lax.rem(step, 2)).start()

        section(1, step)

        @pl.when(valid(step))
        def _():
            pair_copy(1, lax.rem(step, 2)).start()

        return carry

    lax.fori_loop(0, last + 1, round_, 0)


def reduce_gradients(operands, groups, chunks, out_shapes, tokens, collective_id=0):
    landing = [pltpu.VMEM((2,) + piece_shape(st[0], st[1]), jnp.float32) for st in STAGES if st[1].startswith("rs")]
    apps = max(len(g["lhs"]) for g in groups)
    scratch = [
        pltpu.VMEM((2, apps, 2, tokens, CORE_ROWS), jnp.bfloat16),
        pltpu.VMEM((2, apps, tokens, LANES), jnp.bfloat16),
        pltpu.VMEM((OWN_SLOTS, CORE_ROWS, LANES), jnp.float32),
        pltpu.VMEM((2, CORE_ROWS, LANES), jnp.float32),
        pltpu.VMEM((2, CORE_ROWS, LANES), jnp.float32),
        pltpu.VMEM((AG_SLOTS, CORE_ROWS, LANES), jnp.float32),
        *landing,
        pltpu.SemaphoreType.DMA((2, apps, 3)),
        pltpu.SemaphoreType.DMA((len(STAGES),)),
        pltpu.SemaphoreType.DMA((len(STAGES), 2)),
        pltpu.SemaphoreType.DMA((2,)),
        pltpu.SemaphoreType.DMA((2, 2)),
        pltpu.SemaphoreType.DMA((2,)),
        pltpu.SemaphoreType.DMA((2,)),
        pltpu.SemaphoreType.DMA((2, 2)),
        pltpu.SemaphoreType.REGULAR((2, 5)),
    ]
    flops = sum(2 * g["count"] * len(g["lhs"]) * TILE_ROWS * LANES * tokens for g in groups)
    return pl.pallas_call(
        functools.partial(reduce_kernel, groups, chunks, len(operands), len(out_shapes)),
        out_shape=[jax.ShapeDtypeStruct(shape, jnp.float32) for shape in out_shapes],
        in_specs=[pl.BlockSpec(memory_space=pl.ANY)] * len(operands),
        out_specs=[pl.BlockSpec(memory_space=pl.ANY)] * len(out_shapes),
        scratch_shapes=scratch,
        compiler_params=pltpu.CompilerParams(
            collective_id=collective_id, has_side_effects=True, vmem_limit_bytes=60 * 1024 * 1024),
        cost_estimate=pl.CostEstimate(flops=flops, bytes_accessed=128 * 1024 * 1024, transcendentals=0),
        name="reduce_gradients",
    )(*operands)


def gradient_groups(width, ff):
    groups = []

    def add(count, lhs, rhs, out, place):
        start = groups[-1]["start"] + groups[-1]["count"] if groups else 0
        groups.append(dict(start=start, count=count, lhs=lhs, rhs=rhs, out=out, place=place))

    def tall(local):
        return TILE_ROWS * local, 0

    def wide(local):
        return TILE_ROWS * lax.rem(local, width // TILE_ROWS), LANES * lax.div(local, width // TILE_ROWS)

    def attention(layer):
        base = 6 * layer
        for out in range(3):
            add(width // TILE_ROWS, [base], [base + 1 + out], (out, layer), tall)
        add(width // TILE_ROWS, [base + 4], [base + 5], (3, layer), tall)

    attention(1)
    add(ff // TILE_ROWS, [14, 18], [15, 19], (5, None), tall)
    add(ff // TILE_ROWS, [12, 16], [13, 17], (4, None), wide)
    attention(0)
    return groups, sum(group["count"] for group in groups)


def local_operands(x_init, cot_out, w_query, w_key, w_value, w_proj, w_up, w_down):
    batch, seq, width = x_init.shape
    x_in = [x_init.reshape(batch * seq, width), None]
    d_act = cot_out.reshape(batch * seq, width)
    kept = []
    for layer in (0, 1):
        normed, query, key_act, value = project_qkv(x_in[layer], w_query, w_key, w_value, layer)
        probs, mixed, hidden, normed2 = attend(x_in[layer], query, key_act, value, w_proj, layer, seq)
        kept.append((normed, query, key_act, value, probs, mixed, hidden, normed2))
        if layer == 0:
            pre_act, act_0, x_in[1] = mlp_forward(hidden, normed2, w_up, w_down)
    attn, mlp = [None, None], [None, None]
    for layer in (1, 0):
        normed, query, key_act, value, probs, mixed, hidden, normed2 = kept[layer]
        if layer == 1:
            d_pre, d_hidden, act = mlp_backward(d_act, hidden, normed2, w_up, w_down, True, "mlp_both")
        else:
            d_pre, d_hidden = mlp_backward(d_act, hidden, pre_act, w_up, w_down, False, "mlp_backward")
            act = act_0
        mlp[layer] = (normed2, d_pre, act, d_act)
        d_query, d_key, d_value = attend_backward(d_hidden, query, key_act, value, probs, w_proj, layer, seq)
        d_act = project_backward(x_in[layer], d_hidden, d_query, d_key, d_value, w_query, w_key, w_value, layer)
        attn[layer] = (normed, d_query, d_key, d_value, mixed, d_hidden)
    return [*attn[0], *attn[1], *mlp[0], *mlp[1]], d_act.reshape(batch, seq, width)


def solution(mesh):
    def local_step(x_init, cot_out, w_query, w_key, w_value, w_proj, w_up, w_down):
        operands, d_init = local_operands(x_init, cot_out, w_query, w_key, w_value, w_proj, w_up, w_down)
        groups, chunks = gradient_groups(x_init.shape[2], w_up.shape[1])
        shapes = [w_query.shape, w_key.shape, w_value.shape, w_proj.shape, w_up.shape, w_down.shape]
        grads = reduce_gradients(operands, groups, chunks, shapes, operands[0].shape[0])
        return (*grads, d_init)

    data_spec = P("data")
    full_spec = P()
    in_specs = (data_spec, data_spec, full_spec, full_spec, full_spec, full_spec, full_spec, full_spec)
    out_specs = (full_spec, full_spec, full_spec, full_spec, full_spec, full_spec, data_spec)
    return jax.shard_map(local_step, mesh=mesh, in_specs=in_specs, out_specs=out_specs, check_vma=False)
```

```python
import functools

import jax
import jax.numpy as jnp
from jax import lax
from jax.experimental import pallas as pl
from jax.experimental.pallas import tpu as pltpu
from jax.sharding import PartitionSpec as P

EPS = 1e-6
HEAD_DIM = 64
PAIR = 2 * HEAD_DIM
FF_BLOCK = 512
OUT_BLOCK = 256
GELU_A = (2.0 / 3.141592653589793) ** 0.5
GELU_B = 0.044715
MIB = 1024 * 1024


def dot(lhs, rhs, lhs_dim, rhs_dim):
    return lax.dot_general(lhs, rhs, (((lhs_dim,), (rhs_dim,)), ((), ())), preferred_element_type=jnp.float32)


def rms_norm(x_f32):
    return x_f32 * lax.rsqrt(jnp.mean(x_f32 * x_f32, axis=-1, keepdims=True) + EPS)


def rms_backward(x_f32, d_out):
    scale = lax.rsqrt(jnp.mean(x_f32 * x_f32, axis=-1, keepdims=True) + EPS)
    inner = jnp.mean(x_f32 * d_out, axis=-1, keepdims=True)
    return scale * d_out - x_f32 * (scale * scale * scale * inner)


def gelu_parts(pre):
    square = pre * pre
    tanh = jnp.tanh(GELU_A * (pre + GELU_B * pre * square))
    half = 0.5 * (1.0 + tanh)
    slope = half + 0.5 * pre * (1.0 - tanh * tanh) * (GELU_A + (3.0 * GELU_A * GELU_B) * square)
    return pre * half, slope


def call(kernel, grid, in_specs, outs, scratch=(), flops=0, moved=0, name=None):
    return pl.pallas_call(
        kernel,
        grid=grid,
        in_specs=in_specs,
        out_specs=[spec for _, spec in outs],
        out_shape=[shape for shape, _ in outs],
        scratch_shapes=list(scratch),
        compiler_params=pltpu.CompilerParams(vmem_limit_bytes=60 * MIB, dimension_semantics=("arbitrary",) * len(grid)),
        cost_estimate=pl.CostEstimate(flops=flops, bytes_accessed=moved, transcendentals=0),
        name=name,
    )


def whole(shape):
    return pl.BlockSpec(shape, lambda *_: (0,) * len(shape), pipeline_mode=pl.Buffered(1))


def bf16(*shape):
    return jax.ShapeDtypeStruct(shape, jnp.bfloat16)


def project_qkv(x_act, w_query, w_key, w_value, layer):
    tokens, width = x_act.shape

    def kernel(x_ref, wq_ref, wk_ref, wv_ref, u_ref, q_ref, k_ref, v_ref):
        @pl.when(pl.program_id(0) == 0)
        def _():
            u_ref[...] = rms_norm(x_ref[...].astype(jnp.float32)).astype(jnp.bfloat16)

        for w_ref, o_ref in ((wq_ref, q_ref), (wk_ref, k_ref), (wv_ref, v_ref)):
            o_ref[...] = dot(u_ref[...], w_ref[...], 1, 0).astype(jnp.bfloat16)

    weight = pl.BlockSpec((None, width, OUT_BLOCK), lambda i: (layer, 0, i))
    block = pl.BlockSpec((tokens, OUT_BLOCK), lambda i: (0, i))
    return call(
        kernel, (width // OUT_BLOCK,), [whole((tokens, width)), weight, weight, weight],
        [(bf16(tokens, width), whole((tokens, width)))] + [(bf16(tokens, width), block)] * 3,
        flops=6 * tokens * width * width, moved=14 * tokens * width, name=f"qkv_{layer}")(x_act, w_query, w_key, w_value)


def attend(x_act, query, key_act, value, w_proj, layer, seq):
    tokens, width = x_act.shape
    heads = width // HEAD_DIM

    def kernel(x_ref, q_ref, k_ref, v_ref, wo_ref, p_ref, mix_ref, h_ref, n_ref):
        low = lax.broadcasted_iota(jnp.int32, (seq, PAIR), 1) < HEAD_DIM

        def pair(j, carry):
            lanes = pl.ds(pl.multiple_of(PAIR * j, PAIR), PAIR)
            q_pair, k_pair, v_pair = q_ref[:, lanes], k_ref[:, lanes], v_ref[:, lanes]
            total = None
            for side in range(2):
                mask = low if side == 0 else jnp.logical_not(low)
                scores = dot(jnp.where(mask, q_pair, 0), k_pair, 1, 1) * HEAD_DIM ** -0.5
                top = jnp.max(scores, axis=-1, keepdims=True)
                raised = jnp.exp(scores - top)
                inverse = 1.0 / jnp.sum(raised, axis=-1, keepdims=True)
                probs = (raised * inverse).astype(jnp.bfloat16)
                p_ref[2 * j + side] = probs
                part = dot(probs, jnp.where(mask, v_pair, 0), 1, 0)
                total = part if total is None else total + part
            mix_ref[:, lanes] = total.astype(jnp.bfloat16)
            return carry

        lax.fori_loop(0, heads // 2, pair, 0)
        attn = dot(mix_ref[...], wo_ref[...], 1, 0).astype(jnp.bfloat16)
        hidden = (x_ref[...].astype(jnp.float32) + attn.astype(jnp.float32)).astype(jnp.bfloat16)
        h_ref[...] = hidden
        n_ref[...] = rms_norm(hidden.astype(jnp.float32)).astype(jnp.bfloat16)

    row = pl.BlockSpec((seq, width), lambda i: (i, 0))
    weight = pl.BlockSpec((None, width, width), lambda i: (layer, 0, 0), pipeline_mode=pl.Buffered(1))
    probs = pl.BlockSpec((None, heads, seq, seq), lambda i: (i, 0, 0, 0))
    act = (bf16(tokens, width), row)
    return call(
        kernel, (tokens // seq,), [row, row, row, row, weight], [(bf16(tokens // seq, heads, seq, seq), probs), act, act, act],
        flops=2 * tokens * width * (width + 2 * seq), moved=20 * tokens * width, name=f"attend_{layer}",
    )(x_act, query, key_act, value, w_proj)


def mlp_forward(hidden, normed2, w_up, w_down):
    tokens, width = hidden.shape
    ff = w_up.shape[1]
    steps = ff // FF_BLOCK

    def kernel(h_ref, n_ref, w1_ref, w2_ref, pre_ref, act_ref, x_ref, acc_ref):
        i = pl.program_id(0)
        pre = dot(n_ref[...], w1_ref[...], 1, 0).astype(jnp.bfloat16)
        pre_ref[...] = pre
        act = gelu_parts(pre.astype(jnp.float32))[0].astype(jnp.bfloat16)
        act_ref[...] = act
        part = dot(act, w2_ref[...], 1, 0)

        @pl.when(i == 0)
        def _():
            acc_ref[...] = part

        @pl.when(i > 0)
        def _():
            acc_ref[...] += part

        @pl.when(i == steps - 1)
        def _():
            out = acc_ref[...].astype(jnp.bfloat16).astype(jnp.float32)
            x_ref[...] = (h_ref[...].astype(jnp.float32) + out).astype(jnp.bfloat16)

    full = whole((tokens, width))
    up = pl.BlockSpec((width, FF_BLOCK), lambda i: (0, i))
    down = pl.BlockSpec((FF_BLOCK, width), lambda i: (i, 0))
    wide = pl.BlockSpec((tokens, FF_BLOCK), lambda i: (0, i))
    return call(
        kernel, (steps,), [full, full, up, down],
        [(bf16(tokens, ff), wide), (bf16(tokens, ff), wide), (bf16(tokens, width), full)],
        [pltpu.VMEM((tokens, width), jnp.float32)], flops=4 * tokens * width * ff, moved=4 * tokens * ff + 4 * width * ff,
        name="mlp_forward")(hidden, normed2, w_up, w_down)


def mlp_backward(d_next, hidden, feed, w_up, w_down, replay, name):
    tokens, width = hidden.shape
    ff = w_up.shape[1]
    steps = ff // FF_BLOCK

    def kernel(d_ref, h_ref, feed_ref, w1_ref, w2_ref, *refs):
        outs, acc_ref = refs[:-1], refs[-1]
        i = pl.program_id(0)
        if replay:
            pre = dot(feed_ref[...], w1_ref[...], 1, 0).astype(jnp.bfloat16)
        else:
            pre = feed_ref[...]
        act, slope = gelu_parts(pre.astype(jnp.float32))
        if replay:
            outs[2][...] = act.astype(jnp.bfloat16)
        d_act = dot(d_ref[...], w2_ref[...], 1, 1).astype(jnp.bfloat16)
        d_pre = (d_act.astype(jnp.float32) * slope).astype(jnp.bfloat16)
        outs[0][...] = d_pre
        part = dot(d_pre, w1_ref[...], 1, 1)

        @pl.when(i == 0)
        def _():
            acc_ref[...] = part

        @pl.when(i > 0)
        def _():
            acc_ref[...] += part

        @pl.when(i == steps - 1)
        def _():
            d_normed = acc_ref[...].astype(jnp.bfloat16).astype(jnp.float32)
            back = rms_backward(h_ref[...].astype(jnp.float32), d_normed)
            outs[1][...] = (d_ref[...].astype(jnp.float32) + back).astype(jnp.bfloat16)

    full = whole((tokens, width))
    up = pl.BlockSpec((width, FF_BLOCK), lambda i: (0, i))
    down = pl.BlockSpec((FF_BLOCK, width), lambda i: (i, 0))
    wide = pl.BlockSpec((tokens, FF_BLOCK), lambda i: (0, i))
    outs = [(bf16(tokens, ff), wide), (bf16(tokens, width), full)] + ([(bf16(tokens, ff), wide)] if replay else [])
    return call(
        kernel, (steps,), [full, full, full if replay else wide, up, down], outs,
        [pltpu.VMEM((tokens, width), jnp.float32)], flops=(6 if replay else 4) * tokens * width * ff,
        moved=4 * tokens * ff + 4 * width * ff, name=name)(d_next, hidden, feed, w_up, w_down)


def pair_backward(q_pair, k_pair, v_pair, d_pair, low, probs_of):
    sums = [None] * 3
    for side in range(2):
        mask = low if side == 0 else jnp.logical_not(low)
        d_side = jnp.where(mask, d_pair, 0)
        probs_16 = probs_of(side)
        probs_32 = probs_16.astype(jnp.float32)
        d_probs = dot(d_side, v_pair, 1, 1).astype(jnp.bfloat16).astype(jnp.float32)
        row_dot = jnp.sum(d_probs * probs_32, axis=-1, keepdims=True)
        d_scores = (probs_32 * (d_probs - row_dot) * HEAD_DIM ** -0.5).astype(jnp.bfloat16)
        parts = (dot(d_scores, jnp.where(mask, k_pair, 0), 1, 0),
                 dot(d_scores, jnp.where(mask, q_pair, 0), 0, 0),
                 dot(probs_16, d_side, 0, 0))
        sums = [part if total is None else total + part for total, part in zip(sums, parts)]
    return sums


def attend_backward(d_hidden, query, key_act, value, probs, w_proj, layer, seq):
    tokens, width = d_hidden.shape
    heads = width // HEAD_DIM

    def kernel(d_ref, q_ref, k_ref, v_ref, p_ref, wo_ref, dq_ref, dk_ref, dv_ref, mix_ref):
        mix_ref[...] = dot(d_ref[...], wo_ref[...], 1, 1).astype(jnp.bfloat16)
        low = lax.broadcasted_iota(jnp.int32, (seq, PAIR), 1) < HEAD_DIM

        def pair(j, carry):
            lanes = pl.ds(pl.multiple_of(PAIR * j, PAIR), PAIR)
            q_pair, k_pair, v_pair, d_pair = q_ref[:, lanes], k_ref[:, lanes], v_ref[:, lanes], mix_ref[:, lanes]
            sums = pair_backward(q_pair, k_pair, v_pair, d_pair, low, lambda side: p_ref[2 * j + side])
            for ref, total in zip((dq_ref, dk_ref, dv_ref), sums):
                ref[:, lanes] = total.astype(jnp.bfloat16)
            return carry

        lax.fori_loop(0, heads // 2, pair, 0)

    row = pl.BlockSpec((seq, width), lambda i: (i, 0))
    weight = pl.BlockSpec((None, width, width), lambda i: (layer, 0, 0), pipeline_mode=pl.Buffered(1))
    block = pl.BlockSpec((None, heads, seq, seq), lambda i: (i, 0, 0, 0))
    act = (bf16(tokens, width), row)
    return call(
        kernel, (tokens // seq,), [row, row, row, row, block, weight], [act, act, act],
        [pltpu.VMEM((seq, width), jnp.bfloat16)], flops=2 * tokens * width * (width + 4 * seq), moved=24 * tokens * width,
        name=f"attend_backward_{layer}")(d_hidden, query, key_act, value, probs, w_proj)


def project_backward(x_act, d_hidden, d_query, d_key, d_value, w_query, w_key, w_value, layer):
    tokens, width = x_act.shape
    steps = width // OUT_BLOCK

    def kernel(x_ref, d_ref, dq_ref, dk_ref, dv_ref, wq_ref, wk_ref, wv_ref, o_ref, sum_ref):
        i = pl.program_id(0)
        total = dot(dq_ref[...], wq_ref[...], 1, 1) + dot(dk_ref[...], wk_ref[...], 1, 1) + dot(dv_ref[...], wv_ref[...], 1, 1)
        sum_ref[:, pl.ds(pl.multiple_of(OUT_BLOCK * i, OUT_BLOCK), OUT_BLOCK)] = total.astype(jnp.bfloat16)

        @pl.when(i == steps - 1)
        def _():
            back = rms_backward(x_ref[...].astype(jnp.float32), sum_ref[...].astype(jnp.float32))
            o_ref[...] = (d_ref[...].astype(jnp.float32) + back).astype(jnp.bfloat16)

    full = whole((tokens, width))
    weight = pl.BlockSpec((None, OUT_BLOCK, width), lambda i: (layer, i, 0))
    return call(
        kernel, (steps,), [full] * 5 + [weight] * 3, [(bf16(tokens, width), full)],
        [pltpu.VMEM((tokens, width), jnp.bfloat16)], flops=6 * tokens * width * width, moved=18 * tokens * width,
        name=f"project_backward_{layer}")(x_act, d_hidden, d_query, d_key, d_value, w_query, w_key, w_value)[0]


MESH = pl.DeviceIdType.MESH
LANES = 1024
SET_ROWS = 128
CORE_ROWS = 2 * SET_ROWS
TILE_ROWS = 2 * CORE_ROWS
OWN_SLOTS = 8
AG_SLOTS = 10
TYPES = {
    "p1": (0, 0, 80, "xyz"),
    "q1": (0, 80, 48, "zxy"),
    "p2": (1, 128, 80, "yxz"),
    "q2": (1, 208, 48, "zyx"),
}
WRITE_AT = 11


def stage_list():
    stages = []
    for name, (_, _, _, order) in TYPES.items():
        if order[2] == "z":
            plan = [("rs1", 1), ("rs2", 2), ("rsz", 3), ("agz", 6), ("ag2", 9), ("ag1", 10)]
        else:
            plan = [("rsz", 1), ("rs1", 4), ("rs2", 5), ("ag2", 6), ("ag1", 7), ("agz", 8)]
        for kind, at in plan:
            if kind in ("rsz", "agz"):
                for step in range(3):
                    for way in (0, 1):
                        stages.append((name, kind, step, way, at + step))
            else:
                stages.append((name, kind, 0, 0, at))
    return stages


STAGES = stage_list()


def piece_shape(name, kind):
    rows, order = TYPES[name][2], TYPES[name][3]
    if order[2] == "z":
        return {"rs1": (rows, 512), "rs2": (rows, 256), "rsz": (rows // 2, 128)}[kind]
    return {"rsz": (rows // 2, 512), "rs1": (rows // 2, 256), "rs2": (rows // 2, 128)}[kind]


def between(step, first, count):
    return jnp.logical_and(step >= first, step < first + count)


class Backward:
    PB_1, MB, AB, PB_0 = 0, 4, 12, 21
    ROWS = 256

    def __init__(self, at, big, total_buf, w_buf, p_buf, sem, drain):
        self.at, self.big, self.total, self.w, self.p, self.sem, self.drain = at, big, total_buf, w_buf, p_buf, sem, drain
        self.tokens, self.width = at["x_0"].shape
        self.heads = at["probs_0"].shape[1]
        self.seq = at["probs_0"].shape[2]

    def load(self, name, dest, sem, *index):
        ref = self.at[name]
        return pltpu.make_async_copy(ref.at[index] if index else ref, dest, self.sem.at[sem])

    def store(self, src, name, sem, *index):
        ref = self.at[name]
        return pltpu.make_async_copy(src, ref.at[index] if index else ref, self.drain.at[sem])

    def row_blocks(self, fn):
        def body(block, carry):
            fn(pl.ds(pl.multiple_of(self.ROWS * block, self.ROWS), self.ROWS))
            return carry
        lax.fori_loop(0, self.tokens // self.ROWS, body, 0)

    def input_loads(self, layer):
        spot = 4 if layer else 5
        copies = [self.load(f"d{kind}_{layer}", self.big.at[i], i) for i, kind in enumerate("qkv")]
        copies.append(self.load(f"x_{layer}", self.big.at[spot], 3))
        if layer:
            copies.append(self.load("dh_1", self.big.at[5], 4))
        return copies

    def weight_loads(self, layer, block):
        rows = pl.ds(pl.multiple_of(OUT_BLOCK * block, OUT_BLOCK), OUT_BLOCK)
        slot = lax.rem(block, 2)
        return [self.load(name, self.w.at[slot, i], 5 + 3 * slot + i, layer, rows) for i, name in enumerate(("wq", "wk", "wv"))]

    def input_block(self, layer, block):
        big, blocks = self.big, self.width // OUT_BLOCK
        slot = lax.rem(block, 2)

        @pl.when(block == 0)
        def _():
            for copy in self.input_loads(layer):
                copy.wait()
        for copy in self.weight_loads(layer, block):
            copy.wait()

        @pl.when(block + 1 < blocks)
        def _():
            for copy in self.weight_loads(layer, block + 1):
                copy.start()
        lanes = pl.ds(pl.multiple_of(OUT_BLOCK * block, OUT_BLOCK), OUT_BLOCK)

        def product(rows):
            total = dot(big[0, rows], self.w[slot, 0], 1, 1) + dot(big[1, rows], self.w[slot, 1], 1, 1)
            big[3, rows, lanes] = (total + dot(big[2, rows], self.w[slot, 2], 1, 1)).astype(jnp.bfloat16)
        self.row_blocks(product)

        @pl.when(block == blocks - 1)
        def _():
            x_at, d_at = (4, 5) if layer else (5, 4)

            def close(rows):
                back = rms_backward(big[x_at, rows].astype(jnp.float32), big[3, rows].astype(jnp.float32))
                big[3, rows] = (big[d_at, rows].astype(jnp.float32) + back).astype(jnp.bfloat16)
                if layer:
                    self.total[rows] = jnp.zeros((self.ROWS, self.width), jnp.float32)
            self.row_blocks(close)
            self.store(big.at[3], f"dx_{layer}", 0).start()
            if layer:
                self.load("h_0", big.at[4], 3).start()
                for copy in self.mlp_loads(0):
                    copy.start()

    def mlp_loads(self, block):
        slot = lax.rem(block, 2)
        lanes = pl.ds(pl.multiple_of(FF_BLOCK * block, FF_BLOCK), FF_BLOCK)
        half = pl.ds(pl.multiple_of(FF_BLOCK * slot, FF_BLOCK), FF_BLOCK)
        return [self.load("w_up", self.big.at[0, :, half], 5 + 3 * slot, slice(None), lanes),
                self.load("pre_0", self.big.at[1, :, half], 6 + 3 * slot, slice(None), lanes),
                self.load("w_down", self.big.at[5, half], 7 + 3 * slot, lanes)]

    def mlp_store(self, block):
        half = pl.ds(pl.multiple_of(FF_BLOCK * lax.rem(block, 2), FF_BLOCK), FF_BLOCK)
        lanes = pl.ds(pl.multiple_of(FF_BLOCK * block, FF_BLOCK), FF_BLOCK)
        return self.store(self.big.at[2, :, half], "dpre_0", 1, slice(None), lanes)

    def mlp_block(self, block):
        big, blocks = self.big, self.at["w_up"].shape[1] // FF_BLOCK

        @pl.when(block == 0)
        def _():
            self.store(big.at[3], "dx_1", 0).wait()
            self.load("h_0", big.at[4], 3).wait()
        for copy in self.mlp_loads(block):
            copy.wait()

        @pl.when(block + 1 < blocks)
        def _():
            for copy in self.mlp_loads(block + 1):
                copy.start()

        @pl.when(block > 0)
        def _():
            self.mlp_store(block - 1).wait()
        half = pl.ds(pl.multiple_of(FF_BLOCK * lax.rem(block, 2), FF_BLOCK), FF_BLOCK)

        def product(rows):
            d_act = dot(big[3, rows], big[5, half], 1, 1).astype(jnp.bfloat16).astype(jnp.float32)
            slope = gelu_parts(big[1, rows, half].astype(jnp.float32))[1]
            d_pre = (d_act * slope).astype(jnp.bfloat16)
            big[2, rows, half] = d_pre
            self.total[rows] += dot(d_pre, big[0, :, half], 1, 1)
        self.row_blocks(product)
        self.mlp_store(block).start()

        @pl.when(block == blocks - 1)
        def _():
            def close(rows):
                d_normed = self.total[rows].astype(jnp.bfloat16).astype(jnp.float32)
                back = rms_backward(big[4, rows].astype(jnp.float32), d_normed)
                big[4, rows] = (big[3, rows].astype(jnp.float32) + back).astype(jnp.bfloat16)
            self.row_blocks(close)
            self.store(big.at[4], "dh_0", 2).start()
            self.load("wo", big.at[0], 4, 0).start()
            for copy in self.seq_loads(0) + self.probs_loads(0):
                copy.start()

    def seq_loads(self, seq):
        rows = pl.ds(pl.multiple_of(self.seq * seq, self.seq), self.seq)
        return [self.load(f"{kind}_0", self.big.at[1 + lax.rem(seq, 2), pl.ds(self.seq * i, self.seq)], i, rows)
                for i, kind in enumerate("qkv")]

    def probs_loads(self, piece):
        half = self.heads // 2
        heads = pl.ds(half * lax.rem(piece, 2), half)
        return [self.load("probs_0", self.p.at[lax.rem(piece, 2)], 5 + lax.rem(piece, 2), lax.div(piece, 2), heads)]

    def seq_stores(self, piece):
        seq, half = lax.div(piece, 2), lax.rem(piece, 2)
        rows = pl.ds(pl.multiple_of(self.seq * seq, self.seq), self.seq)
        lanes = pl.ds(pl.multiple_of(self.width // 2 * half, PAIR), self.width // 2)
        spot = 5 - 2 * lax.rem(seq, 2)
        return [self.store(self.big.at[spot, pl.ds(self.seq * i, self.seq), lanes], f"d{kind}_0", 3 + i, rows, lanes)
                for i, kind in enumerate("qkv")]

    def attention_piece(self, piece):
        big, pieces = self.big, 2 * (self.tokens // self.seq)
        seq, half = lax.div(piece, 2), lax.rem(piece, 2)
        spot, out = 1 + lax.rem(seq, 2), 5 - 2 * lax.rem(seq, 2)

        @pl.when(piece == 0)
        def _():
            self.mlp_store(self.at["w_up"].shape[1] // FF_BLOCK - 1).wait()
            self.store(big.at[4], "dh_0", 2).wait()
            self.load("wo", big.at[0], 4, 0).wait()

        @pl.when(piece > 0)
        def _():
            for copy in self.seq_stores(piece - 1):
                copy.wait()
        for copy in self.probs_loads(piece):
            copy.wait()

        @pl.when(piece + 1 < pieces)
        def _():
            for copy in self.probs_loads(piece + 1):
                copy.start()
        mixed = pl.ds(3 * self.seq, self.seq)

        @pl.when(half == 0)
        def _():
            for copy in self.seq_loads(seq):
                copy.wait()

            @pl.when(piece + 2 < pieces)
            def _():
                for copy in self.seq_loads(seq + 1):
                    copy.start()
            rows = pl.ds(pl.multiple_of(self.seq * seq, self.seq), self.seq)
            big[spot, mixed] = dot(big[4, rows], big[0], 1, 1).astype(jnp.bfloat16)
        low = lax.broadcasted_iota(jnp.int32, (self.seq, PAIR), 1) < HEAD_DIM
        pairs = self.heads // 4

        def pair(j, carry):
            lanes = pl.ds(pl.multiple_of(PAIR * (pairs * half + j), PAIR), PAIR)
            q_pair, k_pair, v_pair, d_pair = (big[spot, pl.ds(self.seq * i, self.seq), lanes] for i in range(4))
            for i, total in enumerate(pair_backward(q_pair, k_pair, v_pair, d_pair, low, lambda side: self.p[half, 2 * j + side])):
                big[out, pl.ds(self.seq * i, self.seq), lanes] = total.astype(jnp.bfloat16)
            return carry
        lax.fori_loop(0, pairs, pair, 0)
        for copy in self.seq_stores(piece):
            copy.start()

    def item(self, step):
        blocks = self.width // OUT_BLOCK
        pieces = 2 * (self.tokens // self.seq)

        @pl.when(step == self.PB_1)
        def _():
            for copy in self.input_loads(1) + self.weight_loads(1, 0):
                copy.start()
        pl.when(between(step, self.PB_1, blocks))(lambda: self.input_block(1, step - self.PB_1))
        pl.when(between(step, self.MB, 8))(lambda: self.mlp_block(step - self.MB))
        pl.when(between(step, self.AB, pieces))(lambda: self.attention_piece(step - self.AB))

        @pl.when(step == self.PB_0 - 1)
        def _():
            for copy in self.seq_stores(pieces - 1):
                copy.wait()
            for copy in self.input_loads(0) + self.weight_loads(0, 0):
                copy.start()
        pl.when(between(step, self.PB_0, blocks))(lambda: self.input_block(0, step - self.PB_0))

        @pl.when(step == self.PB_0 + blocks)
        def _():
            self.store(self.big.at[3], "dx_0", 0).wait()


def finish_kernel(groups, chunks, in_names, out_names, remote, *refs):
    names = [*in_names, *out_names]
    at, scratch = dict(zip(names, refs[:len(names)])), refs[len(names):]
    (big, total_buf, w_buf, p_buf, item_sem, drain_sem), scratch = scratch[:6], scratch[6:]
    backward = Backward(at, big, total_buf, w_buf, p_buf, item_sem, drain_sem)
    if not remote:
        lax.fori_loop(0, chunks + WRITE_AT + 1, lambda step, carry: backward.item(step) or carry, 0)
        return
    (lhs_buf, rhs_buf, own, part, part_in, gath), scratch = scratch[:6], scratch[6:]
    land_keys = [key for key, st in enumerate(STAGES) if st[1].startswith("rs")]
    landing = dict(zip(land_keys, scratch[:len(land_keys)]))
    load_sem, send_sem, recv_sem, pair_send, pair_recv, out_sem, out_send, out_recv, credit = scratch[len(land_keys):]

    me = lax.axis_index("data")
    core = lax.rem(me, 2)
    coord = {"x": lax.rem(lax.div(me, 2), 2), "y": lax.rem(lax.div(me, 4), 2)}
    z = lax.div(me, 8)
    partner = me + 1 - 2 * core
    near = {"x": me + 2 - 4 * coord["x"], "y": me + 4 - 8 * coord["y"]}
    up_ok, down_ok = z < 3, z > 0
    peers = [(partner, 0, None), (near["x"], 1, None), (near["y"], 2, None), (me + 8, 3, up_ok), (me - 8, 4, down_ok)]

    def guarded(cond, fn):
        if cond is None:
            fn()
        else:
            pl.when(cond)(fn)

    barrier = pltpu.get_barrier_semaphore()
    for dev, _, cond in peers:
        guarded(cond, lambda dev=dev: pl.semaphore_signal(barrier, inc=1, device_id=(dev,), device_id_type=MESH))
    inner = jnp.logical_and(up_ok, down_ok)
    guarded(inner, lambda: pl.semaphore_wait(barrier, 5))
    guarded(jnp.logical_not(inner), lambda: pl.semaphore_wait(barrier, 4))

    def region(name, kind, which):
        _, row, rows, order = TYPES[name]
        if order[2] == "z":
            h1, h2 = coord[order[0]], coord[order[1]]
            if kind == "1":
                return pl.ds(row, rows), pl.ds(pl.multiple_of(512 * which, 128), 512)
            if kind == "2":
                return pl.ds(row, rows), pl.ds(pl.multiple_of(512 * h1 + 256 * which, 128), 256)
            first = pl.multiple_of(row + (rows // 2) * lax.div(which, 2), 8)
            lane = pl.multiple_of(512 * h1 + 256 * h2 + 128 * lax.rem(which, 2), 128)
            return pl.ds(first, rows // 2), pl.ds(lane, 128)
        h1 = coord[order[1]]
        if kind == "z":
            first = pl.multiple_of(row + (rows // 2) * lax.div(which, 2), 8)
            return pl.ds(first, rows // 2), pl.ds(pl.multiple_of(512 * lax.rem(which, 2), 128), 512)
        first = pl.multiple_of(row + (rows // 2) * lax.div(z, 2), 8)
        if kind == "1":
            return pl.ds(first, rows // 2), pl.ds(pl.multiple_of(512 * lax.rem(z, 2) + 256 * which, 128), 256)
        lane = pl.multiple_of(512 * lax.rem(z, 2) + 256 * h1 + 128 * which, 128)
        return pl.ds(first, rows // 2), pl.ds(lane, 128)

    def exchange_axis(name, kind):
        order = TYPES[name][3]
        dims = order[:2] if order[2] == "z" else order[1:]
        return dims[int(kind) - 1]

    def plan(key, chunk, parity):
        name, kind, step, way, _ = STAGES[key]
        mine, slot = lax.rem(chunk, OWN_SLOTS), lax.rem(chunk, AG_SLOTS)
        if kind in ("rs1", "rs2"):
            axis = exchange_axis(name, kind[2])
            src, keep = region(name, kind[2], 1 - coord[axis]), region(name, kind[2], coord[axis])
            dev, send_ok, recv_ok = near[axis], None, None
            sent = own.at[mine, src[0], src[1]]
        elif kind in ("ag1", "ag2"):
            axis = exchange_axis(name, kind[2])
            src = keep = region(name, kind[2], coord[axis])
            dev, send_ok, recv_ok = near[axis], None, None
            sent = gath.at[slot, src[0], src[1]]
        elif kind == "rsz":
            if way:
                dev, k_send, k_keep = me + 8, z + 3 - step, z + 2 - step
                send_ok, recv_ok = k_send <= 3, jnp.logical_and(k_keep <= 3, down_ok)
            else:
                dev, k_send, k_keep = me - 8, z - 3 + step, z - 2 + step
                send_ok, recv_ok = k_send >= 0, jnp.logical_and(k_keep >= 0, up_ok)
            src, keep = region(name, "z", k_send), region(name, "z", k_keep)
            sent = own.at[mine, src[0], src[1]]
        else:
            if way:
                dev, k_send, k_keep = me + 8, z - step, z - 1 - step
                send_ok, recv_ok = jnp.logical_and(k_send >= 0, up_ok), k_keep >= 0
            else:
                dev, k_send, k_keep = me - 8, z + step, z + 1 + step
                send_ok, recv_ok = jnp.logical_and(k_send <= 3, down_ok), k_keep <= 3
            src, keep = region(name, "z", k_send), region(name, "z", k_keep)
            sent = gath.at[slot, src[0], src[1]]
        sems = dict(send_sem=send_sem.at[key], recv_sem=recv_sem.at[key, parity], device_id=(dev,), device_id_type=MESH)
        if kind.startswith("rs"):
            target = landing[key].at[parity]
            send = lambda: pltpu.make_async_remote_copy(src_ref=sent, dst_ref=target, **sems)
            recv = lambda: pltpu.make_async_remote_copy(
                src_ref=own.at[mine, keep[0], keep[1]], dst_ref=target, **sems)

            def arrive():
                own[mine, keep[0], keep[1]] += landing[key][parity]
        else:
            send = lambda: pltpu.make_async_remote_copy(src_ref=sent, dst_ref=sent, **sems)
            recv = lambda: pltpu.make_async_remote_copy(
                src_ref=gath.at[slot, keep[0], keep[1]], dst_ref=gath.at[slot, keep[0], keep[1]], **sems)
            arrive = None
        return send, recv, send_ok, recv_ok, arrive

    def finish(name, chunk):
        order = TYPES[name][3]
        reg = region(name, "z", z) if order[2] == "z" else region(name, "2", coord[order[2]])
        gath[lax.rem(chunk, AG_SLOTS), reg[0], reg[1]] = own[lax.rem(chunk, OWN_SLOTS), reg[0], reg[1]]

    def valid(chunk):
        return jnp.logical_and(chunk >= 0, chunk < chunks)

    def set_rows(half):
        return pl.ds(half * SET_ROWS, SET_ROWS)

    def pair_copy(half, parity):
        return pltpu.make_async_remote_copy(
            src_ref=part.at[parity, set_rows(half)], dst_ref=part_in.at[parity, set_rows(half)],
            send_sem=pair_send.at[half], recv_sem=pair_recv.at[half, parity], device_id=(partner,), device_id_type=MESH)

    def out_copies(half, group, local, whose):
        out, layer = group["out"]
        ref = at[out] if layer is None else at[out].at[layer]
        rows, cols = group["place"](local)
        first = pl.multiple_of(rows + CORE_ROWS * whose + half * SET_ROWS, SET_ROWS)
        return ref.at[pl.ds(first, SET_ROWS), pl.ds(pl.multiple_of(cols, 128), LANES)]

    def write_copies(half, chunk, dest):
        slot = lax.rem(chunk, AG_SLOTS)
        src = gath.at[slot, set_rows(half)]
        here = pltpu.make_async_copy(src, dest, out_sem.at[half])
        there = pltpu.make_async_remote_copy(
            src_ref=src, dst_ref=dest, send_sem=out_send.at[half], recv_sem=out_recv.at[half, lax.rem(chunk, 2)],
            device_id=(partner,), device_id_type=MESH)
        return here, there

    def load_copies(group, local, slot):
        rows, cols = group["place"](local)
        copies = []
        for app, (lhs, rhs) in enumerate(zip(group["lhs"], group["rhs"])):
            for whose in (0, 1):
                first = rows + CORE_ROWS * (core if whose == 0 else 1 - core)
                copies.append(pltpu.make_async_copy(
                    at[lhs].at[:, pl.ds(pl.multiple_of(first, CORE_ROWS), CORE_ROWS)],
                    lhs_buf.at[slot, app, whose], load_sem.at[slot, app, whose]))
            copies.append(pltpu.make_async_copy(
                at[rhs].at[:, pl.ds(pl.multiple_of(cols, 128), LANES)], rhs_buf.at[slot, app], load_sem.at[slot, app, 2]))
        return copies

    def for_group(chunk, fn):
        for group in groups:
            inside = jnp.logical_and(chunk >= group["start"], chunk < group["start"] + group["count"])
            pl.when(inside)(functools.partial(fn, group, chunk - group["start"]))

    def two_apps(chunk):
        flags = [jnp.logical_and(chunk >= g["start"], chunk < g["start"] + g["count"]) for g in groups if len(g["lhs"]) == 2]
        return functools.reduce(jnp.logical_or, flags)

    def start_load(chunk):
        def go(group, local):
            for copy in load_copies(group, local, lax.rem(chunk, 2)):
                copy.start()
        for_group(chunk, go)

    def wait_load(chunk):
        slot = lax.rem(chunk, 2)
        any_two = next(g for g in groups if len(g["lhs"]) == 2)
        copies = load_copies(any_two, 0, slot)
        for copy in copies[:3]:
            copy.wait()

        @pl.when(two_apps(chunk))
        def _():
            for copy in copies[3:]:
                copy.wait()

    def tile(chunk):
        slot, mine, parity = lax.rem(chunk, 2), lax.rem(chunk, OWN_SLOTS), lax.rem(chunk, 2)

        def product(app, whose):
            return lax.dot_general(lhs_buf[slot, app, whose], rhs_buf[slot, app], (((0,), (0,)), ((), ())),
                                   preferred_element_type=jnp.float32)

        own[mine] = product(0, 0)
        part[parity] = product(0, 1)

        @pl.when(two_apps(chunk))
        def _():
            own[mine] += product(1, 0)
            part[parity] += product(1, 1)

    last = chunks + WRITE_AT

    def section(half, step):
        before = lax.rem(step + 1, 2)
        now = lax.rem(step, 2)

        @pl.when(valid(step - 1))
        def _():
            copy = pair_copy(half, before)
            copy.wait_send()
            copy.wait_recv()
            mine = lax.rem(step - 1, OWN_SLOTS)
            own[mine, set_rows(half)] += part_in[before, set_rows(half)]

        names = [name for name in TYPES if TYPES[name][0] == half]
        keys = [key for key, st in enumerate(STAGES) if st[0] in names]
        finals = {name: max(st[4] for st in STAGES if st[0] == name and st[1].startswith("rs")) for name in names}
        for key in keys:
            name, at = STAGES[key][0], STAGES[key][4]
            chunk = step - 1 - at

            @pl.when(valid(chunk))
            def _(key=key, chunk=chunk):
                send, recv, send_ok, recv_ok, arrive = plan(key, chunk, before)

                def arrived():
                    recv().wait_recv()
                    if arrive is not None:
                        arrive()
                guarded(recv_ok, arrived)
                guarded(send_ok, lambda: send().wait_send())
        for name in names:
            chunk = step - 1 - finals[name]
            pl.when(valid(chunk))(functools.partial(finish, name, chunk))

        done = step - 1 - WRITE_AT

        @pl.when(valid(done))
        def _():
            here, there = write_copies(half, done, out_copies(half, groups[0], 0, 0))
            here.wait()
            there.wait_send()
            there.wait_recv()

        @pl.when(step < last)
        def _():
            for dev, way, cond in peers:
                to = way if way < 3 else 7 - way
                guarded(cond, lambda dev=dev, to=to: pl.semaphore_signal(
                    credit.at[half, to], inc=1, device_id=(dev,), device_id_type=MESH))

        @pl.when(step > 0)
        def _():
            for dev, way, cond in peers:
                guarded(cond, lambda way=way: pl.semaphore_wait(credit.at[half, way], 1))

        for key in reversed(keys):
            chunk = step - STAGES[key][4]

            @pl.when(valid(chunk))
            def _(key=key, chunk=chunk):
                send, recv, send_ok, recv_ok, arrive = plan(key, chunk, now)
                guarded(send_ok, lambda: send().start())

        out_chunk = step - WRITE_AT

        @pl.when(valid(out_chunk))
        def _():
            def go(group, local):
                for copy in write_copies(half, out_chunk, out_copies(half, group, local, core)):
                    copy.start()
            for_group(out_chunk, go)

    start_load(jnp.int32(0))

    def round_(step, carry):
        section(0, step)

        @pl.when(valid(step))
        def _():
            pl.when(step + 1 < chunks)(lambda: start_load(step + 1))
            wait_load(step)
            tile(step)
            pair_copy(0, lax.rem(step, 2)).start()

        section(1, step)

        @pl.when(valid(step))
        def _():
            pair_copy(1, lax.rem(step, 2)).start()

        backward.item(step)
        return carry

    lax.fori_loop(0, last + 1, round_, 0)


def finish_backward(inputs, groups, chunks, weights, tokens, seq, collective_id=0, remote=True):
    width, ff = inputs["w_up"].shape
    landing = [pltpu.VMEM((2,) + piece_shape(st[0], st[1]), jnp.float32) for st in STAGES if st[1].startswith("rs")]
    apps = 2
    outs = {name: jax.ShapeDtypeStruct(shape, jnp.float32) for name, shape in weights.items()}
    for name in ("dx_0", "dx_1", "dh_0", "dq_0", "dk_0", "dv_0"):
        outs[name] = bf16(tokens, width)
    outs["dpre_0"] = bf16(tokens, ff)
    heads = width // HEAD_DIM
    scratch = [
        pltpu.VMEM((6, tokens, width), jnp.bfloat16),
        pltpu.VMEM((tokens, width), jnp.float32),
        pltpu.VMEM((2, 3, OUT_BLOCK, width), jnp.bfloat16),
        pltpu.VMEM((2, heads // 2, seq, seq), jnp.bfloat16),
        pltpu.SemaphoreType.DMA((11,)),
        pltpu.SemaphoreType.DMA((6,)),
    ]
    if remote:
        scratch += [
            pltpu.VMEM((2, apps, 2, tokens, CORE_ROWS), jnp.bfloat16),
            pltpu.VMEM((2, apps, tokens, LANES), jnp.bfloat16),
            pltpu.VMEM((OWN_SLOTS, CORE_ROWS, LANES), jnp.float32),
            pltpu.VMEM((2, CORE_ROWS, LANES), jnp.float32),
            pltpu.VMEM((2, CORE_ROWS, LANES), jnp.float32),
            pltpu.VMEM((AG_SLOTS, CORE_ROWS, LANES), jnp.float32),
            *landing,
            pltpu.SemaphoreType.DMA((2, apps, 3)),
            pltpu.SemaphoreType.DMA((len(STAGES),)),
            pltpu.SemaphoreType.DMA((len(STAGES), 2)),
            pltpu.SemaphoreType.DMA((2,)),
            pltpu.SemaphoreType.DMA((2, 2)),
            pltpu.SemaphoreType.DMA((2,)),
            pltpu.SemaphoreType.DMA((2,)),
            pltpu.SemaphoreType.DMA((2, 2)),
            pltpu.SemaphoreType.REGULAR((2, 5)),
        ]
    params = dict(collective_id=collective_id, has_side_effects=True) if remote else {}
    results = pl.pallas_call(
        functools.partial(finish_kernel, groups, chunks, list(inputs), list(outs), remote),
        out_shape=list(outs.values()),
        in_specs=[pl.BlockSpec(memory_space=pl.ANY)] * len(inputs),
        out_specs=[pl.BlockSpec(memory_space=pl.ANY)] * len(outs),
        scratch_shapes=scratch,
        compiler_params=pltpu.CompilerParams(vmem_limit_bytes=67_043_328, **params),
        cost_estimate=pl.CostEstimate(flops=20 * tokens * width * ff, bytes_accessed=256 * MIB, transcendentals=0),
        name="finish_backward",
    )(*inputs.values())
    return dict(zip(outs, results))


def gradient_groups(width, ff):
    groups = []

    def add(count, lhs, rhs, out, place):
        start = groups[-1]["start"] + groups[-1]["count"] if groups else 0
        groups.append(dict(start=start, count=count, lhs=lhs, rhs=rhs, out=out, place=place))

    def tall(local):
        return TILE_ROWS * local, 0

    def wide(local):
        return TILE_ROWS * lax.rem(local, width // TILE_ROWS), LANES * lax.div(local, width // TILE_ROWS)

    def attention(layer):
        for out, kind in enumerate("qkv"):
            add(width // TILE_ROWS, [f"u_{layer}"], [f"d{kind}_{layer}"], (f"g_{kind}", layer), tall)
        add(width // TILE_ROWS, [f"mixed_{layer}"], [f"dh_{layer}"], ("g_o", layer), tall)

    attention(1)
    add(ff // TILE_ROWS, ["act_0", "act_1"], ["dx_1", "cot"], ("g_down", None), tall)
    add(ff // TILE_ROWS, ["n_0", "n_1"], ["dpre_0", "dpre_1"], ("g_up", None), wide)
    attention(0)
    return groups, sum(group["count"] for group in groups)


def local_operands(x_init, cot_out, w_query, w_key, w_value, w_proj, w_up, w_down):
    batch, seq, width = x_init.shape
    tokens = batch * seq
    at = {"x_0": x_init.reshape(tokens, width), "cot": cot_out.reshape(tokens, width)}
    for layer in (0, 1):
        x_in = at[f"x_{layer}"]
        at[f"u_{layer}"], query, key_act, value = project_qkv(x_in, w_query, w_key, w_value, layer)
        probs, at[f"mixed_{layer}"], hidden, at[f"n_{layer}"] = attend(x_in, query, key_act, value, w_proj, layer, seq)
        if layer == 0:
            at.update(q_0=query, k_0=key_act, v_0=value, probs_0=probs, h_0=hidden)
            at["pre_0"], at["act_0"], at["x_1"] = mlp_forward(hidden, at["n_0"], w_up, w_down)
    at["dpre_1"], at["dh_1"], at["act_1"] = mlp_backward(at["cot"], hidden, at["n_1"], w_up, w_down, True, "mlp_both")
    at["dq_1"], at["dk_1"], at["dv_1"] = attend_backward(at["dh_1"], query, key_act, value, probs, w_proj, 1, seq)
    at.update(wq=w_query, wk=w_key, wv=w_value, wo=w_proj, w_up=w_up, w_down=w_down)
    return at


def solution(mesh):
    def local_step(x_init, cot_out, w_query, w_key, w_value, w_proj, w_up, w_down):
        batch, seq, width = x_init.shape
        inputs = local_operands(x_init, cot_out, w_query, w_key, w_value, w_proj, w_up, w_down)
        groups, chunks = gradient_groups(width, w_up.shape[1])
        weights = dict(g_q=w_query.shape, g_k=w_key.shape, g_v=w_value.shape, g_o=w_proj.shape, g_up=w_up.shape, g_down=w_down.shape)
        res = finish_backward(inputs, groups, chunks, weights, batch * seq, seq)
        return (*(res[name] for name in weights), res["dx_0"].reshape(x_init.shape))

    data_spec = P("data")
    full_spec = P()
    in_specs = (data_spec, data_spec, full_spec, full_spec, full_spec, full_spec, full_spec, full_spec)
    out_specs = (full_spec, full_spec, full_spec, full_spec, full_spec, full_spec, data_spec)
    return jax.shard_map(local_step, mesh=mesh, in_specs=in_specs, out_specs=out_specs, check_vma=False)
```

```python
import functools

import jax
import jax.numpy as jnp
from jax import lax
from jax.experimental import pallas as pl
from jax.experimental.pallas import tpu as pltpu
from jax.sharding import PartitionSpec as P

EPS = 1e-6
HEAD_DIM = 64
PAIR = 2 * HEAD_DIM
FF_BLOCK = 512
OUT_BLOCK = 256
GELU_A = (2.0 / 3.141592653589793) ** 0.5
GELU_B = 0.044715
SOFTMAX_SCALE = HEAD_DIM ** -0.5 * 1.4426950408889634
MIB = 1024 * 1024


def dot(lhs, rhs, lhs_dim, rhs_dim):
    return lax.dot_general(lhs, rhs, (((lhs_dim,), (rhs_dim,)), ((), ())), preferred_element_type=jnp.float32)


def rms_norm(x_f32):
    return x_f32 * lax.rsqrt(jnp.mean(x_f32 * x_f32, axis=-1, keepdims=True) + EPS)


def rms_backward(x_f32, d_out):
    scale = lax.rsqrt(jnp.mean(x_f32 * x_f32, axis=-1, keepdims=True) + EPS)
    inner = jnp.mean(x_f32 * d_out, axis=-1, keepdims=True)
    return scale * d_out - x_f32 * (scale * scale * scale * inner)


def gelu_parts(pre):
    square = pre * pre
    tanh = jnp.tanh(GELU_A * (pre + GELU_B * pre * square))
    half = 0.5 * (1.0 + tanh)
    slope = half + 0.5 * pre * (1.0 - tanh * tanh) * (GELU_A + (3.0 * GELU_A * GELU_B) * square)
    return pre * half, slope


def bf16(*shape):
    return jax.ShapeDtypeStruct(shape, jnp.bfloat16)


def pair_backward(q_pair, k_pair, v_pair, d_pair, low, probs_of):
    sums = [None] * 3
    for side in range(2):
        mask = low if side == 0 else jnp.logical_not(low)
        d_side = jnp.where(mask, d_pair, 0)
        probs_16 = probs_of(side)
        probs_32 = probs_16.astype(jnp.float32)
        d_probs = dot(v_pair, d_side, 1, 1).astype(jnp.bfloat16).astype(jnp.float32)
        row_dot = jnp.sum(d_probs * probs_32, axis=0, keepdims=True)
        d_scores = (probs_32 * (d_probs - row_dot) * HEAD_DIM ** -0.5).astype(jnp.bfloat16)
        parts = (dot(d_scores, jnp.where(mask, k_pair, 0), 0, 0),
                 dot(d_scores, jnp.where(mask, q_pair, 0), 1, 0),
                 dot(probs_16, d_side, 1, 0))
        sums = [part if total is None else total + part for total, part in zip(sums, parts)]
    return sums


def pair_forward(q_pair, k_pair, v_pair, low, keep):
    total = None
    for side in range(2):
        mask = low if side == 0 else jnp.logical_not(low)
        scores = dot(k_pair, jnp.where(mask, q_pair, 0), 1, 1)
        top = jnp.max(scores, axis=0, keepdims=True)
        raised = jnp.exp2((scores - top) * SOFTMAX_SCALE)
        inverse = 1.0 / jnp.sum(raised, axis=0, keepdims=True)
        probs = (raised * inverse).astype(jnp.bfloat16)
        keep(side, probs)
        part = dot(probs, jnp.where(mask, v_pair, 0), 0, 0)
        total = part if total is None else total + part
    return total


FRONT_OUTS = ("u_0", "q_0", "k_0", "v_0", "probs_0", "mixed_0", "h_0", "n_0", "pre_0", "act_0", "x_1",
              "u_1", "mixed_1", "n_1", "act_1", "dpre_1", "dh_1", "dq_1", "dk_1", "dv_1")
ROW_BUFFERS = ("u", "q", "k", "v", "mixed", "h", "n", "x", "dh", "dmix", "dq", "dk", "dv")
PAIRS_AT_ONCE = 2
WIDE_BLOCK = 1024


def front_kernel(batch, seq, in_names, *refs):
    at = dict(zip((*in_names, *FRONT_OUTS), refs))
    refs = refs[len(at):]
    x_all, cot_all, w_in, w_out, w_up, w_down, probs, pre, act = refs[:9]
    row = dict(zip(ROW_BUFFERS, refs[9:]))
    load_sem, out_sem = refs[9 + len(ROW_BUFFERS):]
    width, ff = w_up.shape
    heads = width // HEAD_DIM
    loads = {"x": pltpu.make_async_copy(at["x_0"], x_all, load_sem.at[0])}
    for layer in (0, 1):
        for i, name in enumerate(("wq", "wk", "wv")):
            loads[f"{name}_{layer}"] = pltpu.make_async_copy(at[name].at[layer], w_in.at[layer, i], load_sem.at[1 + 4 * layer + i])
        loads[f"wo_{layer}"] = pltpu.make_async_copy(at["wo"].at[layer], w_out.at[layer], load_sem.at[4 + 4 * layer])
    loads["w_up"] = pltpu.make_async_copy(at["w_up"], w_up, load_sem.at[9])
    loads["w_down"] = pltpu.make_async_copy(at["w_down"], w_down, load_sem.at[10])
    loads["cot"] = pltpu.make_async_copy(at["cot"], cot_all, load_sem.at[11])
    for name in ("x", "wq_0", "wk_0", "wv_0", "wo_0", "w_up", "w_down", "wq_1", "wk_1", "wv_1", "wo_1", "cot"):
        loads[name].start()
    holders = {"probs_0": probs, "pre_0": pre, "act_0": act, "act_1": act, "dpre_1": pre, "x_1": row["x"]}
    for name in FRONT_OUTS:
        holders.setdefault(name, row.get(name[:-2]))

    def store(name, index):
        src = holders[name]
        rows = pl.ds(pl.multiple_of(seq * index, seq), seq)
        dest = at[name].at[index] if name == "probs_0" else at[name].at[rows]
        return pltpu.make_async_copy(src, dest, out_sem.at[FRONT_OUTS.index(name)])

    def one_sequence(index, carry):
        rows = pl.ds(pl.multiple_of(seq * index, seq), seq)
        first = index == 0
        low = lax.broadcasted_iota(jnp.int32, (seq, PAIR), 1) < HEAD_DIM

        def need(*names):
            @pl.when(first)
            def _():
                for name in names:
                    loads[name].wait()

        def free(*names, same=False):
            for name in names:
                if same:
                    store(name, index).wait()
                else:
                    pl.when(index > 0)(lambda name=name: store(name, index - 1).wait())

        def send(*names):
            for name in names:
                store(name, index).start()

        def over(count, fn):
            lax.fori_loop(0, count, lambda j, carry: fn(j) or carry, 0)

        def attention(layer):
            x_in = x_all[rows] if layer == 0 else row["x"][...]
            row["u"][...] = rms_norm(x_in.astype(jnp.float32)).astype(jnp.bfloat16)
            for i, kind in enumerate("qkv"):
                need(f"w{kind}_{layer}")
                row[kind][...] = dot(row["u"][...], w_in[layer, i], 1, 0).astype(jnp.bfloat16)

            def pairs(j):
                for extra in range(PAIRS_AT_ONCE):
                    which = PAIRS_AT_ONCE * j + extra
                    lanes = pl.ds(pl.multiple_of(PAIR * which, PAIR), PAIR)

                    def keep(side, value):
                        probs[2 * which + side] = value
                    out = pair_forward(row["q"][:, lanes], row["k"][:, lanes], row["v"][:, lanes], low, keep)
                    row["mixed"][:, lanes] = out.astype(jnp.bfloat16)
            over(heads // 2 // PAIRS_AT_ONCE, pairs)
            need(f"wo_{layer}")
            attn = dot(row["mixed"][...], w_out[layer], 1, 0).astype(jnp.bfloat16)
            hidden = (x_in.astype(jnp.float32) + attn.astype(jnp.float32)).astype(jnp.bfloat16)
            row["h"][...] = hidden
            row["n"][...] = rms_norm(hidden.astype(jnp.float32)).astype(jnp.bfloat16)

        need("x")
        free("u_1")
        free("dq_1", "dk_1", "dv_1", "mixed_1", "n_1", "dh_1")
        attention(0)
        send("u_0", "q_0", "k_0", "v_0", "probs_0", "mixed_0", "h_0", "n_0")
        need("w_up")
        free("act_1", "dpre_1")

        def up(j):
            lanes = pl.ds(pl.multiple_of(WIDE_BLOCK * j, WIDE_BLOCK), WIDE_BLOCK)
            raw = dot(row["n"][...], w_up[:, lanes], 1, 0).astype(jnp.bfloat16)
            pre[:, lanes] = raw
            act[:, lanes] = gelu_parts(raw.astype(jnp.float32))[0].astype(jnp.bfloat16)
        over(ff // WIDE_BLOCK, up)
        send("pre_0", "act_0")
        need("w_down")

        def down(j):
            lanes = pl.ds(pl.multiple_of(OUT_BLOCK * j, OUT_BLOCK), OUT_BLOCK)
            out = dot(act[...], w_down[:, lanes], 1, 0).astype(jnp.bfloat16).astype(jnp.float32)
            row["x"][:, lanes] = (row["h"][:, lanes].astype(jnp.float32) + out).astype(jnp.bfloat16)
        over(width // OUT_BLOCK, down)
        send("x_1")
        free("u_0", "q_0", "k_0", "v_0", "probs_0", "mixed_0", "h_0", "n_0", same=True)
        attention(1)
        send("u_1", "mixed_1", "n_1")
        need("cot")
        free("pre_0", "act_0", same=True)

        def both(j):
            lanes = pl.ds(pl.multiple_of(WIDE_BLOCK * j, WIDE_BLOCK), WIDE_BLOCK)
            raw = dot(row["n"][...], w_up[:, lanes], 1, 0).astype(jnp.bfloat16).astype(jnp.float32)
            d_act = dot(cot_all[rows], w_down[lanes], 1, 1).astype(jnp.bfloat16).astype(jnp.float32)
            out, slope = gelu_parts(raw)
            act[:, lanes] = out.astype(jnp.bfloat16)
            pre[:, lanes] = (d_act * slope).astype(jnp.bfloat16)
        over(ff // WIDE_BLOCK, both)
        send("act_1", "dpre_1")

        def back(j):
            lanes = pl.ds(pl.multiple_of(OUT_BLOCK * j, OUT_BLOCK), OUT_BLOCK)
            row["dmix"][:, lanes] = dot(pre[...], w_up[lanes], 1, 1).astype(jnp.bfloat16)
        over(width // OUT_BLOCK, back)
        d_hidden = cot_all[rows].astype(jnp.float32) + rms_backward(
            row["h"][...].astype(jnp.float32), row["dmix"][...].astype(jnp.float32))
        row["dh"][...] = d_hidden.astype(jnp.bfloat16)
        send("dh_1")
        row["dmix"][...] = dot(row["dh"][...], w_out[1], 1, 1).astype(jnp.bfloat16)

        def pairs_back(j):
            for extra in range(PAIRS_AT_ONCE):
                which = PAIRS_AT_ONCE * j + extra
                lanes = pl.ds(pl.multiple_of(PAIR * which, PAIR), PAIR)
                sums = pair_backward(*(row[name][:, lanes] for name in ("q", "k", "v", "dmix")), low,
                                     lambda side: probs[2 * which + side])
                for name, total in zip(("dq", "dk", "dv"), sums):
                    row[name][:, lanes] = total.astype(jnp.bfloat16)
        over(heads // 2 // PAIRS_AT_ONCE, pairs_back)
        send("dq_1", "dk_1", "dv_1")
        free("x_1", same=True)
        return carry

    lax.fori_loop(0, batch, one_sequence, 0)
    for name in ("u_1", "mixed_1", "n_1", "act_1", "dpre_1", "dh_1", "dq_1", "dk_1", "dv_1"):
        store(name, batch - 1).wait()


def front(inputs, batch, seq):
    tokens, width = inputs["x_0"].shape
    ff = inputs["w_up"].shape[1]
    heads = width // HEAD_DIM
    shapes = []
    for name in FRONT_OUTS:
        if name == "probs_0":
            shapes.append(bf16(batch, heads, seq, seq))
        else:
            shapes.append(bf16(tokens, ff if name[:-2] in ("pre", "act", "dpre") else width))
    block = lambda *shape: pltpu.VMEM(shape, jnp.bfloat16)
    scratch = [
        block(tokens, width), block(tokens, width), block(2, 3, width, width), block(2, width, width), block(width, ff),
        block(ff, width), block(heads, seq, seq), block(seq, ff), block(seq, ff),
        *[block(seq, width) for _ in ROW_BUFFERS],
        pltpu.SemaphoreType.DMA((12,)), pltpu.SemaphoreType.DMA((len(FRONT_OUTS),)),
    ]
    outs = pl.pallas_call(
        functools.partial(front_kernel, batch, seq, tuple(inputs)),
        out_shape=shapes,
        in_specs=[pl.BlockSpec(memory_space=pl.ANY)] * len(inputs),
        out_specs=[pl.BlockSpec(memory_space=pl.ANY)] * len(shapes),
        scratch_shapes=scratch,
        compiler_params=pltpu.CompilerParams(vmem_limit_bytes=67_043_328),
        cost_estimate=pl.CostEstimate(flops=22 * tokens * width * ff // 2, bytes_accessed=100 * MIB, transcendentals=0),
        name="front",
    )(*inputs.values())
    return dict(zip(FRONT_OUTS, outs))


MESH = pl.DeviceIdType.MESH
LANES = 1024
SET_ROWS = 128
CORE_ROWS = 2 * SET_ROWS
TILE_ROWS = 2 * CORE_ROWS
OWN_SLOTS = 8
AG_SLOTS = 10
TYPES = {
    "p1": (0, 0, 80, "xyz"),
    "q1": (0, 80, 48, "zxy"),
    "p2": (1, 128, 80, "yxz"),
    "q2": (1, 208, 48, "zyx"),
}
WRITE_AT = 11


def stage_list():
    stages = []
    for name, (_, _, _, order) in TYPES.items():
        if order[2] == "z":
            plan = [("rs1", 1), ("rs2", 2), ("rsz", 3), ("agz", 6), ("ag2", 9), ("ag1", 10)]
        else:
            plan = [("rsz", 1), ("rs1", 4), ("rs2", 5), ("ag2", 6), ("ag1", 7), ("agz", 8)]
        for kind, at in plan:
            if kind in ("rsz", "agz"):
                for step in range(3):
                    for way in (0, 1):
                        stages.append((name, kind, step, way, at + step))
            else:
                stages.append((name, kind, 0, 0, at))
    return stages


STAGES = stage_list()


def piece_shape(name, kind):
    rows, order = TYPES[name][2], TYPES[name][3]
    if order[2] == "z":
        return {"rs1": (rows, 512), "rs2": (rows, 256), "rsz": (rows // 2, 128)}[kind]
    return {"rsz": (rows // 2, 512), "rs1": (rows // 2, 256), "rs2": (rows // 2, 128)}[kind]


def between(step, first, count):
    return jnp.logical_and(step >= first, step < first + count)


class Backward:
    PB_1, MB, AB, PB_0 = 2, 6, 14, 23
    ROWS = 256

    def __init__(self, at, big, total_buf, w_buf, p_buf, sem, drain):
        self.at, self.big, self.total, self.w, self.p, self.sem, self.drain = at, big, total_buf, w_buf, p_buf, sem, drain
        self.tokens, self.width = at["x_0"].shape
        self.heads = at["probs_0"].shape[1]
        self.seq = at["probs_0"].shape[2]

    def load(self, name, dest, sem, *index):
        ref = self.at[name]
        return pltpu.make_async_copy(ref.at[index] if index else ref, dest, self.sem.at[sem])

    def store(self, src, name, sem, *index):
        ref = self.at[name]
        return pltpu.make_async_copy(src, ref.at[index] if index else ref, self.drain.at[sem])

    def row_blocks(self, fn):
        def body(block, carry):
            fn(pl.ds(pl.multiple_of(self.ROWS * block, self.ROWS), self.ROWS))
            return carry
        lax.fori_loop(0, self.tokens // self.ROWS, body, 0)

    def input_loads(self, layer):
        spot = 4 if layer else 5
        copies = [self.load(f"d{kind}_{layer}", self.big.at[i], i) for i, kind in enumerate("qkv")]
        copies.append(self.load(f"x_{layer}", self.big.at[spot], 3))
        if layer:
            copies.append(self.load("dh_1", self.big.at[5], 4))
        return copies

    def weight_loads(self, layer, block):
        rows = pl.ds(pl.multiple_of(OUT_BLOCK * block, OUT_BLOCK), OUT_BLOCK)
        slot = lax.rem(block, 2)
        return [self.load(name, self.w.at[slot, i], 5 + 3 * slot + i, layer, rows) for i, name in enumerate(("wq", "wk", "wv"))]

    def input_block(self, layer, block):
        big, blocks = self.big, self.width // OUT_BLOCK
        slot = lax.rem(block, 2)

        @pl.when(block == 0)
        def _():
            for copy in self.input_loads(layer):
                copy.wait()
        for copy in self.weight_loads(layer, block):
            copy.wait()

        @pl.when(block + 1 < blocks)
        def _():
            for copy in self.weight_loads(layer, block + 1):
                copy.start()
        lanes = pl.ds(pl.multiple_of(OUT_BLOCK * block, OUT_BLOCK), OUT_BLOCK)

        def product(rows):
            total = dot(big[0, rows], self.w[slot, 0], 1, 1) + dot(big[1, rows], self.w[slot, 1], 1, 1)
            big[3, rows, lanes] = (total + dot(big[2, rows], self.w[slot, 2], 1, 1)).astype(jnp.bfloat16)
        self.row_blocks(product)

        @pl.when(block == blocks - 1)
        def _():
            x_at, d_at = (4, 5) if layer else (5, 4)

            def close(rows):
                back = rms_backward(big[x_at, rows].astype(jnp.float32), big[3, rows].astype(jnp.float32))
                big[3, rows] = (big[d_at, rows].astype(jnp.float32) + back).astype(jnp.bfloat16)
                if layer:
                    self.total[rows] = jnp.zeros((self.ROWS, self.width), jnp.float32)
            self.row_blocks(close)
            self.store(big.at[3], f"dx_{layer}", 0).start()
            if layer:
                self.load("h_0", big.at[4], 3).start()
                for copy in self.mlp_loads(0):
                    copy.start()

    def mlp_loads(self, block):
        slot = lax.rem(block, 2)
        lanes = pl.ds(pl.multiple_of(FF_BLOCK * block, FF_BLOCK), FF_BLOCK)
        half = pl.ds(pl.multiple_of(FF_BLOCK * slot, FF_BLOCK), FF_BLOCK)
        return [self.load("w_up", self.big.at[0, :, half], 5 + 3 * slot, slice(None), lanes),
                self.load("pre_0", self.big.at[1, :, half], 6 + 3 * slot, slice(None), lanes),
                self.load("w_down", self.big.at[5, half], 7 + 3 * slot, lanes)]

    def mlp_store(self, block):
        half = pl.ds(pl.multiple_of(FF_BLOCK * lax.rem(block, 2), FF_BLOCK), FF_BLOCK)
        lanes = pl.ds(pl.multiple_of(FF_BLOCK * block, FF_BLOCK), FF_BLOCK)
        return self.store(self.big.at[2, :, half], "dpre_0", 1, slice(None), lanes)

    def mlp_block(self, block):
        big, blocks = self.big, self.at["w_up"].shape[1] // FF_BLOCK

        @pl.when(block == 0)
        def _():
            self.store(big.at[3], "dx_1", 0).wait()
            self.load("h_0", big.at[4], 3).wait()
        for copy in self.mlp_loads(block):
            copy.wait()

        @pl.when(block + 1 < blocks)
        def _():
            for copy in self.mlp_loads(block + 1):
                copy.start()

        @pl.when(block > 0)
        def _():
            self.mlp_store(block - 1).wait()
        half = pl.ds(pl.multiple_of(FF_BLOCK * lax.rem(block, 2), FF_BLOCK), FF_BLOCK)

        def product(rows):
            d_act = dot(big[3, rows], big[5, half], 1, 1).astype(jnp.bfloat16).astype(jnp.float32)
            slope = gelu_parts(big[1, rows, half].astype(jnp.float32))[1]
            d_pre = (d_act * slope).astype(jnp.bfloat16)
            big[2, rows, half] = d_pre
            self.total[rows] += dot(d_pre, big[0, :, half], 1, 1)
        self.row_blocks(product)
        self.mlp_store(block).start()

        @pl.when(block == blocks - 1)
        def _():
            def close(rows):
                d_normed = self.total[rows].astype(jnp.bfloat16).astype(jnp.float32)
                back = rms_backward(big[4, rows].astype(jnp.float32), d_normed)
                big[4, rows] = (big[3, rows].astype(jnp.float32) + back).astype(jnp.bfloat16)
            self.row_blocks(close)
            self.store(big.at[4], "dh_0", 2).start()
            self.load("wo", big.at[0], 4, 0).start()
            for copy in self.seq_loads(0) + self.probs_loads(0):
                copy.start()

    def seq_loads(self, seq):
        rows = pl.ds(pl.multiple_of(self.seq * seq, self.seq), self.seq)
        return [self.load(f"{kind}_0", self.big.at[1 + lax.rem(seq, 2), pl.ds(self.seq * i, self.seq)], i, rows)
                for i, kind in enumerate("qkv")]

    def probs_loads(self, piece):
        half = self.heads // 2
        heads = pl.ds(half * lax.rem(piece, 2), half)
        return [self.load("probs_0", self.p.at[lax.rem(piece, 2)], 5 + lax.rem(piece, 2), lax.div(piece, 2), heads)]

    def seq_stores(self, piece):
        seq, half = lax.div(piece, 2), lax.rem(piece, 2)
        rows = pl.ds(pl.multiple_of(self.seq * seq, self.seq), self.seq)
        lanes = pl.ds(pl.multiple_of(self.width // 2 * half, PAIR), self.width // 2)
        spot = 5 - 2 * lax.rem(seq, 2)
        return [self.store(self.big.at[spot, pl.ds(self.seq * i, self.seq), lanes], f"d{kind}_0", 3 + i, rows, lanes)
                for i, kind in enumerate("qkv")]

    def attention_piece(self, piece):
        big, pieces = self.big, 2 * (self.tokens // self.seq)
        seq, half = lax.div(piece, 2), lax.rem(piece, 2)
        spot, out = 1 + lax.rem(seq, 2), 5 - 2 * lax.rem(seq, 2)

        @pl.when(piece == 0)
        def _():
            self.mlp_store(self.at["w_up"].shape[1] // FF_BLOCK - 1).wait()
            self.store(big.at[4], "dh_0", 2).wait()
            self.load("wo", big.at[0], 4, 0).wait()

        @pl.when(piece > 0)
        def _():
            for copy in self.seq_stores(piece - 1):
                copy.wait()
        for copy in self.probs_loads(piece):
            copy.wait()

        @pl.when(piece + 1 < pieces)
        def _():
            for copy in self.probs_loads(piece + 1):
                copy.start()
        mixed = pl.ds(3 * self.seq, self.seq)

        @pl.when(half == 0)
        def _():
            for copy in self.seq_loads(seq):
                copy.wait()

            @pl.when(piece + 2 < pieces)
            def _():
                for copy in self.seq_loads(seq + 1):
                    copy.start()
            rows = pl.ds(pl.multiple_of(self.seq * seq, self.seq), self.seq)
            big[spot, mixed] = dot(big[4, rows], big[0], 1, 1).astype(jnp.bfloat16)
        low = lax.broadcasted_iota(jnp.int32, (self.seq, PAIR), 1) < HEAD_DIM
        pairs = self.heads // 4

        def pair(j, carry):
            lanes = pl.ds(pl.multiple_of(PAIR * (pairs * half + j), PAIR), PAIR)
            q_pair, k_pair, v_pair, d_pair = (big[spot, pl.ds(self.seq * i, self.seq), lanes] for i in range(4))
            for i, total in enumerate(pair_backward(q_pair, k_pair, v_pair, d_pair, low, lambda side: self.p[half, 2 * j + side])):
                big[out, pl.ds(self.seq * i, self.seq), lanes] = total.astype(jnp.bfloat16)
            return carry
        lax.fori_loop(0, pairs, pair, 0)
        for copy in self.seq_stores(piece):
            copy.start()

    def item(self, step):
        blocks = self.width // OUT_BLOCK
        pieces = 2 * (self.tokens // self.seq)

        @pl.when(step == self.PB_1)
        def _():
            for copy in self.input_loads(1) + self.weight_loads(1, 0):
                copy.start()
        pl.when(between(step, self.PB_1, blocks))(lambda: self.input_block(1, step - self.PB_1))
        pl.when(between(step, self.MB, 8))(lambda: self.mlp_block(step - self.MB))
        pl.when(between(step, self.AB, pieces))(lambda: self.attention_piece(step - self.AB))

        @pl.when(step == self.PB_0 - 1)
        def _():
            for copy in self.seq_stores(pieces - 1):
                copy.wait()
            for copy in self.input_loads(0) + self.weight_loads(0, 0):
                copy.start()
        pl.when(between(step, self.PB_0, blocks))(lambda: self.input_block(0, step - self.PB_0))

        @pl.when(step == self.PB_0 + blocks)
        def _():
            self.store(self.big.at[3], "dx_0", 0).wait()


def finish_kernel(groups, chunks, in_names, out_names, remote, *refs):
    names = [*in_names, *out_names]
    at, scratch = dict(zip(names, refs[:len(names)])), refs[len(names):]
    (big, total_buf, w_buf, p_buf, item_sem, drain_sem), scratch = scratch[:6], scratch[6:]
    backward = Backward(at, big, total_buf, w_buf, p_buf, item_sem, drain_sem)
    if not remote:
        lax.fori_loop(0, chunks + WRITE_AT + 1, lambda step, carry: backward.item(step) or carry, 0)
        return
    (lhs_buf, rhs_buf, own, part, part_in, gath), scratch = scratch[:6], scratch[6:]
    land_keys = [key for key, st in enumerate(STAGES) if st[1].startswith("rs")]
    landing = dict(zip(land_keys, scratch[:len(land_keys)]))
    load_sem, send_sem, recv_sem, pair_send, pair_recv, out_sem, out_send, out_recv, credit = scratch[len(land_keys):]

    me = lax.axis_index("data")
    core = lax.rem(me, 2)
    coord = {"x": lax.rem(lax.div(me, 2), 2), "y": lax.rem(lax.div(me, 4), 2)}
    z = lax.div(me, 8)
    partner = me + 1 - 2 * core
    near = {"x": me + 2 - 4 * coord["x"], "y": me + 4 - 8 * coord["y"]}
    up_ok, down_ok = z < 3, z > 0
    peers = [(partner, 0, None), (near["x"], 1, None), (near["y"], 2, None), (me + 8, 3, up_ok), (me - 8, 4, down_ok)]

    def guarded(cond, fn):
        if cond is None:
            fn()
        else:
            pl.when(cond)(fn)

    barrier = pltpu.get_barrier_semaphore()
    for dev, _, cond in peers:
        guarded(cond, lambda dev=dev: pl.semaphore_signal(barrier, inc=1, device_id=(dev,), device_id_type=MESH))
    inner = jnp.logical_and(up_ok, down_ok)
    guarded(inner, lambda: pl.semaphore_wait(barrier, 5))
    guarded(jnp.logical_not(inner), lambda: pl.semaphore_wait(barrier, 4))

    def region(name, kind, which):
        _, row, rows, order = TYPES[name]
        if order[2] == "z":
            h1, h2 = coord[order[0]], coord[order[1]]
            if kind == "1":
                return pl.ds(row, rows), pl.ds(pl.multiple_of(512 * which, 128), 512)
            if kind == "2":
                return pl.ds(row, rows), pl.ds(pl.multiple_of(512 * h1 + 256 * which, 128), 256)
            first = pl.multiple_of(row + (rows // 2) * lax.div(which, 2), 8)
            lane = pl.multiple_of(512 * h1 + 256 * h2 + 128 * lax.rem(which, 2), 128)
            return pl.ds(first, rows // 2), pl.ds(lane, 128)
        h1 = coord[order[1]]
        if kind == "z":
            first = pl.multiple_of(row + (rows // 2) * lax.div(which, 2), 8)
            return pl.ds(first, rows // 2), pl.ds(pl.multiple_of(512 * lax.rem(which, 2), 128), 512)
        first = pl.multiple_of(row + (rows // 2) * lax.div(z, 2), 8)
        if kind == "1":
            return pl.ds(first, rows // 2), pl.ds(pl.multiple_of(512 * lax.rem(z, 2) + 256 * which, 128), 256)
        lane = pl.multiple_of(512 * lax.rem(z, 2) + 256 * h1 + 128 * which, 128)
        return pl.ds(first, rows // 2), pl.ds(lane, 128)

    def exchange_axis(name, kind):
        order = TYPES[name][3]
        dims = order[:2] if order[2] == "z" else order[1:]
        return dims[int(kind) - 1]

    def plan(key, chunk, parity):
        name, kind, step, way, _ = STAGES[key]
        mine, slot = lax.rem(chunk, OWN_SLOTS), lax.rem(chunk, AG_SLOTS)
        if kind in ("rs1", "rs2"):
            axis = exchange_axis(name, kind[2])
            src, keep = region(name, kind[2], 1 - coord[axis]), region(name, kind[2], coord[axis])
            dev, send_ok, recv_ok = near[axis], None, None
            sent = own.at[mine, src[0], src[1]]
        elif kind in ("ag1", "ag2"):
            axis = exchange_axis(name, kind[2])
            src = keep = region(name, kind[2], coord[axis])
            dev, send_ok, recv_ok = near[axis], None, None
            sent = gath.at[slot, src[0], src[1]]
        elif kind == "rsz":
            if way:
                dev, k_send, k_keep = me + 8, z + 3 - step, z + 2 - step
                send_ok, recv_ok = k_send <= 3, jnp.logical_and(k_keep <= 3, down_ok)
            else:
                dev, k_send, k_keep = me - 8, z - 3 + step, z - 2 + step
                send_ok, recv_ok = k_send >= 0, jnp.logical_and(k_keep >= 0, up_ok)
            src, keep = region(name, "z", k_send), region(name, "z", k_keep)
            sent = own.at[mine, src[0], src[1]]
        else:
            if way:
                dev, k_send, k_keep = me + 8, z - step, z - 1 - step
                send_ok, recv_ok = jnp.logical_and(k_send >= 0, up_ok), k_keep >= 0
            else:
                dev, k_send, k_keep = me - 8, z + step, z + 1 + step
                send_ok, recv_ok = jnp.logical_and(k_send <= 3, down_ok), k_keep <= 3
            src, keep = region(name, "z", k_send), region(name, "z", k_keep)
            sent = gath.at[slot, src[0], src[1]]
        sems = dict(send_sem=send_sem.at[key], recv_sem=recv_sem.at[key, parity], device_id=(dev,), device_id_type=MESH)
        if kind.startswith("rs"):
            target = landing[key].at[parity]
            send = lambda: pltpu.make_async_remote_copy(src_ref=sent, dst_ref=target, **sems)
            recv = lambda: pltpu.make_async_remote_copy(
                src_ref=own.at[mine, keep[0], keep[1]], dst_ref=target, **sems)

            def arrive():
                own[mine, keep[0], keep[1]] += landing[key][parity]
        else:
            send = lambda: pltpu.make_async_remote_copy(src_ref=sent, dst_ref=sent, **sems)
            recv = lambda: pltpu.make_async_remote_copy(
                src_ref=gath.at[slot, keep[0], keep[1]], dst_ref=gath.at[slot, keep[0], keep[1]], **sems)
            arrive = None
        return send, recv, send_ok, recv_ok, arrive

    def finish(name, chunk):
        order = TYPES[name][3]
        reg = region(name, "z", z) if order[2] == "z" else region(name, "2", coord[order[2]])
        gath[lax.rem(chunk, AG_SLOTS), reg[0], reg[1]] = own[lax.rem(chunk, OWN_SLOTS), reg[0], reg[1]]

    def valid(chunk):
        return jnp.logical_and(chunk >= 0, chunk < chunks)

    def set_rows(half):
        return pl.ds(half * SET_ROWS, SET_ROWS)

    def pair_copy(half, parity):
        return pltpu.make_async_remote_copy(
            src_ref=part.at[parity, set_rows(half)], dst_ref=part_in.at[parity, set_rows(half)],
            send_sem=pair_send.at[half], recv_sem=pair_recv.at[half, parity], device_id=(partner,), device_id_type=MESH)

    def out_copies(half, group, local, whose):
        out, layer = group["out"]
        ref = at[out] if layer is None else at[out].at[layer]
        rows, cols = group["place"](local)
        first = pl.multiple_of(rows + CORE_ROWS * whose + half * SET_ROWS, SET_ROWS)
        return ref.at[pl.ds(first, SET_ROWS), pl.ds(pl.multiple_of(cols, 128), LANES)]

    def write_copies(half, chunk, dest):
        slot = lax.rem(chunk, AG_SLOTS)
        src = gath.at[slot, set_rows(half)]
        here = pltpu.make_async_copy(src, dest, out_sem.at[half])
        there = pltpu.make_async_remote_copy(
            src_ref=src, dst_ref=dest, send_sem=out_send.at[half], recv_sem=out_recv.at[half, lax.rem(chunk, 2)],
            device_id=(partner,), device_id_type=MESH)
        return here, there

    def load_copies(group, local, slot):
        rows, cols = group["place"](local)
        copies = []
        for app, (lhs, rhs) in enumerate(zip(group["lhs"], group["rhs"])):
            for whose in (0, 1):
                first = rows + CORE_ROWS * (core if whose == 0 else 1 - core)
                copies.append(pltpu.make_async_copy(
                    at[lhs].at[:, pl.ds(pl.multiple_of(first, CORE_ROWS), CORE_ROWS)],
                    lhs_buf.at[slot, app, whose], load_sem.at[slot, app, whose]))
            copies.append(pltpu.make_async_copy(
                at[rhs].at[:, pl.ds(pl.multiple_of(cols, 128), LANES)], rhs_buf.at[slot, app], load_sem.at[slot, app, 2]))
        return copies

    def for_group(chunk, fn):
        for group in groups:
            inside = jnp.logical_and(chunk >= group["start"], chunk < group["start"] + group["count"])
            pl.when(inside)(functools.partial(fn, group, chunk - group["start"]))

    def two_apps(chunk):
        flags = [jnp.logical_and(chunk >= g["start"], chunk < g["start"] + g["count"]) for g in groups if len(g["lhs"]) == 2]
        return functools.reduce(jnp.logical_or, flags)

    def start_load(chunk):
        def go(group, local):
            for copy in load_copies(group, local, lax.rem(chunk, 2)):
                copy.start()
        for_group(chunk, go)

    def wait_load(chunk):
        slot = lax.rem(chunk, 2)
        any_two = next(g for g in groups if len(g["lhs"]) == 2)
        copies = load_copies(any_two, 0, slot)
        for copy in copies[:3]:
            copy.wait()

        @pl.when(two_apps(chunk))
        def _():
            for copy in copies[3:]:
                copy.wait()

    def tile(chunk):
        slot, mine, parity = lax.rem(chunk, 2), lax.rem(chunk, OWN_SLOTS), lax.rem(chunk, 2)

        def product(app, whose):
            return lax.dot_general(lhs_buf[slot, app, whose], rhs_buf[slot, app], (((0,), (0,)), ((), ())),
                                   preferred_element_type=jnp.float32)

        own[mine] = product(0, 0)
        part[parity] = product(0, 1)

        @pl.when(two_apps(chunk))
        def _():
            own[mine] += product(1, 0)
            part[parity] += product(1, 1)

    last = chunks + WRITE_AT

    def section(half, step):
        before = lax.rem(step + 1, 2)
        now = lax.rem(step, 2)

        @pl.when(valid(step - 1))
        def _():
            copy = pair_copy(half, before)
            copy.wait_send()
            copy.wait_recv()
            mine = lax.rem(step - 1, OWN_SLOTS)
            own[mine, set_rows(half)] += part_in[before, set_rows(half)]

        names = [name for name in TYPES if TYPES[name][0] == half]
        keys = [key for key, st in enumerate(STAGES) if st[0] in names]
        finals = {name: max(st[4] for st in STAGES if st[0] == name and st[1].startswith("rs")) for name in names}
        for key in keys:
            name, at = STAGES[key][0], STAGES[key][4]
            chunk = step - 1 - at

            @pl.when(valid(chunk))
            def _(key=key, chunk=chunk):
                send, recv, send_ok, recv_ok, arrive = plan(key, chunk, before)

                def arrived():
                    recv().wait_recv()
                    if arrive is not None:
                        arrive()
                guarded(recv_ok, arrived)
                guarded(send_ok, lambda: send().wait_send())
        for name in names:
            chunk = step - 1 - finals[name]
            pl.when(valid(chunk))(functools.partial(finish, name, chunk))

        done = step - 1 - WRITE_AT

        @pl.when(valid(done))
        def _():
            here, there = write_copies(half, done, out_copies(half, groups[0], 0, 0))
            here.wait()
            there.wait_send()
            there.wait_recv()

        @pl.when(step < last)
        def _():
            for dev, way, cond in peers:
                to = way if way < 3 else 7 - way
                guarded(cond, lambda dev=dev, to=to: pl.semaphore_signal(
                    credit.at[half, to], inc=1, device_id=(dev,), device_id_type=MESH))

        @pl.when(step > 0)
        def _():
            for dev, way, cond in peers:
                guarded(cond, lambda way=way: pl.semaphore_wait(credit.at[half, way], 1))

        for key in reversed(keys):
            chunk = step - STAGES[key][4]

            @pl.when(valid(chunk))
            def _(key=key, chunk=chunk):
                send, recv, send_ok, recv_ok, arrive = plan(key, chunk, now)
                guarded(send_ok, lambda: send().start())

        out_chunk = step - WRITE_AT

        @pl.when(valid(out_chunk))
        def _():
            def go(group, local):
                for copy in write_copies(half, out_chunk, out_copies(half, group, local, core)):
                    copy.start()
            for_group(out_chunk, go)

    start_load(jnp.int32(0))

    def round_(step, carry):
        section(0, step)

        @pl.when(valid(step))
        def _():
            pl.when(step + 1 < chunks)(lambda: start_load(step + 1))
            wait_load(step)
            tile(step)
            pair_copy(0, lax.rem(step, 2)).start()

        section(1, step)

        @pl.when(valid(step))
        def _():
            pair_copy(1, lax.rem(step, 2)).start()

        backward.item(step)
        return carry

    lax.fori_loop(0, last + 1, round_, 0)


def finish_backward(inputs, groups, chunks, weights, tokens, seq, collective_id=0, remote=True):
    width, ff = inputs["w_up"].shape
    landing = [pltpu.VMEM((2,) + piece_shape(st[0], st[1]), jnp.float32) for st in STAGES if st[1].startswith("rs")]
    apps = 2
    outs = {name: jax.ShapeDtypeStruct(shape, jnp.float32) for name, shape in weights.items()}
    for name in ("dx_0", "dx_1", "dh_0", "dq_0", "dk_0", "dv_0"):
        outs[name] = bf16(tokens, width)
    outs["dpre_0"] = bf16(tokens, ff)
    heads = width // HEAD_DIM
    scratch = [
        pltpu.VMEM((6, tokens, width), jnp.bfloat16),
        pltpu.VMEM((tokens, width), jnp.float32),
        pltpu.VMEM((2, 3, OUT_BLOCK, width), jnp.bfloat16),
        pltpu.VMEM((2, heads // 2, seq, seq), jnp.bfloat16),
        pltpu.SemaphoreType.DMA((11,)),
        pltpu.SemaphoreType.DMA((6,)),
    ]
    if remote:
        scratch += [
            pltpu.VMEM((2, apps, 2, tokens, CORE_ROWS), jnp.bfloat16),
            pltpu.VMEM((2, apps, tokens, LANES), jnp.bfloat16),
            pltpu.VMEM((OWN_SLOTS, CORE_ROWS, LANES), jnp.float32),
            pltpu.VMEM((2, CORE_ROWS, LANES), jnp.float32),
            pltpu.VMEM((2, CORE_ROWS, LANES), jnp.float32),
            pltpu.VMEM((AG_SLOTS, CORE_ROWS, LANES), jnp.float32),
            *landing,
            pltpu.SemaphoreType.DMA((2, apps, 3)),
            pltpu.SemaphoreType.DMA((len(STAGES),)),
            pltpu.SemaphoreType.DMA((len(STAGES), 2)),
            pltpu.SemaphoreType.DMA((2,)),
            pltpu.SemaphoreType.DMA((2, 2)),
            pltpu.SemaphoreType.DMA((2,)),
            pltpu.SemaphoreType.DMA((2,)),
            pltpu.SemaphoreType.DMA((2, 2)),
            pltpu.SemaphoreType.REGULAR((2, 5)),
        ]
    params = dict(collective_id=collective_id, has_side_effects=True) if remote else {}
    results = pl.pallas_call(
        functools.partial(finish_kernel, groups, chunks, list(inputs), list(outs), remote),
        out_shape=list(outs.values()),
        in_specs=[pl.BlockSpec(memory_space=pl.ANY)] * len(inputs),
        out_specs=[pl.BlockSpec(memory_space=pl.ANY)] * len(outs),
        scratch_shapes=scratch,
        compiler_params=pltpu.CompilerParams(vmem_limit_bytes=67_043_328, **params),
        cost_estimate=pl.CostEstimate(flops=20 * tokens * width * ff, bytes_accessed=256 * MIB, transcendentals=0),
        name="finish_backward",
    )(*inputs.values())
    return dict(zip(outs, results))


DELIVER_ROWS = 512
DELIVER_SLOTS = 16
DELIVER_AHEAD = 8


def deliver(arrays):
    def blocks_of(array):
        lead = [(i,) for i in range(array.shape[0])] if len(array.shape) == 3 else [()]
        rows, cols = array.shape[-2:]
        return [(*index, pl.ds(row, DELIVER_ROWS), pl.ds(col, LANES))
                for index in lead for row in range(0, rows, DELIVER_ROWS) for col in range(0, cols, LANES)]

    work = [(i, index) for i, array in enumerate(arrays) for index in blocks_of(array)]
    count = len(arrays)

    def kernel(*refs):
        ins, outs, buf, in_sem, out_sem = refs[:count], refs[count:2 * count], *refs[2 * count:]

        def fetch(t):
            i, index = work[t]
            return pltpu.make_async_copy(ins[i].at[index], buf.at[t % DELIVER_SLOTS], in_sem.at[t % DELIVER_SLOTS])

        def put(t):
            i, index = work[t]
            return pltpu.make_async_copy(buf.at[t % DELIVER_SLOTS], outs[i].at[index], out_sem.at[t % DELIVER_SLOTS])

        for t in range(min(DELIVER_AHEAD, len(work))):
            fetch(t).start()
        for t in range(len(work)):
            if t + DELIVER_AHEAD < len(work):
                if t + DELIVER_AHEAD >= DELIVER_SLOTS:
                    put(t + DELIVER_AHEAD - DELIVER_SLOTS).wait()
                fetch(t + DELIVER_AHEAD).start()
            fetch(t).wait()
            put(t).start()
        for t in range(max(0, len(work) - DELIVER_SLOTS), len(work)):
            put(t).wait()

    return pl.pallas_call(
        kernel,
        out_shape=[jax.ShapeDtypeStruct(array.shape, array.dtype) for array in arrays],
        in_specs=[pl.BlockSpec(memory_space=pl.ANY)] * count,
        out_specs=[pl.BlockSpec(memory_space=pl.ANY)] * count,
        scratch_shapes=[pltpu.VMEM((DELIVER_SLOTS, DELIVER_ROWS, LANES), jnp.float32),
                        pltpu.SemaphoreType.DMA((DELIVER_SLOTS,)), pltpu.SemaphoreType.DMA((DELIVER_SLOTS,))],
        compiler_params=pltpu.CompilerParams(vmem_limit_bytes=67_043_328),
        cost_estimate=pl.CostEstimate(flops=0, bytes_accessed=2 * sum(a.size for a in arrays) * 4, transcendentals=0),
        name="deliver",
    )(*arrays)


def gradient_groups(width, ff):
    groups = []

    def add(count, lhs, rhs, out, place):
        start = groups[-1]["start"] + groups[-1]["count"] if groups else 0
        groups.append(dict(start=start, count=count, lhs=lhs, rhs=rhs, out=out, place=place))

    def tall(local):
        return TILE_ROWS * local, 0

    def wide(local):
        return TILE_ROWS * lax.rem(local, width // TILE_ROWS), LANES * lax.div(local, width // TILE_ROWS)

    def attention(layer):
        for out, kind in enumerate("qkv"):
            add(width // TILE_ROWS, [f"u_{layer}"], [f"d{kind}_{layer}"], (f"g_{kind}", layer), tall)
        add(width // TILE_ROWS, [f"mixed_{layer}"], [f"dh_{layer}"], ("g_o", layer), tall)

    attention(1)
    add(ff // TILE_ROWS, ["act_0", "act_1"], ["dx_1", "cot"], ("g_down", None), tall)
    add(ff // TILE_ROWS, ["n_0", "n_1"], ["dpre_0", "dpre_1"], ("g_up", None), wide)
    attention(0)
    return groups, sum(group["count"] for group in groups)


def local_operands(x_init, cot_out, w_query, w_key, w_value, w_proj, w_up, w_down):
    batch, seq, width = x_init.shape
    tokens = batch * seq
    at = {"x_0": x_init.reshape(tokens, width), "cot": cot_out.reshape(tokens, width)}
    at.update(wq=w_query, wk=w_key, wv=w_value, wo=w_proj, w_up=w_up, w_down=w_down)
    at.update(front(at, batch, seq))
    return at


def solution(mesh):
    def local_step(x_init, cot_out, w_query, w_key, w_value, w_proj, w_up, w_down):
        batch, seq, width = x_init.shape
        inputs = local_operands(x_init, cot_out, w_query, w_key, w_value, w_proj, w_up, w_down)
        groups, chunks = gradient_groups(width, w_up.shape[1])
        weights = dict(g_q=w_query.shape, g_k=w_key.shape, g_v=w_value.shape, g_o=w_proj.shape, g_up=w_up.shape, g_down=w_down.shape)
        res = finish_backward(inputs, groups, chunks, weights, batch * seq, seq)
        return (*deliver([res[name] for name in weights]), res["dx_0"].reshape(x_init.shape))

    data_spec = P("data")
    full_spec = P()
    in_specs = (data_spec, data_spec, full_spec, full_spec, full_spec, full_spec, full_spec, full_spec)
    out_specs = (full_spec, full_spec, full_spec, full_spec, full_spec, full_spec, data_spec)
    return jax.shard_map(local_step, mesh=mesh, in_specs=in_specs, out_specs=out_specs, check_vma=False)
```

```python
import functools

import jax
import jax.numpy as jnp
from jax import lax
from jax.experimental import pallas as pl
from jax.experimental.pallas import tpu as pltpu
from jax.sharding import PartitionSpec as P

EPS = 1e-6
HEAD_DIM = 64
PAIR = 2 * HEAD_DIM
FF_BLOCK = 512
OUT_BLOCK = 256
GELU_A = (2.0 / 3.141592653589793) ** 0.5
GELU_B = 0.044715
SOFTMAX_SCALE = HEAD_DIM ** -0.5 * 1.4426950408889634
MIB = 1024 * 1024


def dot(lhs, rhs, lhs_dim, rhs_dim):
    return lax.dot_general(lhs, rhs, (((lhs_dim,), (rhs_dim,)), ((), ())), preferred_element_type=jnp.float32)


def rms_norm(x_f32):
    return x_f32 * lax.rsqrt(jnp.mean(x_f32 * x_f32, axis=-1, keepdims=True) + EPS)


def rms_backward(x_f32, d_out):
    scale = lax.rsqrt(jnp.mean(x_f32 * x_f32, axis=-1, keepdims=True) + EPS)
    inner = jnp.mean(x_f32 * d_out, axis=-1, keepdims=True)
    return scale * d_out - x_f32 * (scale * scale * scale * inner)


def gelu_parts(pre):
    square = pre * pre
    tanh = jnp.tanh(GELU_A * (pre + GELU_B * pre * square))
    half = 0.5 * (1.0 + tanh)
    slope = half + 0.5 * pre * (1.0 - tanh * tanh) * (GELU_A + (3.0 * GELU_A * GELU_B) * square)
    return pre * half, slope


def bf16(*shape):
    return jax.ShapeDtypeStruct(shape, jnp.bfloat16)


def pair_backward(q_pair, k_pair, v_pair, d_pair, low, probs_of):
    sums = [None] * 3
    for side in range(2):
        mask = low if side == 0 else jnp.logical_not(low)
        d_side = jnp.where(mask, d_pair, 0)
        probs_16 = probs_of(side)
        probs_32 = probs_16.astype(jnp.float32)
        d_probs = dot(v_pair, d_side, 1, 1).astype(jnp.bfloat16).astype(jnp.float32)
        row_dot = jnp.sum(d_probs * probs_32, axis=0, keepdims=True)
        d_scores = (probs_32 * (d_probs - row_dot) * HEAD_DIM ** -0.5).astype(jnp.bfloat16)
        parts = (dot(d_scores, jnp.where(mask, k_pair, 0), 0, 0),
                 dot(d_scores, jnp.where(mask, q_pair, 0), 1, 0),
                 dot(probs_16, d_side, 1, 0))
        sums = [part if total is None else total + part for total, part in zip(sums, parts)]
    return sums


def pair_forward(q_pair, k_pair, v_pair, low, keep):
    parts = []
    for side in range(2):
        mask = low if side == 0 else jnp.logical_not(low)
        scores = dot(k_pair, jnp.where(mask, q_pair, 0), 1, 1)
        top = jnp.max(scores, axis=0, keepdims=True)
        raised = jnp.exp2((scores - top) * SOFTMAX_SCALE)
        inverse = 1.0 / jnp.sum(raised, axis=0, keepdims=True)
        probs = (raised * inverse).astype(jnp.bfloat16)
        keep(side, probs)
        parts.append(dot(probs, v_pair, 0, 0))
    return jnp.where(low, parts[0], parts[1])


FRONT_OUTS = ("u_0", "q_0", "k_0", "v_0", "probs_0", "mixed_0", "h_0", "n_0", "pre_0", "act_0", "x_1",
              "u_1", "mixed_1", "n_1", "act_1", "dpre_1", "dh_1", "dq_1", "dk_1", "dv_1")
ROW_BUFFERS = ("u", "q", "k", "v", "mixed", "h", "n", "x", "dh", "dmix", "dq", "dk", "dv")
PAIRS_AT_ONCE = 1
BACK_AT_ONCE = 1
WIDE_BLOCK = 1024


def front_kernel(batch, seq, in_names, *refs):
    at = dict(zip((*in_names, *FRONT_OUTS), refs))
    refs = refs[len(at):]
    x_all, cot_all, w_in, w_out, w_up, w_down, probs, pre, act = refs[:9]
    row = dict(zip(ROW_BUFFERS, refs[9:]))
    load_sem, out_sem = refs[9 + len(ROW_BUFFERS):]
    width, ff = w_up.shape
    heads = width // HEAD_DIM
    loads = {"x": pltpu.make_async_copy(at["x_0"], x_all, load_sem.at[0])}
    for layer in (0, 1):
        for i, name in enumerate(("wq", "wk", "wv")):
            loads[f"{name}_{layer}"] = pltpu.make_async_copy(at[name].at[layer], w_in.at[layer, i], load_sem.at[1 + 4 * layer + i])
        loads[f"wo_{layer}"] = pltpu.make_async_copy(at["wo"].at[layer], w_out.at[layer], load_sem.at[4 + 4 * layer])
    loads["w_up"] = pltpu.make_async_copy(at["w_up"], w_up, load_sem.at[9])
    loads["w_down"] = pltpu.make_async_copy(at["w_down"], w_down, load_sem.at[10])
    loads["cot"] = pltpu.make_async_copy(at["cot"], cot_all, load_sem.at[11])
    for name in ("x", "wq_0", "wk_0", "wv_0", "wo_0", "w_up", "w_down", "wq_1", "wk_1", "wv_1", "wo_1", "cot"):
        loads[name].start()
    holders = {"probs_0": probs, "pre_0": pre, "act_0": act, "act_1": act, "dpre_1": pre, "x_1": row["x"]}
    for name in FRONT_OUTS:
        holders.setdefault(name, row.get(name[:-2]))

    def store(name, index):
        src = holders[name]
        rows = pl.ds(pl.multiple_of(seq * index, seq), seq)
        dest = at[name].at[index] if name == "probs_0" else at[name].at[rows]
        return pltpu.make_async_copy(src, dest, out_sem.at[FRONT_OUTS.index(name)])

    def one_sequence(index, carry):
        rows = pl.ds(pl.multiple_of(seq * index, seq), seq)
        first = index == 0
        low = lax.broadcasted_iota(jnp.int32, (seq, PAIR), 1) < HEAD_DIM

        def need(*names):
            @pl.when(first)
            def _():
                for name in names:
                    loads[name].wait()

        def free(*names, same=False):
            for name in names:
                if same:
                    store(name, index).wait()
                else:
                    pl.when(index > 0)(lambda name=name: store(name, index - 1).wait())

        def send(*names):
            for name in names:
                store(name, index).start()

        def over(count, fn):
            for j in range(count):
                fn(j)

        def attention(layer):
            x_in = x_all[rows] if layer == 0 else row["x"][...]
            row["u"][...] = rms_norm(x_in.astype(jnp.float32)).astype(jnp.bfloat16)
            for i, kind in enumerate("qkv"):
                need(f"w{kind}_{layer}")
                row[kind][...] = dot(row["u"][...], w_in[layer, i], 1, 0).astype(jnp.bfloat16)

            def pairs(j):
                for extra in range(PAIRS_AT_ONCE):
                    which = PAIRS_AT_ONCE * j + extra
                    lanes = pl.ds(pl.multiple_of(PAIR * which, PAIR), PAIR)

                    def keep(side, value):
                        probs[2 * which + side] = value
                    out = pair_forward(row["q"][:, lanes], row["k"][:, lanes], row["v"][:, lanes], low, keep)
                    row["mixed"][:, lanes] = out.astype(jnp.bfloat16)
            over(heads // 2 // PAIRS_AT_ONCE, pairs)
            need(f"wo_{layer}")
            attn = dot(row["mixed"][...], w_out[layer], 1, 0).astype(jnp.bfloat16)
            hidden = (x_in.astype(jnp.float32) + attn.astype(jnp.float32)).astype(jnp.bfloat16)
            row["h"][...] = hidden
            row["n"][...] = rms_norm(hidden.astype(jnp.float32)).astype(jnp.bfloat16)

        need("x")
        free("u_1")
        free("mixed_1", "n_1", "dh_1")
        attention(0)
        send("u_0", "q_0", "k_0", "v_0", "probs_0", "mixed_0", "h_0", "n_0")
        need("w_up")
        free("act_1", "dpre_1")

        def up(j):
            lanes = pl.ds(pl.multiple_of(WIDE_BLOCK * j, WIDE_BLOCK), WIDE_BLOCK)
            raw = dot(row["n"][...], w_up[:, lanes], 1, 0).astype(jnp.bfloat16)
            pre[:, lanes] = raw
            act[:, lanes] = gelu_parts(raw.astype(jnp.float32))[0].astype(jnp.bfloat16)
        over(ff // WIDE_BLOCK, up)
        send("pre_0", "act_0")
        need("w_down")

        def down(j):
            lanes = pl.ds(pl.multiple_of(OUT_BLOCK * j, OUT_BLOCK), OUT_BLOCK)
            out = dot(act[...], w_down[:, lanes], 1, 0).astype(jnp.bfloat16).astype(jnp.float32)
            row["x"][:, lanes] = (row["h"][:, lanes].astype(jnp.float32) + out).astype(jnp.bfloat16)
        over(width // OUT_BLOCK, down)
        send("x_1")
        free("u_0", "q_0", "k_0", "v_0", "probs_0", "mixed_0", "h_0", "n_0", same=True)
        attention(1)
        send("u_1", "mixed_1", "n_1")
        need("cot")
        free("pre_0", "act_0", same=True)

        def both(j):
            lanes = pl.ds(pl.multiple_of(WIDE_BLOCK * j, WIDE_BLOCK), WIDE_BLOCK)
            raw = dot(row["n"][...], w_up[:, lanes], 1, 0).astype(jnp.bfloat16).astype(jnp.float32)
            d_act = dot(cot_all[rows], w_down[lanes], 1, 1).astype(jnp.bfloat16).astype(jnp.float32)
            out, slope = gelu_parts(raw)
            act[:, lanes] = out.astype(jnp.bfloat16)
            pre[:, lanes] = (d_act * slope).astype(jnp.bfloat16)
        over(ff // WIDE_BLOCK, both)
        send("act_1", "dpre_1")

        def back(j):
            lanes = pl.ds(pl.multiple_of(OUT_BLOCK * j, OUT_BLOCK), OUT_BLOCK)
            row["dmix"][:, lanes] = dot(pre[...], w_up[lanes], 1, 1).astype(jnp.bfloat16)
        over(width // OUT_BLOCK, back)
        d_hidden = cot_all[rows].astype(jnp.float32) + rms_backward(
            row["h"][...].astype(jnp.float32), row["dmix"][...].astype(jnp.float32))
        row["dh"][...] = d_hidden.astype(jnp.bfloat16)
        send("dh_1")
        row["dmix"][...] = dot(row["dh"][...], w_out[1], 1, 1).astype(jnp.bfloat16)

        free("dq_1", "dk_1", "dv_1")

        def pairs_back(j):
            for extra in range(BACK_AT_ONCE):
                which = BACK_AT_ONCE * j + extra
                lanes = pl.ds(pl.multiple_of(PAIR * which, PAIR), PAIR)
                sums = pair_backward(*(row[name][:, lanes] for name in ("q", "k", "v", "dmix")), low,
                                     lambda side: probs[2 * which + side])
                for name, total in zip(("dq", "dk", "dv"), sums):
                    row[name][:, lanes] = total.astype(jnp.bfloat16)
        over(heads // 2 // BACK_AT_ONCE, pairs_back)
        send("dq_1", "dk_1", "dv_1")
        free("x_1", same=True)
        return carry

    lax.fori_loop(0, batch, one_sequence, 0)
    for name in ("u_1", "mixed_1", "n_1", "act_1", "dpre_1", "dh_1", "dq_1", "dk_1", "dv_1"):
        store(name, batch - 1).wait()


def front(inputs, batch, seq):
    tokens, width = inputs["x_0"].shape
    ff = inputs["w_up"].shape[1]
    heads = width // HEAD_DIM
    shapes = []
    for name in FRONT_OUTS:
        if name == "probs_0":
            shapes.append(bf16(batch, heads, seq, seq))
        else:
            shapes.append(bf16(tokens, ff if name[:-2] in ("pre", "act", "dpre") else width))
    block = lambda *shape: pltpu.VMEM(shape, jnp.bfloat16)
    scratch = [
        block(tokens, width), block(tokens, width), block(2, 3, width, width), block(2, width, width), block(width, ff),
        block(ff, width), block(heads, seq, seq), block(seq, ff), block(seq, ff),
        *[block(seq, width) for _ in ROW_BUFFERS],
        pltpu.SemaphoreType.DMA((12,)), pltpu.SemaphoreType.DMA((len(FRONT_OUTS),)),
    ]
    outs = pl.pallas_call(
        functools.partial(front_kernel, batch, seq, tuple(inputs)),
        out_shape=shapes,
        in_specs=[pl.BlockSpec(memory_space=pl.ANY)] * len(inputs),
        out_specs=[pl.BlockSpec(memory_space=pl.ANY)] * len(shapes),
        scratch_shapes=scratch,
        compiler_params=pltpu.CompilerParams(vmem_limit_bytes=67_043_328),
        cost_estimate=pl.CostEstimate(flops=22 * tokens * width * ff // 2, bytes_accessed=100 * MIB, transcendentals=0),
        name="front",
    )(*inputs.values())
    return dict(zip(FRONT_OUTS, outs))


MESH = pl.DeviceIdType.MESH
LANES = 1024
SET_ROWS = 128
CORE_ROWS = 2 * SET_ROWS
TILE_ROWS = 2 * CORE_ROWS
OWN_SLOTS = 8
AG_SLOTS = 10
TYPES = {
    "p1": (0, 0, 80, "xyz"),
    "q1": (0, 80, 48, "zxy"),
    "p2": (1, 128, 80, "yxz"),
    "q2": (1, 208, 48, "zyx"),
}
WRITE_AT = 11


def stage_list():
    stages = []
    for name, (_, _, _, order) in TYPES.items():
        if order[2] == "z":
            plan = [("rs1", 1), ("rs2", 2), ("rsz", 3), ("agz", 6), ("ag2", 9), ("ag1", 10)]
        else:
            plan = [("rsz", 1), ("rs1", 4), ("rs2", 5), ("ag2", 6), ("ag1", 7), ("agz", 8)]
        for kind, at in plan:
            if kind in ("rsz", "agz"):
                for step in range(3):
                    for way in (0, 1):
                        stages.append((name, kind, step, way, at + step))
            else:
                stages.append((name, kind, 0, 0, at))
    return stages


STAGES = stage_list()


def piece_shape(name, kind):
    rows, order = TYPES[name][2], TYPES[name][3]
    if order[2] == "z":
        return {"rs1": (rows, 512), "rs2": (rows, 256), "rsz": (rows // 2, 128)}[kind]
    return {"rsz": (rows // 2, 512), "rs1": (rows // 2, 256), "rs2": (rows // 2, 128)}[kind]


def between(step, first, count):
    return jnp.logical_and(step >= first, step < first + count)


class Backward:
    PB_1, MB, AB, PB_0 = 2, 6, 14, 23
    ROWS = 256

    def __init__(self, at, big, total_buf, w_buf, p_buf, sem, drain):
        self.at, self.big, self.total, self.w, self.p, self.sem, self.drain = at, big, total_buf, w_buf, p_buf, sem, drain
        self.tokens, self.width = at["x_0"].shape
        self.heads = at["probs_0"].shape[1]
        self.seq = at["probs_0"].shape[2]

    def load(self, name, dest, sem, *index):
        ref = self.at[name]
        return pltpu.make_async_copy(ref.at[index] if index else ref, dest, self.sem.at[sem])

    def store(self, src, name, sem, *index):
        ref = self.at[name]
        return pltpu.make_async_copy(src, ref.at[index] if index else ref, self.drain.at[sem])

    def row_blocks(self, fn):
        def body(block, carry):
            fn(pl.ds(pl.multiple_of(self.ROWS * block, self.ROWS), self.ROWS))
            return carry
        lax.fori_loop(0, self.tokens // self.ROWS, body, 0)

    def input_loads(self, layer):
        spot = 4 if layer else 5
        copies = [self.load(f"d{kind}_{layer}", self.big.at[i], i) for i, kind in enumerate("qkv")]
        copies.append(self.load(f"x_{layer}", self.big.at[spot], 3))
        if layer:
            copies.append(self.load("dh_1", self.big.at[5], 4))
        return copies

    def weight_loads(self, layer, block):
        rows = pl.ds(pl.multiple_of(OUT_BLOCK * block, OUT_BLOCK), OUT_BLOCK)
        slot = lax.rem(block, 2)
        return [self.load(name, self.w.at[slot, i], 5 + 3 * slot + i, layer, rows) for i, name in enumerate(("wq", "wk", "wv"))]

    def input_block(self, layer, block):
        big, blocks = self.big, self.width // OUT_BLOCK
        slot = lax.rem(block, 2)

        @pl.when(block == 0)
        def _():
            for copy in self.input_loads(layer):
                copy.wait()
        for copy in self.weight_loads(layer, block):
            copy.wait()

        @pl.when(block + 1 < blocks)
        def _():
            for copy in self.weight_loads(layer, block + 1):
                copy.start()
        lanes = pl.ds(pl.multiple_of(OUT_BLOCK * block, OUT_BLOCK), OUT_BLOCK)

        def product(rows):
            total = dot(big[0, rows], self.w[slot, 0], 1, 1) + dot(big[1, rows], self.w[slot, 1], 1, 1)
            big[3, rows, lanes] = (total + dot(big[2, rows], self.w[slot, 2], 1, 1)).astype(jnp.bfloat16)
        self.row_blocks(product)

        @pl.when(block == blocks - 1)
        def _():
            x_at, d_at = (4, 5) if layer else (5, 4)

            def close(rows):
                back = rms_backward(big[x_at, rows].astype(jnp.float32), big[3, rows].astype(jnp.float32))
                big[3, rows] = (big[d_at, rows].astype(jnp.float32) + back).astype(jnp.bfloat16)
                if layer:
                    self.total[rows] = jnp.zeros((self.ROWS, self.width), jnp.float32)
            self.row_blocks(close)
            self.store(big.at[3], f"dx_{layer}", 0).start()
            if layer:
                self.load("h_0", big.at[4], 3).start()
                for copy in self.mlp_loads(0):
                    copy.start()

    def mlp_loads(self, block):
        slot = lax.rem(block, 2)
        lanes = pl.ds(pl.multiple_of(FF_BLOCK * block, FF_BLOCK), FF_BLOCK)
        half = pl.ds(pl.multiple_of(FF_BLOCK * slot, FF_BLOCK), FF_BLOCK)
        return [self.load("w_up", self.big.at[0, :, half], 5 + 3 * slot, slice(None), lanes),
                self.load("pre_0", self.big.at[1, :, half], 6 + 3 * slot, slice(None), lanes),
                self.load("w_down", self.big.at[5, half], 7 + 3 * slot, lanes)]

    def mlp_store(self, block):
        half = pl.ds(pl.multiple_of(FF_BLOCK * lax.rem(block, 2), FF_BLOCK), FF_BLOCK)
        lanes = pl.ds(pl.multiple_of(FF_BLOCK * block, FF_BLOCK), FF_BLOCK)
        return self.store(self.big.at[2, :, half], "dpre_0", 1, slice(None), lanes)

    def mlp_block(self, block):
        big, blocks = self.big, self.at["w_up"].shape[1] // FF_BLOCK

        @pl.when(block == 0)
        def _():
            self.store(big.at[3], "dx_1", 0).wait()
            self.load("h_0", big.at[4], 3).wait()
        for copy in self.mlp_loads(block):
            copy.wait()

        @pl.when(block + 1 < blocks)
        def _():
            for copy in self.mlp_loads(block + 1):
                copy.start()

        @pl.when(block > 0)
        def _():
            self.mlp_store(block - 1).wait()
        half = pl.ds(pl.multiple_of(FF_BLOCK * lax.rem(block, 2), FF_BLOCK), FF_BLOCK)

        def product(rows):
            d_act = dot(big[3, rows], big[5, half], 1, 1).astype(jnp.bfloat16).astype(jnp.float32)
            slope = gelu_parts(big[1, rows, half].astype(jnp.float32))[1]
            d_pre = (d_act * slope).astype(jnp.bfloat16)
            big[2, rows, half] = d_pre
            self.total[rows] += dot(d_pre, big[0, :, half], 1, 1)
        self.row_blocks(product)
        self.mlp_store(block).start()

        @pl.when(block == blocks - 1)
        def _():
            def close(rows):
                d_normed = self.total[rows].astype(jnp.bfloat16).astype(jnp.float32)
                back = rms_backward(big[4, rows].astype(jnp.float32), d_normed)
                big[4, rows] = (big[3, rows].astype(jnp.float32) + back).astype(jnp.bfloat16)
            self.row_blocks(close)
            self.store(big.at[4], "dh_0", 2).start()
            self.load("wo", big.at[0], 4, 0).start()
            for copy in self.seq_loads(0) + self.probs_loads(0):
                copy.start()

    def seq_loads(self, seq):
        rows = pl.ds(pl.multiple_of(self.seq * seq, self.seq), self.seq)
        return [self.load(f"{kind}_0", self.big.at[1 + lax.rem(seq, 2), pl.ds(self.seq * i, self.seq)], i, rows)
                for i, kind in enumerate("qkv")]

    def probs_loads(self, piece):
        half = self.heads // 2
        heads = pl.ds(half * lax.rem(piece, 2), half)
        return [self.load("probs_0", self.p.at[lax.rem(piece, 2)], 5 + lax.rem(piece, 2), lax.div(piece, 2), heads)]

    def seq_stores(self, piece):
        seq, half = lax.div(piece, 2), lax.rem(piece, 2)
        rows = pl.ds(pl.multiple_of(self.seq * seq, self.seq), self.seq)
        lanes = pl.ds(pl.multiple_of(self.width // 2 * half, PAIR), self.width // 2)
        spot = 5 - 2 * lax.rem(seq, 2)
        return [self.store(self.big.at[spot, pl.ds(self.seq * i, self.seq), lanes], f"d{kind}_0", 3 + i, rows, lanes)
                for i, kind in enumerate("qkv")]

    def attention_piece(self, piece):
        big, pieces = self.big, 2 * (self.tokens // self.seq)
        seq, half = lax.div(piece, 2), lax.rem(piece, 2)
        spot, out = 1 + lax.rem(seq, 2), 5 - 2 * lax.rem(seq, 2)

        @pl.when(piece == 0)
        def _():
            self.mlp_store(self.at["w_up"].shape[1] // FF_BLOCK - 1).wait()
            self.store(big.at[4], "dh_0", 2).wait()
            self.load("wo", big.at[0], 4, 0).wait()

        @pl.when(piece > 0)
        def _():
            for copy in self.seq_stores(piece - 1):
                copy.wait()
        for copy in self.probs_loads(piece):
            copy.wait()

        @pl.when(piece + 1 < pieces)
        def _():
            for copy in self.probs_loads(piece + 1):
                copy.start()
        mixed = pl.ds(3 * self.seq, self.seq)

        @pl.when(half == 0)
        def _():
            for copy in self.seq_loads(seq):
                copy.wait()

            @pl.when(piece + 2 < pieces)
            def _():
                for copy in self.seq_loads(seq + 1):
                    copy.start()
            rows = pl.ds(pl.multiple_of(self.seq * seq, self.seq), self.seq)
            big[spot, mixed] = dot(big[4, rows], big[0], 1, 1).astype(jnp.bfloat16)
        low = lax.broadcasted_iota(jnp.int32, (self.seq, PAIR), 1) < HEAD_DIM
        pairs = self.heads // 4

        def pair(j, carry):
            lanes = pl.ds(pl.multiple_of(PAIR * (pairs * half + j), PAIR), PAIR)
            q_pair, k_pair, v_pair, d_pair = (big[spot, pl.ds(self.seq * i, self.seq), lanes] for i in range(4))
            for i, total in enumerate(pair_backward(q_pair, k_pair, v_pair, d_pair, low, lambda side: self.p[half, 2 * j + side])):
                big[out, pl.ds(self.seq * i, self.seq), lanes] = total.astype(jnp.bfloat16)
            return carry
        lax.fori_loop(0, pairs, pair, 0)
        for copy in self.seq_stores(piece):
            copy.start()

    def item(self, step):
        blocks = self.width // OUT_BLOCK
        pieces = 2 * (self.tokens // self.seq)

        @pl.when(step == self.PB_1)
        def _():
            for copy in self.input_loads(1) + self.weight_loads(1, 0):
                copy.start()
        pl.when(between(step, self.PB_1, blocks))(lambda: self.input_block(1, step - self.PB_1))
        pl.when(between(step, self.MB, 8))(lambda: self.mlp_block(step - self.MB))
        pl.when(between(step, self.AB, pieces))(lambda: self.attention_piece(step - self.AB))

        @pl.when(step == self.PB_0 - 1)
        def _():
            for copy in self.seq_stores(pieces - 1):
                copy.wait()
            for copy in self.input_loads(0) + self.weight_loads(0, 0):
                copy.start()
        pl.when(between(step, self.PB_0, blocks))(lambda: self.input_block(0, step - self.PB_0))

        @pl.when(step == self.PB_0 + blocks)
        def _():
            self.store(self.big.at[3], "dx_0", 0).wait()


def finish_kernel(groups, chunks, in_names, out_names, remote, *refs):
    names = [*in_names, *out_names]
    at, scratch = dict(zip(names, refs[:len(names)])), refs[len(names):]
    (big, total_buf, w_buf, p_buf, item_sem, drain_sem), scratch = scratch[:6], scratch[6:]
    backward = Backward(at, big, total_buf, w_buf, p_buf, item_sem, drain_sem)
    if not remote:
        lax.fori_loop(0, chunks + WRITE_AT + 1, lambda step, carry: backward.item(step) or carry, 0)
        return
    (lhs_buf, rhs_buf, own, part, part_in, gath), scratch = scratch[:6], scratch[6:]
    land_keys = [key for key, st in enumerate(STAGES) if st[1].startswith("rs")]
    landing = dict(zip(land_keys, scratch[:len(land_keys)]))
    load_sem, send_sem, recv_sem, pair_send, pair_recv, out_sem, out_send, out_recv, credit = scratch[len(land_keys):]

    me = lax.axis_index("data")
    core = lax.rem(me, 2)
    coord = {"x": lax.rem(lax.div(me, 2), 2), "y": lax.rem(lax.div(me, 4), 2)}
    z = lax.div(me, 8)
    partner = me + 1 - 2 * core
    near = {"x": me + 2 - 4 * coord["x"], "y": me + 4 - 8 * coord["y"]}
    up_ok, down_ok = z < 3, z > 0
    peers = [(partner, 0, None), (near["x"], 1, None), (near["y"], 2, None), (me + 8, 3, up_ok), (me - 8, 4, down_ok)]

    def guarded(cond, fn):
        if cond is None:
            fn()
        else:
            pl.when(cond)(fn)

    barrier = pltpu.get_barrier_semaphore()
    for dev, _, cond in peers:
        guarded(cond, lambda dev=dev: pl.semaphore_signal(barrier, inc=1, device_id=(dev,), device_id_type=MESH))
    inner = jnp.logical_and(up_ok, down_ok)
    guarded(inner, lambda: pl.semaphore_wait(barrier, 5))
    guarded(jnp.logical_not(inner), lambda: pl.semaphore_wait(barrier, 4))

    def region(name, kind, which):
        _, row, rows, order = TYPES[name]
        if order[2] == "z":
            h1, h2 = coord[order[0]], coord[order[1]]
            if kind == "1":
                return pl.ds(row, rows), pl.ds(pl.multiple_of(512 * which, 128), 512)
            if kind == "2":
                return pl.ds(row, rows), pl.ds(pl.multiple_of(512 * h1 + 256 * which, 128), 256)
            first = pl.multiple_of(row + (rows // 2) * lax.div(which, 2), 8)
            lane = pl.multiple_of(512 * h1 + 256 * h2 + 128 * lax.rem(which, 2), 128)
            return pl.ds(first, rows // 2), pl.ds(lane, 128)
        h1 = coord[order[1]]
        if kind == "z":
            first = pl.multiple_of(row + (rows // 2) * lax.div(which, 2), 8)
            return pl.ds(first, rows // 2), pl.ds(pl.multiple_of(512 * lax.rem(which, 2), 128), 512)
        first = pl.multiple_of(row + (rows // 2) * lax.div(z, 2), 8)
        if kind == "1":
            return pl.ds(first, rows // 2), pl.ds(pl.multiple_of(512 * lax.rem(z, 2) + 256 * which, 128), 256)
        lane = pl.multiple_of(512 * lax.rem(z, 2) + 256 * h1 + 128 * which, 128)
        return pl.ds(first, rows // 2), pl.ds(lane, 128)

    def exchange_axis(name, kind):
        order = TYPES[name][3]
        dims = order[:2] if order[2] == "z" else order[1:]
        return dims[int(kind) - 1]

    def plan(key, chunk, parity):
        name, kind, step, way, _ = STAGES[key]
        mine, slot = lax.rem(chunk, OWN_SLOTS), lax.rem(chunk, AG_SLOTS)
        if kind in ("rs1", "rs2"):
            axis = exchange_axis(name, kind[2])
            src, keep = region(name, kind[2], 1 - coord[axis]), region(name, kind[2], coord[axis])
            dev, send_ok, recv_ok = near[axis], None, None
            sent = own.at[mine, src[0], src[1]]
        elif kind in ("ag1", "ag2"):
            axis = exchange_axis(name, kind[2])
            src = keep = region(name, kind[2], coord[axis])
            dev, send_ok, recv_ok = near[axis], None, None
            sent = gath.at[slot, src[0], src[1]]
        elif kind == "rsz":
            if way:
                dev, k_send, k_keep = me + 8, z + 3 - step, z + 2 - step
                send_ok, recv_ok = k_send <= 3, jnp.logical_and(k_keep <= 3, down_ok)
            else:
                dev, k_send, k_keep = me - 8, z - 3 + step, z - 2 + step
                send_ok, recv_ok = k_send >= 0, jnp.logical_and(k_keep >= 0, up_ok)
            src, keep = region(name, "z", k_send), region(name, "z", k_keep)
            sent = own.at[mine, src[0], src[1]]
        else:
            if way:
                dev, k_send, k_keep = me + 8, z - step, z - 1 - step
                send_ok, recv_ok = jnp.logical_and(k_send >= 0, up_ok), k_keep >= 0
            else:
                dev, k_send, k_keep = me - 8, z + step, z + 1 + step
                send_ok, recv_ok = jnp.logical_and(k_send <= 3, down_ok), k_keep <= 3
            src, keep = region(name, "z", k_send), region(name, "z", k_keep)
            sent = gath.at[slot, src[0], src[1]]
        sems = dict(send_sem=send_sem.at[key], recv_sem=recv_sem.at[key, parity], device_id=(dev,), device_id_type=MESH)
        if kind.startswith("rs"):
            target = landing[key].at[parity]
            send = lambda: pltpu.make_async_remote_copy(src_ref=sent, dst_ref=target, **sems)
            recv = lambda: pltpu.make_async_remote_copy(
                src_ref=own.at[mine, keep[0], keep[1]], dst_ref=target, **sems)

            def arrive():
                own[mine, keep[0], keep[1]] += landing[key][parity]
        else:
            send = lambda: pltpu.make_async_remote_copy(src_ref=sent, dst_ref=sent, **sems)
            recv = lambda: pltpu.make_async_remote_copy(
                src_ref=gath.at[slot, keep[0], keep[1]], dst_ref=gath.at[slot, keep[0], keep[1]], **sems)
            arrive = None
        return send, recv, send_ok, recv_ok, arrive

    def finish(name, chunk):
        order = TYPES[name][3]
        reg = region(name, "z", z) if order[2] == "z" else region(name, "2", coord[order[2]])
        gath[lax.rem(chunk, AG_SLOTS), reg[0], reg[1]] = own[lax.rem(chunk, OWN_SLOTS), reg[0], reg[1]]

    def valid(chunk):
        return jnp.logical_and(chunk >= 0, chunk < chunks)

    def set_rows(half):
        return pl.ds(half * SET_ROWS, SET_ROWS)

    def pair_copy(half, parity):
        return pltpu.make_async_remote_copy(
            src_ref=part.at[parity, set_rows(half)], dst_ref=part_in.at[parity, set_rows(half)],
            send_sem=pair_send.at[half], recv_sem=pair_recv.at[half, parity], device_id=(partner,), device_id_type=MESH)

    def out_copies(half, group, local, whose):
        out, layer = group["out"]
        ref = at[out] if layer is None else at[out].at[layer]
        rows, cols = group["place"](local)
        first = pl.multiple_of(rows + CORE_ROWS * whose + half * SET_ROWS, SET_ROWS)
        return ref.at[pl.ds(first, SET_ROWS), pl.ds(pl.multiple_of(cols, 128), LANES)]

    def write_copies(half, chunk, dest):
        slot = lax.rem(chunk, AG_SLOTS)
        src = gath.at[slot, set_rows(half)]
        here = pltpu.make_async_copy(src, dest, out_sem.at[half])
        there = pltpu.make_async_remote_copy(
            src_ref=src, dst_ref=dest, send_sem=out_send.at[half], recv_sem=out_recv.at[half, lax.rem(chunk, 2)],
            device_id=(partner,), device_id_type=MESH)
        return here, there

    def load_copies(group, local, slot):
        rows, cols = group["place"](local)
        copies = []
        for app, (lhs, rhs) in enumerate(zip(group["lhs"], group["rhs"])):
            for whose in (0, 1):
                first = rows + CORE_ROWS * (core if whose == 0 else 1 - core)
                copies.append(pltpu.make_async_copy(
                    at[lhs].at[:, pl.ds(pl.multiple_of(first, CORE_ROWS), CORE_ROWS)],
                    lhs_buf.at[slot, app, whose], load_sem.at[slot, app, whose]))
            copies.append(pltpu.make_async_copy(
                at[rhs].at[:, pl.ds(pl.multiple_of(cols, 128), LANES)], rhs_buf.at[slot, app], load_sem.at[slot, app, 2]))
        return copies

    def for_group(chunk, fn):
        for group in groups:
            inside = jnp.logical_and(chunk >= group["start"], chunk < group["start"] + group["count"])
            pl.when(inside)(functools.partial(fn, group, chunk - group["start"]))

    def two_apps(chunk):
        flags = [jnp.logical_and(chunk >= g["start"], chunk < g["start"] + g["count"]) for g in groups if len(g["lhs"]) == 2]
        return functools.reduce(jnp.logical_or, flags)

    def start_load(chunk):
        def go(group, local):
            for copy in load_copies(group, local, lax.rem(chunk, 2)):
                copy.start()
        for_group(chunk, go)

    def wait_load(chunk):
        slot = lax.rem(chunk, 2)
        any_two = next(g for g in groups if len(g["lhs"]) == 2)
        copies = load_copies(any_two, 0, slot)
        for copy in copies[:3]:
            copy.wait()

        @pl.when(two_apps(chunk))
        def _():
            for copy in copies[3:]:
                copy.wait()

    def tile(chunk):
        slot, mine, parity = lax.rem(chunk, 2), lax.rem(chunk, OWN_SLOTS), lax.rem(chunk, 2)

        def product(app, whose):
            return lax.dot_general(lhs_buf[slot, app, whose], rhs_buf[slot, app], (((0,), (0,)), ((), ())),
                                   preferred_element_type=jnp.float32)

        own[mine] = product(0, 0)
        part[parity] = product(0, 1)

        @pl.when(two_apps(chunk))
        def _():
            own[mine] += product(1, 0)
            part[parity] += product(1, 1)

    last = chunks + WRITE_AT

    def section(half, step):
        before = lax.rem(step + 1, 2)
        now = lax.rem(step, 2)

        @pl.when(valid(step - 1))
        def _():
            copy = pair_copy(half, before)
            copy.wait_send()
            copy.wait_recv()
            mine = lax.rem(step - 1, OWN_SLOTS)
            own[mine, set_rows(half)] += part_in[before, set_rows(half)]

        names = [name for name in TYPES if TYPES[name][0] == half]
        keys = [key for key, st in enumerate(STAGES) if st[0] in names]
        finals = {name: max(st[4] for st in STAGES if st[0] == name and st[1].startswith("rs")) for name in names}
        for key in keys:
            name, at = STAGES[key][0], STAGES[key][4]
            chunk = step - 1 - at

            @pl.when(valid(chunk))
            def _(key=key, chunk=chunk):
                send, recv, send_ok, recv_ok, arrive = plan(key, chunk, before)

                def arrived():
                    recv().wait_recv()
                    if arrive is not None:
                        arrive()
                guarded(recv_ok, arrived)
                guarded(send_ok, lambda: send().wait_send())
        for name in names:
            chunk = step - 1 - finals[name]
            pl.when(valid(chunk))(functools.partial(finish, name, chunk))

        done = step - 1 - WRITE_AT

        @pl.when(valid(done))
        def _():
            here, there = write_copies(half, done, out_copies(half, groups[0], 0, 0))
            here.wait()
            there.wait_send()
            there.wait_recv()

        @pl.when(step < last)
        def _():
            for dev, way, cond in peers:
                to = way if way < 3 else 7 - way
                guarded(cond, lambda dev=dev, to=to: pl.semaphore_signal(
                    credit.at[half, to], inc=1, device_id=(dev,), device_id_type=MESH))

        @pl.when(step > 0)
        def _():
            for dev, way, cond in peers:
                guarded(cond, lambda way=way: pl.semaphore_wait(credit.at[half, way], 1))

        for key in reversed(keys):
            chunk = step - STAGES[key][4]

            @pl.when(valid(chunk))
            def _(key=key, chunk=chunk):
                send, recv, send_ok, recv_ok, arrive = plan(key, chunk, now)
                guarded(send_ok, lambda: send().start())

        out_chunk = step - WRITE_AT

        @pl.when(valid(out_chunk))
        def _():
            def go(group, local):
                for copy in write_copies(half, out_chunk, out_copies(half, group, local, core)):
                    copy.start()
            for_group(out_chunk, go)

    start_load(jnp.int32(0))

    def round_(step, carry):
        section(0, step)

        @pl.when(valid(step))
        def _():
            pl.when(step + 1 < chunks)(lambda: start_load(step + 1))
            wait_load(step)
            tile(step)
            pair_copy(0, lax.rem(step, 2)).start()

        section(1, step)

        @pl.when(valid(step))
        def _():
            pair_copy(1, lax.rem(step, 2)).start()

        backward.item(step)
        return carry

    lax.fori_loop(0, last + 1, round_, 0)


def finish_backward(inputs, groups, chunks, weights, tokens, seq, collective_id=0, remote=True):
    width, ff = inputs["w_up"].shape
    landing = [pltpu.VMEM((2,) + piece_shape(st[0], st[1]), jnp.float32) for st in STAGES if st[1].startswith("rs")]
    apps = 2
    outs = {name: jax.ShapeDtypeStruct(shape, jnp.float32) for name, shape in weights.items()}
    for name in ("dx_0", "dx_1", "dh_0", "dq_0", "dk_0", "dv_0"):
        outs[name] = bf16(tokens, width)
    outs["dpre_0"] = bf16(tokens, ff)
    heads = width // HEAD_DIM
    scratch = [
        pltpu.VMEM((6, tokens, width), jnp.bfloat16),
        pltpu.VMEM((tokens, width), jnp.float32),
        pltpu.VMEM((2, 3, OUT_BLOCK, width), jnp.bfloat16),
        pltpu.VMEM((2, heads // 2, seq, seq), jnp.bfloat16),
        pltpu.SemaphoreType.DMA((11,)),
        pltpu.SemaphoreType.DMA((6,)),
    ]
    if remote:
        scratch += [
            pltpu.VMEM((2, apps, 2, tokens, CORE_ROWS), jnp.bfloat16),
            pltpu.VMEM((2, apps, tokens, LANES), jnp.bfloat16),
            pltpu.VMEM((OWN_SLOTS, CORE_ROWS, LANES), jnp.float32),
            pltpu.VMEM((2, CORE_ROWS, LANES), jnp.float32),
            pltpu.VMEM((2, CORE_ROWS, LANES), jnp.float32),
            pltpu.VMEM((AG_SLOTS, CORE_ROWS, LANES), jnp.float32),
            *landing,
            pltpu.SemaphoreType.DMA((2, apps, 3)),
            pltpu.SemaphoreType.DMA((len(STAGES),)),
            pltpu.SemaphoreType.DMA((len(STAGES), 2)),
            pltpu.SemaphoreType.DMA((2,)),
            pltpu.SemaphoreType.DMA((2, 2)),
            pltpu.SemaphoreType.DMA((2,)),
            pltpu.SemaphoreType.DMA((2,)),
            pltpu.SemaphoreType.DMA((2, 2)),
            pltpu.SemaphoreType.REGULAR((2, 5)),
        ]
    params = dict(collective_id=collective_id, has_side_effects=True) if remote else {}
    results = pl.pallas_call(
        functools.partial(finish_kernel, groups, chunks, list(inputs), list(outs), remote),
        out_shape=list(outs.values()),
        in_specs=[pl.BlockSpec(memory_space=pl.ANY)] * len(inputs),
        out_specs=[pl.BlockSpec(memory_space=pl.ANY)] * len(outs),
        scratch_shapes=scratch,
        compiler_params=pltpu.CompilerParams(vmem_limit_bytes=67_043_328, **params),
        cost_estimate=pl.CostEstimate(flops=20 * tokens * width * ff, bytes_accessed=256 * MIB, transcendentals=0),
        name="finish_backward",
    )(*inputs.values())
    return dict(zip(outs, results))


DELIVER_ROWS = 512
DELIVER_SLOTS = 16
DELIVER_AHEAD = 8


def deliver(arrays):
    def blocks_of(array):
        lead = [(i,) for i in range(array.shape[0])] if len(array.shape) == 3 else [()]
        rows, cols = array.shape[-2:]
        return [(*index, pl.ds(row, DELIVER_ROWS), pl.ds(col, LANES))
                for index in lead for row in range(0, rows, DELIVER_ROWS) for col in range(0, cols, LANES)]

    work = [(i, index) for i, array in enumerate(arrays) for index in blocks_of(array)]
    count = len(arrays)

    def kernel(*refs):
        ins, outs, buf, in_sem, out_sem = refs[:count], refs[count:2 * count], *refs[2 * count:]

        def fetch(t):
            i, index = work[t]
            return pltpu.make_async_copy(ins[i].at[index], buf.at[t % DELIVER_SLOTS], in_sem.at[t % DELIVER_SLOTS])

        def put(t):
            i, index = work[t]
            return pltpu.make_async_copy(buf.at[t % DELIVER_SLOTS], outs[i].at[index], out_sem.at[t % DELIVER_SLOTS])

        for t in range(min(DELIVER_AHEAD, len(work))):
            fetch(t).start()
        for t in range(len(work)):
            if t + DELIVER_AHEAD < len(work):
                if t + DELIVER_AHEAD >= DELIVER_SLOTS:
                    put(t + DELIVER_AHEAD - DELIVER_SLOTS).wait()
                fetch(t + DELIVER_AHEAD).start()
            fetch(t).wait()
            put(t).start()
        for t in range(max(0, len(work) - DELIVER_SLOTS), len(work)):
            put(t).wait()

    return pl.pallas_call(
        kernel,
        out_shape=[jax.ShapeDtypeStruct(array.shape, array.dtype) for array in arrays],
        in_specs=[pl.BlockSpec(memory_space=pl.ANY)] * count,
        out_specs=[pl.BlockSpec(memory_space=pl.ANY)] * count,
        scratch_shapes=[pltpu.VMEM((DELIVER_SLOTS, DELIVER_ROWS, LANES), jnp.float32),
                        pltpu.SemaphoreType.DMA((DELIVER_SLOTS,)), pltpu.SemaphoreType.DMA((DELIVER_SLOTS,))],
        compiler_params=pltpu.CompilerParams(vmem_limit_bytes=67_043_328),
        cost_estimate=pl.CostEstimate(flops=0, bytes_accessed=2 * sum(a.size for a in arrays) * 4, transcendentals=0),
        name="deliver",
    )(*arrays)


def gradient_groups(width, ff):
    groups = []

    def add(count, lhs, rhs, out, place):
        start = groups[-1]["start"] + groups[-1]["count"] if groups else 0
        groups.append(dict(start=start, count=count, lhs=lhs, rhs=rhs, out=out, place=place))

    def tall(local):
        return TILE_ROWS * local, 0

    def wide(local):
        return TILE_ROWS * lax.rem(local, width // TILE_ROWS), LANES * lax.div(local, width // TILE_ROWS)

    def attention(layer):
        for out, kind in enumerate("qkv"):
            add(width // TILE_ROWS, [f"u_{layer}"], [f"d{kind}_{layer}"], (f"g_{kind}", layer), tall)
        add(width // TILE_ROWS, [f"mixed_{layer}"], [f"dh_{layer}"], ("g_o", layer), tall)

    attention(1)
    add(ff // TILE_ROWS, ["act_0", "act_1"], ["dx_1", "cot"], ("g_down", None), tall)
    add(ff // TILE_ROWS, ["n_0", "n_1"], ["dpre_0", "dpre_1"], ("g_up", None), wide)
    attention(0)
    return groups, sum(group["count"] for group in groups)


def local_operands(x_init, cot_out, w_query, w_key, w_value, w_proj, w_up, w_down):
    batch, seq, width = x_init.shape
    tokens = batch * seq
    at = {"x_0": x_init.reshape(tokens, width), "cot": cot_out.reshape(tokens, width)}
    at.update(wq=w_query, wk=w_key, wv=w_value, wo=w_proj, w_up=w_up, w_down=w_down)
    at.update(front(at, batch, seq))
    return at


def solution(mesh):
    def local_step(x_init, cot_out, w_query, w_key, w_value, w_proj, w_up, w_down):
        batch, seq, width = x_init.shape
        inputs = local_operands(x_init, cot_out, w_query, w_key, w_value, w_proj, w_up, w_down)
        groups, chunks = gradient_groups(width, w_up.shape[1])
        weights = dict(g_q=w_query.shape, g_k=w_key.shape, g_v=w_value.shape, g_o=w_proj.shape, g_up=w_up.shape, g_down=w_down.shape)
        res = finish_backward(inputs, groups, chunks, weights, batch * seq, seq)
        return (*deliver([res[name] for name in weights]), res["dx_0"].reshape(x_init.shape))

    data_spec = P("data")
    full_spec = P()
    in_specs = (data_spec, data_spec, full_spec, full_spec, full_spec, full_spec, full_spec, full_spec)
    out_specs = (full_spec, full_spec, full_spec, full_spec, full_spec, full_spec, data_spec)
    return jax.shard_map(local_step, mesh=mesh, in_specs=in_specs, out_specs=out_specs, check_vma=False)
```

```python
import functools

import jax
import jax.numpy as jnp
from jax import lax
from jax.experimental import pallas as pl
from jax.experimental.pallas import tpu as pltpu
from jax.sharding import PartitionSpec as P

EPS = 1e-6
HEAD_DIM = 64
PAIR = 2 * HEAD_DIM
FF_BLOCK = 512
OUT_BLOCK = 256
GELU_A = (2.0 / 3.141592653589793) ** 0.5
GELU_B = 0.044715
SOFTMAX_SCALE = HEAD_DIM ** -0.5 * 1.4426950408889634
MIB = 1024 * 1024


def dot(lhs, rhs, lhs_dim, rhs_dim):
    return lax.dot_general(lhs, rhs, (((lhs_dim,), (rhs_dim,)), ((), ())), preferred_element_type=jnp.float32)


def rms_norm(x_f32):
    return x_f32 * lax.rsqrt(jnp.mean(x_f32 * x_f32, axis=-1, keepdims=True) + EPS)


def rms_backward(x_f32, d_out):
    scale = lax.rsqrt(jnp.mean(x_f32 * x_f32, axis=-1, keepdims=True) + EPS)
    inner = jnp.mean(x_f32 * d_out, axis=-1, keepdims=True)
    return scale * d_out - x_f32 * (scale * scale * scale * inner)


def gelu_parts(pre):
    square = pre * pre
    tanh = jnp.tanh(GELU_A * (pre + GELU_B * pre * square))
    half = 0.5 * (1.0 + tanh)
    slope = half + 0.5 * pre * (1.0 - tanh * tanh) * (GELU_A + (3.0 * GELU_A * GELU_B) * square)
    return pre * half, slope


def bf16(*shape):
    return jax.ShapeDtypeStruct(shape, jnp.bfloat16)


def pair_backward(q_pair, k_pair, v_pair, d_pair, low, probs_of):
    sums = [None] * 3
    for side in range(2):
        mask = low if side == 0 else jnp.logical_not(low)
        d_side = jnp.where(mask, d_pair, 0)
        probs_16 = probs_of(side)
        probs_32 = probs_16.astype(jnp.float32)
        d_probs = dot(v_pair, d_side, 1, 1).astype(jnp.bfloat16).astype(jnp.float32)
        row_dot = jnp.sum(d_probs * probs_32, axis=0, keepdims=True)
        d_scores = (probs_32 * (d_probs - row_dot) * HEAD_DIM ** -0.5).astype(jnp.bfloat16)
        parts = (dot(d_scores, jnp.where(mask, k_pair, 0), 0, 0),
                 dot(d_scores, jnp.where(mask, q_pair, 0), 1, 0),
                 dot(probs_16, d_side, 1, 0))
        sums = [part if total is None else total + part for total, part in zip(sums, parts)]
    return sums


def backward_stages(pair_of, probs_of, put, low):
    masks = (low, jnp.logical_not(low))

    def from_mixed(j, _=None):
        _, _, v_pair, d_pair = pair_of(j)
        return [dot(v_pair, jnp.where(mask, d_pair, 0), 1, 1).astype(jnp.bfloat16) for mask in masks]

    def through(j, made):
        out = []
        for side, d_probs in enumerate(made):
            d_probs, probs = d_probs.astype(jnp.float32), probs_of(j, side).astype(jnp.float32)
            row_dot = jnp.sum(d_probs * probs, axis=0, keepdims=True)
            out.append((probs * (d_probs - row_dot) * HEAD_DIM ** -0.5).astype(jnp.bfloat16))
        return out

    def to_inputs(j, made):
        q_pair, k_pair, _, d_pair = pair_of(j)
        sides = [(dot(d_scores, k_pair, 0, 0), dot(d_scores, q_pair, 1, 0), dot(probs_of(j, side), d_pair, 1, 0))
                 for side, d_scores in enumerate(made)]
        put(j, [jnp.where(low, first, second) for first, second in zip(*sides)])
    return from_mixed, through, to_inputs


def forward_stages(pair_of, keep, put, low):
    def scores(j, _=None):
        q_pair, k_pair, _ = pair_of(j)
        return [dot(k_pair, jnp.where(mask, q_pair, 0), 1, 1) for mask in (low, jnp.logical_not(low))]

    def soften(j, made):
        out = []
        for side, score in enumerate(made):
            top = jnp.max(score, axis=0, keepdims=True)
            raised = jnp.exp2((score - top) * SOFTMAX_SCALE)
            inverse = 1.0 / jnp.sum(raised, axis=0, keepdims=True)
            out.append((raised * inverse).astype(jnp.bfloat16))
            keep(j, side, out[-1])
        return out

    def mix(j, made):
        first, second = (dot(probs, pair_of(j)[2], 0, 0) for probs in made)
        put(j, jnp.where(low, first, second))
    return scores, soften, mix


def in_units(first, stages, size):
    def lift(stage):
        return lambda unit, made: [stage(size * unit + i, made[i]) for i in range(size)]
    return (lambda unit: first(unit) or [None] * size, *map(lift, stages))


def staged(count, stages):
    made = [None] * count
    for turn in range(count + len(stages) - 1):
        for depth, stage in enumerate(stages):
            j = turn - depth
            if 0 <= j < count:
                made[j] = stage(j, made[j]) if depth else stage(j)


FRONT_OUTS = ("u_0", "q_0", "k_0", "v_0", "probs_0", "mixed_0", "h_0", "n_0", "pre_0", "act_0", "x_1",
              "u_1", "mixed_1", "n_1", "act_1", "dpre_1", "dh_1", "dq_1", "dk_1", "dv_1")
ROW_BUFFERS = ("u", "q", "k", "v", "mixed", "h", "n", "x", "dh", "dmix", "dq", "dk", "dv")
WIDE_BLOCK = 1024


def front_kernel(batch, seq, in_names, *refs):
    at = dict(zip((*in_names, *FRONT_OUTS), refs))
    refs = refs[len(at):]
    x_all, cot_all, w_in, w_out, w_up, w_down, probs, pre, act = refs[:9]
    row = dict(zip(ROW_BUFFERS, refs[9:]))
    load_sem, out_sem = refs[9 + len(ROW_BUFFERS):]
    width, ff = w_up.shape
    heads = width // HEAD_DIM
    loads = {"x": pltpu.make_async_copy(at["x_0"], x_all, load_sem.at[0])}
    for layer in (0, 1):
        for i, name in enumerate(("wq", "wk", "wv")):
            loads[f"{name}_{layer}"] = pltpu.make_async_copy(at[name].at[layer], w_in.at[layer, i], load_sem.at[1 + 4 * layer + i])
        loads[f"wo_{layer}"] = pltpu.make_async_copy(at["wo"].at[layer], w_out.at[layer], load_sem.at[4 + 4 * layer])
    loads["w_up"] = pltpu.make_async_copy(at["w_up"], w_up, load_sem.at[9])
    loads["w_down"] = pltpu.make_async_copy(at["w_down"], w_down, load_sem.at[10])
    loads["cot"] = pltpu.make_async_copy(at["cot"], cot_all, load_sem.at[11])
    for name in ("x", "wq_0", "wk_0", "wv_0"):
        loads[name].start()
    holders = {"probs_0": probs, "pre_0": pre, "act_0": act, "act_1": act, "dpre_1": pre, "x_1": row["x"]}
    for name in FRONT_OUTS:
        holders.setdefault(name, row.get(name[:-2]))

    def store(name, index):
        src = holders[name]
        rows = pl.ds(pl.multiple_of(seq * index, seq), seq)
        dest = at[name].at[index] if name == "probs_0" else at[name].at[rows]
        return pltpu.make_async_copy(src, dest, out_sem.at[FRONT_OUTS.index(name)])

    def one_sequence(index, carry):
        rows = pl.ds(pl.multiple_of(seq * index, seq), seq)
        first = index == 0
        low = lax.broadcasted_iota(jnp.int32, (seq, PAIR), 1) < HEAD_DIM

        def need(*names):
            @pl.when(first)
            def _():
                for name in names:
                    loads[name].wait()

        def launch(*names):
            @pl.when(first)
            def _():
                for name in names:
                    loads[name].start()

        def free(*names, same=False):
            for name in names:
                if same:
                    store(name, index).wait()
                else:
                    pl.when(index > 0)(lambda name=name: store(name, index - 1).wait())

        def send(*names):
            for name in names:
                store(name, index).start()

        def over(count, fn):
            for j in range(count):
                fn(j)

        def wide(j):
            return pl.ds(WIDE_BLOCK * j, WIDE_BLOCK)

        def attention(layer):
            x_in = x_all[rows] if layer == 0 else row["x"][...]
            row["u"][...] = rms_norm(x_in.astype(jnp.float32)).astype(jnp.bfloat16)
            need(*(f"w{kind}_{layer}" for kind in "qkv"))
            if layer == 0:
                launch("wo_0", "w_up")

            def project(unit):
                lanes = pl.ds(OUT_BLOCK * unit, OUT_BLOCK)
                for i, kind in enumerate("qkv"):
                    row[kind][:, lanes] = dot(row["u"][...], w_in[layer, i, :, lanes], 1, 0).astype(jnp.bfloat16)

            def pair_of(j):
                return tuple(row[kind][:, PAIR * j:PAIR * (j + 1)] for kind in "qkv")

            def keep(j, side, value):
                probs[2 * j + side] = value

            def put(j, value):
                row["mixed"][:, PAIR * j:PAIR * (j + 1)] = value.astype(jnp.bfloat16)
            size = OUT_BLOCK // PAIR
            staged(heads // 2 // size, in_units(project, forward_stages(pair_of, keep, put, low), size))
            need(f"wo_{layer}")
            attn = dot(row["mixed"][...], w_out[layer], 1, 0).astype(jnp.bfloat16)
            hidden = (x_in.astype(jnp.float32) + attn.astype(jnp.float32)).astype(jnp.bfloat16)
            row["h"][...] = hidden
            row["n"][...] = rms_norm(hidden.astype(jnp.float32)).astype(jnp.bfloat16)

        need("x")
        free("u_1")
        free("mixed_1", "n_1", "dh_1")
        attention(0)
        send("u_0", "q_0", "k_0", "v_0", "probs_0", "mixed_0", "h_0", "n_0")
        need("w_up")
        launch("w_down", "wq_1", "wk_1", "wv_1", "wo_1", "cot")
        free("act_1", "dpre_1")

        def raw_block(j):
            return dot(row["n"][...], w_up[:, wide(j)], 1, 0).astype(jnp.bfloat16)

        def up(j, raw):
            pre[:, wide(j)] = raw
            act[:, wide(j)] = gelu_parts(raw.astype(jnp.float32))[0].astype(jnp.bfloat16)
        staged(ff // WIDE_BLOCK, (raw_block, up))
        send("pre_0", "act_0")
        need("w_down")

        def down(j):
            lanes = pl.ds(pl.multiple_of(OUT_BLOCK * j, OUT_BLOCK), OUT_BLOCK)
            out = dot(act[...], w_down[:, lanes], 1, 0).astype(jnp.bfloat16).astype(jnp.float32)
            row["x"][:, lanes] = (row["h"][:, lanes].astype(jnp.float32) + out).astype(jnp.bfloat16)
        over(width // OUT_BLOCK, down)
        send("x_1")
        free("u_0", "q_0", "k_0", "v_0", "probs_0", "mixed_0", "h_0", "n_0", same=True)
        attention(1)
        send("u_1", "mixed_1", "n_1")
        need("cot")
        free("pre_0", "act_0", same=True)

        def both_blocks(j):
            return raw_block(j), dot(cot_all[rows], w_down[wide(j)], 1, 1).astype(jnp.bfloat16)

        def both(j, made):
            raw, d_act = made
            out, slope = gelu_parts(raw.astype(jnp.float32))
            act[:, wide(j)] = out.astype(jnp.bfloat16)
            pre[:, wide(j)] = (d_act.astype(jnp.float32) * slope).astype(jnp.bfloat16)
        staged(ff // WIDE_BLOCK, (both_blocks, both))
        send("act_1", "dpre_1")

        def back(j):
            lanes = pl.ds(pl.multiple_of(OUT_BLOCK * j, OUT_BLOCK), OUT_BLOCK)
            row["dmix"][:, lanes] = dot(pre[...], w_up[lanes], 1, 1).astype(jnp.bfloat16)
        over(width // OUT_BLOCK, back)
        d_hidden = cot_all[rows].astype(jnp.float32) + rms_backward(
            row["h"][...].astype(jnp.float32), row["dmix"][...].astype(jnp.float32))
        row["dh"][...] = d_hidden.astype(jnp.bfloat16)
        send("dh_1")

        free("dq_1", "dk_1", "dv_1")

        def unmix(unit):
            lanes = pl.ds(OUT_BLOCK * unit, OUT_BLOCK)
            row["dmix"][:, lanes] = dot(row["dh"][...], w_out[1, lanes], 1, 1).astype(jnp.bfloat16)

        def back_of(j):
            return tuple(row[kind][:, PAIR * j:PAIR * (j + 1)] for kind in ("q", "k", "v", "dmix"))

        def put_back(j, values):
            for name, value in zip(("dq", "dk", "dv"), values):
                row[name][:, PAIR * j:PAIR * (j + 1)] = value.astype(jnp.bfloat16)
        size = OUT_BLOCK // PAIR
        stages = backward_stages(back_of, lambda j, side: probs[2 * j + side], put_back, low)
        staged(heads // 2 // size, in_units(unmix, stages, size))
        send("dq_1", "dk_1", "dv_1")
        free("x_1", same=True)
        return carry

    lax.fori_loop(0, batch, one_sequence, 0)
    for name in ("u_1", "mixed_1", "n_1", "act_1", "dpre_1", "dh_1", "dq_1", "dk_1", "dv_1"):
        store(name, batch - 1).wait()


def front(inputs, batch, seq):
    tokens, width = inputs["x_0"].shape
    ff = inputs["w_up"].shape[1]
    heads = width // HEAD_DIM
    shapes = []
    for name in FRONT_OUTS:
        if name == "probs_0":
            shapes.append(bf16(batch, heads, seq, seq))
        else:
            shapes.append(bf16(tokens, ff if name[:-2] in ("pre", "act", "dpre") else width))
    block = lambda *shape: pltpu.VMEM(shape, jnp.bfloat16)
    scratch = [
        block(tokens, width), block(tokens, width), block(2, 3, width, width), block(2, width, width), block(width, ff),
        block(ff, width), block(heads, seq, seq), block(seq, ff), block(seq, ff),
        *[block(seq, width) for _ in ROW_BUFFERS],
        pltpu.SemaphoreType.DMA((12,)), pltpu.SemaphoreType.DMA((len(FRONT_OUTS),)),
    ]
    outs = pl.pallas_call(
        functools.partial(front_kernel, batch, seq, tuple(inputs)),
        out_shape=shapes,
        in_specs=[pl.BlockSpec(memory_space=pl.ANY)] * len(inputs),
        out_specs=[pl.BlockSpec(memory_space=pl.ANY)] * len(shapes),
        scratch_shapes=scratch,
        compiler_params=pltpu.CompilerParams(vmem_limit_bytes=67_043_328),
        cost_estimate=pl.CostEstimate(flops=22 * tokens * width * ff // 2, bytes_accessed=100 * MIB, transcendentals=0),
        name="front",
    )(*inputs.values())
    return dict(zip(FRONT_OUTS, outs))


MESH = pl.DeviceIdType.MESH
LANES = 1024
SET_ROWS = 128
CORE_ROWS = 2 * SET_ROWS
TILE_ROWS = 2 * CORE_ROWS
OWN_SLOTS = 8
AG_SLOTS = 10
TYPES = {
    "p1": (0, 0, 80, "xyz"),
    "q1": (0, 80, 48, "zxy"),
    "p2": (1, 128, 80, "yxz"),
    "q2": (1, 208, 48, "zyx"),
}
WRITE_AT = 11


def stage_list():
    stages = []
    for name, (_, _, _, order) in TYPES.items():
        if order[2] == "z":
            plan = [("rs1", 1), ("rs2", 2), ("rsz", 3), ("agz", 6), ("ag2", 9), ("ag1", 10)]
        else:
            plan = [("rsz", 1), ("rs1", 4), ("rs2", 5), ("ag2", 6), ("ag1", 7), ("agz", 8)]
        for kind, at in plan:
            if kind in ("rsz", "agz"):
                for step in range(3):
                    for way in (0, 1):
                        stages.append((name, kind, step, way, at + step))
            else:
                stages.append((name, kind, 0, 0, at))
    return stages


STAGES = stage_list()


def piece_shape(name, kind):
    rows, order = TYPES[name][2], TYPES[name][3]
    if order[2] == "z":
        return {"rs1": (rows, 512), "rs2": (rows, 256), "rsz": (rows // 2, 128)}[kind]
    return {"rsz": (rows // 2, 512), "rs1": (rows // 2, 256), "rs2": (rows // 2, 128)}[kind]


def between(step, first, count):
    return jnp.logical_and(step >= first, step < first + count)


class Backward:
    PB_1, MB, AB, PB_0 = 2, 6, 14, 23
    ROWS = 256

    def __init__(self, at, big, total_buf, w_buf, p_buf, sem, drain):
        self.at, self.big, self.total, self.w, self.p, self.sem, self.drain = at, big, total_buf, w_buf, p_buf, sem, drain
        self.tokens, self.width = at["x_0"].shape
        self.heads = at["probs_0"].shape[1]
        self.seq = at["probs_0"].shape[2]

    def load(self, name, dest, sem, *index):
        ref = self.at[name]
        return pltpu.make_async_copy(ref.at[index] if index else ref, dest, self.sem.at[sem])

    def store(self, src, name, sem, *index):
        ref = self.at[name]
        return pltpu.make_async_copy(src, ref.at[index] if index else ref, self.drain.at[sem])

    def row_blocks(self, fn):
        def body(block, carry):
            fn(pl.ds(pl.multiple_of(self.ROWS * block, self.ROWS), self.ROWS))
            return carry
        lax.fori_loop(0, self.tokens // self.ROWS, body, 0)

    def input_loads(self, layer):
        spot = 4 if layer else 5
        copies = [self.load(f"d{kind}_{layer}", self.big.at[i], i) for i, kind in enumerate("qkv")]
        copies.append(self.load(f"x_{layer}", self.big.at[spot], 3))
        if layer:
            copies.append(self.load("dh_1", self.big.at[5], 4))
        return copies

    def weight_loads(self, layer, block):
        rows = pl.ds(pl.multiple_of(OUT_BLOCK * block, OUT_BLOCK), OUT_BLOCK)
        slot = lax.rem(block, 2)
        return [self.load(name, self.w.at[slot, i], 5 + 3 * slot + i, layer, rows) for i, name in enumerate(("wq", "wk", "wv"))]

    def input_block(self, layer, block):
        big, blocks = self.big, self.width // OUT_BLOCK
        slot = lax.rem(block, 2)

        @pl.when(block == 0)
        def _():
            for copy in self.input_loads(layer):
                copy.wait()
        for copy in self.weight_loads(layer, block):
            copy.wait()

        @pl.when(block + 1 < blocks)
        def _():
            for copy in self.weight_loads(layer, block + 1):
                copy.start()
        lanes = pl.ds(pl.multiple_of(OUT_BLOCK * block, OUT_BLOCK), OUT_BLOCK)

        def product(rows):
            total = dot(big[0, rows], self.w[slot, 0], 1, 1) + dot(big[1, rows], self.w[slot, 1], 1, 1)
            big[3, rows, lanes] = (total + dot(big[2, rows], self.w[slot, 2], 1, 1)).astype(jnp.bfloat16)
        self.row_blocks(product)

        @pl.when(block == blocks - 1)
        def _():
            x_at, d_at = (4, 5) if layer else (5, 4)

            def close(rows):
                back = rms_backward(big[x_at, rows].astype(jnp.float32), big[3, rows].astype(jnp.float32))
                big[3, rows] = (big[d_at, rows].astype(jnp.float32) + back).astype(jnp.bfloat16)
                if layer:
                    self.total[rows] = jnp.zeros((self.ROWS, self.width), jnp.float32)
            self.row_blocks(close)
            self.store(big.at[3], f"dx_{layer}", 0).start()
            if layer:
                self.load("h_0", big.at[4], 3).start()
                for copy in self.mlp_loads(0):
                    copy.start()

    def mlp_loads(self, block):
        slot = lax.rem(block, 2)
        lanes = pl.ds(pl.multiple_of(FF_BLOCK * block, FF_BLOCK), FF_BLOCK)
        half = pl.ds(pl.multiple_of(FF_BLOCK * slot, FF_BLOCK), FF_BLOCK)
        return [self.load("w_up", self.big.at[0, :, half], 5 + 3 * slot, slice(None), lanes),
                self.load("pre_0", self.big.at[1, :, half], 6 + 3 * slot, slice(None), lanes),
                self.load("w_down", self.big.at[5, half], 7 + 3 * slot, lanes)]

    def mlp_store(self, block):
        half = pl.ds(pl.multiple_of(FF_BLOCK * lax.rem(block, 2), FF_BLOCK), FF_BLOCK)
        lanes = pl.ds(pl.multiple_of(FF_BLOCK * block, FF_BLOCK), FF_BLOCK)
        return self.store(self.big.at[2, :, half], "dpre_0", 1, slice(None), lanes)

    def mlp_block(self, block):
        big, blocks = self.big, self.at["w_up"].shape[1] // FF_BLOCK

        @pl.when(block == 0)
        def _():
            self.store(big.at[3], "dx_1", 0).wait()
            self.load("h_0", big.at[4], 3).wait()
        for copy in self.mlp_loads(block):
            copy.wait()

        @pl.when(block + 1 < blocks)
        def _():
            for copy in self.mlp_loads(block + 1):
                copy.start()

        @pl.when(block > 0)
        def _():
            self.mlp_store(block - 1).wait()
        half = pl.ds(pl.multiple_of(FF_BLOCK * lax.rem(block, 2), FF_BLOCK), FF_BLOCK)

        def product(rows):
            d_act = dot(big[3, rows], big[5, half], 1, 1).astype(jnp.bfloat16).astype(jnp.float32)
            slope = gelu_parts(big[1, rows, half].astype(jnp.float32))[1]
            d_pre = (d_act * slope).astype(jnp.bfloat16)
            big[2, rows, half] = d_pre
            self.total[rows] += dot(d_pre, big[0, :, half], 1, 1)
        self.row_blocks(product)
        self.mlp_store(block).start()

        @pl.when(block == blocks - 1)
        def _():
            def close(rows):
                d_normed = self.total[rows].astype(jnp.bfloat16).astype(jnp.float32)
                back = rms_backward(big[4, rows].astype(jnp.float32), d_normed)
                big[4, rows] = (big[3, rows].astype(jnp.float32) + back).astype(jnp.bfloat16)
            self.row_blocks(close)
            self.store(big.at[4], "dh_0", 2).start()
            self.load("wo", big.at[0], 4, 0).start()
            for copy in self.seq_loads(0) + self.probs_loads(0):
                copy.start()

    def seq_loads(self, seq):
        rows = pl.ds(pl.multiple_of(self.seq * seq, self.seq), self.seq)
        return [self.load(f"{kind}_0", self.big.at[1 + lax.rem(seq, 2), pl.ds(self.seq * i, self.seq)], i, rows)
                for i, kind in enumerate("qkv")]

    def probs_loads(self, piece):
        half = self.heads // 2
        heads = pl.ds(half * lax.rem(piece, 2), half)
        return [self.load("probs_0", self.p.at[lax.rem(piece, 2)], 5 + lax.rem(piece, 2), lax.div(piece, 2), heads)]

    def seq_stores(self, piece):
        seq, half = lax.div(piece, 2), lax.rem(piece, 2)
        rows = pl.ds(pl.multiple_of(self.seq * seq, self.seq), self.seq)
        lanes = pl.ds(pl.multiple_of(self.width // 2 * half, PAIR), self.width // 2)
        spot = 5 - 2 * lax.rem(seq, 2)
        return [self.store(self.big.at[spot, pl.ds(self.seq * i, self.seq), lanes], f"d{kind}_0", 3 + i, rows, lanes)
                for i, kind in enumerate("qkv")]

    def attention_piece(self, piece):
        big, pieces = self.big, 2 * (self.tokens // self.seq)
        seq, half = lax.div(piece, 2), lax.rem(piece, 2)
        spot, out = 1 + lax.rem(seq, 2), 5 - 2 * lax.rem(seq, 2)

        @pl.when(piece == 0)
        def _():
            self.mlp_store(self.at["w_up"].shape[1] // FF_BLOCK - 1).wait()
            self.store(big.at[4], "dh_0", 2).wait()
            self.load("wo", big.at[0], 4, 0).wait()

        @pl.when(piece > 0)
        def _():
            for copy in self.seq_stores(piece - 1):
                copy.wait()
        for copy in self.probs_loads(piece):
            copy.wait()

        @pl.when(piece + 1 < pieces)
        def _():
            for copy in self.probs_loads(piece + 1):
                copy.start()
        mixed = pl.ds(3 * self.seq, self.seq)

        @pl.when(half == 0)
        def _():
            for copy in self.seq_loads(seq):
                copy.wait()

            @pl.when(piece + 2 < pieces)
            def _():
                for copy in self.seq_loads(seq + 1):
                    copy.start()
            rows = pl.ds(pl.multiple_of(self.seq * seq, self.seq), self.seq)
            big[spot, mixed] = dot(big[4, rows], big[0], 1, 1).astype(jnp.bfloat16)
        low = lax.broadcasted_iota(jnp.int32, (self.seq, PAIR), 1) < HEAD_DIM
        pairs = self.heads // 4

        def pair(j, carry):
            lanes = pl.ds(pl.multiple_of(PAIR * (pairs * half + j), PAIR), PAIR)
            q_pair, k_pair, v_pair, d_pair = (big[spot, pl.ds(self.seq * i, self.seq), lanes] for i in range(4))
            for i, total in enumerate(pair_backward(q_pair, k_pair, v_pair, d_pair, low, lambda side: self.p[half, 2 * j + side])):
                big[out, pl.ds(self.seq * i, self.seq), lanes] = total.astype(jnp.bfloat16)
            return carry
        lax.fori_loop(0, pairs, pair, 0)
        for copy in self.seq_stores(piece):
            copy.start()

    def item(self, step):
        blocks = self.width // OUT_BLOCK
        pieces = 2 * (self.tokens // self.seq)

        @pl.when(step == self.PB_1)
        def _():
            for copy in self.input_loads(1) + self.weight_loads(1, 0):
                copy.start()
        pl.when(between(step, self.PB_1, blocks))(lambda: self.input_block(1, step - self.PB_1))
        pl.when(between(step, self.MB, 8))(lambda: self.mlp_block(step - self.MB))
        pl.when(between(step, self.AB, pieces))(lambda: self.attention_piece(step - self.AB))

        @pl.when(step == self.PB_0 - 1)
        def _():
            for copy in self.seq_stores(pieces - 1):
                copy.wait()
            for copy in self.input_loads(0) + self.weight_loads(0, 0):
                copy.start()
        pl.when(between(step, self.PB_0, blocks))(lambda: self.input_block(0, step - self.PB_0))

        @pl.when(step == self.PB_0 + blocks)
        def _():
            self.store(self.big.at[3], "dx_0", 0).wait()


def finish_kernel(groups, chunks, in_names, out_names, remote, *refs):
    names = [*in_names, *out_names]
    at, scratch = dict(zip(names, refs[:len(names)])), refs[len(names):]
    (big, total_buf, w_buf, p_buf, item_sem, drain_sem), scratch = scratch[:6], scratch[6:]
    backward = Backward(at, big, total_buf, w_buf, p_buf, item_sem, drain_sem)
    if not remote:
        lax.fori_loop(0, chunks + WRITE_AT + 1, lambda step, carry: backward.item(step) or carry, 0)
        return
    (lhs_buf, rhs_buf, own, part, part_in, gath), scratch = scratch[:6], scratch[6:]
    land_keys = [key for key, st in enumerate(STAGES) if st[1].startswith("rs")]
    landing = dict(zip(land_keys, scratch[:len(land_keys)]))
    load_sem, send_sem, recv_sem, pair_send, pair_recv, out_sem, out_send, out_recv, credit = scratch[len(land_keys):]

    me = lax.axis_index("data")
    core = lax.rem(me, 2)
    coord = {"x": lax.rem(lax.div(me, 2), 2), "y": lax.rem(lax.div(me, 4), 2)}
    z = lax.div(me, 8)
    partner = me + 1 - 2 * core
    near = {"x": me + 2 - 4 * coord["x"], "y": me + 4 - 8 * coord["y"]}
    up_ok, down_ok = z < 3, z > 0
    peers = [(partner, 0, None), (near["x"], 1, None), (near["y"], 2, None), (me + 8, 3, up_ok), (me - 8, 4, down_ok)]

    def guarded(cond, fn):
        if cond is None:
            fn()
        else:
            pl.when(cond)(fn)

    barrier = pltpu.get_barrier_semaphore()
    for dev, _, cond in peers:
        guarded(cond, lambda dev=dev: pl.semaphore_signal(barrier, inc=1, device_id=(dev,), device_id_type=MESH))
    inner = jnp.logical_and(up_ok, down_ok)
    guarded(inner, lambda: pl.semaphore_wait(barrier, 5))
    guarded(jnp.logical_not(inner), lambda: pl.semaphore_wait(barrier, 4))

    def region(name, kind, which):
        _, row, rows, order = TYPES[name]
        if order[2] == "z":
            h1, h2 = coord[order[0]], coord[order[1]]
            if kind == "1":
                return pl.ds(row, rows), pl.ds(pl.multiple_of(512 * which, 128), 512)
            if kind == "2":
                return pl.ds(row, rows), pl.ds(pl.multiple_of(512 * h1 + 256 * which, 128), 256)
            first = pl.multiple_of(row + (rows // 2) * lax.div(which, 2), 8)
            lane = pl.multiple_of(512 * h1 + 256 * h2 + 128 * lax.rem(which, 2), 128)
            return pl.ds(first, rows // 2), pl.ds(lane, 128)
        h1 = coord[order[1]]
        if kind == "z":
            first = pl.multiple_of(row + (rows // 2) * lax.div(which, 2), 8)
            return pl.ds(first, rows // 2), pl.ds(pl.multiple_of(512 * lax.rem(which, 2), 128), 512)
        first = pl.multiple_of(row + (rows // 2) * lax.div(z, 2), 8)
        if kind == "1":
            return pl.ds(first, rows // 2), pl.ds(pl.multiple_of(512 * lax.rem(z, 2) + 256 * which, 128), 256)
        lane = pl.multiple_of(512 * lax.rem(z, 2) + 256 * h1 + 128 * which, 128)
        return pl.ds(first, rows // 2), pl.ds(lane, 128)

    def exchange_axis(name, kind):
        order = TYPES[name][3]
        dims = order[:2] if order[2] == "z" else order[1:]
        return dims[int(kind) - 1]

    def plan(key, chunk, parity):
        name, kind, step, way, _ = STAGES[key]
        mine, slot = lax.rem(chunk, OWN_SLOTS), lax.rem(chunk, AG_SLOTS)
        if kind in ("rs1", "rs2"):
            axis = exchange_axis(name, kind[2])
            src, keep = region(name, kind[2], 1 - coord[axis]), region(name, kind[2], coord[axis])
            dev, send_ok, recv_ok = near[axis], None, None
            sent = own.at[mine, src[0], src[1]]
        elif kind in ("ag1", "ag2"):
            axis = exchange_axis(name, kind[2])
            src = keep = region(name, kind[2], coord[axis])
            dev, send_ok, recv_ok = near[axis], None, None
            sent = gath.at[slot, src[0], src[1]]
        elif kind == "rsz":
            if way:
                dev, k_send, k_keep = me + 8, z + 3 - step, z + 2 - step
                send_ok, recv_ok = k_send <= 3, jnp.logical_and(k_keep <= 3, down_ok)
            else:
                dev, k_send, k_keep = me - 8, z - 3 + step, z - 2 + step
                send_ok, recv_ok = k_send >= 0, jnp.logical_and(k_keep >= 0, up_ok)
            src, keep = region(name, "z", k_send), region(name, "z", k_keep)
            sent = own.at[mine, src[0], src[1]]
        else:
            if way:
                dev, k_send, k_keep = me + 8, z - step, z - 1 - step
                send_ok, recv_ok = jnp.logical_and(k_send >= 0, up_ok), k_keep >= 0
            else:
                dev, k_send, k_keep = me - 8, z + step, z + 1 + step
                send_ok, recv_ok = jnp.logical_and(k_send <= 3, down_ok), k_keep <= 3
            src, keep = region(name, "z", k_send), region(name, "z", k_keep)
            sent = gath.at[slot, src[0], src[1]]
        sems = dict(send_sem=send_sem.at[key], recv_sem=recv_sem.at[key, parity], device_id=(dev,), device_id_type=MESH)
        if kind.startswith("rs"):
            target = landing[key].at[parity]
            send = lambda: pltpu.make_async_remote_copy(src_ref=sent, dst_ref=target, **sems)
            recv = lambda: pltpu.make_async_remote_copy(
                src_ref=own.at[mine, keep[0], keep[1]], dst_ref=target, **sems)

            def arrive():
                own[mine, keep[0], keep[1]] += landing[key][parity]
        else:
            send = lambda: pltpu.make_async_remote_copy(src_ref=sent, dst_ref=sent, **sems)
            recv = lambda: pltpu.make_async_remote_copy(
                src_ref=gath.at[slot, keep[0], keep[1]], dst_ref=gath.at[slot, keep[0], keep[1]], **sems)
            arrive = None
        return send, recv, send_ok, recv_ok, arrive

    def finish(name, chunk):
        order = TYPES[name][3]
        reg = region(name, "z", z) if order[2] == "z" else region(name, "2", coord[order[2]])
        gath[lax.rem(chunk, AG_SLOTS), reg[0], reg[1]] = own[lax.rem(chunk, OWN_SLOTS), reg[0], reg[1]]

    def valid(chunk):
        return jnp.logical_and(chunk >= 0, chunk < chunks)

    def set_rows(half):
        return pl.ds(half * SET_ROWS, SET_ROWS)

    def pair_copy(half, parity):
        return pltpu.make_async_remote_copy(
            src_ref=part.at[parity, set_rows(half)], dst_ref=part_in.at[parity, set_rows(half)],
            send_sem=pair_send.at[half], recv_sem=pair_recv.at[half, parity], device_id=(partner,), device_id_type=MESH)

    def out_copies(half, group, local, whose):
        out, layer = group["out"]
        ref = at[out] if layer is None else at[out].at[layer]
        rows, cols = group["place"](local)
        first = pl.multiple_of(rows + CORE_ROWS * whose + half * SET_ROWS, SET_ROWS)
        return ref.at[pl.ds(first, SET_ROWS), pl.ds(pl.multiple_of(cols, 128), LANES)]

    def write_copies(half, chunk, dest):
        slot = lax.rem(chunk, AG_SLOTS)
        src = gath.at[slot, set_rows(half)]
        here = pltpu.make_async_copy(src, dest, out_sem.at[half])
        there = pltpu.make_async_remote_copy(
            src_ref=src, dst_ref=dest, send_sem=out_send.at[half], recv_sem=out_recv.at[half, lax.rem(chunk, 2)],
            device_id=(partner,), device_id_type=MESH)
        return here, there

    def load_copies(group, local, slot):
        rows, cols = group["place"](local)
        copies = []
        for app, (lhs, rhs) in enumerate(zip(group["lhs"], group["rhs"])):
            for whose in (0, 1):
                first = rows + CORE_ROWS * (core if whose == 0 else 1 - core)
                copies.append(pltpu.make_async_copy(
                    at[lhs].at[:, pl.ds(pl.multiple_of(first, CORE_ROWS), CORE_ROWS)],
                    lhs_buf.at[slot, app, whose], load_sem.at[slot, app, whose]))
            copies.append(pltpu.make_async_copy(
                at[rhs].at[:, pl.ds(pl.multiple_of(cols, 128), LANES)], rhs_buf.at[slot, app], load_sem.at[slot, app, 2]))
        return copies

    def for_group(chunk, fn):
        for group in groups:
            inside = jnp.logical_and(chunk >= group["start"], chunk < group["start"] + group["count"])
            pl.when(inside)(functools.partial(fn, group, chunk - group["start"]))

    def two_apps(chunk):
        flags = [jnp.logical_and(chunk >= g["start"], chunk < g["start"] + g["count"]) for g in groups if len(g["lhs"]) == 2]
        return functools.reduce(jnp.logical_or, flags)

    def start_load(chunk):
        def go(group, local):
            for copy in load_copies(group, local, lax.rem(chunk, 2)):
                copy.start()
        for_group(chunk, go)

    def wait_load(chunk):
        slot = lax.rem(chunk, 2)
        any_two = next(g for g in groups if len(g["lhs"]) == 2)
        copies = load_copies(any_two, 0, slot)
        for copy in copies[:3]:
            copy.wait()

        @pl.when(two_apps(chunk))
        def _():
            for copy in copies[3:]:
                copy.wait()

    def tile(chunk):
        slot, mine, parity = lax.rem(chunk, 2), lax.rem(chunk, OWN_SLOTS), lax.rem(chunk, 2)

        def product(app, whose):
            return lax.dot_general(lhs_buf[slot, app, whose], rhs_buf[slot, app], (((0,), (0,)), ((), ())),
                                   preferred_element_type=jnp.float32)

        own[mine] = product(0, 0)
        part[parity] = product(0, 1)

        @pl.when(two_apps(chunk))
        def _():
            own[mine] += product(1, 0)
            part[parity] += product(1, 1)

    last = chunks + WRITE_AT

    def section(half, step):
        before = lax.rem(step + 1, 2)
        now = lax.rem(step, 2)

        @pl.when(valid(step - 1))
        def _():
            copy = pair_copy(half, before)
            copy.wait_send()
            copy.wait_recv()
            mine = lax.rem(step - 1, OWN_SLOTS)
            own[mine, set_rows(half)] += part_in[before, set_rows(half)]

        names = [name for name in TYPES if TYPES[name][0] == half]
        keys = [key for key, st in enumerate(STAGES) if st[0] in names]
        finals = {name: max(st[4] for st in STAGES if st[0] == name and st[1].startswith("rs")) for name in names}
        for key in keys:
            name, at = STAGES[key][0], STAGES[key][4]
            chunk = step - 1 - at

            @pl.when(valid(chunk))
            def _(key=key, chunk=chunk):
                send, recv, send_ok, recv_ok, arrive = plan(key, chunk, before)

                def arrived():
                    recv().wait_recv()
                    if arrive is not None:
                        arrive()
                guarded(recv_ok, arrived)
                guarded(send_ok, lambda: send().wait_send())
        for name in names:
            chunk = step - 1 - finals[name]
            pl.when(valid(chunk))(functools.partial(finish, name, chunk))

        done = step - 1 - WRITE_AT

        @pl.when(valid(done))
        def _():
            here, there = write_copies(half, done, out_copies(half, groups[0], 0, 0))
            here.wait()
            there.wait_send()
            there.wait_recv()

        @pl.when(step < last)
        def _():
            for dev, way, cond in peers:
                to = way if way < 3 else 7 - way
                guarded(cond, lambda dev=dev, to=to: pl.semaphore_signal(
                    credit.at[half, to], inc=1, device_id=(dev,), device_id_type=MESH))

        @pl.when(step > 0)
        def _():
            for dev, way, cond in peers:
                guarded(cond, lambda way=way: pl.semaphore_wait(credit.at[half, way], 1))

        for key in reversed(keys):
            chunk = step - STAGES[key][4]

            @pl.when(valid(chunk))
            def _(key=key, chunk=chunk):
                send, recv, send_ok, recv_ok, arrive = plan(key, chunk, now)
                guarded(send_ok, lambda: send().start())

        out_chunk = step - WRITE_AT

        @pl.when(valid(out_chunk))
        def _():
            def go(group, local):
                for copy in write_copies(half, out_chunk, out_copies(half, group, local, core)):
                    copy.start()
            for_group(out_chunk, go)

    start_load(jnp.int32(0))

    def round_(step, carry):
        section(0, step)

        @pl.when(valid(step))
        def _():
            pl.when(step + 1 < chunks)(lambda: start_load(step + 1))
            wait_load(step)
            tile(step)
            pair_copy(0, lax.rem(step, 2)).start()

        section(1, step)

        @pl.when(valid(step))
        def _():
            pair_copy(1, lax.rem(step, 2)).start()

        backward.item(step)
        return carry

    lax.fori_loop(0, last + 1, round_, 0)


def finish_backward(inputs, groups, chunks, weights, tokens, seq, collective_id=0, remote=True):
    width, ff = inputs["w_up"].shape
    landing = [pltpu.VMEM((2,) + piece_shape(st[0], st[1]), jnp.float32) for st in STAGES if st[1].startswith("rs")]
    apps = 2
    outs = {name: jax.ShapeDtypeStruct(shape, jnp.float32) for name, shape in weights.items()}
    for name in ("dx_0", "dx_1", "dh_0", "dq_0", "dk_0", "dv_0"):
        outs[name] = bf16(tokens, width)
    outs["dpre_0"] = bf16(tokens, ff)
    heads = width // HEAD_DIM
    scratch = [
        pltpu.VMEM((6, tokens, width), jnp.bfloat16),
        pltpu.VMEM((tokens, width), jnp.float32),
        pltpu.VMEM((2, 3, OUT_BLOCK, width), jnp.bfloat16),
        pltpu.VMEM((2, heads // 2, seq, seq), jnp.bfloat16),
        pltpu.SemaphoreType.DMA((11,)),
        pltpu.SemaphoreType.DMA((6,)),
    ]
    if remote:
        scratch += [
            pltpu.VMEM((2, apps, 2, tokens, CORE_ROWS), jnp.bfloat16),
            pltpu.VMEM((2, apps, tokens, LANES), jnp.bfloat16),
            pltpu.VMEM((OWN_SLOTS, CORE_ROWS, LANES), jnp.float32),
            pltpu.VMEM((2, CORE_ROWS, LANES), jnp.float32),
            pltpu.VMEM((2, CORE_ROWS, LANES), jnp.float32),
            pltpu.VMEM((AG_SLOTS, CORE_ROWS, LANES), jnp.float32),
            *landing,
            pltpu.SemaphoreType.DMA((2, apps, 3)),
            pltpu.SemaphoreType.DMA((len(STAGES),)),
            pltpu.SemaphoreType.DMA((len(STAGES), 2)),
            pltpu.SemaphoreType.DMA((2,)),
            pltpu.SemaphoreType.DMA((2, 2)),
            pltpu.SemaphoreType.DMA((2,)),
            pltpu.SemaphoreType.DMA((2,)),
            pltpu.SemaphoreType.DMA((2, 2)),
            pltpu.SemaphoreType.REGULAR((2, 5)),
        ]
    params = dict(collective_id=collective_id, has_side_effects=True) if remote else {}
    results = pl.pallas_call(
        functools.partial(finish_kernel, groups, chunks, list(inputs), list(outs), remote),
        out_shape=list(outs.values()),
        in_specs=[pl.BlockSpec(memory_space=pl.ANY)] * len(inputs),
        out_specs=[pl.BlockSpec(memory_space=pl.ANY)] * len(outs),
        scratch_shapes=scratch,
        compiler_params=pltpu.CompilerParams(vmem_limit_bytes=67_043_328, **params),
        cost_estimate=pl.CostEstimate(flops=20 * tokens * width * ff, bytes_accessed=256 * MIB, transcendentals=0),
        name="finish_backward",
    )(*inputs.values())
    return dict(zip(outs, results))


DELIVER_ROWS = 512
DELIVER_SLOTS = 16
DELIVER_AHEAD = 8


def deliver(arrays, small):
    def blocks_of(array):
        lead = [(i,) for i in range(array.shape[0])] if len(array.shape) == 3 else [()]
        rows, cols = array.shape[-2:]
        return [(*index, pl.ds(row, DELIVER_ROWS), pl.ds(col, LANES))
                for index in lead for row in range(0, rows, DELIVER_ROWS) for col in range(0, cols, LANES)]

    work = [(i, index) for i, array in enumerate(arrays) for index in blocks_of(array)]
    count = len(arrays) + 1

    def kernel(*refs):
        ins, outs, buf, whole_buf, in_sem, out_sem, whole_sem = refs[:count], refs[count:2 * count], *refs[2 * count:]
        whole_in = pltpu.make_async_copy(ins[-1], whole_buf, whole_sem.at[0])
        whole_out = pltpu.make_async_copy(whole_buf, outs[-1], whole_sem.at[1])

        def fetch(t):
            i, index = work[t]
            return pltpu.make_async_copy(ins[i].at[index], buf.at[t % DELIVER_SLOTS], in_sem.at[t % DELIVER_SLOTS])

        def put(t):
            i, index = work[t]
            return pltpu.make_async_copy(buf.at[t % DELIVER_SLOTS], outs[i].at[index], out_sem.at[t % DELIVER_SLOTS])

        whole_in.start()
        for t in range(min(DELIVER_AHEAD, len(work))):
            fetch(t).start()
        whole_in.wait()
        whole_out.start()
        for t in range(len(work)):
            if t + DELIVER_AHEAD < len(work):
                if t + DELIVER_AHEAD >= DELIVER_SLOTS:
                    put(t + DELIVER_AHEAD - DELIVER_SLOTS).wait()
                fetch(t + DELIVER_AHEAD).start()
            fetch(t).wait()
            put(t).start()
        for t in range(max(0, len(work) - DELIVER_SLOTS), len(work)):
            put(t).wait()
        whole_out.wait()

    return pl.pallas_call(
        kernel,
        out_shape=[jax.ShapeDtypeStruct(array.shape, array.dtype) for array in (*arrays, small)],
        in_specs=[pl.BlockSpec(memory_space=pl.ANY)] * count,
        out_specs=[pl.BlockSpec(memory_space=pl.ANY)] * count,
        scratch_shapes=[pltpu.VMEM((DELIVER_SLOTS, DELIVER_ROWS, LANES), jnp.float32), pltpu.VMEM(small.shape, small.dtype),
                        pltpu.SemaphoreType.DMA((DELIVER_SLOTS,)), pltpu.SemaphoreType.DMA((DELIVER_SLOTS,)),
                        pltpu.SemaphoreType.DMA((2,))],
        compiler_params=pltpu.CompilerParams(vmem_limit_bytes=67_043_328),
        cost_estimate=pl.CostEstimate(flops=0, bytes_accessed=2 * sum(a.size for a in arrays) * 4, transcendentals=0),
        name="deliver",
    )(*arrays, small)


def gradient_groups(width, ff):
    groups = []

    def add(count, lhs, rhs, out, place):
        start = groups[-1]["start"] + groups[-1]["count"] if groups else 0
        groups.append(dict(start=start, count=count, lhs=lhs, rhs=rhs, out=out, place=place))

    def tall(local):
        return TILE_ROWS * local, 0

    def wide(local):
        return TILE_ROWS * lax.rem(local, width // TILE_ROWS), LANES * lax.div(local, width // TILE_ROWS)

    def attention(layer):
        for out, kind in enumerate("qkv"):
            add(width // TILE_ROWS, [f"u_{layer}"], [f"d{kind}_{layer}"], (f"g_{kind}", layer), tall)
        add(width // TILE_ROWS, [f"mixed_{layer}"], [f"dh_{layer}"], ("g_o", layer), tall)

    attention(1)
    add(ff // TILE_ROWS, ["act_0", "act_1"], ["dx_1", "cot"], ("g_down", None), tall)
    add(ff // TILE_ROWS, ["n_0", "n_1"], ["dpre_0", "dpre_1"], ("g_up", None), wide)
    attention(0)
    return groups, sum(group["count"] for group in groups)


def local_operands(x_init, cot_out, w_query, w_key, w_value, w_proj, w_up, w_down):
    batch, seq, width = x_init.shape
    tokens = batch * seq
    at = {"x_0": x_init.reshape(tokens, width), "cot": cot_out.reshape(tokens, width)}
    at.update(wq=w_query, wk=w_key, wv=w_value, wo=w_proj, w_up=w_up, w_down=w_down)
    at.update(front(at, batch, seq))
    return at


def solution(mesh):
    def local_step(x_init, cot_out, w_query, w_key, w_value, w_proj, w_up, w_down):
        batch, seq, width = x_init.shape
        inputs = local_operands(x_init, cot_out, w_query, w_key, w_value, w_proj, w_up, w_down)
        groups, chunks = gradient_groups(width, w_up.shape[1])
        weights = dict(g_q=w_query.shape, g_k=w_key.shape, g_v=w_value.shape, g_o=w_proj.shape, g_up=w_up.shape, g_down=w_down.shape)
        res = finish_backward(inputs, groups, chunks, weights, batch * seq, seq)
        *grads, d_init = deliver([res[name] for name in weights], res["dx_0"])
        return (*grads, d_init.reshape(x_init.shape))

    data_spec = P("data")
    full_spec = P()
    in_specs = (data_spec, data_spec, full_spec, full_spec, full_spec, full_spec, full_spec, full_spec)
    out_specs = (full_spec, full_spec, full_spec, full_spec, full_spec, full_spec, data_spec)
    return jax.shard_map(local_step, mesh=mesh, in_specs=in_specs, out_specs=out_specs, check_vma=False)
```

```python
import functools

import jax
import jax.numpy as jnp
from jax import lax
from jax.experimental import pallas as pl
from jax.experimental.pallas import tpu as pltpu
from jax.sharding import PartitionSpec as P

EPS = 1e-6
HEAD_DIM = 64
PAIR = 2 * HEAD_DIM
FF_BLOCK = 512
OUT_BLOCK = 256
GELU_A = (2.0 / 3.141592653589793) ** 0.5
GELU_B = 0.044715
SOFTMAX_SCALE = HEAD_DIM ** -0.5 * 1.4426950408889634
MIB = 1024 * 1024


def dot(lhs, rhs, lhs_dim, rhs_dim):
    return lax.dot_general(lhs, rhs, (((lhs_dim,), (rhs_dim,)), ((), ())), preferred_element_type=jnp.float32)


def rms_norm(x_f32):
    return x_f32 * lax.rsqrt(jnp.mean(x_f32 * x_f32, axis=-1, keepdims=True) + EPS)


def rms_backward(x_f32, d_out):
    scale = lax.rsqrt(jnp.mean(x_f32 * x_f32, axis=-1, keepdims=True) + EPS)
    inner = jnp.mean(x_f32 * d_out, axis=-1, keepdims=True)
    return scale * d_out - x_f32 * (scale * scale * scale * inner)


def gelu_parts(pre):
    square = pre * pre
    tanh = jnp.tanh(GELU_A * (pre + GELU_B * pre * square))
    half = 0.5 * (1.0 + tanh)
    slope = half + 0.5 * pre * (1.0 - tanh * tanh) * (GELU_A + (3.0 * GELU_A * GELU_B) * square)
    return pre * half, slope


def bf16(*shape):
    return jax.ShapeDtypeStruct(shape, jnp.bfloat16)


def backward_stages(pair_of, probs_of, put, low):
    masks = (low, jnp.logical_not(low))

    def from_mixed(j, _=None):
        _, _, v_pair, d_pair = pair_of(j)
        return [dot(v_pair, jnp.where(mask, d_pair, 0), 1, 1).astype(jnp.bfloat16) for mask in masks]

    def through(j, made):
        out = []
        for side, d_probs in enumerate(made):
            d_probs, probs = d_probs.astype(jnp.float32), probs_of(j, side).astype(jnp.float32)
            row_dot = jnp.sum(d_probs * probs, axis=0, keepdims=True)
            out.append((probs * (d_probs - row_dot) * HEAD_DIM ** -0.5).astype(jnp.bfloat16))
        return out

    def to_inputs(j, made):
        q_pair, k_pair, _, d_pair = pair_of(j)
        sides = [(dot(d_scores, k_pair, 0, 0), dot(d_scores, q_pair, 1, 0), dot(probs_of(j, side), d_pair, 1, 0))
                 for side, d_scores in enumerate(made)]
        put(j, [jnp.where(low, first, second) for first, second in zip(*sides)])
    return from_mixed, through, to_inputs


def forward_stages(pair_of, keep, put, low):
    def scores(j, _=None):
        q_pair, k_pair, _ = pair_of(j)
        return [dot(k_pair, jnp.where(mask, q_pair, 0), 1, 1) for mask in (low, jnp.logical_not(low))]

    def soften(j, made):
        out = []
        for side, score in enumerate(made):
            top = jnp.max(score, axis=0, keepdims=True)
            raised = jnp.exp2((score - top) * SOFTMAX_SCALE)
            inverse = 1.0 / jnp.sum(raised, axis=0, keepdims=True)
            out.append((raised * inverse).astype(jnp.bfloat16))
            keep(j, side, out[-1])
        return out

    def mix(j, made):
        first, second = (dot(probs, pair_of(j)[2], 0, 0) for probs in made)
        put(j, jnp.where(low, first, second))
    return scores, soften, mix


def in_units(first, stages, size):
    def lift(stage):
        return lambda unit, made: [stage(size * unit + i, made[i]) for i in range(size)]
    return (lambda unit: first(unit) or [None] * size, *map(lift, stages))


def staged(count, stages):
    made = [None] * count
    for turn in range(count + len(stages) - 1):
        for depth, stage in enumerate(stages):
            j = turn - depth
            if 0 <= j < count:
                made[j] = stage(j, made[j]) if depth else stage(j)


FRONT_OUTS = ("u_0", "q_0", "k_0", "v_0", "probs_0", "mixed_0", "h_0", "n_0", "pre_0", "act_0", "x_1",
              "u_1", "q_1", "k_1", "v_1", "probs_1", "mixed_1", "n_1", "act_1", "dpre_1", "dh_1")
ROW_BUFFERS = ("u", "q", "k", "v", "mixed", "h", "n", "x", "dh", "dn")
WIDE_BLOCK = 1024


def front_kernel(batch, seq, in_names, *refs):
    at = dict(zip((*in_names, *FRONT_OUTS), refs))
    refs = refs[len(at):]
    x_all, cot_all, w_in, w_out, w_up, w_down, probs, pre, act = refs[:9]
    row = dict(zip(ROW_BUFFERS, refs[9:]))
    load_sem, out_sem = refs[9 + len(ROW_BUFFERS):]
    width, ff = w_up.shape
    heads = width // HEAD_DIM
    loads = {"x": pltpu.make_async_copy(at["x_0"], x_all, load_sem.at[0])}
    for layer in (0, 1):
        for i, name in enumerate(("wq", "wk", "wv")):
            loads[f"{name}_{layer}"] = pltpu.make_async_copy(at[name].at[layer], w_in.at[layer, i], load_sem.at[1 + 4 * layer + i])
        loads[f"wo_{layer}"] = pltpu.make_async_copy(at["wo"].at[layer], w_out.at[layer], load_sem.at[4 + 4 * layer])
    loads["w_up"] = pltpu.make_async_copy(at["w_up"], w_up, load_sem.at[9])
    loads["w_down"] = pltpu.make_async_copy(at["w_down"], w_down, load_sem.at[10])
    loads["cot"] = pltpu.make_async_copy(at["cot"], cot_all, load_sem.at[11])
    for name in ("x", "wq_0", "wk_0", "wv_0"):
        loads[name].start()
    holders = {"probs_0": probs, "probs_1": probs, "pre_0": pre, "act_0": act, "act_1": act, "dpre_1": pre, "x_1": row["x"]}
    for name in FRONT_OUTS:
        holders.setdefault(name, row.get(name[:-2]))

    def store(name, index):
        src = holders[name]
        rows = pl.ds(pl.multiple_of(seq * index, seq), seq)
        dest = at[name].at[index] if name.startswith("probs") else at[name].at[rows]
        return pltpu.make_async_copy(src, dest, out_sem.at[FRONT_OUTS.index(name)])

    def one_sequence(index, carry):
        rows = pl.ds(pl.multiple_of(seq * index, seq), seq)
        first = index == 0
        low = lax.broadcasted_iota(jnp.int32, (seq, PAIR), 1) < HEAD_DIM

        def need(*names):
            @pl.when(first)
            def _():
                for name in names:
                    loads[name].wait()

        def launch(*names):
            @pl.when(first)
            def _():
                for name in names:
                    loads[name].start()

        def free(*names, same=False):
            for name in names:
                if same:
                    store(name, index).wait()
                else:
                    pl.when(index > 0)(lambda name=name: store(name, index - 1).wait())

        def send(*names):
            for name in names:
                store(name, index).start()

        def over(count, fn):
            for j in range(count):
                fn(j)

        def wide(j):
            return pl.ds(WIDE_BLOCK * j, WIDE_BLOCK)

        def attention(layer):
            x_in = x_all[rows] if layer == 0 else row["x"][...]
            row["u"][...] = rms_norm(x_in.astype(jnp.float32)).astype(jnp.bfloat16)
            need(*(f"w{kind}_{layer}" for kind in "qkv"))
            if layer == 0:
                launch("wo_0", "w_up")

            def project(unit):
                lanes = pl.ds(OUT_BLOCK * unit, OUT_BLOCK)
                for i, kind in enumerate("qkv"):
                    row[kind][:, lanes] = dot(row["u"][...], w_in[layer, i, :, lanes], 1, 0).astype(jnp.bfloat16)

            def pair_of(j):
                return tuple(row[kind][:, PAIR * j:PAIR * (j + 1)] for kind in "qkv")

            def keep(j, side, value):
                probs[2 * j + side] = value

            def put(j, value):
                row["mixed"][:, PAIR * j:PAIR * (j + 1)] = value.astype(jnp.bfloat16)
            size = OUT_BLOCK // PAIR
            staged(heads // 2 // size, in_units(project, forward_stages(pair_of, keep, put, low), size))
            need(f"wo_{layer}")
            attn = dot(row["mixed"][...], w_out[layer], 1, 0).astype(jnp.bfloat16)
            hidden = (x_in.astype(jnp.float32) + attn.astype(jnp.float32)).astype(jnp.bfloat16)
            row["h"][...] = hidden
            row["n"][...] = rms_norm(hidden.astype(jnp.float32)).astype(jnp.bfloat16)

        need("x")
        free("u_1", "q_1", "k_1", "v_1", "probs_1", "mixed_1", "n_1", "dh_1")
        attention(0)
        send("u_0", "q_0", "k_0", "v_0", "probs_0", "mixed_0", "h_0", "n_0")
        need("w_up")
        launch("w_down", "wq_1", "wk_1", "wv_1", "wo_1", "cot")
        free("act_1", "dpre_1")

        def raw_block(j):
            return dot(row["n"][...], w_up[:, wide(j)], 1, 0).astype(jnp.bfloat16)

        def up(j, raw):
            pre[:, wide(j)] = raw
            act[:, wide(j)] = gelu_parts(raw.astype(jnp.float32))[0].astype(jnp.bfloat16)
        staged(ff // WIDE_BLOCK, (raw_block, up))
        send("pre_0", "act_0")
        need("w_down")

        def down(j):
            lanes = pl.ds(pl.multiple_of(OUT_BLOCK * j, OUT_BLOCK), OUT_BLOCK)
            out = dot(act[...], w_down[:, lanes], 1, 0).astype(jnp.bfloat16).astype(jnp.float32)
            row["x"][:, lanes] = (row["h"][:, lanes].astype(jnp.float32) + out).astype(jnp.bfloat16)
        over(width // OUT_BLOCK, down)
        send("x_1")
        free("u_0", "q_0", "k_0", "v_0", "probs_0", "mixed_0", "h_0", "n_0", same=True)
        attention(1)
        send("u_1", "q_1", "k_1", "v_1", "probs_1", "mixed_1", "n_1")
        need("cot")
        free("pre_0", "act_0", same=True)

        def both_blocks(j):
            return raw_block(j), dot(cot_all[rows], w_down[wide(j)], 1, 1).astype(jnp.bfloat16)

        def both(j, made):
            raw, d_act = made
            out, slope = gelu_parts(raw.astype(jnp.float32))
            act[:, wide(j)] = out.astype(jnp.bfloat16)
            pre[:, wide(j)] = (d_act.astype(jnp.float32) * slope).astype(jnp.bfloat16)
        staged(ff // WIDE_BLOCK, (both_blocks, both))
        send("act_1", "dpre_1")

        def back(j):
            lanes = pl.ds(pl.multiple_of(OUT_BLOCK * j, OUT_BLOCK), OUT_BLOCK)
            row["dn"][:, lanes] = dot(pre[...], w_up[lanes], 1, 1).astype(jnp.bfloat16)
        over(width // OUT_BLOCK, back)
        d_hidden = cot_all[rows].astype(jnp.float32) + rms_backward(
            row["h"][...].astype(jnp.float32), row["dn"][...].astype(jnp.float32))
        row["dh"][...] = d_hidden.astype(jnp.bfloat16)
        send("dh_1")
        free("x_1", same=True)
        return carry

    lax.fori_loop(0, batch, one_sequence, 0)
    for name in ("u_1", "q_1", "k_1", "v_1", "probs_1", "mixed_1", "n_1", "act_1", "dpre_1", "dh_1"):
        store(name, batch - 1).wait()


def front(inputs, batch, seq):
    tokens, width = inputs["x_0"].shape
    ff = inputs["w_up"].shape[1]
    heads = width // HEAD_DIM
    shapes = []
    for name in FRONT_OUTS:
        if name.startswith("probs"):
            shapes.append(bf16(batch, heads, seq, seq))
        else:
            shapes.append(bf16(tokens, ff if name[:-2] in ("pre", "act", "dpre") else width))
    block = lambda *shape: pltpu.VMEM(shape, jnp.bfloat16)
    scratch = [
        block(tokens, width), block(tokens, width), block(2, 3, width, width), block(2, width, width), block(width, ff),
        block(ff, width), block(heads, seq, seq), block(seq, ff), block(seq, ff),
        *[block(seq, width) for _ in ROW_BUFFERS],
        pltpu.SemaphoreType.DMA((12,)), pltpu.SemaphoreType.DMA((len(FRONT_OUTS),)),
    ]
    outs = pl.pallas_call(
        functools.partial(front_kernel, batch, seq, tuple(inputs)),
        out_shape=shapes,
        in_specs=[pl.BlockSpec(memory_space=pl.ANY)] * len(inputs),
        out_specs=[pl.BlockSpec(memory_space=pl.ANY)] * len(shapes),
        scratch_shapes=scratch,
        compiler_params=pltpu.CompilerParams(vmem_limit_bytes=67_043_328),
        cost_estimate=pl.CostEstimate(flops=22 * tokens * width * ff // 2, bytes_accessed=100 * MIB, transcendentals=0),
        name="front",
    )(*inputs.values())
    return dict(zip(FRONT_OUTS, outs))


MESH = pl.DeviceIdType.MESH
LANES = 1024
SET_ROWS = 128
CORE_ROWS = 2 * SET_ROWS
TILE_ROWS = 2 * CORE_ROWS
OWN_SLOTS = 8
AG_SLOTS = 10
TYPES = {
    "p1": (0, 0, 80, "xyz"),
    "q1": (0, 80, 48, "zxy"),
    "p2": (1, 128, 80, "yxz"),
    "q2": (1, 208, 48, "zyx"),
}
WRITE_AT = 11


def stage_list():
    stages = []
    for name, (_, _, _, order) in TYPES.items():
        if order[2] == "z":
            plan = [("rs1", 1), ("rs2", 2), ("rsz", 3), ("agz", 6), ("ag2", 9), ("ag1", 10)]
        else:
            plan = [("rsz", 1), ("rs1", 4), ("rs2", 5), ("ag2", 6), ("ag1", 7), ("agz", 8)]
        for kind, at in plan:
            if kind in ("rsz", "agz"):
                for step in range(3):
                    for way in (0, 1):
                        stages.append((name, kind, step, way, at + step))
            else:
                stages.append((name, kind, 0, 0, at))
    return stages


STAGES = stage_list()


def piece_shape(name, kind):
    rows, order = TYPES[name][2], TYPES[name][3]
    if order[2] == "z":
        return {"rs1": (rows, 512), "rs2": (rows, 256), "rsz": (rows // 2, 128)}[kind]
    return {"rsz": (rows // 2, 512), "rs1": (rows // 2, 256), "rs2": (rows // 2, 128)}[kind]


def between(step, first, count):
    return jnp.logical_and(step >= first, step < first + count)


class Backward:
    PB_1, MB, AB, PB_0 = 4, 6, 14, 23
    ROWS = 256

    def __init__(self, at, big, total_buf, w_buf, p_buf, sem, drain):
        self.at, self.big, self.total, self.w, self.p, self.sem, self.drain = at, big, total_buf, w_buf, p_buf, sem, drain
        self.tokens, self.width = at["x_0"].shape
        self.heads = at["probs_0"].shape[1]
        self.seq = at["probs_0"].shape[2]
        self.seqs = self.tokens // self.seq

    def load(self, name, dest, sem, *index):
        ref = self.at[name]
        return pltpu.make_async_copy(ref.at[index] if index else ref, dest, self.sem.at[sem])

    def store(self, src, name, sem, *index):
        ref = self.at[name]
        return pltpu.make_async_copy(src, ref.at[index] if index else ref, self.drain.at[sem])

    def row_blocks(self, fn):
        def body(block, carry):
            fn(pl.ds(pl.multiple_of(self.ROWS * block, self.ROWS), self.ROWS))
            return carry
        lax.fori_loop(0, self.tokens // self.ROWS, body, 0)

    def input_loads(self, layer):
        copies = [self.load(f"d{kind}_{layer}", self.big.at[i], i) for i, kind in enumerate("qkv")]
        return copies + [self.load(f"x_{layer}", self.big.at[5], 3)]

    def weight_loads(self, layer, block):
        rows = pl.ds(pl.multiple_of(OUT_BLOCK * block, OUT_BLOCK), OUT_BLOCK)
        slot = lax.rem(block, 2)
        return [self.load(name, self.w.at[slot, i], 5 + 3 * slot + i, layer, rows) for i, name in enumerate(("wq", "wk", "wv"))]

    def input_block(self, layer, block):
        big, blocks = self.big, self.width // OUT_BLOCK
        slot = lax.rem(block, 2)

        @pl.when(block == 0)
        def _():
            for copy in self.input_loads(layer):
                copy.wait()
        for copy in self.weight_loads(layer, block):
            copy.wait()

        @pl.when(block + 1 < blocks)
        def _():
            for copy in self.weight_loads(layer, block + 1):
                copy.start()
        lanes = pl.ds(pl.multiple_of(OUT_BLOCK * block, OUT_BLOCK), OUT_BLOCK)

        def product(rows):
            total = dot(big[0, rows], self.w[slot, 0], 1, 1) + dot(big[1, rows], self.w[slot, 1], 1, 1)
            big[3, rows, lanes] = (total + dot(big[2, rows], self.w[slot, 2], 1, 1)).astype(jnp.bfloat16)
        self.row_blocks(product)

        @pl.when(block == blocks - 1)
        def _():
            def close(rows):
                back = rms_backward(big[5, rows].astype(jnp.float32), big[3, rows].astype(jnp.float32))
                big[3, rows] = (big[4, rows].astype(jnp.float32) + back).astype(jnp.bfloat16)
                if layer:
                    self.total[rows] = jnp.zeros((self.ROWS, self.width), jnp.float32)
            self.row_blocks(close)
            self.store(big.at[3], f"dx_{layer}", 0).start()
            if layer:
                self.load("h_0", big.at[4], 3).start()
                for copy in self.mlp_loads(0):
                    copy.start()

    def mlp_loads(self, block):
        slot = lax.rem(block, 2)
        lanes = pl.ds(pl.multiple_of(FF_BLOCK * block, FF_BLOCK), FF_BLOCK)
        half = pl.ds(pl.multiple_of(FF_BLOCK * slot, FF_BLOCK), FF_BLOCK)
        return [self.load("w_up", self.big.at[0, :, half], 5 + 3 * slot, slice(None), lanes),
                self.load("pre_0", self.big.at[1, :, half], 6 + 3 * slot, slice(None), lanes),
                self.load("w_down", self.big.at[5, half], 7 + 3 * slot, lanes)]

    def mlp_store(self, block):
        half = pl.ds(pl.multiple_of(FF_BLOCK * lax.rem(block, 2), FF_BLOCK), FF_BLOCK)
        lanes = pl.ds(pl.multiple_of(FF_BLOCK * block, FF_BLOCK), FF_BLOCK)
        return self.store(self.big.at[2, :, half], "dpre_0", 1, slice(None), lanes)

    def mlp_block(self, block):
        big, blocks = self.big, self.at["w_up"].shape[1] // FF_BLOCK

        @pl.when(block == 0)
        def _():
            self.store(big.at[3], "dx_1", 0).wait()
            self.load("h_0", big.at[4], 3).wait()
        for copy in self.mlp_loads(block):
            copy.wait()

        @pl.when(block + 1 < blocks)
        def _():
            for copy in self.mlp_loads(block + 1):
                copy.start()

        @pl.when(block > 0)
        def _():
            self.mlp_store(block - 1).wait()
        half = pl.ds(pl.multiple_of(FF_BLOCK * lax.rem(block, 2), FF_BLOCK), FF_BLOCK)

        def product(rows):
            d_act = dot(big[3, rows], big[5, half], 1, 1).astype(jnp.bfloat16).astype(jnp.float32)
            slope = gelu_parts(big[1, rows, half].astype(jnp.float32))[1]
            d_pre = (d_act * slope).astype(jnp.bfloat16)
            big[2, rows, half] = d_pre
            self.total[rows] += dot(d_pre, big[0, :, half], 1, 1)
        self.row_blocks(product)
        self.mlp_store(block).start()

        @pl.when(block == blocks - 1)
        def _():
            def close(rows):
                d_normed = self.total[rows].astype(jnp.bfloat16).astype(jnp.float32)
                back = rms_backward(big[4, rows].astype(jnp.float32), d_normed)
                big[4, rows] = (big[3, rows].astype(jnp.float32) + back).astype(jnp.bfloat16)
            self.row_blocks(close)
            self.store(big.at[4], "dh_0", 2).start()
            self.load("wo", big.at[0], 4, 0).start()
            for copy in self.piece_loads(0, 0):
                copy.start()

    def where(self, piece):
        seq, half = lax.rem(piece, self.seqs), lax.div(piece, self.seqs)
        rows = pl.ds(pl.multiple_of(self.seq * seq, self.seq), self.seq)
        lanes = pl.ds(pl.multiple_of(self.width // 2 * half, self.width // 2), self.width // 2)
        return seq, half, rows, lanes

    def piece_loads(self, layer, piece):
        seq, half, rows, lanes = self.where(piece)
        near = pl.ds(0, self.width // 2)
        copies = [self.load(f"{kind}_{layer}", self.big.at[1 + lax.rem(piece, 2), pl.ds(self.seq * i, self.seq), near], i, rows, lanes)
                  for i, kind in enumerate("qkv")]
        heads = pl.ds(self.heads // 2 * half, self.heads // 2)
        return copies + [self.load(f"probs_{layer}", self.p.at[lax.rem(piece, 2)], 5, seq, heads)]

    def piece_stores(self, layer, piece):
        _, _, rows, lanes = self.where(piece)
        near, spot = pl.ds(0, self.width // 2), 5 - 2 * lax.rem(piece, 2)
        return [self.store(self.big.at[spot, pl.ds(self.seq * i, self.seq), near], f"d{kind}_{layer}", 3 + i, rows, lanes)
                for i, kind in enumerate("qkv")]

    def attention_piece(self, layer, piece):
        big, p_buf, pieces = self.big, self.p, 2 * self.seqs
        _, half, rows, _ = self.where(piece)
        parity = lax.rem(piece, 2)
        spot, out = 1 + parity, 5 - 2 * parity

        @pl.when(piece == 0)
        def _():
            if layer == 0:
                self.mlp_store(self.at["w_up"].shape[1] // FF_BLOCK - 1).wait()
                self.store(big.at[4], "dh_0", 2).wait()
            else:
                self.load("dh_1", big.at[4], 3).wait()
            self.load("wo", big.at[0], 4, layer).wait()
        waiting = piece > 0
        if layer == 1:
            waiting = jnp.logical_and(waiting, piece != self.seqs)

        @pl.when(waiting)
        def _():
            for copy in self.piece_stores(layer, piece - 1):
                copy.wait()
        for copy in self.piece_loads(layer, piece):
            copy.wait()

        @pl.when(piece + 1 < pieces)
        def _():
            for copy in self.piece_loads(layer, piece + 1):
                copy.start()
        low = lax.broadcasted_iota(jnp.int32, (self.seq, PAIR), 1) < HEAD_DIM

        def unmix(unit):
            w_rows = pl.ds(pl.multiple_of(self.width // 2 * half + OUT_BLOCK * unit, OUT_BLOCK), OUT_BLOCK)
            d_mixed = dot(big[4, rows], big[0, w_rows], 1, 1)
            big[spot, pl.ds(3 * self.seq, self.seq), pl.ds(OUT_BLOCK * unit, OUT_BLOCK)] = d_mixed.astype(jnp.bfloat16)

        def pair_of(j):
            return tuple(big[spot, pl.ds(self.seq * i, self.seq), pl.ds(PAIR * j, PAIR)] for i in range(4))

        def put(j, values):
            for i, value in enumerate(values):
                big[out, pl.ds(self.seq * i, self.seq), pl.ds(PAIR * j, PAIR)] = value.astype(jnp.bfloat16)
        size = OUT_BLOCK // PAIR
        stages = backward_stages(pair_of, lambda j, side: p_buf[parity, 2 * j + side], put, low)
        staged(self.heads // 4 // size, in_units(unmix, stages, size))
        for copy in self.piece_stores(layer, piece):
            copy.start()

    def begin(self):
        self.load("dh_1", self.big.at[4], 3).start()
        self.load("wo", self.big.at[0], 4, 1).start()
        for copy in self.piece_loads(1, 0):
            copy.start()

    def before_load(self, step):
        @pl.when(step == 1)
        def _():
            for copy in self.piece_stores(1, self.seqs - 1):
                copy.wait()

    def item(self, step):
        blocks = self.width // OUT_BLOCK
        pieces = 2 * self.seqs

        @pl.when(step < 3)
        def _():
            first = jnp.where(step == 0, 0, self.seqs + self.seqs // 2 * (step - 1))
            count = jnp.where(step == 0, self.seqs, self.seqs // 2)
            lax.fori_loop(first, first + count, lambda piece, carry: self.attention_piece(1, piece) or carry, 0)

        @pl.when(step == 3)
        def _():
            for copy in self.piece_stores(1, pieces - 1):
                copy.wait()
            for copy in self.input_loads(1) + self.weight_loads(1, 0):
                copy.start()

        @pl.when(between(step, self.PB_1, 2))
        def _():
            first = blocks // 2 * (step - self.PB_1)
            lax.fori_loop(first, first + blocks // 2, lambda block, carry: self.input_block(1, block) or carry, 0)
        pl.when(between(step, self.MB, 8))(lambda: self.mlp_block(step - self.MB))
        pl.when(between(step, self.AB, pieces))(lambda: self.attention_piece(0, step - self.AB))

        @pl.when(step == self.PB_0 - 1)
        def _():
            for copy in self.piece_stores(0, pieces - 1):
                copy.wait()
            for copy in self.input_loads(0) + self.weight_loads(0, 0):
                copy.start()
        pl.when(between(step, self.PB_0, blocks))(lambda: self.input_block(0, step - self.PB_0))

        @pl.when(step == self.PB_0 + blocks)
        def _():
            self.store(self.big.at[3], "dx_0", 0).wait()


def finish_kernel(groups, chunks, in_names, out_names, remote, *refs):
    names = [*in_names, *out_names]
    at, scratch = dict(zip(names, refs[:len(names)])), refs[len(names):]
    (big, total_buf, w_buf, p_buf, item_sem, drain_sem), scratch = scratch[:6], scratch[6:]
    backward = Backward(at, big, total_buf, w_buf, p_buf, item_sem, drain_sem)
    if not remote:
        backward.begin()

        def alone(step, carry):
            backward.before_load(step)
            backward.item(step)
            return carry
        lax.fori_loop(0, chunks + WRITE_AT + 1, alone, 0)
        return
    (lhs_buf, rhs_buf, own, part, part_in, gath), scratch = scratch[:6], scratch[6:]
    land_keys = [key for key, st in enumerate(STAGES) if st[1].startswith("rs")]
    landing = dict(zip(land_keys, scratch[:len(land_keys)]))
    load_sem, send_sem, recv_sem, pair_send, pair_recv, out_sem, out_send, out_recv, credit = scratch[len(land_keys):]

    me = lax.axis_index("data")
    core = lax.rem(me, 2)
    coord = {"x": lax.rem(lax.div(me, 2), 2), "y": lax.rem(lax.div(me, 4), 2)}
    z = lax.div(me, 8)
    partner = me + 1 - 2 * core
    near = {"x": me + 2 - 4 * coord["x"], "y": me + 4 - 8 * coord["y"]}
    up_ok, down_ok = z < 3, z > 0
    peers = [(partner, 0, None), (near["x"], 1, None), (near["y"], 2, None), (me + 8, 3, up_ok), (me - 8, 4, down_ok)]

    def guarded(cond, fn):
        if cond is None:
            fn()
        else:
            pl.when(cond)(fn)

    barrier = pltpu.get_barrier_semaphore()
    for dev, _, cond in peers:
        guarded(cond, lambda dev=dev: pl.semaphore_signal(barrier, inc=1, device_id=(dev,), device_id_type=MESH))
    inner = jnp.logical_and(up_ok, down_ok)
    guarded(inner, lambda: pl.semaphore_wait(barrier, 5))
    guarded(jnp.logical_not(inner), lambda: pl.semaphore_wait(barrier, 4))

    def region(name, kind, which):
        _, row, rows, order = TYPES[name]
        if order[2] == "z":
            h1, h2 = coord[order[0]], coord[order[1]]
            if kind == "1":
                return pl.ds(row, rows), pl.ds(pl.multiple_of(512 * which, 128), 512)
            if kind == "2":
                return pl.ds(row, rows), pl.ds(pl.multiple_of(512 * h1 + 256 * which, 128), 256)
            first = pl.multiple_of(row + (rows // 2) * lax.div(which, 2), 8)
            lane = pl.multiple_of(512 * h1 + 256 * h2 + 128 * lax.rem(which, 2), 128)
            return pl.ds(first, rows // 2), pl.ds(lane, 128)
        h1 = coord[order[1]]
        if kind == "z":
            first = pl.multiple_of(row + (rows // 2) * lax.div(which, 2), 8)
            return pl.ds(first, rows // 2), pl.ds(pl.multiple_of(512 * lax.rem(which, 2), 128), 512)
        first = pl.multiple_of(row + (rows // 2) * lax.div(z, 2), 8)
        if kind == "1":
            return pl.ds(first, rows // 2), pl.ds(pl.multiple_of(512 * lax.rem(z, 2) + 256 * which, 128), 256)
        lane = pl.multiple_of(512 * lax.rem(z, 2) + 256 * h1 + 128 * which, 128)
        return pl.ds(first, rows // 2), pl.ds(lane, 128)

    def exchange_axis(name, kind):
        order = TYPES[name][3]
        dims = order[:2] if order[2] == "z" else order[1:]
        return dims[int(kind) - 1]

    def plan(key, chunk, parity):
        name, kind, step, way, _ = STAGES[key]
        mine, slot = lax.rem(chunk, OWN_SLOTS), lax.rem(chunk, AG_SLOTS)
        if kind in ("rs1", "rs2"):
            axis = exchange_axis(name, kind[2])
            src, keep = region(name, kind[2], 1 - coord[axis]), region(name, kind[2], coord[axis])
            dev, send_ok, recv_ok = near[axis], None, None
            sent = own.at[mine, src[0], src[1]]
        elif kind in ("ag1", "ag2"):
            axis = exchange_axis(name, kind[2])
            src = keep = region(name, kind[2], coord[axis])
            dev, send_ok, recv_ok = near[axis], None, None
            sent = gath.at[slot, src[0], src[1]]
        elif kind == "rsz":
            if way:
                dev, k_send, k_keep = me + 8, z + 3 - step, z + 2 - step
                send_ok, recv_ok = k_send <= 3, jnp.logical_and(k_keep <= 3, down_ok)
            else:
                dev, k_send, k_keep = me - 8, z - 3 + step, z - 2 + step
                send_ok, recv_ok = k_send >= 0, jnp.logical_and(k_keep >= 0, up_ok)
            src, keep = region(name, "z", k_send), region(name, "z", k_keep)
            sent = own.at[mine, src[0], src[1]]
        else:
            if way:
                dev, k_send, k_keep = me + 8, z - step, z - 1 - step
                send_ok, recv_ok = jnp.logical_and(k_send >= 0, up_ok), k_keep >= 0
            else:
                dev, k_send, k_keep = me - 8, z + step, z + 1 + step
                send_ok, recv_ok = jnp.logical_and(k_send <= 3, down_ok), k_keep <= 3
            src, keep = region(name, "z", k_send), region(name, "z", k_keep)
            sent = gath.at[slot, src[0], src[1]]
        sems = dict(send_sem=send_sem.at[key], recv_sem=recv_sem.at[key, parity], device_id=(dev,), device_id_type=MESH)
        if kind.startswith("rs"):
            target = landing[key].at[parity]
            send = lambda: pltpu.make_async_remote_copy(src_ref=sent, dst_ref=target, **sems)
            recv = lambda: pltpu.make_async_remote_copy(
                src_ref=own.at[mine, keep[0], keep[1]], dst_ref=target, **sems)

            def arrive():
                own[mine, keep[0], keep[1]] += landing[key][parity]
        else:
            send = lambda: pltpu.make_async_remote_copy(src_ref=sent, dst_ref=sent, **sems)
            recv = lambda: pltpu.make_async_remote_copy(
                src_ref=gath.at[slot, keep[0], keep[1]], dst_ref=gath.at[slot, keep[0], keep[1]], **sems)
            arrive = None
        return send, recv, send_ok, recv_ok, arrive

    def finish(name, chunk):
        order = TYPES[name][3]
        reg = region(name, "z", z) if order[2] == "z" else region(name, "2", coord[order[2]])
        gath[lax.rem(chunk, AG_SLOTS), reg[0], reg[1]] = own[lax.rem(chunk, OWN_SLOTS), reg[0], reg[1]]

    def valid(chunk):
        return jnp.logical_and(chunk >= 0, chunk < chunks)

    def set_rows(half):
        return pl.ds(half * SET_ROWS, SET_ROWS)

    def pair_copy(half, parity):
        return pltpu.make_async_remote_copy(
            src_ref=part.at[parity, set_rows(half)], dst_ref=part_in.at[parity, set_rows(half)],
            send_sem=pair_send.at[half], recv_sem=pair_recv.at[half, parity], device_id=(partner,), device_id_type=MESH)

    half_lanes = LANES // 2

    def outlets(half, group, local, whose):
        out, layer = group["out"]
        ref = at[out] if layer is None else at[out].at[layer]
        rows, cols = group["place"](local)
        if not group["narrow"]:
            first = pl.multiple_of(rows + CORE_ROWS * whose + half * SET_ROWS, SET_ROWS)
            return [(pl.ds(0, LANES), ref.at[pl.ds(first, SET_ROWS), pl.ds(pl.multiple_of(cols, 128), LANES)])]
        places = []
        for sub in (0, 1):
            first = pl.multiple_of(2 * CORE_ROWS * whose + CORE_ROWS * sub + half * SET_ROWS, SET_ROWS)
            places.append((pl.ds(half_lanes * sub, half_lanes), ref.at[pl.ds(first, SET_ROWS), pl.ds(cols, half_lanes)]))
        return places

    def write_copies(half, chunk, lanes, dest):
        slot = lax.rem(chunk, AG_SLOTS)
        src = gath.at[slot, set_rows(half), lanes]
        here = pltpu.make_async_copy(src, dest, out_sem.at[half])
        there = pltpu.make_async_remote_copy(
            src_ref=src, dst_ref=dest, send_sem=out_send.at[half], recv_sem=out_recv.at[half, lax.rem(chunk, 2)],
            device_id=(partner,), device_id_type=MESH)
        return here, there

    def load_copies(group, local, slot):
        rows, cols = group["place"](local)
        narrow = group["narrow"]
        lhs, rhs = [], []
        for sub in range(2 if narrow else len(group["lhs"])):
            for whose in (0, 1):
                owner = core if whose == 0 else 1 - core
                first = 2 * CORE_ROWS * owner + CORE_ROWS * sub if narrow else rows + CORE_ROWS * owner
                source = at[group["lhs"][0 if narrow else sub]]
                lhs.append(pltpu.make_async_copy(
                    source.at[:, pl.ds(pl.multiple_of(first, CORE_ROWS), CORE_ROWS)],
                    lhs_buf.at[slot, sub, whose], load_sem.at[slot, sub, whose]))
        for app, name in enumerate(group["rhs"]):
            size = half_lanes if narrow else LANES
            rhs.append(pltpu.make_async_copy(
                at[name].at[:, pl.ds(pl.multiple_of(cols, 128), size)], rhs_buf.at[slot, app, :, pl.ds(0, size)],
                load_sem.at[slot, app, 2]))
        return lhs, rhs

    def for_group(chunk, fn):
        for group in groups:
            inside = jnp.logical_and(chunk >= group["start"], chunk < group["start"] + group["count"])
            pl.when(inside)(functools.partial(fn, group, chunk - group["start"]))

    def among(chunk, chosen):
        flags = [jnp.logical_and(chunk >= g["start"], chunk < g["start"] + g["count"]) for g in groups if chosen(g)]
        return functools.reduce(jnp.logical_or, flags)

    def is_two(group):
        return len(group["lhs"]) == 2

    def is_narrow(group):
        return group["narrow"]

    def start_load(chunk):
        def go(group, local):
            for copy in sum(load_copies(group, local, lax.rem(chunk, 2)), []):
                copy.start()
        for_group(chunk, go)

    def wait_load(chunk):
        slot = lax.rem(chunk, 2)
        two_lhs, two_rhs = load_copies(next(filter(is_two, groups)), 0, slot)
        slim_lhs, slim_rhs = load_copies(next(filter(is_narrow, groups)), 0, slot)
        for copy in two_lhs[:2]:
            copy.wait()

        @pl.when(jnp.logical_not(among(chunk, is_narrow)))
        def _():
            two_rhs[0].wait()

        @pl.when(among(chunk, is_narrow))
        def _():
            for copy in slim_rhs + slim_lhs[2:]:
                copy.wait()

        @pl.when(among(chunk, is_two))
        def _():
            for copy in two_lhs[2:] + two_rhs[1:]:
                copy.wait()

    def tile(chunk):
        slot, mine, parity = lax.rem(chunk, 2), lax.rem(chunk, OWN_SLOTS), lax.rem(chunk, 2)

        def product(sub, whose, rhs):
            return dot(lhs_buf[slot, sub, whose], rhs, 0, 0)

        @pl.when(among(chunk, is_narrow))
        def _():
            for sub in (0, 1):
                lanes, rhs = pl.ds(half_lanes * sub, half_lanes), rhs_buf[slot, 0, :, pl.ds(0, half_lanes)]
                own[mine, :, lanes] = product(sub, 0, rhs)
                part[parity, :, lanes] = product(sub, 1, rhs)

        @pl.when(jnp.logical_not(among(chunk, is_narrow)))
        def _():
            own[mine] = product(0, 0, rhs_buf[slot, 0])
            part[parity] = product(0, 1, rhs_buf[slot, 0])

        @pl.when(among(chunk, is_two))
        def _():
            own[mine] += product(1, 0, rhs_buf[slot, 1])
            part[parity] += product(1, 1, rhs_buf[slot, 1])

    last = chunks + WRITE_AT

    def section(half, step):
        before = lax.rem(step + 1, 2)
        now = lax.rem(step, 2)

        @pl.when(valid(step - 1))
        def _():
            copy = pair_copy(half, before)
            copy.wait_send()
            copy.wait_recv()
            mine = lax.rem(step - 1, OWN_SLOTS)
            own[mine, set_rows(half)] += part_in[before, set_rows(half)]

        names = [name for name in TYPES if TYPES[name][0] == half]
        keys = [key for key, st in enumerate(STAGES) if st[0] in names]
        finals = {name: max(st[4] for st in STAGES if st[0] == name and st[1].startswith("rs")) for name in names}
        for key in keys:
            name, at = STAGES[key][0], STAGES[key][4]
            chunk = step - 1 - at

            @pl.when(valid(chunk))
            def _(key=key, chunk=chunk):
                send, recv, send_ok, recv_ok, arrive = plan(key, chunk, before)

                def arrived():
                    recv().wait_recv()
                    if arrive is not None:
                        arrive()
                guarded(recv_ok, arrived)
                guarded(send_ok, lambda: send().wait_send())
        for name in names:
            chunk = step - 1 - finals[name]
            pl.when(valid(chunk))(functools.partial(finish, name, chunk))

        done = step - 1 - WRITE_AT

        @pl.when(valid(done))
        def _():
            (lanes, dest), = outlets(half, groups[0], 0, 0)
            here, there = write_copies(half, done, lanes, dest)
            here.wait()
            there.wait_send()
            there.wait_recv()

        @pl.when(step < last)
        def _():
            for dev, way, cond in peers:
                to = way if way < 3 else 7 - way
                guarded(cond, lambda dev=dev, to=to: pl.semaphore_signal(
                    credit.at[half, to], inc=1, device_id=(dev,), device_id_type=MESH))

        @pl.when(step > 0)
        def _():
            for dev, way, cond in peers:
                guarded(cond, lambda way=way: pl.semaphore_wait(credit.at[half, way], 1))

        for key in reversed(keys):
            chunk = step - STAGES[key][4]

            @pl.when(valid(chunk))
            def _(key=key, chunk=chunk):
                send, recv, send_ok, recv_ok, arrive = plan(key, chunk, now)
                guarded(send_ok, lambda: send().start())

        out_chunk = step - WRITE_AT

        @pl.when(valid(out_chunk))
        def _():
            def go(group, local):
                for lanes, dest in outlets(half, group, local, core):
                    for copy in write_copies(half, out_chunk, lanes, dest):
                        copy.start()
            for_group(out_chunk, go)

    backward.begin()
    start_load(jnp.int32(0))

    def round_(step, carry):
        section(0, step)

        @pl.when(valid(step))
        def _():
            backward.before_load(step)
            pl.when(step + 1 < chunks)(lambda: start_load(step + 1))
            wait_load(step)
            tile(step)
            pair_copy(0, lax.rem(step, 2)).start()

        section(1, step)

        @pl.when(valid(step))
        def _():
            pair_copy(1, lax.rem(step, 2)).start()

        backward.item(step)
        return carry

    lax.fori_loop(0, last + 1, round_, 0)


def finish_backward(inputs, groups, chunks, weights, tokens, seq, collective_id=0, remote=True):
    width, ff = inputs["w_up"].shape
    landing = [pltpu.VMEM((2,) + piece_shape(st[0], st[1]), jnp.float32) for st in STAGES if st[1].startswith("rs")]
    apps = 2
    outs = {name: jax.ShapeDtypeStruct(shape, jnp.float32) for name, shape in weights.items()}
    for name in ("dx_0", "dx_1", "dh_0", "dq_0", "dk_0", "dv_0", "dq_1", "dk_1", "dv_1"):
        outs[name] = bf16(tokens, width)
    outs["dpre_0"] = bf16(tokens, ff)
    heads = width // HEAD_DIM
    scratch = [
        pltpu.VMEM((6, tokens, width), jnp.bfloat16),
        pltpu.VMEM((tokens, width), jnp.float32),
        pltpu.VMEM((2, 3, OUT_BLOCK, width), jnp.bfloat16),
        pltpu.VMEM((2, heads // 2, seq, seq), jnp.bfloat16),
        pltpu.SemaphoreType.DMA((11,)),
        pltpu.SemaphoreType.DMA((6,)),
    ]
    if remote:
        scratch += [
            pltpu.VMEM((2, apps, 2, tokens, CORE_ROWS), jnp.bfloat16),
            pltpu.VMEM((2, apps, tokens, LANES), jnp.bfloat16),
            pltpu.VMEM((OWN_SLOTS, CORE_ROWS, LANES), jnp.float32),
            pltpu.VMEM((2, CORE_ROWS, LANES), jnp.float32),
            pltpu.VMEM((2, CORE_ROWS, LANES), jnp.float32),
            pltpu.VMEM((AG_SLOTS, CORE_ROWS, LANES), jnp.float32),
            *landing,
            pltpu.SemaphoreType.DMA((2, apps, 3)),
            pltpu.SemaphoreType.DMA((len(STAGES),)),
            pltpu.SemaphoreType.DMA((len(STAGES), 2)),
            pltpu.SemaphoreType.DMA((2,)),
            pltpu.SemaphoreType.DMA((2, 2)),
            pltpu.SemaphoreType.DMA((2,)),
            pltpu.SemaphoreType.DMA((2,)),
            pltpu.SemaphoreType.DMA((2, 2)),
            pltpu.SemaphoreType.REGULAR((2, 5)),
        ]
    params = dict(collective_id=collective_id, has_side_effects=True) if remote else {}
    results = pl.pallas_call(
        functools.partial(finish_kernel, groups, chunks, list(inputs), list(outs), remote),
        out_shape=list(outs.values()),
        in_specs=[pl.BlockSpec(memory_space=pl.ANY)] * len(inputs),
        out_specs=[pl.BlockSpec(memory_space=pl.ANY)] * len(outs),
        scratch_shapes=scratch,
        compiler_params=pltpu.CompilerParams(vmem_limit_bytes=67_043_328, **params),
        cost_estimate=pl.CostEstimate(flops=20 * tokens * width * ff, bytes_accessed=256 * MIB, transcendentals=0),
        name="finish_backward",
    )(*inputs.values())
    return dict(zip(outs, results))


DELIVER_ROWS = 512
DELIVER_SLOTS = 16
DELIVER_AHEAD = 8


def deliver(arrays, small):
    def blocks_of(array):
        lead = [(i,) for i in range(array.shape[0])] if len(array.shape) == 3 else [()]
        rows, cols = array.shape[-2:]
        return [(*index, pl.ds(row, DELIVER_ROWS), pl.ds(col, LANES))
                for index in lead for row in range(0, rows, DELIVER_ROWS) for col in range(0, cols, LANES)]

    work = [(i, index) for i, array in enumerate(arrays) for index in blocks_of(array)]
    count = len(arrays) + 1

    def kernel(*refs):
        ins, outs, buf, whole_buf, in_sem, out_sem, whole_sem = refs[:count], refs[count:2 * count], *refs[2 * count:]
        whole_in = pltpu.make_async_copy(ins[-1], whole_buf, whole_sem.at[0])
        whole_out = pltpu.make_async_copy(whole_buf, outs[-1], whole_sem.at[1])

        def fetch(t):
            i, index = work[t]
            return pltpu.make_async_copy(ins[i].at[index], buf.at[t % DELIVER_SLOTS], in_sem.at[t % DELIVER_SLOTS])

        def put(t):
            i, index = work[t]
            return pltpu.make_async_copy(buf.at[t % DELIVER_SLOTS], outs[i].at[index], out_sem.at[t % DELIVER_SLOTS])

        whole_in.start()
        for t in range(min(DELIVER_AHEAD, len(work))):
            fetch(t).start()
        whole_in.wait()
        whole_out.start()
        for t in range(len(work)):
            if t + DELIVER_AHEAD < len(work):
                if t + DELIVER_AHEAD >= DELIVER_SLOTS:
                    put(t + DELIVER_AHEAD - DELIVER_SLOTS).wait()
                fetch(t + DELIVER_AHEAD).start()
            fetch(t).wait()
            put(t).start()
        for t in range(max(0, len(work) - DELIVER_SLOTS), len(work)):
            put(t).wait()
        whole_out.wait()

    return pl.pallas_call(
        kernel,
        out_shape=[jax.ShapeDtypeStruct(array.shape, array.dtype) for array in (*arrays, small)],
        in_specs=[pl.BlockSpec(memory_space=pl.ANY)] * count,
        out_specs=[pl.BlockSpec(memory_space=pl.ANY)] * count,
        scratch_shapes=[pltpu.VMEM((DELIVER_SLOTS, DELIVER_ROWS, LANES), jnp.float32), pltpu.VMEM(small.shape, small.dtype),
                        pltpu.SemaphoreType.DMA((DELIVER_SLOTS,)), pltpu.SemaphoreType.DMA((DELIVER_SLOTS,)),
                        pltpu.SemaphoreType.DMA((2,))],
        compiler_params=pltpu.CompilerParams(vmem_limit_bytes=67_043_328),
        cost_estimate=pl.CostEstimate(flops=0, bytes_accessed=2 * sum(a.size for a in arrays) * 4, transcendentals=0),
        name="deliver",
    )(*arrays, small)


def gradient_groups(width, ff):
    groups = []

    def add(count, lhs, rhs, out, place, narrow=False):
        start = groups[-1]["start"] + groups[-1]["count"] if groups else 0
        groups.append(dict(start=start, count=count, lhs=lhs, rhs=rhs, out=out, place=place, narrow=narrow))

    def tall(local):
        return TILE_ROWS * local, 0

    def wide(local):
        return TILE_ROWS * lax.rem(local, width // TILE_ROWS), LANES * lax.div(local, width // TILE_ROWS)

    add(width // TILE_ROWS, ["mixed_1"], ["dh_1"], ("g_o", 1), tall)
    for half in (0, 1):
        for kind in "qkv":
            add(1, ["u_1"], [f"d{kind}_1"], (f"g_{kind}", 1), lambda local, half=half: (0, width // 2 * half), narrow=True)
    add(ff // TILE_ROWS, ["act_0", "act_1"], ["dx_1", "cot"], ("g_down", None), tall)
    add(ff // TILE_ROWS, ["n_0", "n_1"], ["dpre_0", "dpre_1"], ("g_up", None), wide)
    for kind in "qkv":
        add(width // TILE_ROWS, ["u_0"], [f"d{kind}_0"], (f"g_{kind}", 0), tall)
    add(width // TILE_ROWS, ["mixed_0"], ["dh_0"], ("g_o", 0), tall)
    return groups, sum(group["count"] for group in groups)


def local_operands(x_init, cot_out, w_query, w_key, w_value, w_proj, w_up, w_down):
    batch, seq, width = x_init.shape
    tokens = batch * seq
    at = {"x_0": x_init.reshape(tokens, width), "cot": cot_out.reshape(tokens, width)}
    at.update(wq=w_query, wk=w_key, wv=w_value, wo=w_proj, w_up=w_up, w_down=w_down)
    at.update(front(at, batch, seq))
    return at


def solution(mesh):
    def local_step(x_init, cot_out, w_query, w_key, w_value, w_proj, w_up, w_down):
        batch, seq, width = x_init.shape
        inputs = local_operands(x_init, cot_out, w_query, w_key, w_value, w_proj, w_up, w_down)
        groups, chunks = gradient_groups(width, w_up.shape[1])
        weights = dict(g_q=w_query.shape, g_k=w_key.shape, g_v=w_value.shape, g_o=w_proj.shape, g_up=w_up.shape, g_down=w_down.shape)
        res = finish_backward(inputs, groups, chunks, weights, batch * seq, seq)
        *grads, d_init = deliver([res[name] for name in weights], res["dx_0"])
        return (*grads, d_init.reshape(x_init.shape))

    data_spec = P("data")
    full_spec = P()
    in_specs = (data_spec, data_spec, full_spec, full_spec, full_spec, full_spec, full_spec, full_spec)
    out_specs = (full_spec, full_spec, full_spec, full_spec, full_spec, full_spec, data_spec)
    return jax.shard_map(local_step, mesh=mesh, in_specs=in_specs, out_specs=out_specs, check_vma=False)
```

```python
import functools

import jax
import jax.numpy as jnp
from jax import lax
from jax.experimental import pallas as pl
from jax.experimental.pallas import tpu as pltpu
from jax.sharding import PartitionSpec as P

EPS = 1e-6
HEAD_DIM = 64
PAIR = 2 * HEAD_DIM
FF_BLOCK = 512
OUT_BLOCK = 256
GELU_A = (2.0 / 3.141592653589793) ** 0.5
GELU_B = 0.044715
SOFTMAX_SCALE = HEAD_DIM ** -0.5 * 1.4426950408889634
MIB = 1024 * 1024


def dot(lhs, rhs, lhs_dim, rhs_dim):
    return lax.dot_general(lhs, rhs, (((lhs_dim,), (rhs_dim,)), ((), ())), preferred_element_type=jnp.float32)


def rms_norm(x_f32):
    return x_f32 * lax.rsqrt(jnp.mean(x_f32 * x_f32, axis=-1, keepdims=True) + EPS)


def rms_backward(x_f32, d_out):
    scale = lax.rsqrt(jnp.mean(x_f32 * x_f32, axis=-1, keepdims=True) + EPS)
    inner = jnp.mean(x_f32 * d_out, axis=-1, keepdims=True)
    return scale * d_out - x_f32 * (scale * scale * scale * inner)


def gelu_parts(pre):
    square = pre * pre
    tanh = jnp.tanh(GELU_A * (pre + GELU_B * pre * square))
    half = 0.5 * (1.0 + tanh)
    slope = half + 0.5 * pre * (1.0 - tanh * tanh) * (GELU_A + (3.0 * GELU_A * GELU_B) * square)
    return pre * half, slope


def bf16(*shape):
    return jax.ShapeDtypeStruct(shape, jnp.bfloat16)


def backward_stages(pair_of, probs_of, put, low):
    masks = (low, jnp.logical_not(low))

    def from_mixed(j, _=None):
        _, _, v_pair, d_pair = pair_of(j)
        return [dot(v_pair, jnp.where(mask, d_pair, 0), 1, 1).astype(jnp.bfloat16) for mask in masks]

    def through(j, made):
        out = []
        for side, d_probs in enumerate(made):
            d_probs, probs = d_probs.astype(jnp.float32), probs_of(j, side).astype(jnp.float32)
            row_dot = jnp.sum(d_probs * probs, axis=0, keepdims=True)
            out.append((probs * (d_probs - row_dot) * HEAD_DIM ** -0.5).astype(jnp.bfloat16))
        return out

    def to_inputs(j, made):
        q_pair, k_pair, _, d_pair = pair_of(j)
        sides = [(dot(d_scores, k_pair, 0, 0), dot(d_scores, q_pair, 1, 0), dot(probs_of(j, side), d_pair, 1, 0))
                 for side, d_scores in enumerate(made)]
        put(j, [jnp.where(low, first, second) for first, second in zip(*sides)])
    return from_mixed, through, to_inputs


def forward_stages(pair_of, keep, put, low):
    def scores(j, _=None):
        q_pair, k_pair, _ = pair_of(j)
        return [dot(k_pair, jnp.where(mask, q_pair, 0), 1, 1) for mask in (low, jnp.logical_not(low))]

    def soften(j, made):
        out = []
        for side, score in enumerate(made):
            top = jnp.max(score, axis=0, keepdims=True)
            raised = jnp.exp2((score - top) * SOFTMAX_SCALE)
            inverse = 1.0 / jnp.sum(raised, axis=0, keepdims=True)
            out.append((raised * inverse).astype(jnp.bfloat16))
            keep(j, side, out[-1])
        return out

    def mix(j, made):
        first, second = (dot(probs, pair_of(j)[2], 0, 0) for probs in made)
        put(j, jnp.where(low, first, second))
    return scores, soften, mix


def in_units(first, stages, size):
    def lift(stage):
        return lambda unit, made: [stage(size * unit + i, made[i]) for i in range(size)]
    return (lambda unit: first(unit) or [None] * size, *map(lift, stages))


def staged(count, stages):
    made = [None] * count
    for turn in range(count + len(stages) - 1):
        for depth, stage in enumerate(stages):
            j = turn - depth
            if 0 <= j < count:
                made[j] = stage(j, made[j]) if depth else stage(j)


FRONT_OUTS = ("u_0", "q_0", "k_0", "v_0", "probs_0", "mixed_0", "h_0", "n_0", "pre_0", "act_0", "x_1",
              "u_1", "q_1", "k_1", "v_1", "probs_1", "mixed_1", "n_1", "act_1", "dpre_1", "dh_1", "dqa_1", "dka_1", "dva_1")
ROW_BUFFERS = ("u", "q", "k", "v", "mixed", "h", "n", "x", "dh", "dn")
HALF_BUFFERS = ("dqa", "dka", "dva")
WIDE_BLOCK = 1024


def front_kernel(batch, seq, in_names, *refs):
    at = dict(zip((*in_names, *FRONT_OUTS), refs))
    refs = refs[len(at):]
    x_all, cot_all, w_in, w_out, w_up, w_down, probs, pre, act = refs[:9]
    row = dict(zip((*ROW_BUFFERS, *HALF_BUFFERS), refs[9:]))
    load_sem, out_sem = refs[9 + len(row):]
    width, ff = w_up.shape
    heads = width // HEAD_DIM
    loads = {"x": pltpu.make_async_copy(at["x_0"], x_all, load_sem.at[0])}
    for layer in (0, 1):
        for i, name in enumerate(("wq", "wk", "wv")):
            loads[f"{name}_{layer}"] = pltpu.make_async_copy(at[name].at[layer], w_in.at[layer, i], load_sem.at[1 + 4 * layer + i])
        loads[f"wo_{layer}"] = pltpu.make_async_copy(at["wo"].at[layer], w_out.at[layer], load_sem.at[4 + 4 * layer])
    loads["w_up"] = pltpu.make_async_copy(at["w_up"], w_up, load_sem.at[9])
    loads["w_down"] = pltpu.make_async_copy(at["w_down"], w_down, load_sem.at[10])
    loads["cot"] = pltpu.make_async_copy(at["cot"], cot_all, load_sem.at[11])
    for name in ("x", "wq_0", "wk_0", "wv_0"):
        loads[name].start()
    holders = {"probs_0": probs, "probs_1": probs, "pre_0": pre, "act_0": act, "act_1": act, "dpre_1": pre, "x_1": row["x"]}
    for name in FRONT_OUTS:
        holders.setdefault(name, row.get(name[:-2]))

    def store(name, index):
        src = holders[name]
        rows = pl.ds(pl.multiple_of(seq * index, seq), seq)
        dest = at[name].at[index] if name.startswith("probs") else at[name].at[rows]
        return pltpu.make_async_copy(src, dest, out_sem.at[FRONT_OUTS.index(name)])

    def one_sequence(index, carry):
        rows = pl.ds(pl.multiple_of(seq * index, seq), seq)
        first = index == 0
        low = lax.broadcasted_iota(jnp.int32, (seq, PAIR), 1) < HEAD_DIM

        def need(*names):
            @pl.when(first)
            def _():
                for name in names:
                    loads[name].wait()

        def launch(*names):
            @pl.when(first)
            def _():
                for name in names:
                    loads[name].start()

        def free(*names, same=False):
            for name in names:
                if same:
                    store(name, index).wait()
                else:
                    pl.when(index > 0)(lambda name=name: store(name, index - 1).wait())

        def send(*names):
            for name in names:
                store(name, index).start()

        def over(count, fn):
            for j in range(count):
                fn(j)

        def wide(j):
            return pl.ds(WIDE_BLOCK * j, WIDE_BLOCK)

        def attention(layer):
            x_in = x_all[rows] if layer == 0 else row["x"][...]
            row["u"][...] = rms_norm(x_in.astype(jnp.float32)).astype(jnp.bfloat16)
            need(*(f"w{kind}_{layer}" for kind in "qkv"))
            if layer == 0:
                launch("wo_0", "w_up")

            def project(unit):
                lanes = pl.ds(OUT_BLOCK * unit, OUT_BLOCK)
                for i, kind in enumerate("qkv"):
                    row[kind][:, lanes] = dot(row["u"][...], w_in[layer, i, :, lanes], 1, 0).astype(jnp.bfloat16)

            def pair_of(j):
                return tuple(row[kind][:, PAIR * j:PAIR * (j + 1)] for kind in "qkv")

            def keep(j, side, value):
                probs[2 * j + side] = value

            def put(j, value):
                row["mixed"][:, PAIR * j:PAIR * (j + 1)] = value.astype(jnp.bfloat16)
            size = OUT_BLOCK // PAIR
            staged(heads // 2 // size, in_units(project, forward_stages(pair_of, keep, put, low), size))
            need(f"wo_{layer}")
            attn = dot(row["mixed"][...], w_out[layer], 1, 0).astype(jnp.bfloat16)
            hidden = (x_in.astype(jnp.float32) + attn.astype(jnp.float32)).astype(jnp.bfloat16)
            row["h"][...] = hidden
            row["n"][...] = rms_norm(hidden.astype(jnp.float32)).astype(jnp.bfloat16)

        need("x")
        free("u_1", "q_1", "k_1", "v_1", "probs_1", "mixed_1", "n_1", "dh_1")
        attention(0)
        send("u_0", "q_0", "k_0", "v_0", "probs_0", "mixed_0", "h_0", "n_0")
        need("w_up")
        launch("w_down", "wq_1", "wk_1", "wv_1", "wo_1", "cot")
        free("act_1", "dpre_1")

        def raw_block(j):
            return dot(row["n"][...], w_up[:, wide(j)], 1, 0).astype(jnp.bfloat16)

        def up(j, raw):
            pre[:, wide(j)] = raw
            act[:, wide(j)] = gelu_parts(raw.astype(jnp.float32))[0].astype(jnp.bfloat16)
        staged(ff // WIDE_BLOCK, (raw_block, up))
        send("pre_0", "act_0")
        need("w_down")

        def down(j):
            lanes = pl.ds(pl.multiple_of(OUT_BLOCK * j, OUT_BLOCK), OUT_BLOCK)
            out = dot(act[...], w_down[:, lanes], 1, 0).astype(jnp.bfloat16).astype(jnp.float32)
            row["x"][:, lanes] = (row["h"][:, lanes].astype(jnp.float32) + out).astype(jnp.bfloat16)
        over(width // OUT_BLOCK, down)
        send("x_1")
        free("u_0", "q_0", "k_0", "v_0", "probs_0", "mixed_0", "h_0", "n_0", same=True)
        attention(1)
        send("u_1", "q_1", "k_1", "v_1", "probs_1", "mixed_1", "n_1")
        need("cot")
        free("pre_0", "act_0", same=True)

        def both_blocks(j):
            return raw_block(j), dot(cot_all[rows], w_down[wide(j)], 1, 1).astype(jnp.bfloat16)

        def both(j, made):
            raw, d_act = made
            out, slope = gelu_parts(raw.astype(jnp.float32))
            act[:, wide(j)] = out.astype(jnp.bfloat16)
            pre[:, wide(j)] = (d_act.astype(jnp.float32) * slope).astype(jnp.bfloat16)
        staged(ff // WIDE_BLOCK, (both_blocks, both))
        send("act_1", "dpre_1")

        def back(j):
            lanes = pl.ds(pl.multiple_of(OUT_BLOCK * j, OUT_BLOCK), OUT_BLOCK)
            row["dn"][:, lanes] = dot(pre[...], w_up[lanes], 1, 1).astype(jnp.bfloat16)
        over(width // OUT_BLOCK, back)
        d_hidden = cot_all[rows].astype(jnp.float32) + rms_backward(
            row["h"][...].astype(jnp.float32), row["dn"][...].astype(jnp.float32))
        row["dh"][...] = d_hidden.astype(jnp.bfloat16)
        send("dh_1")
        free("dqa_1", "dka_1", "dva_1")

        def unmix(unit):
            lanes = pl.ds(OUT_BLOCK * unit, OUT_BLOCK)
            row["dn"][:, lanes] = dot(row["dh"][...], w_out[1, lanes], 1, 1).astype(jnp.bfloat16)

        def back_of(j):
            return tuple(row[kind][:, PAIR * j:PAIR * (j + 1)] for kind in ("q", "k", "v", "dn"))

        def put_back(j, values):
            for name, value in zip(HALF_BUFFERS, values):
                row[name][:, PAIR * j:PAIR * (j + 1)] = value.astype(jnp.bfloat16)
        size = OUT_BLOCK // PAIR
        stages = backward_stages(back_of, lambda j, side: probs[2 * j + side], put_back, low)
        staged(heads // 4 // size, in_units(unmix, stages, size))
        send("dqa_1", "dka_1", "dva_1")
        free("x_1", same=True)
        return carry

    lax.fori_loop(0, batch, one_sequence, 0)
    for name in ("u_1", "q_1", "k_1", "v_1", "probs_1", "mixed_1", "n_1", "act_1", "dpre_1", "dh_1", "dqa_1", "dka_1", "dva_1"):
        store(name, batch - 1).wait()


def front(inputs, batch, seq):
    tokens, width = inputs["x_0"].shape
    ff = inputs["w_up"].shape[1]
    heads = width // HEAD_DIM
    shapes = []
    for name in FRONT_OUTS:
        if name.startswith("probs"):
            shapes.append(bf16(batch, heads, seq, seq))
        else:
            wide = ff if name[:-2] in ("pre", "act", "dpre") else width
            shapes.append(bf16(tokens, width // 2 if name[:-2] in HALF_BUFFERS else wide))
    block = lambda *shape: pltpu.VMEM(shape, jnp.bfloat16)
    scratch = [
        block(tokens, width), block(tokens, width), block(2, 3, width, width), block(2, width, width), block(width, ff),
        block(ff, width), block(heads, seq, seq), block(seq, ff), block(seq, ff),
        *[block(seq, width) for _ in ROW_BUFFERS], *[block(seq, width // 2) for _ in HALF_BUFFERS],
        pltpu.SemaphoreType.DMA((12,)), pltpu.SemaphoreType.DMA((len(FRONT_OUTS),)),
    ]
    outs = pl.pallas_call(
        functools.partial(front_kernel, batch, seq, tuple(inputs)),
        out_shape=shapes,
        in_specs=[pl.BlockSpec(memory_space=pl.ANY)] * len(inputs),
        out_specs=[pl.BlockSpec(memory_space=pl.ANY)] * len(shapes),
        scratch_shapes=scratch,
        compiler_params=pltpu.CompilerParams(vmem_limit_bytes=67_043_328),
        cost_estimate=pl.CostEstimate(flops=22 * tokens * width * ff // 2, bytes_accessed=100 * MIB, transcendentals=0),
        name="front",
    )(*inputs.values())
    return dict(zip(FRONT_OUTS, outs))


MESH = pl.DeviceIdType.MESH
LANES = 1024
SET_ROWS = 128
CORE_ROWS = 2 * SET_ROWS
TILE_ROWS = 2 * CORE_ROWS
OWN_SLOTS = 8
AG_SLOTS = 10
TYPES = {
    "p1": (0, 0, 80, "xyz"),
    "q1": (0, 80, 48, "zxy"),
    "p2": (1, 128, 80, "yxz"),
    "q2": (1, 208, 48, "zyx"),
}
WRITE_AT = 11


def stage_list():
    stages = []
    for name, (_, _, _, order) in TYPES.items():
        if order[2] == "z":
            plan = [("rs1", 1), ("rs2", 2), ("rsz", 3), ("agz", 6), ("ag2", 9), ("ag1", 10)]
        else:
            plan = [("rsz", 1), ("rs1", 4), ("rs2", 5), ("ag2", 6), ("ag1", 7), ("agz", 8)]
        for kind, at in plan:
            if kind in ("rsz", "agz"):
                for step in range(3):
                    for way in (0, 1):
                        stages.append((name, kind, step, way, at + step))
            else:
                stages.append((name, kind, 0, 0, at))
    return stages


STAGES = stage_list()


def piece_shape(name, kind):
    rows, order = TYPES[name][2], TYPES[name][3]
    if order[2] == "z":
        return {"rs1": (rows, 512), "rs2": (rows, 256), "rsz": (rows // 2, 128)}[kind]
    return {"rsz": (rows // 2, 512), "rs1": (rows // 2, 256), "rs2": (rows // 2, 128)}[kind]


def between(step, first, count):
    return jnp.logical_and(step >= first, step < first + count)


class Backward:
    PB_1, MB, AB, PB_0 = 4, 6, 14, 23
    ROWS = 256

    def __init__(self, at, big, total_buf, w_buf, p_buf, sem, drain):
        self.at, self.big, self.total, self.w, self.p, self.sem, self.drain = at, big, total_buf, w_buf, p_buf, sem, drain
        self.tokens, self.width = at["x_0"].shape
        self.heads = at["probs_0"].shape[1]
        self.seq = at["probs_0"].shape[2]
        self.seqs = self.tokens // self.seq

    def load(self, name, dest, sem, *index):
        ref = self.at[name]
        return pltpu.make_async_copy(ref.at[index] if index else ref, dest, self.sem.at[sem])

    def store(self, src, name, sem, *index):
        ref = self.at[name]
        return pltpu.make_async_copy(src, ref.at[index] if index else ref, self.drain.at[sem])

    def row_blocks(self, fn):
        def body(block, carry):
            fn(pl.ds(pl.multiple_of(self.ROWS * block, self.ROWS), self.ROWS))
            return carry
        lax.fori_loop(0, self.tokens // self.ROWS, body, 0)

    def input_loads(self, layer):
        copies = [self.load(f"x_{layer}", self.big.at[5], 3)]
        for i, kind in enumerate("qkv"):
            if layer:
                half = self.width // 2
                copies.append(self.load(f"d{kind}a_1", self.big.at[i, :, pl.ds(0, half)], i))
                copies.append(self.load(f"d{kind}b_1", self.big.at[i, :, pl.ds(half, half)], 11 + i))
            else:
                copies.append(self.load(f"d{kind}_0", self.big.at[i], i))
        return copies

    def weight_loads(self, layer, block):
        rows = pl.ds(pl.multiple_of(OUT_BLOCK * block, OUT_BLOCK), OUT_BLOCK)
        slot = lax.rem(block, 2)
        return [self.load(name, self.w.at[slot, i], 5 + 3 * slot + i, layer, rows) for i, name in enumerate(("wq", "wk", "wv"))]

    def input_block(self, layer, block):
        big, blocks = self.big, self.width // OUT_BLOCK
        slot = lax.rem(block, 2)

        @pl.when(block == 0)
        def _():
            for copy in self.input_loads(layer):
                copy.wait()
        for copy in self.weight_loads(layer, block):
            copy.wait()

        @pl.when(block + 1 < blocks)
        def _():
            for copy in self.weight_loads(layer, block + 1):
                copy.start()
        lanes = pl.ds(pl.multiple_of(OUT_BLOCK * block, OUT_BLOCK), OUT_BLOCK)

        def product(rows):
            total = dot(big[0, rows], self.w[slot, 0], 1, 1) + dot(big[1, rows], self.w[slot, 1], 1, 1)
            big[3, rows, lanes] = (total + dot(big[2, rows], self.w[slot, 2], 1, 1)).astype(jnp.bfloat16)
        self.row_blocks(product)

        @pl.when(block == blocks - 1)
        def _():
            def close(rows):
                back = rms_backward(big[5, rows].astype(jnp.float32), big[3, rows].astype(jnp.float32))
                big[3, rows] = (big[4, rows].astype(jnp.float32) + back).astype(jnp.bfloat16)
                if layer:
                    self.total[rows] = jnp.zeros((self.ROWS, self.width), jnp.float32)
            self.row_blocks(close)
            self.store(big.at[3], f"dx_{layer}", 0).start()
            if layer:
                self.load("h_0", big.at[4], 3).start()
                for copy in self.mlp_loads(0):
                    copy.start()

    def mlp_loads(self, block):
        slot = lax.rem(block, 2)
        lanes = pl.ds(pl.multiple_of(FF_BLOCK * block, FF_BLOCK), FF_BLOCK)
        half = pl.ds(pl.multiple_of(FF_BLOCK * slot, FF_BLOCK), FF_BLOCK)
        return [self.load("w_up", self.big.at[0, :, half], 5 + 3 * slot, slice(None), lanes),
                self.load("pre_0", self.big.at[1, :, half], 6 + 3 * slot, slice(None), lanes),
                self.load("w_down", self.big.at[5, half], 7 + 3 * slot, lanes)]

    def mlp_store(self, block):
        half = pl.ds(pl.multiple_of(FF_BLOCK * lax.rem(block, 2), FF_BLOCK), FF_BLOCK)
        lanes = pl.ds(pl.multiple_of(FF_BLOCK * block, FF_BLOCK), FF_BLOCK)
        return self.store(self.big.at[2, :, half], "dpre_0", 1, slice(None), lanes)

    def mlp_block(self, block):
        big, blocks = self.big, self.at["w_up"].shape[1] // FF_BLOCK

        @pl.when(block == 0)
        def _():
            self.store(big.at[3], "dx_1", 0).wait()
            self.load("h_0", big.at[4], 3).wait()
        for copy in self.mlp_loads(block):
            copy.wait()

        @pl.when(block + 1 < blocks)
        def _():
            for copy in self.mlp_loads(block + 1):
                copy.start()

        @pl.when(block > 0)
        def _():
            self.mlp_store(block - 1).wait()
        half = pl.ds(pl.multiple_of(FF_BLOCK * lax.rem(block, 2), FF_BLOCK), FF_BLOCK)

        def product(rows):
            d_act = dot(big[3, rows], big[5, half], 1, 1).astype(jnp.bfloat16).astype(jnp.float32)
            slope = gelu_parts(big[1, rows, half].astype(jnp.float32))[1]
            d_pre = (d_act * slope).astype(jnp.bfloat16)
            big[2, rows, half] = d_pre
            self.total[rows] += dot(d_pre, big[0, :, half], 1, 1)
        self.row_blocks(product)
        self.mlp_store(block).start()

        @pl.when(block == blocks - 1)
        def _():
            def close(rows):
                d_normed = self.total[rows].astype(jnp.bfloat16).astype(jnp.float32)
                back = rms_backward(big[4, rows].astype(jnp.float32), d_normed)
                big[4, rows] = (big[3, rows].astype(jnp.float32) + back).astype(jnp.bfloat16)
            self.row_blocks(close)
            self.store(big.at[4], "dh_0", 2).start()
            self.load("wo", big.at[0], 4, 0).start()
            for copy in self.piece_loads(0, 0):
                copy.start()

    def where(self, piece):
        seq, half = lax.rem(piece, self.seqs), lax.div(piece, self.seqs)
        rows = pl.ds(pl.multiple_of(self.seq * seq, self.seq), self.seq)
        lanes = pl.ds(pl.multiple_of(self.width // 2 * half, self.width // 2), self.width // 2)
        return seq, half, rows, lanes

    def piece_loads(self, layer, piece):
        seq, half, rows, lanes = self.where(piece)
        near = pl.ds(0, self.width // 2)
        copies = [self.load(f"{kind}_{layer}", self.big.at[1 + lax.rem(piece, 2), pl.ds(self.seq * i, self.seq), near], i, rows, lanes)
                  for i, kind in enumerate("qkv")]
        heads = pl.ds(self.heads // 2 * half, self.heads // 2)
        return copies + [self.load(f"probs_{layer}", self.p.at[lax.rem(piece, 2)], 5, seq, heads)]

    def piece_stores(self, layer, piece):
        _, _, rows, lanes = self.where(piece)
        near, spot = pl.ds(0, self.width // 2), 5 - 2 * lax.rem(piece, 2)
        sources = [self.big.at[spot, pl.ds(self.seq * i, self.seq), near] for i in range(3)]
        if layer:
            return [self.store(src, f"d{kind}b_1", 3 + i, rows) for i, (src, kind) in enumerate(zip(sources, "qkv"))]
        return [self.store(src, f"d{kind}_0", 3 + i, rows, lanes) for i, (src, kind) in enumerate(zip(sources, "qkv"))]

    def attention_piece(self, layer, piece):
        big, p_buf, pieces = self.big, self.p, 2 * self.seqs
        _, half, rows, _ = self.where(piece)
        parity = lax.rem(piece, 2)
        spot, out = 1 + parity, 5 - 2 * parity

        start = self.seqs * layer

        @pl.when(piece == start)
        def _():
            if layer == 0:
                self.mlp_store(self.at["w_up"].shape[1] // FF_BLOCK - 1).wait()
                self.store(big.at[4], "dh_0", 2).wait()
            else:
                self.load("dh_1", big.at[4], 3).wait()
            self.load("wo", big.at[0], 4, layer).wait()

        @pl.when(piece > start)
        def _():
            for copy in self.piece_stores(layer, piece - 1):
                copy.wait()
        for copy in self.piece_loads(layer, piece):
            copy.wait()

        @pl.when(piece + 1 < pieces)
        def _():
            for copy in self.piece_loads(layer, piece + 1):
                copy.start()
        low = lax.broadcasted_iota(jnp.int32, (self.seq, PAIR), 1) < HEAD_DIM

        def unmix(unit):
            w_rows = pl.ds(pl.multiple_of(self.width // 2 * half + OUT_BLOCK * unit, OUT_BLOCK), OUT_BLOCK)
            d_mixed = dot(big[4, rows], big[0, w_rows], 1, 1)
            big[spot, pl.ds(3 * self.seq, self.seq), pl.ds(OUT_BLOCK * unit, OUT_BLOCK)] = d_mixed.astype(jnp.bfloat16)

        def pair_of(j):
            return tuple(big[spot, pl.ds(self.seq * i, self.seq), pl.ds(PAIR * j, PAIR)] for i in range(4))

        def put(j, values):
            for i, value in enumerate(values):
                big[out, pl.ds(self.seq * i, self.seq), pl.ds(PAIR * j, PAIR)] = value.astype(jnp.bfloat16)
        size = OUT_BLOCK // PAIR
        stages = backward_stages(pair_of, lambda j, side: p_buf[parity, 2 * j + side], put, low)
        staged(self.heads // 4 // size, in_units(unmix, stages, size))
        for copy in self.piece_stores(layer, piece):
            copy.start()

    def begin(self):
        self.load("dh_1", self.big.at[4], 3).start()
        self.load("wo", self.big.at[0], 4, 1).start()
        for copy in self.piece_loads(1, self.seqs):
            copy.start()

    def item(self, step):
        blocks = self.width // OUT_BLOCK
        pieces = 2 * self.seqs

        @pl.when(step < 3)
        def _():
            first = self.seqs + step
            count = jnp.where(step == 2, self.seqs - 2, 1)
            lax.fori_loop(first, first + count, lambda piece, carry: self.attention_piece(1, piece) or carry, 0)

        @pl.when(step == 3)
        def _():
            for copy in self.piece_stores(1, pieces - 1):
                copy.wait()
            for copy in self.input_loads(1) + self.weight_loads(1, 0):
                copy.start()

        @pl.when(between(step, self.PB_1, 2))
        def _():
            first = blocks // 2 * (step - self.PB_1)
            lax.fori_loop(first, first + blocks // 2, lambda block, carry: self.input_block(1, block) or carry, 0)
        pl.when(between(step, self.MB, 8))(lambda: self.mlp_block(step - self.MB))
        pl.when(between(step, self.AB, pieces))(lambda: self.attention_piece(0, step - self.AB))

        @pl.when(step == self.PB_0 - 1)
        def _():
            for copy in self.piece_stores(0, pieces - 1):
                copy.wait()
            for copy in self.input_loads(0) + self.weight_loads(0, 0):
                copy.start()
        pl.when(between(step, self.PB_0, blocks))(lambda: self.input_block(0, step - self.PB_0))

        @pl.when(step == self.PB_0 + blocks)
        def _():
            self.store(self.big.at[3], "dx_0", 0).wait()


def finish_kernel(groups, chunks, in_names, out_names, remote, *refs):
    names = [*in_names, *out_names]
    at, scratch = dict(zip(names, refs[:len(names)])), refs[len(names):]
    (big, total_buf, w_buf, p_buf, item_sem, drain_sem), scratch = scratch[:6], scratch[6:]
    backward = Backward(at, big, total_buf, w_buf, p_buf, item_sem, drain_sem)
    if not remote:
        backward.begin()

        def alone(step, carry):
            backward.item(step)
            return carry
        lax.fori_loop(0, chunks + WRITE_AT + 1, alone, 0)
        return
    (lhs_buf, rhs_buf, own, part, part_in, gath), scratch = scratch[:6], scratch[6:]
    land_keys = [key for key, st in enumerate(STAGES) if st[1].startswith("rs")]
    landing = dict(zip(land_keys, scratch[:len(land_keys)]))
    load_sem, send_sem, recv_sem, pair_send, pair_recv, out_sem, out_send, out_recv, credit = scratch[len(land_keys):]

    me = lax.axis_index("data")
    core = lax.rem(me, 2)
    coord = {"x": lax.rem(lax.div(me, 2), 2), "y": lax.rem(lax.div(me, 4), 2)}
    z = lax.div(me, 8)
    partner = me + 1 - 2 * core
    near = {"x": me + 2 - 4 * coord["x"], "y": me + 4 - 8 * coord["y"]}
    up_ok, down_ok = z < 3, z > 0
    peers = [(partner, 0, None), (near["x"], 1, None), (near["y"], 2, None), (me + 8, 3, up_ok), (me - 8, 4, down_ok)]

    def guarded(cond, fn):
        if cond is None:
            fn()
        else:
            pl.when(cond)(fn)

    barrier = pltpu.get_barrier_semaphore()
    for dev, _, cond in peers:
        guarded(cond, lambda dev=dev: pl.semaphore_signal(barrier, inc=1, device_id=(dev,), device_id_type=MESH))
    inner = jnp.logical_and(up_ok, down_ok)
    guarded(inner, lambda: pl.semaphore_wait(barrier, 5))
    guarded(jnp.logical_not(inner), lambda: pl.semaphore_wait(barrier, 4))

    def region(name, kind, which):
        _, row, rows, order = TYPES[name]
        if order[2] == "z":
            h1, h2 = coord[order[0]], coord[order[1]]
            if kind == "1":
                return pl.ds(row, rows), pl.ds(pl.multiple_of(512 * which, 128), 512)
            if kind == "2":
                return pl.ds(row, rows), pl.ds(pl.multiple_of(512 * h1 + 256 * which, 128), 256)
            first = pl.multiple_of(row + (rows // 2) * lax.div(which, 2), 8)
            lane = pl.multiple_of(512 * h1 + 256 * h2 + 128 * lax.rem(which, 2), 128)
            return pl.ds(first, rows // 2), pl.ds(lane, 128)
        h1 = coord[order[1]]
        if kind == "z":
            first = pl.multiple_of(row + (rows // 2) * lax.div(which, 2), 8)
            return pl.ds(first, rows // 2), pl.ds(pl.multiple_of(512 * lax.rem(which, 2), 128), 512)
        first = pl.multiple_of(row + (rows // 2) * lax.div(z, 2), 8)
        if kind == "1":
            return pl.ds(first, rows // 2), pl.ds(pl.multiple_of(512 * lax.rem(z, 2) + 256 * which, 128), 256)
        lane = pl.multiple_of(512 * lax.rem(z, 2) + 256 * h1 + 128 * which, 128)
        return pl.ds(first, rows // 2), pl.ds(lane, 128)

    def exchange_axis(name, kind):
        order = TYPES[name][3]
        dims = order[:2] if order[2] == "z" else order[1:]
        return dims[int(kind) - 1]

    def plan(key, chunk, parity):
        name, kind, step, way, _ = STAGES[key]
        mine, slot = lax.rem(chunk, OWN_SLOTS), lax.rem(chunk, AG_SLOTS)
        if kind in ("rs1", "rs2"):
            axis = exchange_axis(name, kind[2])
            src, keep = region(name, kind[2], 1 - coord[axis]), region(name, kind[2], coord[axis])
            dev, send_ok, recv_ok = near[axis], None, None
            sent = own.at[mine, src[0], src[1]]
        elif kind in ("ag1", "ag2"):
            axis = exchange_axis(name, kind[2])
            src = keep = region(name, kind[2], coord[axis])
            dev, send_ok, recv_ok = near[axis], None, None
            sent = gath.at[slot, src[0], src[1]]
        elif kind == "rsz":
            if way:
                dev, k_send, k_keep = me + 8, z + 3 - step, z + 2 - step
                send_ok, recv_ok = k_send <= 3, jnp.logical_and(k_keep <= 3, down_ok)
            else:
                dev, k_send, k_keep = me - 8, z - 3 + step, z - 2 + step
                send_ok, recv_ok = k_send >= 0, jnp.logical_and(k_keep >= 0, up_ok)
            src, keep = region(name, "z", k_send), region(name, "z", k_keep)
            sent = own.at[mine, src[0], src[1]]
        else:
            if way:
                dev, k_send, k_keep = me + 8, z - step, z - 1 - step
                send_ok, recv_ok = jnp.logical_and(k_send >= 0, up_ok), k_keep >= 0
            else:
                dev, k_send, k_keep = me - 8, z + step, z + 1 + step
                send_ok, recv_ok = jnp.logical_and(k_send <= 3, down_ok), k_keep <= 3
            src, keep = region(name, "z", k_send), region(name, "z", k_keep)
            sent = gath.at[slot, src[0], src[1]]
        sems = dict(send_sem=send_sem.at[key], recv_sem=recv_sem.at[key, parity], device_id=(dev,), device_id_type=MESH)
        if kind.startswith("rs"):
            target = landing[key].at[parity]
            send = lambda: pltpu.make_async_remote_copy(src_ref=sent, dst_ref=target, **sems)
            recv = lambda: pltpu.make_async_remote_copy(
                src_ref=own.at[mine, keep[0], keep[1]], dst_ref=target, **sems)

            def arrive():
                own[mine, keep[0], keep[1]] += landing[key][parity]
        else:
            send = lambda: pltpu.make_async_remote_copy(src_ref=sent, dst_ref=sent, **sems)
            recv = lambda: pltpu.make_async_remote_copy(
                src_ref=gath.at[slot, keep[0], keep[1]], dst_ref=gath.at[slot, keep[0], keep[1]], **sems)
            arrive = None
        return send, recv, send_ok, recv_ok, arrive

    def finish(name, chunk):
        order = TYPES[name][3]
        reg = region(name, "z", z) if order[2] == "z" else region(name, "2", coord[order[2]])
        gath[lax.rem(chunk, AG_SLOTS), reg[0], reg[1]] = own[lax.rem(chunk, OWN_SLOTS), reg[0], reg[1]]

    def valid(chunk):
        return jnp.logical_and(chunk >= 0, chunk < chunks)

    def set_rows(half):
        return pl.ds(half * SET_ROWS, SET_ROWS)

    def pair_copy(half, parity):
        return pltpu.make_async_remote_copy(
            src_ref=part.at[parity, set_rows(half)], dst_ref=part_in.at[parity, set_rows(half)],
            send_sem=pair_send.at[half], recv_sem=pair_recv.at[half, parity], device_id=(partner,), device_id_type=MESH)

    half_lanes = LANES // 2

    def outlets(half, group, local, whose):
        out, layer = group["out"]
        ref = at[out] if layer is None else at[out].at[layer]
        rows, cols = group["place"](local)
        if not group["narrow"]:
            first = pl.multiple_of(rows + CORE_ROWS * whose + half * SET_ROWS, SET_ROWS)
            return [(pl.ds(0, LANES), ref.at[pl.ds(first, SET_ROWS), pl.ds(pl.multiple_of(cols, 128), LANES)])]
        places = []
        for sub in (0, 1):
            first = pl.multiple_of(2 * CORE_ROWS * whose + CORE_ROWS * sub + half * SET_ROWS, SET_ROWS)
            places.append((pl.ds(half_lanes * sub, half_lanes), ref.at[pl.ds(first, SET_ROWS), pl.ds(cols, half_lanes)]))
        return places

    def write_copies(half, chunk, lanes, dest):
        slot = lax.rem(chunk, AG_SLOTS)
        src = gath.at[slot, set_rows(half), lanes]
        here = pltpu.make_async_copy(src, dest, out_sem.at[half])
        there = pltpu.make_async_remote_copy(
            src_ref=src, dst_ref=dest, send_sem=out_send.at[half], recv_sem=out_recv.at[half, lax.rem(chunk, 2)],
            device_id=(partner,), device_id_type=MESH)
        return here, there

    def load_copies(group, local, slot):
        rows, cols = group["place"](local)
        narrow = group["narrow"]
        lhs, rhs = [], []
        for sub in range(2 if narrow else len(group["lhs"])):
            for whose in (0, 1):
                owner = core if whose == 0 else 1 - core
                first = 2 * CORE_ROWS * owner + CORE_ROWS * sub if narrow else rows + CORE_ROWS * owner
                source = at[group["lhs"][0 if narrow else sub]]
                lhs.append(pltpu.make_async_copy(
                    source.at[:, pl.ds(pl.multiple_of(first, CORE_ROWS), CORE_ROWS)],
                    lhs_buf.at[slot, sub, whose], load_sem.at[slot, sub, whose]))
        for app, name in enumerate(group["rhs"]):
            size = half_lanes if narrow else LANES
            rhs.append(pltpu.make_async_copy(
                at[name].at[:, pl.ds(0 if narrow else pl.multiple_of(cols, 128), size)], rhs_buf.at[slot, app, :, pl.ds(0, size)],
                load_sem.at[slot, app, 2]))
        return lhs, rhs

    def for_group(chunk, fn):
        for group in groups:
            inside = jnp.logical_and(chunk >= group["start"], chunk < group["start"] + group["count"])
            pl.when(inside)(functools.partial(fn, group, chunk - group["start"]))

    def among(chunk, chosen):
        flags = [jnp.logical_and(chunk >= g["start"], chunk < g["start"] + g["count"]) for g in groups if chosen(g)]
        return functools.reduce(jnp.logical_or, flags)

    def is_two(group):
        return len(group["lhs"]) == 2

    def is_narrow(group):
        return group["narrow"]

    def start_load(chunk):
        def go(group, local):
            for copy in sum(load_copies(group, local, lax.rem(chunk, 2)), []):
                copy.start()
        for_group(chunk, go)

    def wait_load(chunk):
        slot = lax.rem(chunk, 2)
        two_lhs, two_rhs = load_copies(next(filter(is_two, groups)), 0, slot)
        slim_lhs, slim_rhs = load_copies(next(filter(is_narrow, groups)), 0, slot)
        for copy in two_lhs[:2]:
            copy.wait()

        @pl.when(jnp.logical_not(among(chunk, is_narrow)))
        def _():
            two_rhs[0].wait()

        @pl.when(among(chunk, is_narrow))
        def _():
            for copy in slim_rhs + slim_lhs[2:]:
                copy.wait()

        @pl.when(among(chunk, is_two))
        def _():
            for copy in two_lhs[2:] + two_rhs[1:]:
                copy.wait()

    def tile(chunk):
        slot, mine, parity = lax.rem(chunk, 2), lax.rem(chunk, OWN_SLOTS), lax.rem(chunk, 2)

        def product(sub, whose, rhs):
            return dot(lhs_buf[slot, sub, whose], rhs, 0, 0)

        @pl.when(among(chunk, is_narrow))
        def _():
            for sub in (0, 1):
                lanes, rhs = pl.ds(half_lanes * sub, half_lanes), rhs_buf[slot, 0, :, pl.ds(0, half_lanes)]
                own[mine, :, lanes] = product(sub, 0, rhs)
                part[parity, :, lanes] = product(sub, 1, rhs)

        @pl.when(jnp.logical_not(among(chunk, is_narrow)))
        def _():
            own[mine] = product(0, 0, rhs_buf[slot, 0])
            part[parity] = product(0, 1, rhs_buf[slot, 0])

        @pl.when(among(chunk, is_two))
        def _():
            own[mine] += product(1, 0, rhs_buf[slot, 1])
            part[parity] += product(1, 1, rhs_buf[slot, 1])

    last = chunks + WRITE_AT

    def section(half, step):
        before = lax.rem(step + 1, 2)
        now = lax.rem(step, 2)

        @pl.when(valid(step - 1))
        def _():
            copy = pair_copy(half, before)
            copy.wait_send()
            copy.wait_recv()
            mine = lax.rem(step - 1, OWN_SLOTS)
            own[mine, set_rows(half)] += part_in[before, set_rows(half)]

        names = [name for name in TYPES if TYPES[name][0] == half]
        keys = [key for key, st in enumerate(STAGES) if st[0] in names]
        finals = {name: max(st[4] for st in STAGES if st[0] == name and st[1].startswith("rs")) for name in names}
        for key in keys:
            name, at = STAGES[key][0], STAGES[key][4]
            chunk = step - 1 - at

            @pl.when(valid(chunk))
            def _(key=key, chunk=chunk):
                send, recv, send_ok, recv_ok, arrive = plan(key, chunk, before)

                def arrived():
                    recv().wait_recv()
                    if arrive is not None:
                        arrive()
                guarded(recv_ok, arrived)
                guarded(send_ok, lambda: send().wait_send())
        for name in names:
            chunk = step - 1 - finals[name]
            pl.when(valid(chunk))(functools.partial(finish, name, chunk))

        done = step - 1 - WRITE_AT

        @pl.when(valid(done))
        def _():
            (lanes, dest), = outlets(half, next(filter(is_two, groups)), 0, 0)
            here, there = write_copies(half, done, lanes, dest)
            here.wait()
            there.wait_send()
            there.wait_recv()

        @pl.when(step < last)
        def _():
            for dev, way, cond in peers:
                to = way if way < 3 else 7 - way
                guarded(cond, lambda dev=dev, to=to: pl.semaphore_signal(
                    credit.at[half, to], inc=1, device_id=(dev,), device_id_type=MESH))

        @pl.when(step > 0)
        def _():
            for dev, way, cond in peers:
                guarded(cond, lambda way=way: pl.semaphore_wait(credit.at[half, way], 1))

        for key in reversed(keys):
            chunk = step - STAGES[key][4]

            @pl.when(valid(chunk))
            def _(key=key, chunk=chunk):
                send, recv, send_ok, recv_ok, arrive = plan(key, chunk, now)
                guarded(send_ok, lambda: send().start())

        out_chunk = step - WRITE_AT

        @pl.when(valid(out_chunk))
        def _():
            def go(group, local):
                for lanes, dest in outlets(half, group, local, core):
                    for copy in write_copies(half, out_chunk, lanes, dest):
                        copy.start()
            for_group(out_chunk, go)

    backward.begin()
    start_load(jnp.int32(0))

    def round_(step, carry):
        section(0, step)

        @pl.when(valid(step))
        def _():
            pl.when(step + 1 < chunks)(lambda: start_load(step + 1))
            wait_load(step)
            tile(step)
            pair_copy(0, lax.rem(step, 2)).start()

        section(1, step)

        @pl.when(valid(step))
        def _():
            pair_copy(1, lax.rem(step, 2)).start()

        backward.item(step)
        return carry

    lax.fori_loop(0, last + 1, round_, 0)


def finish_backward(inputs, groups, chunks, weights, tokens, seq, collective_id=0, remote=True):
    width, ff = inputs["w_up"].shape
    landing = [pltpu.VMEM((2,) + piece_shape(st[0], st[1]), jnp.float32) for st in STAGES if st[1].startswith("rs")]
    apps = 2
    outs = {name: jax.ShapeDtypeStruct(shape, jnp.float32) for name, shape in weights.items()}
    for name in ("dx_0", "dx_1", "dh_0", "dq_0", "dk_0", "dv_0"):
        outs[name] = bf16(tokens, width)
    for name in ("dqb_1", "dkb_1", "dvb_1"):
        outs[name] = bf16(tokens, width // 2)
    outs["dpre_0"] = bf16(tokens, ff)
    heads = width // HEAD_DIM
    scratch = [
        pltpu.VMEM((6, tokens, width), jnp.bfloat16),
        pltpu.VMEM((tokens, width), jnp.float32),
        pltpu.VMEM((2, 3, OUT_BLOCK, width), jnp.bfloat16),
        pltpu.VMEM((2, heads // 2, seq, seq), jnp.bfloat16),
        pltpu.SemaphoreType.DMA((14,)),
        pltpu.SemaphoreType.DMA((6,)),
    ]
    if remote:
        scratch += [
            pltpu.VMEM((2, apps, 2, tokens, CORE_ROWS), jnp.bfloat16),
            pltpu.VMEM((2, apps, tokens, LANES), jnp.bfloat16),
            pltpu.VMEM((OWN_SLOTS, CORE_ROWS, LANES), jnp.float32),
            pltpu.VMEM((2, CORE_ROWS, LANES), jnp.float32),
            pltpu.VMEM((2, CORE_ROWS, LANES), jnp.float32),
            pltpu.VMEM((AG_SLOTS, CORE_ROWS, LANES), jnp.float32),
            *landing,
            pltpu.SemaphoreType.DMA((2, apps, 3)),
            pltpu.SemaphoreType.DMA((len(STAGES),)),
            pltpu.SemaphoreType.DMA((len(STAGES), 2)),
            pltpu.SemaphoreType.DMA((2,)),
            pltpu.SemaphoreType.DMA((2, 2)),
            pltpu.SemaphoreType.DMA((2,)),
            pltpu.SemaphoreType.DMA((2,)),
            pltpu.SemaphoreType.DMA((2, 2)),
            pltpu.SemaphoreType.REGULAR((2, 5)),
        ]
    params = dict(collective_id=collective_id, has_side_effects=True) if remote else {}
    results = pl.pallas_call(
        functools.partial(finish_kernel, groups, chunks, list(inputs), list(outs), remote),
        out_shape=list(outs.values()),
        in_specs=[pl.BlockSpec(memory_space=pl.ANY)] * len(inputs),
        out_specs=[pl.BlockSpec(memory_space=pl.ANY)] * len(outs),
        scratch_shapes=scratch,
        compiler_params=pltpu.CompilerParams(vmem_limit_bytes=67_043_328, **params),
        cost_estimate=pl.CostEstimate(flops=20 * tokens * width * ff, bytes_accessed=256 * MIB, transcendentals=0),
        name="finish_backward",
    )(*inputs.values())
    return dict(zip(outs, results))


DELIVER_ROWS = 256
DELIVER_SLOTS = 40
DELIVER_AHEAD = 20


def deliver(arrays, small):
    def blocks_of(array):
        lead = [(i,) for i in range(array.shape[0])] if len(array.shape) == 3 else [()]
        rows, cols = array.shape[-2:]
        return [(*index, pl.ds(row, DELIVER_ROWS), pl.ds(col, LANES))
                for index in lead for row in range(0, rows, DELIVER_ROWS) for col in range(0, cols, LANES)]

    work = [(i, index) for i, array in enumerate(arrays) for index in blocks_of(array)]
    count = len(arrays) + 1

    def kernel(*refs):
        ins, outs, buf, whole_buf, in_sem, out_sem, whole_sem = refs[:count], refs[count:2 * count], *refs[2 * count:]
        whole_in = pltpu.make_async_copy(ins[-1], whole_buf, whole_sem.at[0])
        whole_out = pltpu.make_async_copy(whole_buf, outs[-1], whole_sem.at[1])

        def fetch(t):
            i, index = work[t]
            return pltpu.make_async_copy(ins[i].at[index], buf.at[t % DELIVER_SLOTS], in_sem.at[t % DELIVER_SLOTS])

        def put(t):
            i, index = work[t]
            return pltpu.make_async_copy(buf.at[t % DELIVER_SLOTS], outs[i].at[index], out_sem.at[t % DELIVER_SLOTS])

        whole_in.start()
        for t in range(min(DELIVER_AHEAD, len(work))):
            fetch(t).start()
        whole_in.wait()
        whole_out.start()
        for t in range(len(work)):
            if t + DELIVER_AHEAD < len(work):
                if t + DELIVER_AHEAD >= DELIVER_SLOTS:
                    put(t + DELIVER_AHEAD - DELIVER_SLOTS).wait()
                fetch(t + DELIVER_AHEAD).start()
            fetch(t).wait()
            put(t).start()
        for t in range(max(0, len(work) - DELIVER_SLOTS), len(work)):
            put(t).wait()
        whole_out.wait()

    return pl.pallas_call(
        kernel,
        out_shape=[jax.ShapeDtypeStruct(array.shape, array.dtype) for array in (*arrays, small)],
        in_specs=[pl.BlockSpec(memory_space=pl.ANY)] * count,
        out_specs=[pl.BlockSpec(memory_space=pl.ANY)] * count,
        scratch_shapes=[pltpu.VMEM((DELIVER_SLOTS, DELIVER_ROWS, LANES), jnp.float32), pltpu.VMEM(small.shape, small.dtype),
                        pltpu.SemaphoreType.DMA((DELIVER_SLOTS,)), pltpu.SemaphoreType.DMA((DELIVER_SLOTS,)),
                        pltpu.SemaphoreType.DMA((2,))],
        compiler_params=pltpu.CompilerParams(vmem_limit_bytes=67_043_328),
        cost_estimate=pl.CostEstimate(flops=0, bytes_accessed=2 * sum(a.size for a in arrays) * 4, transcendentals=0),
        name="deliver",
    )(*arrays, small)


def gradient_groups(width, ff):
    groups = []

    def add(count, lhs, rhs, out, place, narrow=False):
        start = groups[-1]["start"] + groups[-1]["count"] if groups else 0
        groups.append(dict(start=start, count=count, lhs=lhs, rhs=rhs, out=out, place=place, narrow=narrow))

    def tall(local):
        return TILE_ROWS * local, 0

    def wide(local):
        return TILE_ROWS * lax.rem(local, width // TILE_ROWS), LANES * lax.div(local, width // TILE_ROWS)

    for half in (0, 1):
        for kind in "qkv":
            add(1, ["u_1"], [f"d{kind}{'ab'[half]}_1"], (f"g_{kind}", 1), lambda local, half=half: (0, width // 2 * half), narrow=True)
        if half == 0:
            add(width // TILE_ROWS, ["mixed_1"], ["dh_1"], ("g_o", 1), tall)
    add(ff // TILE_ROWS, ["act_0", "act_1"], ["dx_1", "cot"], ("g_down", None), tall)
    add(ff // TILE_ROWS, ["n_0", "n_1"], ["dpre_0", "dpre_1"], ("g_up", None), wide)
    for kind in "qkv":
        add(width // TILE_ROWS, ["u_0"], [f"d{kind}_0"], (f"g_{kind}", 0), tall)
    add(width // TILE_ROWS, ["mixed_0"], ["dh_0"], ("g_o", 0), tall)
    return groups, sum(group["count"] for group in groups)


def local_operands(x_init, cot_out, w_query, w_key, w_value, w_proj, w_up, w_down):
    batch, seq, width = x_init.shape
    tokens = batch * seq
    at = {"x_0": x_init.reshape(tokens, width), "cot": cot_out.reshape(tokens, width)}
    at.update(wq=w_query, wk=w_key, wv=w_value, wo=w_proj, w_up=w_up, w_down=w_down)
    at.update(front(at, batch, seq))
    return at


def solution(mesh):
    def local_step(x_init, cot_out, w_query, w_key, w_value, w_proj, w_up, w_down):
        batch, seq, width = x_init.shape
        inputs = local_operands(x_init, cot_out, w_query, w_key, w_value, w_proj, w_up, w_down)
        groups, chunks = gradient_groups(width, w_up.shape[1])
        weights = dict(g_q=w_query.shape, g_k=w_key.shape, g_v=w_value.shape, g_o=w_proj.shape, g_up=w_up.shape, g_down=w_down.shape)
        res = finish_backward(inputs, groups, chunks, weights, batch * seq, seq)
        *grads, d_init = deliver([res[name] for name in weights], res["dx_0"])
        return (*grads, d_init.reshape(x_init.shape))

    data_spec = P("data")
    full_spec = P()
    in_specs = (data_spec, data_spec, full_spec, full_spec, full_spec, full_spec, full_spec, full_spec)
    out_specs = (full_spec, full_spec, full_spec, full_spec, full_spec, full_spec, data_spec)
    return jax.shard_map(local_step, mesh=mesh, in_specs=in_specs, out_specs=out_specs, check_vma=False)
```

```python
import functools

import jax
import jax.numpy as jnp
from jax import lax
from jax.experimental import pallas as pl
from jax.experimental.pallas import tpu as pltpu
from jax.sharding import PartitionSpec as P

EPS = 1e-6
HEAD_DIM = 64
PAIR = 2 * HEAD_DIM
FF_BLOCK = 512
OUT_BLOCK = 256
GELU_A = (2.0 / 3.141592653589793) ** 0.5
GELU_B = 0.044715
SOFTMAX_SCALE = HEAD_DIM ** -0.5 * 1.4426950408889634
MIB = 1024 * 1024


def dot(lhs, rhs, lhs_dim, rhs_dim):
    return lax.dot_general(lhs, rhs, (((lhs_dim,), (rhs_dim,)), ((), ())), preferred_element_type=jnp.float32)


def rms_norm(x_f32):
    return x_f32 * lax.rsqrt(jnp.mean(x_f32 * x_f32, axis=-1, keepdims=True) + EPS)


def rms_backward(x_f32, d_out):
    scale = lax.rsqrt(jnp.mean(x_f32 * x_f32, axis=-1, keepdims=True) + EPS)
    inner = jnp.mean(x_f32 * d_out, axis=-1, keepdims=True)
    return scale * d_out - x_f32 * (scale * scale * scale * inner)


def gelu_parts(pre):
    square = pre * pre
    tanh = jnp.tanh(GELU_A * (pre + GELU_B * pre * square))
    half = 0.5 * (1.0 + tanh)
    slope = half + 0.5 * pre * (1.0 - tanh * tanh) * (GELU_A + (3.0 * GELU_A * GELU_B) * square)
    return pre * half, slope


def bf16(*shape):
    return jax.ShapeDtypeStruct(shape, jnp.bfloat16)


def backward_stages(pair_of, probs_of, put, low):
    masks = (low, jnp.logical_not(low))

    def from_mixed(j, _=None):
        _, _, v_pair, d_pair = pair_of(j)
        return [dot(v_pair, jnp.where(mask, d_pair, 0), 1, 1).astype(jnp.bfloat16) for mask in masks]

    def through(j, made):
        out = []
        for side, d_probs in enumerate(made):
            d_probs, probs = d_probs.astype(jnp.float32), probs_of(j, side).astype(jnp.float32)
            row_dot = jnp.sum(d_probs * probs, axis=0, keepdims=True)
            out.append((probs * (d_probs - row_dot) * HEAD_DIM ** -0.5).astype(jnp.bfloat16))
        return out

    def to_inputs(j, made):
        q_pair, k_pair, _, d_pair = pair_of(j)
        sides = [(dot(d_scores, k_pair, 0, 0), dot(d_scores, q_pair, 1, 0), dot(probs_of(j, side), d_pair, 1, 0))
                 for side, d_scores in enumerate(made)]
        put(j, [jnp.where(low, first, second) for first, second in zip(*sides)])
    return from_mixed, through, to_inputs


def forward_stages(pair_of, keep, put, low):
    def scores(j, _=None):
        q_pair, k_pair, _ = pair_of(j)
        return [dot(k_pair, jnp.where(mask, q_pair, 0), 1, 1) for mask in (low, jnp.logical_not(low))]

    def soften(j, made):
        out = []
        for side, score in enumerate(made):
            top = jnp.max(score, axis=0, keepdims=True)
            raised = jnp.exp2((score - top) * SOFTMAX_SCALE)
            inverse = 1.0 / jnp.sum(raised, axis=0, keepdims=True)
            out.append((raised * inverse).astype(jnp.bfloat16))
            keep(j, side, out[-1])
        return out

    def mix(j, made):
        first, second = (dot(probs, pair_of(j)[2], 0, 0) for probs in made)
        put(j, jnp.where(low, first, second))
    return scores, soften, mix


def in_units(first, stages, size):
    def lift(stage):
        return lambda unit, made: [stage(size * unit + i, made[i]) for i in range(size)]
    return (lambda unit: first(unit) or [None] * size, *map(lift, stages))


def staged(count, stages):
    made = [None] * count
    for turn in range(count + len(stages) - 1):
        for depth, stage in enumerate(stages):
            j = turn - depth
            if 0 <= j < count:
                made[j] = stage(j, made[j]) if depth else stage(j)


FRONT_OUTS = ("u_0", "q_0", "k_0", "v_0", "probs_0", "mixed_0", "h_0", "n_0", "pre_0", "act_0", "x_1",
              "u_1", "q_1", "k_1", "v_1", "probs_1", "mixed_1", "n_1", "act_1", "dpre_1", "dh_1", "dqa_1", "dka_1", "dva_1")
ROW_BUFFERS = ("u", "q", "k", "v", "mixed", "h", "n", "x", "dh", "dn")
HALF_BUFFERS = ("dqa", "dka", "dva")
WIDE_BLOCK = 1024


def front_kernel(batch, seq, in_names, *refs):
    at = dict(zip((*in_names, *FRONT_OUTS), refs))
    refs = refs[len(at):]
    x_all, cot_all, w_in, w_out, w_up, w_down, probs, pre, act = refs[:9]
    row = dict(zip((*ROW_BUFFERS, *HALF_BUFFERS), refs[9:]))
    load_sem, out_sem = refs[9 + len(row):]
    width, ff = w_up.shape
    heads = width // HEAD_DIM
    loads = {"x": pltpu.make_async_copy(at["x_0"], x_all, load_sem.at[0])}
    for layer in (0, 1):
        for i, name in enumerate(("wq", "wk", "wv")):
            loads[f"{name}_{layer}"] = pltpu.make_async_copy(at[name].at[layer], w_in.at[layer, i], load_sem.at[1 + 4 * layer + i])
        loads[f"wo_{layer}"] = pltpu.make_async_copy(at["wo"].at[layer], w_out.at[layer], load_sem.at[4 + 4 * layer])
    loads["w_up"] = pltpu.make_async_copy(at["w_up"], w_up, load_sem.at[9])
    loads["w_down"] = pltpu.make_async_copy(at["w_down"], w_down, load_sem.at[10])
    loads["cot"] = pltpu.make_async_copy(at["cot"], cot_all, load_sem.at[11])
    for name in ("x", "wq_0", "wk_0", "wv_0"):
        loads[name].start()
    holders = {"probs_0": probs, "probs_1": probs, "pre_0": pre, "act_0": act, "act_1": act, "dpre_1": pre, "x_1": row["x"]}
    for name in FRONT_OUTS:
        holders.setdefault(name, row.get(name[:-2]))

    def store(name, index):
        src = holders[name]
        rows = pl.ds(pl.multiple_of(seq * index, seq), seq)
        dest = at[name].at[index] if name.startswith("probs") else at[name].at[rows]
        return pltpu.make_async_copy(src, dest, out_sem.at[FRONT_OUTS.index(name)])

    def one_sequence(index, carry):
        rows = pl.ds(pl.multiple_of(seq * index, seq), seq)
        first = index == 0
        low = lax.broadcasted_iota(jnp.int32, (seq, PAIR), 1) < HEAD_DIM

        def need(*names):
            @pl.when(first)
            def _():
                for name in names:
                    loads[name].wait()

        def launch(*names):
            @pl.when(first)
            def _():
                for name in names:
                    loads[name].start()

        def free(*names, same=False):
            for name in names:
                if same:
                    store(name, index).wait()
                else:
                    pl.when(index > 0)(lambda name=name: store(name, index - 1).wait())

        def send(*names):
            for name in names:
                store(name, index).start()

        def over(count, fn):
            for j in range(count):
                fn(j)

        def wide(j):
            return pl.ds(WIDE_BLOCK * j, WIDE_BLOCK)

        def attention(layer):
            x_in = x_all[rows] if layer == 0 else row["x"][...]
            row["u"][...] = rms_norm(x_in.astype(jnp.float32)).astype(jnp.bfloat16)
            need(*(f"w{kind}_{layer}" for kind in "qkv"))
            if layer == 0:
                launch("wo_0", "w_up")

            def project(unit):
                lanes = pl.ds(OUT_BLOCK * unit, OUT_BLOCK)
                for i, kind in enumerate("qkv"):
                    row[kind][:, lanes] = dot(row["u"][...], w_in[layer, i, :, lanes], 1, 0).astype(jnp.bfloat16)

            def pair_of(j):
                return tuple(row[kind][:, PAIR * j:PAIR * (j + 1)] for kind in "qkv")

            def keep(j, side, value):
                probs[2 * j + side] = value

            def put(j, value):
                row["mixed"][:, PAIR * j:PAIR * (j + 1)] = value.astype(jnp.bfloat16)
            size = OUT_BLOCK // PAIR
            staged(heads // 2 // size, in_units(project, forward_stages(pair_of, keep, put, low), size))
            need(f"wo_{layer}")
            attn = dot(row["mixed"][...], w_out[layer], 1, 0).astype(jnp.bfloat16)
            hidden = (x_in.astype(jnp.float32) + attn.astype(jnp.float32)).astype(jnp.bfloat16)
            row["h"][...] = hidden
            row["n"][...] = rms_norm(hidden.astype(jnp.float32)).astype(jnp.bfloat16)

        need("x")
        free("u_1", "q_1", "k_1", "v_1", "probs_1", "mixed_1", "n_1", "dh_1")
        attention(0)
        send("u_0", "q_0", "k_0", "v_0", "probs_0", "mixed_0", "h_0", "n_0")
        need("w_up")
        launch("w_down", "wq_1", "wk_1", "wv_1", "wo_1", "cot")
        free("act_1", "dpre_1")

        def raw_block(j):
            return dot(row["n"][...], w_up[:, wide(j)], 1, 0).astype(jnp.bfloat16)

        def up(j, raw):
            pre[:, wide(j)] = raw
            act[:, wide(j)] = gelu_parts(raw.astype(jnp.float32))[0].astype(jnp.bfloat16)
        staged(ff // WIDE_BLOCK, (raw_block, up))
        send("pre_0", "act_0")
        need("w_down")

        def down(j):
            lanes = pl.ds(pl.multiple_of(OUT_BLOCK * j, OUT_BLOCK), OUT_BLOCK)
            out = dot(act[...], w_down[:, lanes], 1, 0).astype(jnp.bfloat16).astype(jnp.float32)
            row["x"][:, lanes] = (row["h"][:, lanes].astype(jnp.float32) + out).astype(jnp.bfloat16)
        over(width // OUT_BLOCK, down)
        send("x_1")
        free("u_0", "q_0", "k_0", "v_0", "probs_0", "mixed_0", "h_0", "n_0", same=True)
        attention(1)
        send("u_1", "q_1", "k_1", "v_1", "probs_1", "mixed_1", "n_1")
        need("cot")
        free("pre_0", "act_0", same=True)

        def both_blocks(j):
            return raw_block(j), dot(cot_all[rows], w_down[wide(j)], 1, 1).astype(jnp.bfloat16)

        def both(j, made):
            raw, d_act = made
            out, slope = gelu_parts(raw.astype(jnp.float32))
            act[:, wide(j)] = out.astype(jnp.bfloat16)
            pre[:, wide(j)] = (d_act.astype(jnp.float32) * slope).astype(jnp.bfloat16)
        staged(ff // WIDE_BLOCK, (both_blocks, both))
        send("act_1", "dpre_1")

        def back(j):
            lanes = pl.ds(pl.multiple_of(OUT_BLOCK * j, OUT_BLOCK), OUT_BLOCK)
            row["dn"][:, lanes] = dot(pre[...], w_up[lanes], 1, 1).astype(jnp.bfloat16)
        over(width // OUT_BLOCK, back)
        d_hidden = cot_all[rows].astype(jnp.float32) + rms_backward(
            row["h"][...].astype(jnp.float32), row["dn"][...].astype(jnp.float32))
        row["dh"][...] = d_hidden.astype(jnp.bfloat16)
        send("dh_1")
        free("dqa_1", "dka_1", "dva_1")

        def unmix(unit):
            lanes = pl.ds(OUT_BLOCK * unit, OUT_BLOCK)
            row["dn"][:, lanes] = dot(row["dh"][...], w_out[1, lanes], 1, 1).astype(jnp.bfloat16)

        def back_of(j):
            return tuple(row[kind][:, PAIR * j:PAIR * (j + 1)] for kind in ("q", "k", "v", "dn"))

        def put_back(j, values):
            for name, value in zip(HALF_BUFFERS, values):
                row[name][:, PAIR * j:PAIR * (j + 1)] = value.astype(jnp.bfloat16)
        size = OUT_BLOCK // PAIR
        stages = backward_stages(back_of, lambda j, side: probs[2 * j + side], put_back, low)
        staged(heads // 4 // size, in_units(unmix, stages, size))
        send("dqa_1", "dka_1", "dva_1")
        free("x_1", same=True)
        return carry

    lax.fori_loop(0, batch, one_sequence, 0)
    for name in ("u_1", "q_1", "k_1", "v_1", "probs_1", "mixed_1", "n_1", "act_1", "dpre_1", "dh_1", "dqa_1", "dka_1", "dva_1"):
        store(name, batch - 1).wait()


def front(inputs, batch, seq):
    tokens, width = inputs["x_0"].shape
    ff = inputs["w_up"].shape[1]
    heads = width // HEAD_DIM
    shapes = []
    for name in FRONT_OUTS:
        if name.startswith("probs"):
            shapes.append(bf16(batch, heads, seq, seq))
        else:
            wide = ff if name[:-2] in ("pre", "act", "dpre") else width
            shapes.append(bf16(tokens, width // 2 if name[:-2] in HALF_BUFFERS else wide))
    block = lambda *shape: pltpu.VMEM(shape, jnp.bfloat16)
    scratch = [
        block(tokens, width), block(tokens, width), block(2, 3, width, width), block(2, width, width), block(width, ff),
        block(ff, width), block(heads, seq, seq), block(seq, ff), block(seq, ff),
        *[block(seq, width) for _ in ROW_BUFFERS], *[block(seq, width // 2) for _ in HALF_BUFFERS],
        pltpu.SemaphoreType.DMA((12,)), pltpu.SemaphoreType.DMA((len(FRONT_OUTS),)),
    ]
    outs = pl.pallas_call(
        functools.partial(front_kernel, batch, seq, tuple(inputs)),
        out_shape=shapes,
        in_specs=[pl.BlockSpec(memory_space=pl.ANY)] * len(inputs),
        out_specs=[pl.BlockSpec(memory_space=pl.ANY)] * len(shapes),
        scratch_shapes=scratch,
        compiler_params=pltpu.CompilerParams(vmem_limit_bytes=67_043_328),
        cost_estimate=pl.CostEstimate(flops=22 * tokens * width * ff // 2, bytes_accessed=100 * MIB, transcendentals=0),
        name="front",
    )(*inputs.values())
    return dict(zip(FRONT_OUTS, outs))


MESH = pl.DeviceIdType.MESH
LANES = 1024
SET_ROWS = 128
CORE_ROWS = 2 * SET_ROWS
TILE_ROWS = 2 * CORE_ROWS
OWN_SLOTS = 8
AG_SLOTS = 10
TYPES = {
    "p1": (0, 0, 80, "xyz"),
    "q1": (0, 80, 48, "zxy"),
    "p2": (1, 128, 80, "yxz"),
    "q2": (1, 208, 48, "zyx"),
}
WRITE_AT = 11


def stage_list():
    stages = []
    for name, (_, _, _, order) in TYPES.items():
        if order[2] == "z":
            plan = [("rs1", 1), ("rs2", 2), ("rsz", 3), ("agz", 6), ("ag2", 9), ("ag1", 10)]
        else:
            plan = [("rsz", 1), ("rs1", 4), ("rs2", 5), ("ag2", 6), ("ag1", 7), ("agz", 8)]
        for kind, at in plan:
            if kind in ("rsz", "agz"):
                for step in range(3):
                    for way in (0, 1):
                        stages.append((name, kind, step, way, at + step))
            else:
                stages.append((name, kind, 0, 0, at))
    return stages


STAGES = stage_list()


def piece_shape(name, kind):
    rows, order = TYPES[name][2], TYPES[name][3]
    if order[2] == "z":
        return {"rs1": (rows, 512), "rs2": (rows, 256), "rsz": (rows // 2, 128)}[kind]
    return {"rsz": (rows // 2, 512), "rs1": (rows // 2, 256), "rs2": (rows // 2, 128)}[kind]


def between(step, first, count):
    return jnp.logical_and(step >= first, step < first + count)


class Backward:
    PB_1, MB, AB, PB_0 = 4, 6, 14, 23
    ROWS = 256

    def __init__(self, at, big, total_buf, w_buf, p_buf, sem, drain):
        self.at, self.big, self.total, self.w, self.p, self.sem, self.drain = at, big, total_buf, w_buf, p_buf, sem, drain
        self.tokens, self.width = at["x_0"].shape
        self.heads = at["probs_0"].shape[1]
        self.seq = at["probs_0"].shape[2]
        self.seqs = self.tokens // self.seq

    def load(self, name, dest, sem, *index):
        ref = self.at[name]
        return pltpu.make_async_copy(ref.at[index] if index else ref, dest, self.sem.at[sem])

    def store(self, src, name, sem, *index):
        ref = self.at[name]
        return pltpu.make_async_copy(src, ref.at[index] if index else ref, self.drain.at[sem])

    def row_blocks(self, fn):
        def body(block, carry):
            fn(pl.ds(pl.multiple_of(self.ROWS * block, self.ROWS), self.ROWS))
            return carry
        lax.fori_loop(0, self.tokens // self.ROWS, body, 0)

    def input_loads(self, layer):
        copies = [self.load(f"x_{layer}", self.big.at[5], 3)]
        for i, kind in enumerate("qkv"):
            if layer:
                half = self.width // 2
                copies.append(self.load(f"d{kind}a_1", self.big.at[i, :, pl.ds(0, half)], i))
                copies.append(self.load(f"d{kind}b_1", self.big.at[i, :, pl.ds(half, half)], 11 + i))
            else:
                copies.append(self.load(f"d{kind}_0", self.big.at[i], i))
        return copies

    def weight_loads(self, layer, block):
        rows = pl.ds(pl.multiple_of(OUT_BLOCK * block, OUT_BLOCK), OUT_BLOCK)
        slot = lax.rem(block, 2)
        return [self.load(name, self.w.at[slot, i], 5 + 3 * slot + i, layer, rows) for i, name in enumerate(("wq", "wk", "wv"))]

    def input_block(self, layer, block):
        big, blocks = self.big, self.width // OUT_BLOCK
        slot = lax.rem(block, 2)

        @pl.when(block == 0)
        def _():
            for copy in self.input_loads(layer):
                copy.wait()
        for copy in self.weight_loads(layer, block):
            copy.wait()

        @pl.when(block + 1 < blocks)
        def _():
            for copy in self.weight_loads(layer, block + 1):
                copy.start()
        lanes = pl.ds(pl.multiple_of(OUT_BLOCK * block, OUT_BLOCK), OUT_BLOCK)

        def product(rows):
            total = dot(big[0, rows], self.w[slot, 0], 1, 1) + dot(big[1, rows], self.w[slot, 1], 1, 1)
            big[3, rows, lanes] = (total + dot(big[2, rows], self.w[slot, 2], 1, 1)).astype(jnp.bfloat16)
        self.row_blocks(product)

        @pl.when(block == blocks - 1)
        def _():
            def close(rows):
                back = rms_backward(big[5, rows].astype(jnp.float32), big[3, rows].astype(jnp.float32))
                big[3, rows] = (big[4, rows].astype(jnp.float32) + back).astype(jnp.bfloat16)
                if layer:
                    self.total[rows] = jnp.zeros((self.ROWS, self.width), jnp.float32)
            self.row_blocks(close)
            self.store(big.at[3], f"dx_{layer}", 0).start()
            if layer:
                self.load("h_0", big.at[4], 3).start()
                for copy in self.mlp_loads(0):
                    copy.start()

    def mlp_loads(self, block):
        slot = lax.rem(block, 2)
        lanes = pl.ds(pl.multiple_of(FF_BLOCK * block, FF_BLOCK), FF_BLOCK)
        half = pl.ds(pl.multiple_of(FF_BLOCK * slot, FF_BLOCK), FF_BLOCK)
        return [self.load("w_up", self.big.at[0, :, half], 5 + 3 * slot, slice(None), lanes),
                self.load("pre_0", self.big.at[1, :, half], 6 + 3 * slot, slice(None), lanes),
                self.load("w_down", self.big.at[5, half], 7 + 3 * slot, lanes)]

    def mlp_store(self, block):
        half = pl.ds(pl.multiple_of(FF_BLOCK * lax.rem(block, 2), FF_BLOCK), FF_BLOCK)
        lanes = pl.ds(pl.multiple_of(FF_BLOCK * block, FF_BLOCK), FF_BLOCK)
        return self.store(self.big.at[2, :, half], "dpre_0", 1, slice(None), lanes)

    def mlp_block(self, block):
        big, blocks = self.big, self.at["w_up"].shape[1] // FF_BLOCK

        @pl.when(block == 0)
        def _():
            self.store(big.at[3], "dx_1", 0).wait()
            self.load("h_0", big.at[4], 3).wait()
        for copy in self.mlp_loads(block):
            copy.wait()

        @pl.when(block + 1 < blocks)
        def _():
            for copy in self.mlp_loads(block + 1):
                copy.start()

        @pl.when(block > 0)
        def _():
            self.mlp_store(block - 1).wait()
        half = pl.ds(pl.multiple_of(FF_BLOCK * lax.rem(block, 2), FF_BLOCK), FF_BLOCK)

        def product(rows):
            d_act = dot(big[3, rows], big[5, half], 1, 1).astype(jnp.bfloat16).astype(jnp.float32)
            slope = gelu_parts(big[1, rows, half].astype(jnp.float32))[1]
            d_pre = (d_act * slope).astype(jnp.bfloat16)
            big[2, rows, half] = d_pre
            self.total[rows] += dot(d_pre, big[0, :, half], 1, 1)
        self.row_blocks(product)
        self.mlp_store(block).start()

        @pl.when(block == blocks - 1)
        def _():
            def close(rows):
                d_normed = self.total[rows].astype(jnp.bfloat16).astype(jnp.float32)
                back = rms_backward(big[4, rows].astype(jnp.float32), d_normed)
                big[4, rows] = (big[3, rows].astype(jnp.float32) + back).astype(jnp.bfloat16)
            self.row_blocks(close)
            self.store(big.at[4], "dh_0", 2).start()
            self.load("wo", big.at[0], 4, 0).start()
            for copy in self.piece_loads(0, 0):
                copy.start()

    def where(self, piece):
        seq, half = lax.rem(piece, self.seqs), lax.div(piece, self.seqs)
        rows = pl.ds(pl.multiple_of(self.seq * seq, self.seq), self.seq)
        lanes = pl.ds(pl.multiple_of(self.width // 2 * half, self.width // 2), self.width // 2)
        return seq, half, rows, lanes

    def piece_loads(self, layer, piece):
        seq, half, rows, lanes = self.where(piece)
        near = pl.ds(0, self.width // 2)
        copies = [self.load(f"{kind}_{layer}", self.big.at[1 + lax.rem(piece, 2), pl.ds(self.seq * i, self.seq), near], i, rows, lanes)
                  for i, kind in enumerate("qkv")]
        heads = pl.ds(self.heads // 2 * half, self.heads // 2)
        return copies + [self.load(f"probs_{layer}", self.p.at[lax.rem(piece, 2)], 5, seq, heads)]

    def piece_stores(self, layer, piece):
        _, _, rows, lanes = self.where(piece)
        near, spot = pl.ds(0, self.width // 2), 5 - 2 * lax.rem(piece, 2)
        sources = [self.big.at[spot, pl.ds(self.seq * i, self.seq), near] for i in range(3)]
        if layer:
            return [self.store(src, f"d{kind}b_1", 3 + i, rows) for i, (src, kind) in enumerate(zip(sources, "qkv"))]
        return [self.store(src, f"d{kind}_0", 3 + i, rows, lanes) for i, (src, kind) in enumerate(zip(sources, "qkv"))]

    def attention_piece(self, layer, piece):
        big, p_buf, pieces = self.big, self.p, 2 * self.seqs
        _, half, rows, _ = self.where(piece)
        parity = lax.rem(piece, 2)
        spot, out = 1 + parity, 5 - 2 * parity

        start = self.seqs * layer

        @pl.when(piece == start)
        def _():
            if layer == 0:
                self.mlp_store(self.at["w_up"].shape[1] // FF_BLOCK - 1).wait()
                self.store(big.at[4], "dh_0", 2).wait()
            else:
                self.load("dh_1", big.at[4], 3).wait()
            self.load("wo", big.at[0], 4, layer).wait()

        @pl.when(piece > start)
        def _():
            for copy in self.piece_stores(layer, piece - 1):
                copy.wait()
        for copy in self.piece_loads(layer, piece):
            copy.wait()

        @pl.when(piece + 1 < pieces)
        def _():
            for copy in self.piece_loads(layer, piece + 1):
                copy.start()
        low = lax.broadcasted_iota(jnp.int32, (self.seq, PAIR), 1) < HEAD_DIM

        def unmix(unit):
            w_rows = pl.ds(pl.multiple_of(self.width // 2 * half + OUT_BLOCK * unit, OUT_BLOCK), OUT_BLOCK)
            d_mixed = dot(big[4, rows], big[0, w_rows], 1, 1)
            big[spot, pl.ds(3 * self.seq, self.seq), pl.ds(OUT_BLOCK * unit, OUT_BLOCK)] = d_mixed.astype(jnp.bfloat16)

        def pair_of(j):
            return tuple(big[spot, pl.ds(self.seq * i, self.seq), pl.ds(PAIR * j, PAIR)] for i in range(4))

        def put(j, values):
            for i, value in enumerate(values):
                big[out, pl.ds(self.seq * i, self.seq), pl.ds(PAIR * j, PAIR)] = value.astype(jnp.bfloat16)
        size = OUT_BLOCK // PAIR
        stages = backward_stages(pair_of, lambda j, side: p_buf[parity, 2 * j + side], put, low)
        staged(self.heads // 4 // size, in_units(unmix, stages, size))
        for copy in self.piece_stores(layer, piece):
            copy.start()

    def begin(self):
        self.load("dh_1", self.big.at[4], 3).start()
        self.load("wo", self.big.at[0], 4, 1).start()
        for copy in self.piece_loads(1, self.seqs):
            copy.start()

    def item(self, step):
        blocks = self.width // OUT_BLOCK
        pieces = 2 * self.seqs

        @pl.when(step < 3)
        def _():
            first = self.seqs + step
            count = jnp.where(step == 2, self.seqs - 2, 1)
            lax.fori_loop(first, first + count, lambda piece, carry: self.attention_piece(1, piece) or carry, 0)

        @pl.when(step == 3)
        def _():
            for copy in self.piece_stores(1, pieces - 1):
                copy.wait()
            for copy in self.input_loads(1) + self.weight_loads(1, 0):
                copy.start()

        @pl.when(between(step, self.PB_1, 2))
        def _():
            first = blocks // 2 * (step - self.PB_1)
            lax.fori_loop(first, first + blocks // 2, lambda block, carry: self.input_block(1, block) or carry, 0)
        pl.when(between(step, self.MB, 8))(lambda: self.mlp_block(step - self.MB))
        pl.when(between(step, self.AB, pieces))(lambda: self.attention_piece(0, step - self.AB))

        @pl.when(step == self.PB_0 - 1)
        def _():
            for copy in self.piece_stores(0, pieces - 1):
                copy.wait()
            for copy in self.input_loads(0) + self.weight_loads(0, 0):
                copy.start()
        pl.when(between(step, self.PB_0, blocks))(lambda: self.input_block(0, step - self.PB_0))

        @pl.when(step == self.PB_0 + blocks)
        def _():
            self.store(self.big.at[3], "dx_0", 0).wait()


def finish_kernel(groups, chunks, in_names, out_names, remote, *refs):
    names = [*in_names, *out_names]
    at, scratch = dict(zip(names, refs[:len(names)])), refs[len(names):]
    (big, total_buf, w_buf, p_buf, item_sem, drain_sem), scratch = scratch[:6], scratch[6:]
    backward = Backward(at, big, total_buf, w_buf, p_buf, item_sem, drain_sem)
    if not remote:
        backward.begin()

        def alone(step, carry):
            backward.item(step)
            return carry
        lax.fori_loop(0, chunks + WRITE_AT + 1, alone, 0)
        return
    (lhs_buf, rhs_buf, own, part, part_in, gath), scratch = scratch[:6], scratch[6:]
    land_keys = [key for key, st in enumerate(STAGES) if st[1].startswith("rs")]
    landing = dict(zip(land_keys, scratch[:len(land_keys)]))
    load_sem, send_sem, recv_sem, pair_send, pair_recv, out_sem, out_send, out_recv, credit = scratch[len(land_keys):]

    me = lax.axis_index("data")
    core = lax.rem(me, 2)
    coord = {"x": lax.rem(lax.div(me, 2), 2), "y": lax.rem(lax.div(me, 4), 2)}
    z = lax.div(me, 8)
    partner = me + 1 - 2 * core
    near = {"x": me + 2 - 4 * coord["x"], "y": me + 4 - 8 * coord["y"]}
    up_ok, down_ok = z < 3, z > 0
    peers = [(partner, 0, None), (near["x"], 1, None), (near["y"], 2, None), (me + 8, 3, up_ok), (me - 8, 4, down_ok)]

    def guarded(cond, fn):
        if cond is None:
            fn()
        else:
            pl.when(cond)(fn)

    barrier = pltpu.get_barrier_semaphore()
    for dev, _, cond in peers:
        guarded(cond, lambda dev=dev: pl.semaphore_signal(barrier, inc=1, device_id=(dev,), device_id_type=MESH))
    inner = jnp.logical_and(up_ok, down_ok)
    guarded(inner, lambda: pl.semaphore_wait(barrier, 5))
    guarded(jnp.logical_not(inner), lambda: pl.semaphore_wait(barrier, 4))

    def region(name, kind, which):
        _, row, rows, order = TYPES[name]
        if order[2] == "z":
            h1, h2 = coord[order[0]], coord[order[1]]
            if kind == "1":
                return pl.ds(row, rows), pl.ds(pl.multiple_of(512 * which, 128), 512)
            if kind == "2":
                return pl.ds(row, rows), pl.ds(pl.multiple_of(512 * h1 + 256 * which, 128), 256)
            first = pl.multiple_of(row + (rows // 2) * lax.div(which, 2), 8)
            lane = pl.multiple_of(512 * h1 + 256 * h2 + 128 * lax.rem(which, 2), 128)
            return pl.ds(first, rows // 2), pl.ds(lane, 128)
        h1 = coord[order[1]]
        if kind == "z":
            first = pl.multiple_of(row + (rows // 2) * lax.div(which, 2), 8)
            return pl.ds(first, rows // 2), pl.ds(pl.multiple_of(512 * lax.rem(which, 2), 128), 512)
        first = pl.multiple_of(row + (rows // 2) * lax.div(z, 2), 8)
        if kind == "1":
            return pl.ds(first, rows // 2), pl.ds(pl.multiple_of(512 * lax.rem(z, 2) + 256 * which, 128), 256)
        lane = pl.multiple_of(512 * lax.rem(z, 2) + 256 * h1 + 128 * which, 128)
        return pl.ds(first, rows // 2), pl.ds(lane, 128)

    def exchange_axis(name, kind):
        order = TYPES[name][3]
        dims = order[:2] if order[2] == "z" else order[1:]
        return dims[int(kind) - 1]

    def plan(key, chunk, parity):
        name, kind, step, way, _ = STAGES[key]
        mine, slot = lax.rem(chunk, OWN_SLOTS), lax.rem(chunk, AG_SLOTS)
        if kind in ("rs1", "rs2"):
            axis = exchange_axis(name, kind[2])
            src, keep = region(name, kind[2], 1 - coord[axis]), region(name, kind[2], coord[axis])
            dev, send_ok, recv_ok = near[axis], None, None
            sent = own.at[mine, src[0], src[1]]
        elif kind in ("ag1", "ag2"):
            axis = exchange_axis(name, kind[2])
            src = keep = region(name, kind[2], coord[axis])
            dev, send_ok, recv_ok = near[axis], None, None
            sent = gath.at[slot, src[0], src[1]]
        elif kind == "rsz":
            if way:
                dev, k_send, k_keep = me + 8, z + 3 - step, z + 2 - step
                send_ok, recv_ok = k_send <= 3, jnp.logical_and(k_keep <= 3, down_ok)
            else:
                dev, k_send, k_keep = me - 8, z - 3 + step, z - 2 + step
                send_ok, recv_ok = k_send >= 0, jnp.logical_and(k_keep >= 0, up_ok)
            src, keep = region(name, "z", k_send), region(name, "z", k_keep)
            sent = own.at[mine, src[0], src[1]]
        else:
            if way:
                dev, k_send, k_keep = me + 8, z - step, z - 1 - step
                send_ok, recv_ok = jnp.logical_and(k_send >= 0, up_ok), k_keep >= 0
            else:
                dev, k_send, k_keep = me - 8, z + step, z + 1 + step
                send_ok, recv_ok = jnp.logical_and(k_send <= 3, down_ok), k_keep <= 3
            src, keep = region(name, "z", k_send), region(name, "z", k_keep)
            sent = gath.at[slot, src[0], src[1]]
        sems = dict(send_sem=send_sem.at[key, parity], recv_sem=recv_sem.at[key, parity], device_id=(dev,), device_id_type=MESH)
        if kind.startswith("rs"):
            target = landing[key].at[parity]
            send = lambda: pltpu.make_async_remote_copy(src_ref=sent, dst_ref=target, **sems)
            recv = lambda: pltpu.make_async_remote_copy(
                src_ref=own.at[mine, keep[0], keep[1]], dst_ref=target, **sems)

            def arrive():
                own[mine, keep[0], keep[1]] += landing[key][parity]
        else:
            send = lambda: pltpu.make_async_remote_copy(src_ref=sent, dst_ref=sent, **sems)
            recv = lambda: pltpu.make_async_remote_copy(
                src_ref=gath.at[slot, keep[0], keep[1]], dst_ref=gath.at[slot, keep[0], keep[1]], **sems)
            arrive = None
        return send, recv, send_ok, recv_ok, arrive

    def finish(name, chunk):
        order = TYPES[name][3]
        reg = region(name, "z", z) if order[2] == "z" else region(name, "2", coord[order[2]])
        gath[lax.rem(chunk, AG_SLOTS), reg[0], reg[1]] = own[lax.rem(chunk, OWN_SLOTS), reg[0], reg[1]]

    def valid(chunk):
        return jnp.logical_and(chunk >= 0, chunk < chunks)

    def set_rows(half):
        return pl.ds(half * SET_ROWS, SET_ROWS)

    def pair_copy(half, parity):
        return pltpu.make_async_remote_copy(
            src_ref=part.at[parity, set_rows(half)], dst_ref=part_in.at[parity, set_rows(half)],
            send_sem=pair_send.at[half], recv_sem=pair_recv.at[half, parity], device_id=(partner,), device_id_type=MESH)

    half_lanes = LANES // 2

    def outlets(half, group, local, whose):
        out, layer = group["out"]
        ref = at[out] if layer is None else at[out].at[layer]
        rows, cols = group["place"](local)
        if not group["narrow"]:
            first = pl.multiple_of(rows + CORE_ROWS * whose + half * SET_ROWS, SET_ROWS)
            return [(pl.ds(0, LANES), ref.at[pl.ds(first, SET_ROWS), pl.ds(pl.multiple_of(cols, 128), LANES)])]
        places = []
        for sub in (0, 1):
            first = pl.multiple_of(2 * CORE_ROWS * whose + CORE_ROWS * sub + half * SET_ROWS, SET_ROWS)
            places.append((pl.ds(half_lanes * sub, half_lanes), ref.at[pl.ds(first, SET_ROWS), pl.ds(cols, half_lanes)]))
        return places

    def write_copies(half, chunk, lanes, dest):
        slot = lax.rem(chunk, AG_SLOTS)
        src = gath.at[slot, set_rows(half), lanes]
        here = pltpu.make_async_copy(src, dest, out_sem.at[half])
        there = pltpu.make_async_remote_copy(
            src_ref=src, dst_ref=dest, send_sem=out_send.at[half], recv_sem=out_recv.at[half, lax.rem(chunk, 2)],
            device_id=(partner,), device_id_type=MESH)
        return here, there

    def load_copies(group, local, slot):
        rows, cols = group["place"](local)
        narrow = group["narrow"]
        lhs, rhs = [], []
        for sub in range(2 if narrow else len(group["lhs"])):
            for whose in (0, 1):
                owner = core if whose == 0 else 1 - core
                first = 2 * CORE_ROWS * owner + CORE_ROWS * sub if narrow else rows + CORE_ROWS * owner
                source = at[group["lhs"][0 if narrow else sub]]
                lhs.append(pltpu.make_async_copy(
                    source.at[:, pl.ds(pl.multiple_of(first, CORE_ROWS), CORE_ROWS)],
                    lhs_buf.at[slot, sub, whose], load_sem.at[slot, sub, whose]))
        for app, name in enumerate(group["rhs"]):
            size = half_lanes if narrow else LANES
            rhs.append(pltpu.make_async_copy(
                at[name].at[:, pl.ds(0 if narrow else pl.multiple_of(cols, 128), size)], rhs_buf.at[slot, app, :, pl.ds(0, size)],
                load_sem.at[slot, app, 2]))
        return lhs, rhs

    def for_group(chunk, fn):
        for group in groups:
            inside = jnp.logical_and(chunk >= group["start"], chunk < group["start"] + group["count"])
            pl.when(inside)(functools.partial(fn, group, chunk - group["start"]))

    def among(chunk, chosen):
        flags = [jnp.logical_and(chunk >= g["start"], chunk < g["start"] + g["count"]) for g in groups if chosen(g)]
        return functools.reduce(jnp.logical_or, flags)

    def is_two(group):
        return len(group["lhs"]) == 2

    def is_narrow(group):
        return group["narrow"]

    def start_load(chunk):
        def go(group, local):
            for copy in sum(load_copies(group, local, lax.rem(chunk, 2)), []):
                copy.start()
        for_group(chunk, go)

    def wait_load(chunk):
        slot = lax.rem(chunk, 2)
        two_lhs, two_rhs = load_copies(next(filter(is_two, groups)), 0, slot)
        slim_lhs, slim_rhs = load_copies(next(filter(is_narrow, groups)), 0, slot)
        for copy in two_lhs[:2]:
            copy.wait()

        @pl.when(jnp.logical_not(among(chunk, is_narrow)))
        def _():
            two_rhs[0].wait()

        @pl.when(among(chunk, is_narrow))
        def _():
            for copy in slim_rhs + slim_lhs[2:]:
                copy.wait()

        @pl.when(among(chunk, is_two))
        def _():
            for copy in two_lhs[2:] + two_rhs[1:]:
                copy.wait()

    def tile(chunk):
        slot, mine, parity = lax.rem(chunk, 2), lax.rem(chunk, OWN_SLOTS), lax.rem(chunk, 2)

        def product(sub, whose, rhs):
            return dot(lhs_buf[slot, sub, whose], rhs, 0, 0)

        @pl.when(among(chunk, is_narrow))
        def _():
            for sub in (0, 1):
                lanes, rhs = pl.ds(half_lanes * sub, half_lanes), rhs_buf[slot, 0, :, pl.ds(0, half_lanes)]
                own[mine, :, lanes] = product(sub, 0, rhs)
                part[parity, :, lanes] = product(sub, 1, rhs)

        @pl.when(jnp.logical_not(among(chunk, is_narrow)))
        def _():
            own[mine] = product(0, 0, rhs_buf[slot, 0])
            part[parity] = product(0, 1, rhs_buf[slot, 0])

        @pl.when(among(chunk, is_two))
        def _():
            own[mine] += product(1, 0, rhs_buf[slot, 1])
            part[parity] += product(1, 1, rhs_buf[slot, 1])

    last = chunks + WRITE_AT

    def section(half, step):
        before = lax.rem(step + 1, 2)
        now = lax.rem(step, 2)
        names = [name for name in TYPES if TYPES[name][0] == half]
        at_stage = {}
        for key, (name, _, _, _, at) in enumerate(STAGES):
            if name in names:
                at_stage.setdefault((at, name), []).append(key)
        finals = {name: max(st[4] for st in STAGES if st[0] == name and st[1].startswith("rs")) for name in names}

        def start(at, name):
            chunk = step - at

            @pl.when(valid(chunk))
            def _():
                for key in at_stage[at, name]:
                    send, _, send_ok, _, _ = plan(key, chunk, now)
                    guarded(send_ok, lambda send=send: send().start())

        def finish_stage(at, name):
            chunk = step - 1 - at

            @pl.when(valid(chunk))
            def _():
                for key in at_stage[at, name]:
                    send, recv, send_ok, recv_ok, arrive = plan(key, chunk, before)

                    def arrived(recv=recv, arrive=arrive):
                        recv().wait_recv()
                        if arrive is not None:
                            arrive()
                    guarded(recv_ok, arrived)
                    guarded(send_ok, lambda send=send: send().wait_send())
                if at == finals[name]:
                    finish(name, chunk)

        @pl.when(step > 0)
        def _():
            for dev, way, cond in peers:
                guarded(cond, lambda way=way: pl.semaphore_wait(credit.at[half, way], 1))

        @pl.when(valid(step - 1))
        def _():
            copy = pair_copy(half, before)
            copy.wait_send()
            copy.wait_recv()
            mine = lax.rem(step - 1, OWN_SLOTS)
            own[mine, set_rows(half)] += part_in[before, set_rows(half)]

        done = step - 1 - WRITE_AT

        @pl.when(valid(done))
        def _():
            (lanes, dest), = outlets(half, next(filter(is_two, groups)), 0, 0)
            here, there = write_copies(half, done, lanes, dest)
            here.wait()
            there.wait_send()
            there.wait_recv()

        held = [(1, name) for name in names]
        for at in range(1, WRITE_AT):
            for name in names:
                finish_stage(at, name)
                start(*held.pop(0))
                if at + 1 < WRITE_AT:
                    held.append((at + 1, name))
        out_chunk = step - WRITE_AT

        @pl.when(step < last)
        def _():
            for dev, way, cond in peers:
                to = way if way < 3 else 7 - way
                guarded(cond, lambda dev=dev, to=to: pl.semaphore_signal(
                    credit.at[half, to], inc=1, device_id=(dev,), device_id_type=MESH))

        @pl.when(valid(out_chunk))
        def _():
            def go(group, local):
                for lanes, dest in outlets(half, group, local, core):
                    for copy in write_copies(half, out_chunk, lanes, dest):
                        copy.start()
            for_group(out_chunk, go)

    backward.begin()
    start_load(jnp.int32(0))

    def round_(step, carry):
        section(0, step)

        @pl.when(valid(step))
        def _():
            pl.when(step + 1 < chunks)(lambda: start_load(step + 1))
            wait_load(step)
            tile(step)
            pair_copy(0, lax.rem(step, 2)).start()

        section(1, step)

        @pl.when(valid(step))
        def _():
            pair_copy(1, lax.rem(step, 2)).start()

        backward.item(step)
        return carry

    lax.fori_loop(0, last + 1, round_, 0)


def finish_backward(inputs, groups, chunks, weights, tokens, seq, collective_id=0, remote=True):
    width, ff = inputs["w_up"].shape
    landing = [pltpu.VMEM((2,) + piece_shape(st[0], st[1]), jnp.float32) for st in STAGES if st[1].startswith("rs")]
    apps = 2
    outs = {name: jax.ShapeDtypeStruct(shape, jnp.float32) for name, shape in weights.items()}
    for name in ("dx_0", "dx_1", "dh_0", "dq_0", "dk_0", "dv_0"):
        outs[name] = bf16(tokens, width)
    for name in ("dqb_1", "dkb_1", "dvb_1"):
        outs[name] = bf16(tokens, width // 2)
    outs["dpre_0"] = bf16(tokens, ff)
    heads = width // HEAD_DIM
    scratch = [
        pltpu.VMEM((6, tokens, width), jnp.bfloat16),
        pltpu.VMEM((tokens, width), jnp.float32),
        pltpu.VMEM((2, 3, OUT_BLOCK, width), jnp.bfloat16),
        pltpu.VMEM((2, heads // 2, seq, seq), jnp.bfloat16),
        pltpu.SemaphoreType.DMA((14,)),
        pltpu.SemaphoreType.DMA((6,)),
    ]
    if remote:
        scratch += [
            pltpu.VMEM((2, apps, 2, tokens, CORE_ROWS), jnp.bfloat16),
            pltpu.VMEM((2, apps, tokens, LANES), jnp.bfloat16),
            pltpu.VMEM((OWN_SLOTS, CORE_ROWS, LANES), jnp.float32),
            pltpu.VMEM((2, CORE_ROWS, LANES), jnp.float32),
            pltpu.VMEM((2, CORE_ROWS, LANES), jnp.float32),
            pltpu.VMEM((AG_SLOTS, CORE_ROWS, LANES), jnp.float32),
            *landing,
            pltpu.SemaphoreType.DMA((2, apps, 3)),
            pltpu.SemaphoreType.DMA((len(STAGES), 2)),
            pltpu.SemaphoreType.DMA((len(STAGES), 2)),
            pltpu.SemaphoreType.DMA((2,)),
            pltpu.SemaphoreType.DMA((2, 2)),
            pltpu.SemaphoreType.DMA((2,)),
            pltpu.SemaphoreType.DMA((2,)),
            pltpu.SemaphoreType.DMA((2, 2)),
            pltpu.SemaphoreType.REGULAR((2, 5)),
        ]
    params = dict(collective_id=collective_id, has_side_effects=True) if remote else {}
    results = pl.pallas_call(
        functools.partial(finish_kernel, groups, chunks, list(inputs), list(outs), remote),
        out_shape=list(outs.values()),
        in_specs=[pl.BlockSpec(memory_space=pl.ANY)] * len(inputs),
        out_specs=[pl.BlockSpec(memory_space=pl.ANY)] * len(outs),
        scratch_shapes=scratch,
        compiler_params=pltpu.CompilerParams(vmem_limit_bytes=67_043_328, **params),
        cost_estimate=pl.CostEstimate(flops=20 * tokens * width * ff, bytes_accessed=256 * MIB, transcendentals=0),
        name="finish_backward",
    )(*inputs.values())
    return dict(zip(outs, results))


DELIVER_ROWS = 256
DELIVER_SLOTS = 40
DELIVER_AHEAD = 20


def deliver(arrays, small):
    def blocks_of(array):
        lead = [(i,) for i in range(array.shape[0])] if len(array.shape) == 3 else [()]
        rows, cols = array.shape[-2:]
        return [(*index, pl.ds(row, DELIVER_ROWS), pl.ds(col, LANES))
                for index in lead for row in range(0, rows, DELIVER_ROWS) for col in range(0, cols, LANES)]

    work = [(i, index) for i, array in enumerate(arrays) for index in blocks_of(array)]
    count = len(arrays) + 1

    def kernel(*refs):
        ins, outs, buf, whole_buf, in_sem, out_sem, whole_sem = refs[:count], refs[count:2 * count], *refs[2 * count:]
        whole_in = pltpu.make_async_copy(ins[-1], whole_buf, whole_sem.at[0])
        whole_out = pltpu.make_async_copy(whole_buf, outs[-1], whole_sem.at[1])

        def fetch(t):
            i, index = work[t]
            return pltpu.make_async_copy(ins[i].at[index], buf.at[t % DELIVER_SLOTS], in_sem.at[t % DELIVER_SLOTS])

        def put(t):
            i, index = work[t]
            return pltpu.make_async_copy(buf.at[t % DELIVER_SLOTS], outs[i].at[index], out_sem.at[t % DELIVER_SLOTS])

        whole_in.start()
        for t in range(min(DELIVER_AHEAD, len(work))):
            fetch(t).start()
        whole_in.wait()
        whole_out.start()
        for t in range(len(work)):
            if t + DELIVER_AHEAD < len(work):
                if t + DELIVER_AHEAD >= DELIVER_SLOTS:
                    put(t + DELIVER_AHEAD - DELIVER_SLOTS).wait()
                fetch(t + DELIVER_AHEAD).start()
            fetch(t).wait()
            put(t).start()
        for t in range(max(0, len(work) - DELIVER_SLOTS), len(work)):
            put(t).wait()
        whole_out.wait()

    return pl.pallas_call(
        kernel,
        out_shape=[jax.ShapeDtypeStruct(array.shape, array.dtype) for array in (*arrays, small)],
        in_specs=[pl.BlockSpec(memory_space=pl.ANY)] * count,
        out_specs=[pl.BlockSpec(memory_space=pl.ANY)] * count,
        scratch_shapes=[pltpu.VMEM((DELIVER_SLOTS, DELIVER_ROWS, LANES), jnp.float32), pltpu.VMEM(small.shape, small.dtype),
                        pltpu.SemaphoreType.DMA((DELIVER_SLOTS,)), pltpu.SemaphoreType.DMA((DELIVER_SLOTS,)),
                        pltpu.SemaphoreType.DMA((2,))],
        compiler_params=pltpu.CompilerParams(vmem_limit_bytes=67_043_328),
        cost_estimate=pl.CostEstimate(flops=0, bytes_accessed=2 * sum(a.size for a in arrays) * 4, transcendentals=0),
        name="deliver",
    )(*arrays, small)


def gradient_groups(width, ff):
    groups = []

    def add(count, lhs, rhs, out, place, narrow=False):
        start = groups[-1]["start"] + groups[-1]["count"] if groups else 0
        groups.append(dict(start=start, count=count, lhs=lhs, rhs=rhs, out=out, place=place, narrow=narrow))

    def tall(local):
        return TILE_ROWS * local, 0

    def wide(local):
        return TILE_ROWS * lax.rem(local, width // TILE_ROWS), LANES * lax.div(local, width // TILE_ROWS)

    for half in (0, 1):
        for kind in "qkv":
            add(1, ["u_1"], [f"d{kind}{'ab'[half]}_1"], (f"g_{kind}", 1), lambda local, half=half: (0, width // 2 * half), narrow=True)
        if half == 0:
            add(width // TILE_ROWS, ["mixed_1"], ["dh_1"], ("g_o", 1), tall)
    add(ff // TILE_ROWS, ["act_0", "act_1"], ["dx_1", "cot"], ("g_down", None), tall)
    add(ff // TILE_ROWS, ["n_0", "n_1"], ["dpre_0", "dpre_1"], ("g_up", None), wide)
    for kind in "qkv":
        add(width // TILE_ROWS, ["u_0"], [f"d{kind}_0"], (f"g_{kind}", 0), tall)
    add(width // TILE_ROWS, ["mixed_0"], ["dh_0"], ("g_o", 0), tall)
    return groups, sum(group["count"] for group in groups)


def local_operands(x_init, cot_out, w_query, w_key, w_value, w_proj, w_up, w_down):
    batch, seq, width = x_init.shape
    tokens = batch * seq
    at = {"x_0": x_init.reshape(tokens, width), "cot": cot_out.reshape(tokens, width)}
    at.update(wq=w_query, wk=w_key, wv=w_value, wo=w_proj, w_up=w_up, w_down=w_down)
    at.update(front(at, batch, seq))
    return at


def solution(mesh):
    def local_step(x_init, cot_out, w_query, w_key, w_value, w_proj, w_up, w_down):
        batch, seq, width = x_init.shape
        inputs = local_operands(x_init, cot_out, w_query, w_key, w_value, w_proj, w_up, w_down)
        groups, chunks = gradient_groups(width, w_up.shape[1])
        weights = dict(g_q=w_query.shape, g_k=w_key.shape, g_v=w_value.shape, g_o=w_proj.shape, g_up=w_up.shape, g_down=w_down.shape)
        res = finish_backward(inputs, groups, chunks, weights, batch * seq, seq)
        *grads, d_init = deliver([res[name] for name in weights], res["dx_0"])
        return (*grads, d_init.reshape(x_init.shape))

    data_spec = P("data")
    full_spec = P()
    in_specs = (data_spec, data_spec, full_spec, full_spec, full_spec, full_spec, full_spec, full_spec)
    out_specs = (full_spec, full_spec, full_spec, full_spec, full_spec, full_spec, data_spec)
    return jax.shard_map(local_step, mesh=mesh, in_specs=in_specs, out_specs=out_specs, check_vma=False)
```

```python
import functools

import jax
import jax.numpy as jnp
from jax import lax
from jax.experimental import pallas as pl
from jax.experimental.pallas import tpu as pltpu
from jax.sharding import PartitionSpec as P

EPS = 1e-6
HEAD_DIM = 64
PAIR = 2 * HEAD_DIM
FF_BLOCK = 512
OUT_BLOCK = 256
GELU_A = (2.0 / 3.141592653589793) ** 0.5
GELU_B = 0.044715
SOFTMAX_SCALE = HEAD_DIM ** -0.5 * 1.4426950408889634
MIB = 1024 * 1024


def dot(lhs, rhs, lhs_dim, rhs_dim):
    return lax.dot_general(lhs, rhs, (((lhs_dim,), (rhs_dim,)), ((), ())), preferred_element_type=jnp.float32)


def rms_norm(x_f32):
    return x_f32 * lax.rsqrt(jnp.mean(x_f32 * x_f32, axis=-1, keepdims=True) + EPS)


def rms_backward(x_f32, d_out):
    scale = lax.rsqrt(jnp.mean(x_f32 * x_f32, axis=-1, keepdims=True) + EPS)
    inner = jnp.mean(x_f32 * d_out, axis=-1, keepdims=True)
    return scale * d_out - x_f32 * (scale * scale * scale * inner)


def gelu_parts(pre):
    square = pre * pre
    tanh = jnp.tanh(GELU_A * (pre + GELU_B * pre * square))
    half = 0.5 * (1.0 + tanh)
    slope = half + 0.5 * pre * (1.0 - tanh * tanh) * (GELU_A + (3.0 * GELU_A * GELU_B) * square)
    return pre * half, slope


def bf16(*shape):
    return jax.ShapeDtypeStruct(shape, jnp.bfloat16)


def backward_stages(pair_of, probs_of, put, low):
    masks = (low, jnp.logical_not(low))

    def from_mixed(j, _=None):
        _, _, v_pair, d_pair = pair_of(j)
        return [dot(v_pair, jnp.where(mask, d_pair, 0), 1, 1).astype(jnp.bfloat16) for mask in masks]

    def through(j, made):
        out = []
        for side, d_probs in enumerate(made):
            d_probs, probs = d_probs.astype(jnp.float32), probs_of(j, side).astype(jnp.float32)
            row_dot = jnp.sum(d_probs * probs, axis=0, keepdims=True)
            out.append((probs * (d_probs - row_dot) * HEAD_DIM ** -0.5).astype(jnp.bfloat16))
        return out

    def to_inputs(j, made):
        q_pair, k_pair, _, d_pair = pair_of(j)
        sides = [(dot(d_scores, k_pair, 0, 0), dot(d_scores, q_pair, 1, 0), dot(probs_of(j, side), d_pair, 1, 0))
                 for side, d_scores in enumerate(made)]
        put(j, [jnp.where(low, first, second) for first, second in zip(*sides)])
    return from_mixed, through, to_inputs


def forward_stages(pair_of, keep, put, low):
    def scores(j, _=None):
        q_pair, k_pair, _ = pair_of(j)
        return [dot(k_pair, jnp.where(mask, q_pair, 0), 1, 1) for mask in (low, jnp.logical_not(low))]

    def soften(j, made):
        out = []
        for side, score in enumerate(made):
            top = jnp.max(score, axis=0, keepdims=True)
            raised = jnp.exp2((score - top) * SOFTMAX_SCALE)
            inverse = 1.0 / jnp.sum(raised, axis=0, keepdims=True)
            out.append((raised * inverse).astype(jnp.bfloat16))
            keep(j, side, out[-1])
        return out

    def mix(j, made):
        first, second = (dot(probs, pair_of(j)[2], 0, 0) for probs in made)
        put(j, jnp.where(low, first, second))
    return scores, soften, mix


def in_units(first, stages, size):
    def lift(stage):
        return lambda unit, made: [stage(size * unit + i, made[i]) for i in range(size)]
    return (lambda unit: first(unit) or [None] * size, *map(lift, stages))


def staged(count, stages):
    made = [None] * count
    for turn in range(count + len(stages) - 1):
        for depth, stage in enumerate(stages):
            j = turn - depth
            if 0 <= j < count:
                made[j] = stage(j, made[j]) if depth else stage(j)


FRONT_OUTS = ("u_0", "q_0", "k_0", "v_0", "probs_0", "mixed_0", "h_0", "n_0", "pre_0", "act_0", "x_1",
              "u_1", "q_1", "k_1", "v_1", "probs_1", "mixed_1", "n_1", "act_1", "dpre_1", "dh_1", "dqa_1", "dka_1", "dva_1")
ROW_BUFFERS = ("u", "q", "k", "v", "mixed", "h", "n", "x", "dh", "dn")
HALF_BUFFERS = ("dqa", "dka", "dva")
WIDE_BLOCK = 1024


def front_kernel(batch, seq, in_names, *refs):
    at = dict(zip((*in_names, *FRONT_OUTS), refs))
    refs = refs[len(at):]
    x_all, cot_all, w_in, w_out, w_up, w_down, probs, pre, act = refs[:9]
    row = dict(zip((*ROW_BUFFERS, *HALF_BUFFERS), refs[9:]))
    load_sem, out_sem = refs[9 + len(row):]
    width, ff = w_up.shape
    heads = width // HEAD_DIM
    loads = {"x": pltpu.make_async_copy(at["x_0"], x_all, load_sem.at[0])}
    for layer in (0, 1):
        for i, name in enumerate(("wq", "wk", "wv")):
            loads[f"{name}_{layer}"] = pltpu.make_async_copy(at[name].at[layer], w_in.at[layer, i], load_sem.at[1 + 4 * layer + i])
        loads[f"wo_{layer}"] = pltpu.make_async_copy(at["wo"].at[layer], w_out.at[layer], load_sem.at[4 + 4 * layer])
    loads["w_up"] = pltpu.make_async_copy(at["w_up"], w_up, load_sem.at[9])
    loads["w_down"] = pltpu.make_async_copy(at["w_down"], w_down, load_sem.at[10])
    loads["cot"] = pltpu.make_async_copy(at["cot"], cot_all, load_sem.at[11])
    for name in ("x", "wq_0", "wk_0", "wv_0"):
        loads[name].start()
    holders = {"probs_0": probs, "probs_1": probs, "pre_0": pre, "act_0": act, "act_1": act, "dpre_1": pre, "x_1": row["x"]}
    for name in FRONT_OUTS:
        holders.setdefault(name, row.get(name[:-2]))

    def store(name, index):
        src = holders[name]
        rows = pl.ds(pl.multiple_of(seq * index, seq), seq)
        dest = at[name].at[index] if name.startswith("probs") else at[name].at[rows]
        return pltpu.make_async_copy(src, dest, out_sem.at[FRONT_OUTS.index(name)])

    def one_sequence(index, carry):
        rows = pl.ds(pl.multiple_of(seq * index, seq), seq)
        first = index == 0
        low = lax.broadcasted_iota(jnp.int32, (seq, PAIR), 1) < HEAD_DIM

        def need(*names):
            @pl.when(first)
            def _():
                for name in names:
                    loads[name].wait()

        def launch(*names):
            @pl.when(first)
            def _():
                for name in names:
                    loads[name].start()

        def free(*names, same=False):
            for name in names:
                if same:
                    store(name, index).wait()
                else:
                    pl.when(index > 0)(lambda name=name: store(name, index - 1).wait())

        def send(*names):
            for name in names:
                store(name, index).start()

        def over(count, fn):
            for j in range(count):
                fn(j)

        def wide(j):
            return pl.ds(WIDE_BLOCK * j, WIDE_BLOCK)

        def attention(layer):
            x_in = x_all[rows] if layer == 0 else row["x"][...]
            row["u"][...] = rms_norm(x_in.astype(jnp.float32)).astype(jnp.bfloat16)
            need(*(f"w{kind}_{layer}" for kind in "qkv"))
            if layer == 0:
                launch("wo_0", "w_up")

            def project(unit):
                lanes = pl.ds(OUT_BLOCK * unit, OUT_BLOCK)
                for i, kind in enumerate("qkv"):
                    row[kind][:, lanes] = dot(row["u"][...], w_in[layer, i, :, lanes], 1, 0).astype(jnp.bfloat16)

            def pair_of(j):
                return tuple(row[kind][:, PAIR * j:PAIR * (j + 1)] for kind in "qkv")

            def keep(j, side, value):
                probs[2 * j + side] = value

            def put(j, value):
                row["mixed"][:, PAIR * j:PAIR * (j + 1)] = value.astype(jnp.bfloat16)
            size = OUT_BLOCK // PAIR
            staged(heads // 2 // size, in_units(project, forward_stages(pair_of, keep, put, low), size))
            need(f"wo_{layer}")
            attn = dot(row["mixed"][...], w_out[layer], 1, 0).astype(jnp.bfloat16)
            hidden = (x_in.astype(jnp.float32) + attn.astype(jnp.float32)).astype(jnp.bfloat16)
            row["h"][...] = hidden
            row["n"][...] = rms_norm(hidden.astype(jnp.float32)).astype(jnp.bfloat16)

        need("x")
        free("u_1", "q_1", "k_1", "v_1", "probs_1", "mixed_1", "n_1", "dh_1")
        attention(0)
        send("u_0", "q_0", "k_0", "v_0", "probs_0", "mixed_0", "h_0", "n_0")
        need("w_up")
        launch("w_down", "wq_1", "wk_1", "wv_1", "wo_1", "cot")
        free("act_1", "dpre_1")

        def raw_block(j):
            return dot(row["n"][...], w_up[:, wide(j)], 1, 0).astype(jnp.bfloat16)

        def up(j, raw):
            pre[:, wide(j)] = raw
            act[:, wide(j)] = gelu_parts(raw.astype(jnp.float32))[0].astype(jnp.bfloat16)
        staged(ff // WIDE_BLOCK, (raw_block, up))
        send("pre_0", "act_0")
        need("w_down")

        def down(j):
            lanes = pl.ds(pl.multiple_of(OUT_BLOCK * j, OUT_BLOCK), OUT_BLOCK)
            out = dot(act[...], w_down[:, lanes], 1, 0).astype(jnp.bfloat16).astype(jnp.float32)
            row["x"][:, lanes] = (row["h"][:, lanes].astype(jnp.float32) + out).astype(jnp.bfloat16)
        over(width // OUT_BLOCK, down)
        send("x_1")
        free("u_0", "q_0", "k_0", "v_0", "probs_0", "mixed_0", "h_0", "n_0", same=True)
        attention(1)
        send("u_1", "q_1", "k_1", "v_1", "probs_1", "mixed_1", "n_1")
        need("cot")
        free("pre_0", "act_0", same=True)

        def both_blocks(j):
            return raw_block(j), dot(cot_all[rows], w_down[wide(j)], 1, 1).astype(jnp.bfloat16)

        def both(j, made):
            raw, d_act = made
            out, slope = gelu_parts(raw.astype(jnp.float32))
            act[:, wide(j)] = out.astype(jnp.bfloat16)
            pre[:, wide(j)] = (d_act.astype(jnp.float32) * slope).astype(jnp.bfloat16)
        staged(ff // WIDE_BLOCK, (both_blocks, both))
        send("act_1", "dpre_1")

        def back(j):
            lanes = pl.ds(pl.multiple_of(OUT_BLOCK * j, OUT_BLOCK), OUT_BLOCK)
            row["dn"][:, lanes] = dot(pre[...], w_up[lanes], 1, 1).astype(jnp.bfloat16)
        over(width // OUT_BLOCK, back)
        d_hidden = cot_all[rows].astype(jnp.float32) + rms_backward(
            row["h"][...].astype(jnp.float32), row["dn"][...].astype(jnp.float32))
        row["dh"][...] = d_hidden.astype(jnp.bfloat16)
        send("dh_1")
        free("dqa_1", "dka_1", "dva_1")

        def unmix(unit):
            lanes = pl.ds(OUT_BLOCK * unit, OUT_BLOCK)
            row["dn"][:, lanes] = dot(row["dh"][...], w_out[1, lanes], 1, 1).astype(jnp.bfloat16)

        def back_of(j):
            return tuple(row[kind][:, PAIR * j:PAIR * (j + 1)] for kind in ("q", "k", "v", "dn"))

        def put_back(j, values):
            for name, value in zip(HALF_BUFFERS, values):
                row[name][:, PAIR * j:PAIR * (j + 1)] = value.astype(jnp.bfloat16)
        size = OUT_BLOCK // PAIR
        stages = backward_stages(back_of, lambda j, side: probs[2 * j + side], put_back, low)
        staged(heads // 4 // size, in_units(unmix, stages, size))
        send("dqa_1", "dka_1", "dva_1")
        free("x_1", same=True)
        return carry

    lax.fori_loop(0, batch, one_sequence, 0)
    for name in ("u_1", "q_1", "k_1", "v_1", "probs_1", "mixed_1", "n_1", "act_1", "dpre_1", "dh_1", "dqa_1", "dka_1", "dva_1"):
        store(name, batch - 1).wait()


def front(inputs, batch, seq):
    tokens, width = inputs["x_0"].shape
    ff = inputs["w_up"].shape[1]
    heads = width // HEAD_DIM
    shapes = []
    for name in FRONT_OUTS:
        if name.startswith("probs"):
            shapes.append(bf16(batch, heads, seq, seq))
        else:
            wide = ff if name[:-2] in ("pre", "act", "dpre") else width
            shapes.append(bf16(tokens, width // 2 if name[:-2] in HALF_BUFFERS else wide))
    block = lambda *shape: pltpu.VMEM(shape, jnp.bfloat16)
    scratch = [
        block(tokens, width), block(tokens, width), block(2, 3, width, width), block(2, width, width), block(width, ff),
        block(ff, width), block(heads, seq, seq), block(seq, ff), block(seq, ff),
        *[block(seq, width) for _ in ROW_BUFFERS], *[block(seq, width // 2) for _ in HALF_BUFFERS],
        pltpu.SemaphoreType.DMA((12,)), pltpu.SemaphoreType.DMA((len(FRONT_OUTS),)),
    ]
    outs = pl.pallas_call(
        functools.partial(front_kernel, batch, seq, tuple(inputs)),
        out_shape=shapes,
        in_specs=[pl.BlockSpec(memory_space=pl.ANY)] * len(inputs),
        out_specs=[pl.BlockSpec(memory_space=pl.ANY)] * len(shapes),
        scratch_shapes=scratch,
        compiler_params=pltpu.CompilerParams(vmem_limit_bytes=67_043_328),
        cost_estimate=pl.CostEstimate(flops=22 * tokens * width * ff // 2, bytes_accessed=100 * MIB, transcendentals=0),
        name="front",
    )(*inputs.values())
    return dict(zip(FRONT_OUTS, outs))


MESH = pl.DeviceIdType.MESH
LANES = 1024
SET_ROWS = 128
CORE_ROWS = 2 * SET_ROWS
TILE_ROWS = 2 * CORE_ROWS
OWN_SLOTS = 8
AG_SLOTS = 10
TYPES = {
    "p1": (0, 0, 80, "xyz"),
    "q1": (0, 80, 48, "zxy"),
    "p2": (1, 128, 80, "yxz"),
    "q2": (1, 208, 48, "zyx"),
}
WRITE_AT = 11


def stage_list():
    stages = []
    for name, (_, _, _, order) in TYPES.items():
        if order[2] == "z":
            plan = [("rs1", 1), ("rs2", 2), ("rsz", 3), ("agz", 6), ("ag2", 9), ("ag1", 10)]
        else:
            plan = [("rsz", 1), ("rs1", 4), ("rs2", 5), ("ag2", 6), ("ag1", 7), ("agz", 8)]
        for kind, at in plan:
            if kind in ("rsz", "agz"):
                for step in range(3):
                    for way in (0, 1):
                        stages.append((name, kind, step, way, at + step))
            else:
                stages.append((name, kind, 0, 0, at))
    return stages


STAGES = stage_list()


def piece_shape(name, kind):
    rows, order = TYPES[name][2], TYPES[name][3]
    if order[2] == "z":
        return {"rs1": (rows, 512), "rs2": (rows, 256), "rsz": (rows // 2, 128)}[kind]
    return {"rsz": (rows // 2, 512), "rs1": (rows // 2, 256), "rs2": (rows // 2, 128)}[kind]


def between(step, first, count):
    return jnp.logical_and(step >= first, step < first + count)


class Backward:
    PB_1, MB, AB, PB_0 = 4, 6, 14, 23
    ROWS = 256

    def __init__(self, at, big, total_buf, w_buf, p_buf, sem, drain):
        self.at, self.big, self.total, self.w, self.p, self.sem, self.drain = at, big, total_buf, w_buf, p_buf, sem, drain
        self.tokens, self.width = at["x_0"].shape
        self.heads = at["probs_0"].shape[1]
        self.seq = at["probs_0"].shape[2]
        self.seqs = self.tokens // self.seq

    def load(self, name, dest, sem, *index):
        ref = self.at[name]
        return pltpu.make_async_copy(ref.at[index] if index else ref, dest, self.sem.at[sem])

    def store(self, src, name, sem, *index):
        ref = self.at[name]
        return pltpu.make_async_copy(src, ref.at[index] if index else ref, self.drain.at[sem])

    def row_blocks(self, fn):
        def body(block, carry):
            fn(pl.ds(pl.multiple_of(self.ROWS * block, self.ROWS), self.ROWS))
            return carry
        lax.fori_loop(0, self.tokens // self.ROWS, body, 0)

    def input_loads(self, layer):
        copies = [self.load(f"x_{layer}", self.big.at[5], 3)]
        for i, kind in enumerate("qkv"):
            if layer:
                half = self.width // 2
                copies.append(self.load(f"d{kind}a_1", self.big.at[i, :, pl.ds(0, half)], i))
                copies.append(self.load(f"d{kind}b_1", self.big.at[i, :, pl.ds(half, half)], 11 + i))
            else:
                copies.append(self.load(f"d{kind}_0", self.big.at[i], i))
        return copies

    def weight_loads(self, layer, block):
        rows = pl.ds(pl.multiple_of(OUT_BLOCK * block, OUT_BLOCK), OUT_BLOCK)
        slot = lax.rem(block, 2)
        return [self.load(name, self.w.at[slot, i], 5 + 3 * slot + i, layer, rows) for i, name in enumerate(("wq", "wk", "wv"))]

    def input_block(self, layer, block):
        big, blocks = self.big, self.width // OUT_BLOCK
        slot = lax.rem(block, 2)

        @pl.when(block == 0)
        def _():
            for copy in self.input_loads(layer):
                copy.wait()
        for copy in self.weight_loads(layer, block):
            copy.wait()

        @pl.when(block + 1 < blocks)
        def _():
            for copy in self.weight_loads(layer, block + 1):
                copy.start()
        lanes = pl.ds(pl.multiple_of(OUT_BLOCK * block, OUT_BLOCK), OUT_BLOCK)

        def product(rows):
            total = dot(big[0, rows], self.w[slot, 0], 1, 1) + dot(big[1, rows], self.w[slot, 1], 1, 1)
            big[3, rows, lanes] = (total + dot(big[2, rows], self.w[slot, 2], 1, 1)).astype(jnp.bfloat16)
        self.row_blocks(product)

        @pl.when(block == blocks - 1)
        def _():
            def close(rows):
                back = rms_backward(big[5, rows].astype(jnp.float32), big[3, rows].astype(jnp.float32))
                big[3, rows] = (big[4, rows].astype(jnp.float32) + back).astype(jnp.bfloat16)
                if layer:
                    self.total[rows] = jnp.zeros((self.ROWS, self.width), jnp.float32)
            self.row_blocks(close)
            self.store(big.at[3], f"dx_{layer}", 0).start()
            if layer:
                self.load("h_0", big.at[4], 3).start()
                for copy in self.mlp_loads(0):
                    copy.start()

    def mlp_loads(self, block):
        slot = lax.rem(block, 2)
        lanes = pl.ds(pl.multiple_of(FF_BLOCK * block, FF_BLOCK), FF_BLOCK)
        half = pl.ds(pl.multiple_of(FF_BLOCK * slot, FF_BLOCK), FF_BLOCK)
        return [self.load("w_up", self.big.at[0, :, half], 5 + 3 * slot, slice(None), lanes),
                self.load("pre_0", self.big.at[1, :, half], 6 + 3 * slot, slice(None), lanes),
                self.load("w_down", self.big.at[5, half], 7 + 3 * slot, lanes)]

    def mlp_store(self, block):
        half = pl.ds(pl.multiple_of(FF_BLOCK * lax.rem(block, 2), FF_BLOCK), FF_BLOCK)
        lanes = pl.ds(pl.multiple_of(FF_BLOCK * block, FF_BLOCK), FF_BLOCK)
        return self.store(self.big.at[2, :, half], "dpre_0", 1, slice(None), lanes)

    def mlp_block(self, block):
        big, blocks = self.big, self.at["w_up"].shape[1] // FF_BLOCK

        @pl.when(block == 0)
        def _():
            self.store(big.at[3], "dx_1", 0).wait()
            self.load("h_0", big.at[4], 3).wait()
        for copy in self.mlp_loads(block):
            copy.wait()

        @pl.when(block + 1 < blocks)
        def _():
            for copy in self.mlp_loads(block + 1):
                copy.start()

        @pl.when(block > 0)
        def _():
            self.mlp_store(block - 1).wait()
        half = pl.ds(pl.multiple_of(FF_BLOCK * lax.rem(block, 2), FF_BLOCK), FF_BLOCK)

        def product(rows):
            d_act = dot(big[3, rows], big[5, half], 1, 1).astype(jnp.bfloat16).astype(jnp.float32)
            slope = gelu_parts(big[1, rows, half].astype(jnp.float32))[1]
            d_pre = (d_act * slope).astype(jnp.bfloat16)
            big[2, rows, half] = d_pre
            self.total[rows] += dot(d_pre, big[0, :, half], 1, 1)
        self.row_blocks(product)
        self.mlp_store(block).start()

        @pl.when(block == blocks - 1)
        def _():
            def close(rows):
                d_normed = self.total[rows].astype(jnp.bfloat16).astype(jnp.float32)
                back = rms_backward(big[4, rows].astype(jnp.float32), d_normed)
                big[4, rows] = (big[3, rows].astype(jnp.float32) + back).astype(jnp.bfloat16)
            self.row_blocks(close)
            self.store(big.at[4], "dh_0", 2).start()
            self.load("wo", big.at[0], 4, 0).start()
            for copy in self.piece_loads(0, 0):
                copy.start()

    def where(self, piece):
        seq, half = lax.rem(piece, self.seqs), lax.div(piece, self.seqs)
        rows = pl.ds(pl.multiple_of(self.seq * seq, self.seq), self.seq)
        lanes = pl.ds(pl.multiple_of(self.width // 2 * half, self.width // 2), self.width // 2)
        return seq, half, rows, lanes

    def piece_loads(self, layer, piece):
        seq, half, rows, lanes = self.where(piece)
        near = pl.ds(0, self.width // 2)
        copies = [self.load(f"{kind}_{layer}", self.big.at[1 + lax.rem(piece, 2), pl.ds(self.seq * i, self.seq), near], i, rows, lanes)
                  for i, kind in enumerate("qkv")]
        heads = pl.ds(self.heads // 2 * half, self.heads // 2)
        return copies + [self.load(f"probs_{layer}", self.p.at[lax.rem(piece, 2)], 5, seq, heads)]

    def piece_stores(self, layer, piece):
        _, _, rows, lanes = self.where(piece)
        near, spot = pl.ds(0, self.width // 2), 5 - 2 * lax.rem(piece, 2)
        sources = [self.big.at[spot, pl.ds(self.seq * i, self.seq), near] for i in range(3)]
        if layer:
            return [self.store(src, f"d{kind}b_1", 3 + i, rows) for i, (src, kind) in enumerate(zip(sources, "qkv"))]
        return [self.store(src, f"d{kind}_0", 3 + i, rows, lanes) for i, (src, kind) in enumerate(zip(sources, "qkv"))]

    def attention_piece(self, layer, piece):
        big, p_buf, pieces = self.big, self.p, 2 * self.seqs
        _, half, rows, _ = self.where(piece)
        parity = lax.rem(piece, 2)
        spot, out = 1 + parity, 5 - 2 * parity

        start = self.seqs * layer

        @pl.when(piece == start)
        def _():
            if layer == 0:
                self.mlp_store(self.at["w_up"].shape[1] // FF_BLOCK - 1).wait()
                self.store(big.at[4], "dh_0", 2).wait()
            else:
                self.load("dh_1", big.at[4], 3).wait()
            self.load("wo", big.at[0], 4, layer).wait()

        @pl.when(piece > start)
        def _():
            for copy in self.piece_stores(layer, piece - 1):
                copy.wait()
        for copy in self.piece_loads(layer, piece):
            copy.wait()

        @pl.when(piece + 1 < pieces)
        def _():
            for copy in self.piece_loads(layer, piece + 1):
                copy.start()
        low = lax.broadcasted_iota(jnp.int32, (self.seq, PAIR), 1) < HEAD_DIM

        def unmix(unit):
            w_rows = pl.ds(pl.multiple_of(self.width // 2 * half + OUT_BLOCK * unit, OUT_BLOCK), OUT_BLOCK)
            d_mixed = dot(big[4, rows], big[0, w_rows], 1, 1)
            big[spot, pl.ds(3 * self.seq, self.seq), pl.ds(OUT_BLOCK * unit, OUT_BLOCK)] = d_mixed.astype(jnp.bfloat16)

        def pair_of(j):
            return tuple(big[spot, pl.ds(self.seq * i, self.seq), pl.ds(PAIR * j, PAIR)] for i in range(4))

        def put(j, values):
            for i, value in enumerate(values):
                big[out, pl.ds(self.seq * i, self.seq), pl.ds(PAIR * j, PAIR)] = value.astype(jnp.bfloat16)
        size = OUT_BLOCK // PAIR
        stages = backward_stages(pair_of, lambda j, side: p_buf[parity, 2 * j + side], put, low)
        staged(self.heads // 4 // size, in_units(unmix, stages, size))
        for copy in self.piece_stores(layer, piece):
            copy.start()

    def begin(self):
        self.load("dh_1", self.big.at[4], 3).start()
        self.load("wo", self.big.at[0], 4, 1).start()
        for copy in self.piece_loads(1, self.seqs):
            copy.start()

    def item(self, step):
        blocks = self.width // OUT_BLOCK
        pieces = 2 * self.seqs

        @pl.when(step < 3)
        def _():
            first = self.seqs + step
            count = jnp.where(step == 2, self.seqs - 2, 1)
            lax.fori_loop(first, first + count, lambda piece, carry: self.attention_piece(1, piece) or carry, 0)

        @pl.when(step == 3)
        def _():
            for copy in self.piece_stores(1, pieces - 1):
                copy.wait()
            for copy in self.input_loads(1) + self.weight_loads(1, 0):
                copy.start()

        @pl.when(between(step, self.PB_1, 2))
        def _():
            first = blocks // 2 * (step - self.PB_1)
            lax.fori_loop(first, first + blocks // 2, lambda block, carry: self.input_block(1, block) or carry, 0)
        pl.when(between(step, self.MB, 8))(lambda: self.mlp_block(step - self.MB))
        pl.when(between(step, self.AB, pieces))(lambda: self.attention_piece(0, step - self.AB))

        @pl.when(step == self.PB_0 - 1)
        def _():
            for copy in self.piece_stores(0, pieces - 1):
                copy.wait()
            for copy in self.input_loads(0) + self.weight_loads(0, 0):
                copy.start()
        pl.when(between(step, self.PB_0, blocks))(lambda: self.input_block(0, step - self.PB_0))

        @pl.when(step == self.PB_0 + blocks)
        def _():
            self.store(self.big.at[3], "dx_0", 0).wait()


def finish_kernel(groups, chunks, in_names, out_names, remote, *refs):
    names = [*in_names, *out_names]
    at, scratch = dict(zip(names, refs[:len(names)])), refs[len(names):]
    (big, total_buf, w_buf, p_buf, item_sem, drain_sem), scratch = scratch[:6], scratch[6:]
    backward = Backward(at, big, total_buf, w_buf, p_buf, item_sem, drain_sem)
    if not remote:
        backward.begin()

        def alone(step, carry):
            backward.item(step)
            return carry
        lax.fori_loop(0, chunks + WRITE_AT + 1, alone, 0)
        return
    (lhs_buf, rhs_buf, own, part, part_in, gath), scratch = scratch[:6], scratch[6:]
    land_keys = [key for key, st in enumerate(STAGES) if st[1].startswith("rs")]
    landing = dict(zip(land_keys, scratch[:len(land_keys)]))
    load_sem, send_sem, recv_sem, pair_send, pair_recv, out_sem, out_send, out_recv, credit = scratch[len(land_keys):]

    me = lax.axis_index("data")
    core = lax.rem(me, 2)
    coord = {"x": lax.rem(lax.div(me, 2), 2), "y": lax.rem(lax.div(me, 4), 2)}
    z = lax.div(me, 8)
    partner = me + 1 - 2 * core
    near = {"x": me + 2 - 4 * coord["x"], "y": me + 4 - 8 * coord["y"]}
    up_ok, down_ok = z < 3, z > 0
    peers = [(partner, 0, None), (near["x"], 1, None), (near["y"], 2, None), (me + 8, 3, up_ok), (me - 8, 4, down_ok)]

    def guarded(cond, fn):
        if cond is None:
            fn()
        else:
            pl.when(cond)(fn)

    barrier = pltpu.get_barrier_semaphore()
    for dev, _, cond in peers:
        guarded(cond, lambda dev=dev: pl.semaphore_signal(barrier, inc=1, device_id=(dev,), device_id_type=MESH))
    inner = jnp.logical_and(up_ok, down_ok)
    guarded(inner, lambda: pl.semaphore_wait(barrier, 5))
    guarded(jnp.logical_not(inner), lambda: pl.semaphore_wait(barrier, 4))

    def region(name, kind, which):
        _, row, rows, order = TYPES[name]
        if order[2] == "z":
            h1, h2 = coord[order[0]], coord[order[1]]
            if kind == "1":
                return pl.ds(row, rows), pl.ds(pl.multiple_of(512 * which, 128), 512)
            if kind == "2":
                return pl.ds(row, rows), pl.ds(pl.multiple_of(512 * h1 + 256 * which, 128), 256)
            first = pl.multiple_of(row + (rows // 2) * lax.div(which, 2), 8)
            lane = pl.multiple_of(512 * h1 + 256 * h2 + 128 * lax.rem(which, 2), 128)
            return pl.ds(first, rows // 2), pl.ds(lane, 128)
        h1 = coord[order[1]]
        if kind == "z":
            first = pl.multiple_of(row + (rows // 2) * lax.div(which, 2), 8)
            return pl.ds(first, rows // 2), pl.ds(pl.multiple_of(512 * lax.rem(which, 2), 128), 512)
        first = pl.multiple_of(row + (rows // 2) * lax.div(z, 2), 8)
        if kind == "1":
            return pl.ds(first, rows // 2), pl.ds(pl.multiple_of(512 * lax.rem(z, 2) + 256 * which, 128), 256)
        lane = pl.multiple_of(512 * lax.rem(z, 2) + 256 * h1 + 128 * which, 128)
        return pl.ds(first, rows // 2), pl.ds(lane, 128)

    def exchange_axis(name, kind):
        order = TYPES[name][3]
        dims = order[:2] if order[2] == "z" else order[1:]
        return dims[int(kind) - 1]

    def plan(key, chunk, parity):
        name, kind, step, way, _ = STAGES[key]
        mine, slot = lax.rem(chunk, OWN_SLOTS), lax.rem(chunk, AG_SLOTS)
        if kind in ("rs1", "rs2"):
            axis = exchange_axis(name, kind[2])
            src, keep = region(name, kind[2], 1 - coord[axis]), region(name, kind[2], coord[axis])
            dev, send_ok, recv_ok = near[axis], None, None
            sent = own.at[mine, src[0], src[1]]
        elif kind in ("ag1", "ag2"):
            axis = exchange_axis(name, kind[2])
            src = keep = region(name, kind[2], coord[axis])
            dev, send_ok, recv_ok = near[axis], None, None
            sent = gath.at[slot, src[0], src[1]]
        elif kind == "rsz":
            if way:
                dev, k_send, k_keep = me + 8, z + 3 - step, z + 2 - step
                send_ok, recv_ok = k_send <= 3, jnp.logical_and(k_keep <= 3, down_ok)
            else:
                dev, k_send, k_keep = me - 8, z - 3 + step, z - 2 + step
                send_ok, recv_ok = k_send >= 0, jnp.logical_and(k_keep >= 0, up_ok)
            src, keep = region(name, "z", k_send), region(name, "z", k_keep)
            sent = own.at[mine, src[0], src[1]]
        else:
            if way:
                dev, k_send, k_keep = me + 8, z - step, z - 1 - step
                send_ok, recv_ok = jnp.logical_and(k_send >= 0, up_ok), k_keep >= 0
            else:
                dev, k_send, k_keep = me - 8, z + step, z + 1 + step
                send_ok, recv_ok = jnp.logical_and(k_send <= 3, down_ok), k_keep <= 3
            src, keep = region(name, "z", k_send), region(name, "z", k_keep)
            sent = gath.at[slot, src[0], src[1]]
        sems = dict(send_sem=send_sem.at[key, parity], recv_sem=recv_sem.at[key, parity], device_id=(dev,), device_id_type=MESH)
        if kind.startswith("rs"):
            target = landing[key].at[parity]
            send = lambda: pltpu.make_async_remote_copy(src_ref=sent, dst_ref=target, **sems)
            recv = lambda: pltpu.make_async_remote_copy(
                src_ref=own.at[mine, keep[0], keep[1]], dst_ref=target, **sems)

            def arrive():
                own[mine, keep[0], keep[1]] += landing[key][parity]
        else:
            send = lambda: pltpu.make_async_remote_copy(src_ref=sent, dst_ref=sent, **sems)
            recv = lambda: pltpu.make_async_remote_copy(
                src_ref=gath.at[slot, keep[0], keep[1]], dst_ref=gath.at[slot, keep[0], keep[1]], **sems)
            arrive = None
        return send, recv, send_ok, recv_ok, arrive

    def finish(name, chunk):
        order = TYPES[name][3]
        reg = region(name, "z", z) if order[2] == "z" else region(name, "2", coord[order[2]])
        gath[lax.rem(chunk, AG_SLOTS), reg[0], reg[1]] = own[lax.rem(chunk, OWN_SLOTS), reg[0], reg[1]]

    def valid(chunk):
        return jnp.logical_and(chunk >= 0, chunk < chunks)

    def set_rows(half):
        return pl.ds(half * SET_ROWS, SET_ROWS)

    def pair_copy(half, parity):
        return pltpu.make_async_remote_copy(
            src_ref=part.at[parity, set_rows(half)], dst_ref=part_in.at[parity, set_rows(half)],
            send_sem=pair_send.at[half], recv_sem=pair_recv.at[half, parity], device_id=(partner,), device_id_type=MESH)

    half_lanes = LANES // 2

    def outlets(half, group, local, whose):
        out, layer = group["out"]
        ref = at[out] if layer is None else at[out].at[layer]
        rows, cols = group["place"](local)
        if not group["narrow"]:
            first = pl.multiple_of(rows + CORE_ROWS * whose + half * SET_ROWS, SET_ROWS)
            return [(pl.ds(0, LANES), ref.at[pl.ds(first, SET_ROWS), pl.ds(pl.multiple_of(cols, 128), LANES)])]
        places = []
        for sub in (0, 1):
            first = pl.multiple_of(2 * CORE_ROWS * whose + CORE_ROWS * sub + half * SET_ROWS, SET_ROWS)
            places.append((pl.ds(half_lanes * sub, half_lanes), ref.at[pl.ds(first, SET_ROWS), pl.ds(cols, half_lanes)]))
        return places

    def write_copies(half, chunk, lanes, dest):
        slot = lax.rem(chunk, AG_SLOTS)
        src = gath.at[slot, set_rows(half), lanes]
        here = pltpu.make_async_copy(src, dest, out_sem.at[half])
        there = pltpu.make_async_remote_copy(
            src_ref=src, dst_ref=dest, send_sem=out_send.at[half], recv_sem=out_recv.at[half, lax.rem(chunk, 2)],
            device_id=(partner,), device_id_type=MESH)
        return here, there

    def load_copies(group, local, slot):
        rows, cols = group["place"](local)
        narrow = group["narrow"]
        lhs, rhs = [], []
        for sub in range(2 if narrow else len(group["lhs"])):
            for whose in (0, 1):
                owner = core if whose == 0 else 1 - core
                first = 2 * CORE_ROWS * owner + CORE_ROWS * sub if narrow else rows + CORE_ROWS * owner
                source = at[group["lhs"][0 if narrow else sub]]
                lhs.append(pltpu.make_async_copy(
                    source.at[:, pl.ds(pl.multiple_of(first, CORE_ROWS), CORE_ROWS)],
                    lhs_buf.at[slot, sub, whose], load_sem.at[slot, sub, whose]))
        for app, name in enumerate(group["rhs"]):
            size = half_lanes if narrow else LANES
            rhs.append(pltpu.make_async_copy(
                at[name].at[:, pl.ds(0 if narrow else pl.multiple_of(cols, 128), size)], rhs_buf.at[slot, app, :, pl.ds(0, size)],
                load_sem.at[slot, app, 2]))
        return lhs, rhs

    def for_group(chunk, fn):
        for group in groups:
            inside = jnp.logical_and(chunk >= group["start"], chunk < group["start"] + group["count"])
            pl.when(inside)(functools.partial(fn, group, chunk - group["start"]))

    def among(chunk, chosen):
        flags = [jnp.logical_and(chunk >= g["start"], chunk < g["start"] + g["count"]) for g in groups if chosen(g)]
        return functools.reduce(jnp.logical_or, flags)

    def is_two(group):
        return len(group["lhs"]) == 2

    def is_narrow(group):
        return group["narrow"]

    def start_load(chunk):
        def go(group, local):
            for copy in sum(load_copies(group, local, lax.rem(chunk, 2)), []):
                copy.start()
        for_group(chunk, go)

    def wait_load(chunk):
        slot = lax.rem(chunk, 2)
        two_lhs, two_rhs = load_copies(next(filter(is_two, groups)), 0, slot)
        slim_lhs, slim_rhs = load_copies(next(filter(is_narrow, groups)), 0, slot)
        for copy in two_lhs[:2]:
            copy.wait()

        @pl.when(jnp.logical_not(among(chunk, is_narrow)))
        def _():
            two_rhs[0].wait()

        @pl.when(among(chunk, is_narrow))
        def _():
            for copy in slim_rhs + slim_lhs[2:]:
                copy.wait()

        @pl.when(among(chunk, is_two))
        def _():
            for copy in two_lhs[2:] + two_rhs[1:]:
                copy.wait()

    def tile(chunk):
        slot, mine, parity = lax.rem(chunk, 2), lax.rem(chunk, OWN_SLOTS), lax.rem(chunk, 2)

        def product(sub, whose, rhs):
            return dot(lhs_buf[slot, sub, whose], rhs, 0, 0)

        @pl.when(among(chunk, is_narrow))
        def _():
            for sub in (0, 1):
                lanes, rhs = pl.ds(half_lanes * sub, half_lanes), rhs_buf[slot, 0, :, pl.ds(0, half_lanes)]
                own[mine, :, lanes] = product(sub, 0, rhs)
                part[parity, :, lanes] = product(sub, 1, rhs)

        @pl.when(jnp.logical_not(among(chunk, is_narrow)))
        def _():
            own[mine] = product(0, 0, rhs_buf[slot, 0])
            part[parity] = product(0, 1, rhs_buf[slot, 0])

        @pl.when(among(chunk, is_two))
        def _():
            own[mine] += product(1, 0, rhs_buf[slot, 1])
            part[parity] += product(1, 1, rhs_buf[slot, 1])

    last = chunks + WRITE_AT

    def section(half, step):
        before = lax.rem(step + 1, 2)
        now = lax.rem(step, 2)
        names = [name for name in TYPES if TYPES[name][0] == half]
        at_stage = {}
        for key, (name, _, _, _, at) in enumerate(STAGES):
            if name in names:
                at_stage.setdefault((at, name), []).append(key)
        finals = {name: max(st[4] for st in STAGES if st[0] == name and st[1].startswith("rs")) for name in names}

        def start(at, name):
            chunk = step - at

            @pl.when(valid(chunk))
            def _():
                for key in at_stage[at, name]:
                    send, _, send_ok, _, _ = plan(key, chunk, now)
                    guarded(send_ok, lambda send=send: send().start())

        def finish_stage(at, name):
            chunk = step - 1 - at

            @pl.when(valid(chunk))
            def _():
                for key in at_stage[at, name]:
                    send, recv, send_ok, recv_ok, arrive = plan(key, chunk, before)

                    def arrived(recv=recv, arrive=arrive):
                        recv().wait_recv()
                        if arrive is not None:
                            arrive()
                    guarded(recv_ok, arrived)
                    guarded(send_ok, lambda send=send: send().wait_send())
                if at == finals[name]:
                    finish(name, chunk)

        @pl.when(step > 0)
        def _():
            for dev, way, cond in peers:
                guarded(cond, lambda way=way: pl.semaphore_wait(credit.at[half, way], 1))

        @pl.when(valid(step - 1))
        def _():
            copy = pair_copy(half, before)
            copy.wait_send()
            copy.wait_recv()
            mine = lax.rem(step - 1, OWN_SLOTS)
            own[mine, set_rows(half)] += part_in[before, set_rows(half)]

        done = step - 1 - WRITE_AT

        @pl.when(valid(done))
        def _():
            (lanes, dest), = outlets(half, next(filter(is_two, groups)), 0, 0)
            here, there = write_copies(half, done, lanes, dest)
            here.wait()
            there.wait_send()
            there.wait_recv()

        held = []
        for name in names:
            start(1, name)
        for at in range(1, WRITE_AT):
            for name in names:
                finish_stage(at, name)
                if held:
                    start(*held.pop(0))
                if at + 1 < WRITE_AT:
                    held.append((at + 1, name))
        assert not held
        out_chunk = step - WRITE_AT

        @pl.when(step < last)
        def _():
            for dev, way, cond in peers:
                to = way if way < 3 else 7 - way
                guarded(cond, lambda dev=dev, to=to: pl.semaphore_signal(
                    credit.at[half, to], inc=1, device_id=(dev,), device_id_type=MESH))

        @pl.when(valid(out_chunk))
        def _():
            def go(group, local):
                for lanes, dest in outlets(half, group, local, core):
                    for copy in write_copies(half, out_chunk, lanes, dest):
                        copy.start()
            for_group(out_chunk, go)

    backward.begin()
    start_load(jnp.int32(0))

    def round_(step, carry):
        section(0, step)

        @pl.when(valid(step))
        def _():
            pl.when(step + 1 < chunks)(lambda: start_load(step + 1))
            wait_load(step)
            tile(step)
            pair_copy(0, lax.rem(step, 2)).start()

        section(1, step)

        @pl.when(valid(step))
        def _():
            pair_copy(1, lax.rem(step, 2)).start()

        backward.item(step)
        return carry

    lax.fori_loop(0, last + 1, round_, 0)


def finish_backward(inputs, groups, chunks, weights, tokens, seq, collective_id=0, remote=True):
    width, ff = inputs["w_up"].shape
    landing = [pltpu.VMEM((2,) + piece_shape(st[0], st[1]), jnp.float32) for st in STAGES if st[1].startswith("rs")]
    apps = 2
    outs = {name: jax.ShapeDtypeStruct(shape, jnp.float32) for name, shape in weights.items()}
    for name in ("dx_0", "dx_1", "dh_0", "dq_0", "dk_0", "dv_0"):
        outs[name] = bf16(tokens, width)
    for name in ("dqb_1", "dkb_1", "dvb_1"):
        outs[name] = bf16(tokens, width // 2)
    outs["dpre_0"] = bf16(tokens, ff)
    heads = width // HEAD_DIM
    scratch = [
        pltpu.VMEM((6, tokens, width), jnp.bfloat16),
        pltpu.VMEM((tokens, width), jnp.float32),
        pltpu.VMEM((2, 3, OUT_BLOCK, width), jnp.bfloat16),
        pltpu.VMEM((2, heads // 2, seq, seq), jnp.bfloat16),
        pltpu.SemaphoreType.DMA((14,)),
        pltpu.SemaphoreType.DMA((6,)),
    ]
    if remote:
        scratch += [
            pltpu.VMEM((2, apps, 2, tokens, CORE_ROWS), jnp.bfloat16),
            pltpu.VMEM((2, apps, tokens, LANES), jnp.bfloat16),
            pltpu.VMEM((OWN_SLOTS, CORE_ROWS, LANES), jnp.float32),
            pltpu.VMEM((2, CORE_ROWS, LANES), jnp.float32),
            pltpu.VMEM((2, CORE_ROWS, LANES), jnp.float32),
            pltpu.VMEM((AG_SLOTS, CORE_ROWS, LANES), jnp.float32),
            *landing,
            pltpu.SemaphoreType.DMA((2, apps, 3)),
            pltpu.SemaphoreType.DMA((len(STAGES), 2)),
            pltpu.SemaphoreType.DMA((len(STAGES), 2)),
            pltpu.SemaphoreType.DMA((2,)),
            pltpu.SemaphoreType.DMA((2, 2)),
            pltpu.SemaphoreType.DMA((2,)),
            pltpu.SemaphoreType.DMA((2,)),
            pltpu.SemaphoreType.DMA((2, 2)),
            pltpu.SemaphoreType.REGULAR((2, 5)),
        ]
    params = dict(collective_id=collective_id, has_side_effects=True) if remote else {}
    results = pl.pallas_call(
        functools.partial(finish_kernel, groups, chunks, list(inputs), list(outs), remote),
        out_shape=list(outs.values()),
        in_specs=[pl.BlockSpec(memory_space=pl.ANY)] * len(inputs),
        out_specs=[pl.BlockSpec(memory_space=pl.ANY)] * len(outs),
        scratch_shapes=scratch,
        compiler_params=pltpu.CompilerParams(vmem_limit_bytes=67_043_328, **params),
        cost_estimate=pl.CostEstimate(flops=20 * tokens * width * ff, bytes_accessed=256 * MIB, transcendentals=0),
        name="finish_backward",
    )(*inputs.values())
    return dict(zip(outs, results))


DELIVER_ROWS = 256
DELIVER_SLOTS = 40
DELIVER_AHEAD = 20


def deliver(arrays, small):
    def blocks_of(array):
        lead = [(i,) for i in range(array.shape[0])] if len(array.shape) == 3 else [()]
        rows, cols = array.shape[-2:]
        return [(*index, pl.ds(row, DELIVER_ROWS), pl.ds(col, LANES))
                for index in lead for row in range(0, rows, DELIVER_ROWS) for col in range(0, cols, LANES)]

    work = [(i, index) for i, array in enumerate(arrays) for index in blocks_of(array)]
    count = len(arrays) + 1

    def kernel(*refs):
        ins, outs, buf, whole_buf, in_sem, out_sem, whole_sem = refs[:count], refs[count:2 * count], *refs[2 * count:]
        whole_in = pltpu.make_async_copy(ins[-1], whole_buf, whole_sem.at[0])
        whole_out = pltpu.make_async_copy(whole_buf, outs[-1], whole_sem.at[1])

        def fetch(t):
            i, index = work[t]
            return pltpu.make_async_copy(ins[i].at[index], buf.at[t % DELIVER_SLOTS], in_sem.at[t % DELIVER_SLOTS])

        def put(t):
            i, index = work[t]
            return pltpu.make_async_copy(buf.at[t % DELIVER_SLOTS], outs[i].at[index], out_sem.at[t % DELIVER_SLOTS])

        whole_in.start()
        for t in range(min(DELIVER_AHEAD, len(work))):
            fetch(t).start()
        whole_in.wait()
        whole_out.start()
        for t in range(len(work)):
            if t + DELIVER_AHEAD < len(work):
                if t + DELIVER_AHEAD >= DELIVER_SLOTS:
                    put(t + DELIVER_AHEAD - DELIVER_SLOTS).wait()
                fetch(t + DELIVER_AHEAD).start()
            fetch(t).wait()
            put(t).start()
        for t in range(max(0, len(work) - DELIVER_SLOTS), len(work)):
            put(t).wait()
        whole_out.wait()

    return pl.pallas_call(
        kernel,
        out_shape=[jax.ShapeDtypeStruct(array.shape, array.dtype) for array in (*arrays, small)],
        in_specs=[pl.BlockSpec(memory_space=pl.ANY)] * count,
        out_specs=[pl.BlockSpec(memory_space=pl.ANY)] * count,
        scratch_shapes=[pltpu.VMEM((DELIVER_SLOTS, DELIVER_ROWS, LANES), jnp.float32), pltpu.VMEM(small.shape, small.dtype),
                        pltpu.SemaphoreType.DMA((DELIVER_SLOTS,)), pltpu.SemaphoreType.DMA((DELIVER_SLOTS,)),
                        pltpu.SemaphoreType.DMA((2,))],
        compiler_params=pltpu.CompilerParams(vmem_limit_bytes=67_043_328),
        cost_estimate=pl.CostEstimate(flops=0, bytes_accessed=2 * sum(a.size for a in arrays) * 4, transcendentals=0),
        name="deliver",
    )(*arrays, small)


def gradient_groups(width, ff):
    groups = []

    def add(count, lhs, rhs, out, place, narrow=False):
        start = groups[-1]["start"] + groups[-1]["count"] if groups else 0
        groups.append(dict(start=start, count=count, lhs=lhs, rhs=rhs, out=out, place=place, narrow=narrow))

    def tall(local):
        return TILE_ROWS * local, 0

    def wide(local):
        return TILE_ROWS * lax.rem(local, width // TILE_ROWS), LANES * lax.div(local, width // TILE_ROWS)

    for half in (0, 1):
        for kind in "qkv":
            add(1, ["u_1"], [f"d{kind}{'ab'[half]}_1"], (f"g_{kind}", 1), lambda local, half=half: (0, width // 2 * half), narrow=True)
        if half == 0:
            add(width // TILE_ROWS, ["mixed_1"], ["dh_1"], ("g_o", 1), tall)
    add(ff // TILE_ROWS, ["act_0", "act_1"], ["dx_1", "cot"], ("g_down", None), tall)
    add(ff // TILE_ROWS, ["n_0", "n_1"], ["dpre_0", "dpre_1"], ("g_up", None), wide)
    for kind in "qkv":
        add(width // TILE_ROWS, ["u_0"], [f"d{kind}_0"], (f"g_{kind}", 0), tall)
    add(width // TILE_ROWS, ["mixed_0"], ["dh_0"], ("g_o", 0), tall)
    return groups, sum(group["count"] for group in groups)


def local_operands(x_init, cot_out, w_query, w_key, w_value, w_proj, w_up, w_down):
    batch, seq, width = x_init.shape
    tokens = batch * seq
    at = {"x_0": x_init.reshape(tokens, width), "cot": cot_out.reshape(tokens, width)}
    at.update(wq=w_query, wk=w_key, wv=w_value, wo=w_proj, w_up=w_up, w_down=w_down)
    at.update(front(at, batch, seq))
    return at


def solution(mesh):
    def local_step(x_init, cot_out, w_query, w_key, w_value, w_proj, w_up, w_down):
        batch, seq, width = x_init.shape
        inputs = local_operands(x_init, cot_out, w_query, w_key, w_value, w_proj, w_up, w_down)
        groups, chunks = gradient_groups(width, w_up.shape[1])
        weights = dict(g_q=w_query.shape, g_k=w_key.shape, g_v=w_value.shape, g_o=w_proj.shape, g_up=w_up.shape, g_down=w_down.shape)
        res = finish_backward(inputs, groups, chunks, weights, batch * seq, seq)
        *grads, d_init = deliver([res[name] for name in weights], res["dx_0"])
        return (*grads, d_init.reshape(x_init.shape))

    data_spec = P("data")
    full_spec = P()
    in_specs = (data_spec, data_spec, full_spec, full_spec, full_spec, full_spec, full_spec, full_spec)
    out_specs = (full_spec, full_spec, full_spec, full_spec, full_spec, full_spec, data_spec)
    return jax.shard_map(local_step, mesh=mesh, in_specs=in_specs, out_specs=out_specs, check_vma=False)
```

```python
import functools

import jax
import jax.numpy as jnp
from jax import lax
from jax.experimental import pallas as pl
from jax.experimental.pallas import tpu as pltpu
from jax.sharding import PartitionSpec as P

EPS = 1e-6
HEAD_DIM = 64
PAIR = 2 * HEAD_DIM
FF_BLOCK = 512
OUT_BLOCK = 256
GELU_A = (2.0 / 3.141592653589793) ** 0.5
GELU_B = 0.044715
SOFTMAX_SCALE = HEAD_DIM ** -0.5 * 1.4426950408889634
MIB = 1024 * 1024


def dot(lhs, rhs, lhs_dim, rhs_dim):
    return lax.dot_general(lhs, rhs, (((lhs_dim,), (rhs_dim,)), ((), ())), preferred_element_type=jnp.float32)


def rms_norm(x_f32):
    return x_f32 * lax.rsqrt(jnp.mean(x_f32 * x_f32, axis=-1, keepdims=True) + EPS)


def rms_backward(x_f32, d_out):
    scale = lax.rsqrt(jnp.mean(x_f32 * x_f32, axis=-1, keepdims=True) + EPS)
    inner = jnp.mean(x_f32 * d_out, axis=-1, keepdims=True)
    return scale * d_out - x_f32 * (scale * scale * scale * inner)


def gelu_parts(pre):
    square = pre * pre
    tanh = jnp.tanh(GELU_A * (pre + GELU_B * pre * square))
    half = 0.5 * (1.0 + tanh)
    slope = half + 0.5 * pre * (1.0 - tanh * tanh) * (GELU_A + (3.0 * GELU_A * GELU_B) * square)
    return pre * half, slope


def bf16(*shape):
    return jax.ShapeDtypeStruct(shape, jnp.bfloat16)


def backward_stages(pair_of, probs_of, put, low):
    masks = (low, jnp.logical_not(low))

    def from_mixed(j, _=None):
        _, _, v_pair, d_pair = pair_of(j)
        return [dot(v_pair, jnp.where(mask, d_pair, 0), 1, 1).astype(jnp.bfloat16) for mask in masks]

    def through(j, made):
        out = []
        for side, d_probs in enumerate(made):
            d_probs, probs = d_probs.astype(jnp.float32), probs_of(j, side).astype(jnp.float32)
            row_dot = jnp.sum(d_probs * probs, axis=0, keepdims=True)
            out.append((probs * (d_probs - row_dot) * HEAD_DIM ** -0.5).astype(jnp.bfloat16))
        return out

    def to_inputs(j, made):
        q_pair, k_pair, _, d_pair = pair_of(j)
        sides = [(dot(d_scores, k_pair, 0, 0), dot(d_scores, q_pair, 1, 0), dot(probs_of(j, side), d_pair, 1, 0))
                 for side, d_scores in enumerate(made)]
        put(j, [jnp.where(low, first, second) for first, second in zip(*sides)])
    return from_mixed, through, to_inputs


def forward_stages(pair_of, keep, put, low):
    def scores(j, _=None):
        q_pair, k_pair, _ = pair_of(j)
        return [dot(k_pair, jnp.where(mask, q_pair, 0), 1, 1) for mask in (low, jnp.logical_not(low))]

    def soften(j, made):
        out = []
        for side, score in enumerate(made):
            top = jnp.max(score, axis=0, keepdims=True)
            raised = jnp.exp2((score - top) * SOFTMAX_SCALE)
            inverse = 1.0 / jnp.sum(raised, axis=0, keepdims=True)
            out.append((raised * inverse).astype(jnp.bfloat16))
            keep(j, side, out[-1])
        return out

    def mix(j, made):
        first, second = (dot(probs, pair_of(j)[2], 0, 0) for probs in made)
        put(j, jnp.where(low, first, second))
    return scores, soften, mix


def in_units(first, stages, size):
    def lift(stage):
        return lambda unit, made: [stage(size * unit + i, made[i]) for i in range(size)]
    return (lambda unit: first(unit) or [None] * size, *map(lift, stages))


def staged(count, stages):
    made = [None] * count
    for turn in range(count + len(stages) - 1):
        for depth, stage in enumerate(stages):
            j = turn - depth
            if 0 <= j < count:
                made[j] = stage(j, made[j]) if depth else stage(j)


FRONT_OUTS = ("u_0", "q_0", "k_0", "v_0", "probs_0", "mixed_0", "h_0", "n_0", "pre_0", "act_0", "x_1",
              "u_1", "q_1", "k_1", "v_1", "probs_1", "mixed_1", "n_1", "act_1", "dpre_1", "dh_1", "dqa_1", "dka_1", "dva_1")
ROW_BUFFERS = ("u", "q", "k", "v", "mixed", "h", "n", "x", "dh", "dn")
HALF_BUFFERS = ("dqa", "dka", "dva")
WIDE_BLOCK = 1024


def front_kernel(batch, seq, in_names, *refs):
    at = dict(zip((*in_names, *FRONT_OUTS), refs))
    refs = refs[len(at):]
    x_all, cot_all, w_in, w_out, w_up, w_down, probs, pre, act = refs[:9]
    row = dict(zip((*ROW_BUFFERS, *HALF_BUFFERS), refs[9:]))
    load_sem, out_sem = refs[9 + len(row):]
    width, ff = w_up.shape
    heads = width // HEAD_DIM
    loads = {"x": pltpu.make_async_copy(at["x_0"], x_all, load_sem.at[0])}
    for layer in (0, 1):
        for i, name in enumerate(("wq", "wk", "wv")):
            loads[f"{name}_{layer}"] = pltpu.make_async_copy(at[name].at[layer], w_in.at[layer, i], load_sem.at[1 + 4 * layer + i])
        loads[f"wo_{layer}"] = pltpu.make_async_copy(at["wo"].at[layer], w_out.at[layer], load_sem.at[4 + 4 * layer])
    loads["w_up"] = pltpu.make_async_copy(at["w_up"], w_up, load_sem.at[9])
    loads["w_down"] = pltpu.make_async_copy(at["w_down"], w_down, load_sem.at[10])
    loads["cot"] = pltpu.make_async_copy(at["cot"], cot_all, load_sem.at[11])
    for name in ("x", "wq_0", "wk_0", "wv_0"):
        loads[name].start()
    holders = {"probs_0": probs, "probs_1": probs, "pre_0": pre, "act_0": act, "act_1": act, "dpre_1": pre, "x_1": row["x"]}
    for name in FRONT_OUTS:
        holders.setdefault(name, row.get(name[:-2]))

    def store(name, index):
        src = holders[name]
        rows = pl.ds(pl.multiple_of(seq * index, seq), seq)
        dest = at[name].at[index] if name.startswith("probs") else at[name].at[rows]
        return pltpu.make_async_copy(src, dest, out_sem.at[FRONT_OUTS.index(name)])

    def one_sequence(index, carry):
        rows = pl.ds(pl.multiple_of(seq * index, seq), seq)
        first = index == 0
        low = lax.broadcasted_iota(jnp.int32, (seq, PAIR), 1) < HEAD_DIM

        def need(*names):
            @pl.when(first)
            def _():
                for name in names:
                    loads[name].wait()

        def launch(*names):
            @pl.when(first)
            def _():
                for name in names:
                    loads[name].start()

        def free(*names, same=False):
            for name in names:
                if same:
                    store(name, index).wait()
                else:
                    pl.when(index > 0)(lambda name=name: store(name, index - 1).wait())

        def send(*names):
            for name in names:
                store(name, index).start()

        def over(count, fn):
            for j in range(count):
                fn(j)

        def wide(j):
            return pl.ds(WIDE_BLOCK * j, WIDE_BLOCK)

        def attention(layer):
            x_in = x_all[rows] if layer == 0 else row["x"][...]
            row["u"][...] = rms_norm(x_in.astype(jnp.float32)).astype(jnp.bfloat16)
            need(*(f"w{kind}_{layer}" for kind in "qkv"))
            if layer == 0:
                launch("wo_0", "w_up")

            def project(unit):
                lanes = pl.ds(OUT_BLOCK * unit, OUT_BLOCK)
                for i, kind in enumerate("qkv"):
                    row[kind][:, lanes] = dot(row["u"][...], w_in[layer, i, :, lanes], 1, 0).astype(jnp.bfloat16)

            def pair_of(j):
                return tuple(row[kind][:, PAIR * j:PAIR * (j + 1)] for kind in "qkv")

            def keep(j, side, value):
                probs[2 * j + side] = value

            def put(j, value):
                row["mixed"][:, PAIR * j:PAIR * (j + 1)] = value.astype(jnp.bfloat16)
            size = OUT_BLOCK // PAIR
            staged(heads // 2 // size, in_units(project, forward_stages(pair_of, keep, put, low), size))
            need(f"wo_{layer}")
            attn = dot(row["mixed"][...], w_out[layer], 1, 0).astype(jnp.bfloat16)
            hidden = (x_in.astype(jnp.float32) + attn.astype(jnp.float32)).astype(jnp.bfloat16)
            row["h"][...] = hidden
            row["n"][...] = rms_norm(hidden.astype(jnp.float32)).astype(jnp.bfloat16)

        need("x")
        free("u_1", "q_1", "k_1", "v_1", "probs_1", "mixed_1", "n_1", "dh_1")
        attention(0)
        send("u_0", "q_0", "k_0", "v_0", "probs_0", "mixed_0", "h_0", "n_0")
        need("w_up")
        launch("w_down", "wq_1", "wk_1", "wv_1", "wo_1", "cot")
        free("act_1", "dpre_1")

        def raw_block(j):
            return dot(row["n"][...], w_up[:, wide(j)], 1, 0).astype(jnp.bfloat16)

        def up(j, raw):
            pre[:, wide(j)] = raw
            act[:, wide(j)] = gelu_parts(raw.astype(jnp.float32))[0].astype(jnp.bfloat16)
        staged(ff // WIDE_BLOCK, (raw_block, up))
        send("pre_0", "act_0")
        need("w_down")

        def down(j):
            lanes = pl.ds(pl.multiple_of(OUT_BLOCK * j, OUT_BLOCK), OUT_BLOCK)
            out = dot(act[...], w_down[:, lanes], 1, 0).astype(jnp.bfloat16).astype(jnp.float32)
            row["x"][:, lanes] = (row["h"][:, lanes].astype(jnp.float32) + out).astype(jnp.bfloat16)
        over(width // OUT_BLOCK, down)
        send("x_1")
        free("u_0", "q_0", "k_0", "v_0", "probs_0", "mixed_0", "h_0", "n_0", same=True)
        attention(1)
        send("u_1", "q_1", "k_1", "v_1", "probs_1", "mixed_1", "n_1")
        need("cot")
        free("pre_0", "act_0", same=True)

        def both_blocks(j):
            return raw_block(j), dot(cot_all[rows], w_down[wide(j)], 1, 1).astype(jnp.bfloat16)

        def both(j, made):
            raw, d_act = made
            out, slope = gelu_parts(raw.astype(jnp.float32))
            act[:, wide(j)] = out.astype(jnp.bfloat16)
            pre[:, wide(j)] = (d_act.astype(jnp.float32) * slope).astype(jnp.bfloat16)
        staged(ff // WIDE_BLOCK, (both_blocks, both))
        send("act_1", "dpre_1")

        def back(j):
            lanes = pl.ds(pl.multiple_of(OUT_BLOCK * j, OUT_BLOCK), OUT_BLOCK)
            row["dn"][:, lanes] = dot(pre[...], w_up[lanes], 1, 1).astype(jnp.bfloat16)
        over(width // OUT_BLOCK, back)
        d_hidden = cot_all[rows].astype(jnp.float32) + rms_backward(
            row["h"][...].astype(jnp.float32), row["dn"][...].astype(jnp.float32))
        row["dh"][...] = d_hidden.astype(jnp.bfloat16)
        send("dh_1")
        free("dqa_1", "dka_1", "dva_1")

        def unmix(unit):
            lanes = pl.ds(OUT_BLOCK * unit, OUT_BLOCK)
            row["dn"][:, lanes] = dot(row["dh"][...], w_out[1, lanes], 1, 1).astype(jnp.bfloat16)

        def back_of(j):
            return tuple(row[kind][:, PAIR * j:PAIR * (j + 1)] for kind in ("q", "k", "v", "dn"))

        def put_back(j, values):
            for name, value in zip(HALF_BUFFERS, values):
                row[name][:, PAIR * j:PAIR * (j + 1)] = value.astype(jnp.bfloat16)
        size = OUT_BLOCK // PAIR
        stages = backward_stages(back_of, lambda j, side: probs[2 * j + side], put_back, low)
        staged(heads // 4 // size, in_units(unmix, stages, size))
        send("dqa_1", "dka_1", "dva_1")
        free("x_1", same=True)
        return carry

    lax.fori_loop(0, batch, one_sequence, 0)
    for name in ("u_1", "q_1", "k_1", "v_1", "probs_1", "mixed_1", "n_1", "act_1", "dpre_1", "dh_1", "dqa_1", "dka_1", "dva_1"):
        store(name, batch - 1).wait()


def front(inputs, batch, seq):
    tokens, width = inputs["x_0"].shape
    ff = inputs["w_up"].shape[1]
    heads = width // HEAD_DIM
    shapes = []
    for name in FRONT_OUTS:
        if name.startswith("probs"):
            shapes.append(bf16(batch, heads, seq, seq))
        else:
            wide = ff if name[:-2] in ("pre", "act", "dpre") else width
            shapes.append(bf16(tokens, width // 2 if name[:-2] in HALF_BUFFERS else wide))
    block = lambda *shape: pltpu.VMEM(shape, jnp.bfloat16)
    scratch = [
        block(tokens, width), block(tokens, width), block(2, 3, width, width), block(2, width, width), block(width, ff),
        block(ff, width), block(heads, seq, seq), block(seq, ff), block(seq, ff),
        *[block(seq, width) for _ in ROW_BUFFERS], *[block(seq, width // 2) for _ in HALF_BUFFERS],
        pltpu.SemaphoreType.DMA((12,)), pltpu.SemaphoreType.DMA((len(FRONT_OUTS),)),
    ]
    outs = pl.pallas_call(
        functools.partial(front_kernel, batch, seq, tuple(inputs)),
        out_shape=shapes,
        in_specs=[pl.BlockSpec(memory_space=pl.ANY)] * len(inputs),
        out_specs=[pl.BlockSpec(memory_space=pl.ANY)] * len(shapes),
        scratch_shapes=scratch,
        compiler_params=pltpu.CompilerParams(vmem_limit_bytes=67_043_328),
        cost_estimate=pl.CostEstimate(flops=22 * tokens * width * ff // 2, bytes_accessed=100 * MIB, transcendentals=0),
        name="front",
    )(*inputs.values())
    return dict(zip(FRONT_OUTS, outs))


MESH = pl.DeviceIdType.MESH
LANES = 1024
SET_ROWS = 128
CORE_ROWS = 2 * SET_ROWS
TILE_ROWS = 2 * CORE_ROWS
OWN_SLOTS = 8
AG_SLOTS = 10
TYPES = {
    "p1": (0, 0, 80, "xyz"),
    "q1": (0, 80, 48, "zxy"),
    "p2": (1, 128, 80, "yxz"),
    "q2": (1, 208, 48, "zyx"),
}
WRITE_AT = 11


def stage_list():
    stages = []
    for name, (_, _, _, order) in TYPES.items():
        if order[2] == "z":
            plan = [("rs1", 1), ("rs2", 2), ("rsz", 3), ("agz", 6), ("ag2", 9), ("ag1", 10)]
        else:
            plan = [("rsz", 1), ("rs1", 4), ("rs2", 5), ("ag2", 6), ("ag1", 7), ("agz", 8)]
        for kind, at in plan:
            if kind in ("rsz", "agz"):
                for step in range(3):
                    for way in (0, 1):
                        stages.append((name, kind, step, way, at + step))
            else:
                stages.append((name, kind, 0, 0, at))
    return stages


STAGES = stage_list()


def piece_shape(name, kind):
    rows, order = TYPES[name][2], TYPES[name][3]
    if order[2] == "z":
        return {"rs1": (rows, 512), "rs2": (rows, 256), "rsz": (rows // 2, 128)}[kind]
    return {"rsz": (rows // 2, 512), "rs1": (rows // 2, 256), "rs2": (rows // 2, 128)}[kind]


def between(step, first, count):
    return jnp.logical_and(step >= first, step < first + count)


class Backward:
    PB_1, MB, AB, PB_0 = 3, 6, 14, 23
    ROWS = 256

    def __init__(self, at, big, total_buf, w_buf, p_buf, sem, drain):
        self.at, self.big, self.total, self.w, self.p, self.sem, self.drain = at, big, total_buf, w_buf, p_buf, sem, drain
        self.tokens, self.width = at["x_0"].shape
        self.heads = at["probs_0"].shape[1]
        self.seq = at["probs_0"].shape[2]
        self.seqs = self.tokens // self.seq

    def load(self, name, dest, sem, *index):
        ref = self.at[name]
        return pltpu.make_async_copy(ref.at[index] if index else ref, dest, self.sem.at[sem])

    def store(self, src, name, sem, *index):
        ref = self.at[name]
        return pltpu.make_async_copy(src, ref.at[index] if index else ref, self.drain.at[sem])

    def row_blocks(self, fn):
        def body(block, carry):
            fn(pl.ds(pl.multiple_of(self.ROWS * block, self.ROWS), self.ROWS))
            return carry
        lax.fori_loop(0, self.tokens // self.ROWS, body, 0)

    def input_loads(self, layer):
        copies = [self.load(f"x_{layer}", self.big.at[5], 3)]
        for i, kind in enumerate("qkv"):
            if layer:
                half = self.width // 2
                copies.append(self.load(f"d{kind}a_1", self.big.at[i, :, pl.ds(0, half)], i))
                copies.append(self.load(f"d{kind}b_1", self.big.at[i, :, pl.ds(half, half)], 11 + i))
            else:
                copies.append(self.load(f"d{kind}_0", self.big.at[i], i))
        return copies

    def weight_loads(self, layer, block):
        rows = pl.ds(pl.multiple_of(OUT_BLOCK * block, OUT_BLOCK), OUT_BLOCK)
        slot = lax.rem(block, 2)
        return [self.load(name, self.w.at[slot, i], 5 + 3 * slot + i, layer, rows) for i, name in enumerate(("wq", "wk", "wv"))]

    def input_block(self, layer, block):
        big, blocks = self.big, self.width // OUT_BLOCK
        slot = lax.rem(block, 2)

        @pl.when(block == 0)
        def _():
            for copy in self.input_loads(layer):
                copy.wait()
        for copy in self.weight_loads(layer, block):
            copy.wait()

        @pl.when(block + 1 < blocks)
        def _():
            for copy in self.weight_loads(layer, block + 1):
                copy.start()
        lanes = pl.ds(pl.multiple_of(OUT_BLOCK * block, OUT_BLOCK), OUT_BLOCK)

        def product(rows):
            total = dot(big[0, rows], self.w[slot, 0], 1, 1) + dot(big[1, rows], self.w[slot, 1], 1, 1)
            big[3, rows, lanes] = (total + dot(big[2, rows], self.w[slot, 2], 1, 1)).astype(jnp.bfloat16)
        self.row_blocks(product)

        @pl.when(block == blocks - 1)
        def _():
            def close(rows):
                back = rms_backward(big[5, rows].astype(jnp.float32), big[3, rows].astype(jnp.float32))
                big[3, rows] = (big[4, rows].astype(jnp.float32) + back).astype(jnp.bfloat16)
                if layer:
                    self.total[rows] = jnp.zeros((self.ROWS, self.width), jnp.float32)
            self.row_blocks(close)
            self.store(big.at[3], f"dx_{layer}", 0).start()
            if layer:
                self.load("h_0", big.at[4], 3).start()
                for copy in self.mlp_loads(0):
                    copy.start()

    def mlp_loads(self, block):
        slot = lax.rem(block, 2)
        lanes = pl.ds(pl.multiple_of(FF_BLOCK * block, FF_BLOCK), FF_BLOCK)
        half = pl.ds(pl.multiple_of(FF_BLOCK * slot, FF_BLOCK), FF_BLOCK)
        return [self.load("w_up", self.big.at[0, :, half], 5 + 3 * slot, slice(None), lanes),
                self.load("pre_0", self.big.at[1, :, half], 6 + 3 * slot, slice(None), lanes),
                self.load("w_down", self.big.at[5, half], 7 + 3 * slot, lanes)]

    def mlp_store(self, block):
        half = pl.ds(pl.multiple_of(FF_BLOCK * lax.rem(block, 2), FF_BLOCK), FF_BLOCK)
        lanes = pl.ds(pl.multiple_of(FF_BLOCK * block, FF_BLOCK), FF_BLOCK)
        return self.store(self.big.at[2, :, half], "dpre_0", 1, slice(None), lanes)

    def mlp_block(self, block):
        big, blocks = self.big, self.at["w_up"].shape[1] // FF_BLOCK

        @pl.when(block == 0)
        def _():
            self.store(big.at[3], "dx_1", 0).wait()
            self.load("h_0", big.at[4], 3).wait()
        for copy in self.mlp_loads(block):
            copy.wait()

        @pl.when(block + 1 < blocks)
        def _():
            for copy in self.mlp_loads(block + 1):
                copy.start()

        @pl.when(block > 0)
        def _():
            self.mlp_store(block - 1).wait()
        half = pl.ds(pl.multiple_of(FF_BLOCK * lax.rem(block, 2), FF_BLOCK), FF_BLOCK)

        def product(rows):
            d_act = dot(big[3, rows], big[5, half], 1, 1).astype(jnp.bfloat16).astype(jnp.float32)
            slope = gelu_parts(big[1, rows, half].astype(jnp.float32))[1]
            d_pre = (d_act * slope).astype(jnp.bfloat16)
            big[2, rows, half] = d_pre
            self.total[rows] += dot(d_pre, big[0, :, half], 1, 1)
        self.row_blocks(product)
        self.mlp_store(block).start()

        @pl.when(block == blocks - 1)
        def _():
            def close(rows):
                d_normed = self.total[rows].astype(jnp.bfloat16).astype(jnp.float32)
                back = rms_backward(big[4, rows].astype(jnp.float32), d_normed)
                big[4, rows] = (big[3, rows].astype(jnp.float32) + back).astype(jnp.bfloat16)
            self.row_blocks(close)
            self.store(big.at[4], "dh_0", 2).start()
            self.load("wo", big.at[0], 4, 0).start()
            for copy in self.piece_loads(0, 0):
                copy.start()

    def where(self, piece):
        seq, half = lax.rem(piece, self.seqs), lax.div(piece, self.seqs)
        rows = pl.ds(pl.multiple_of(self.seq * seq, self.seq), self.seq)
        lanes = pl.ds(pl.multiple_of(self.width // 2 * half, self.width // 2), self.width // 2)
        return seq, half, rows, lanes

    def piece_loads(self, layer, piece):
        seq, half, rows, lanes = self.where(piece)
        near = pl.ds(0, self.width // 2)
        copies = [self.load(f"{kind}_{layer}", self.big.at[1 + lax.rem(piece, 2), pl.ds(self.seq * i, self.seq), near], i, rows, lanes)
                  for i, kind in enumerate("qkv")]
        heads = pl.ds(self.heads // 2 * half, self.heads // 2)
        return copies + [self.load(f"probs_{layer}", self.p.at[lax.rem(piece, 2)], 5, seq, heads)]

    def piece_stores(self, layer, piece):
        _, _, rows, lanes = self.where(piece)
        near, spot = pl.ds(0, self.width // 2), 5 - 2 * lax.rem(piece, 2)
        sources = [self.big.at[spot, pl.ds(self.seq * i, self.seq), near] for i in range(3)]
        if layer:
            return [self.store(src, f"d{kind}b_1", 3 + i, rows) for i, (src, kind) in enumerate(zip(sources, "qkv"))]
        return [self.store(src, f"d{kind}_0", 3 + i, rows, lanes) for i, (src, kind) in enumerate(zip(sources, "qkv"))]

    def attention_piece(self, layer, piece):
        big, p_buf, pieces = self.big, self.p, 2 * self.seqs
        _, half, rows, _ = self.where(piece)
        parity = lax.rem(piece, 2)
        spot, out = 1 + parity, 5 - 2 * parity

        start = self.seqs * layer

        @pl.when(piece == start)
        def _():
            if layer == 0:
                self.mlp_store(self.at["w_up"].shape[1] // FF_BLOCK - 1).wait()
                self.store(big.at[4], "dh_0", 2).wait()
            else:
                self.load("dh_1", big.at[4], 3).wait()
            self.load("wo", big.at[0], 4, layer).wait()

        @pl.when(piece > start)
        def _():
            for copy in self.piece_stores(layer, piece - 1):
                copy.wait()
        for copy in self.piece_loads(layer, piece):
            copy.wait()

        @pl.when(piece + 1 < pieces)
        def _():
            for copy in self.piece_loads(layer, piece + 1):
                copy.start()
        low = lax.broadcasted_iota(jnp.int32, (self.seq, PAIR), 1) < HEAD_DIM

        def unmix(unit):
            w_rows = pl.ds(pl.multiple_of(self.width // 2 * half + OUT_BLOCK * unit, OUT_BLOCK), OUT_BLOCK)
            d_mixed = dot(big[4, rows], big[0, w_rows], 1, 1)
            big[spot, pl.ds(3 * self.seq, self.seq), pl.ds(OUT_BLOCK * unit, OUT_BLOCK)] = d_mixed.astype(jnp.bfloat16)

        def pair_of(j):
            return tuple(big[spot, pl.ds(self.seq * i, self.seq), pl.ds(PAIR * j, PAIR)] for i in range(4))

        def put(j, values):
            for i, value in enumerate(values):
                big[out, pl.ds(self.seq * i, self.seq), pl.ds(PAIR * j, PAIR)] = value.astype(jnp.bfloat16)
        size = OUT_BLOCK // PAIR
        stages = backward_stages(pair_of, lambda j, side: p_buf[parity, 2 * j + side], put, low)
        staged(self.heads // 4 // size, in_units(unmix, stages, size))
        for copy in self.piece_stores(layer, piece):
            copy.start()

    def begin(self):
        self.load("dh_1", self.big.at[4], 3).start()
        self.load("wo", self.big.at[0], 4, 1).start()
        for copy in self.piece_loads(1, self.seqs):
            copy.start()

    def item(self, step):
        blocks = self.width // OUT_BLOCK
        pieces = 2 * self.seqs

        @pl.when(step < 3)
        def _():
            first = self.seqs + step
            count = jnp.where(step == 2, self.seqs - 2, 1)
            lax.fori_loop(first, first + count, lambda piece, carry: self.attention_piece(1, piece) or carry, 0)

        @pl.when(step == self.PB_1 - 1)
        def _():
            for copy in self.piece_stores(1, pieces - 1):
                copy.wait()
            for copy in self.input_loads(1) + self.weight_loads(1, 0):
                copy.start()

        @pl.when(between(step, self.PB_1, blocks - 1))
        def _():
            first = step - self.PB_1
            count = jnp.where(first == blocks - 2, 2, 1)
            lax.fori_loop(first, first + count, lambda block, carry: self.input_block(1, block) or carry, 0)
        pl.when(between(step, self.MB, 8))(lambda: self.mlp_block(step - self.MB))
        pl.when(between(step, self.AB, pieces))(lambda: self.attention_piece(0, step - self.AB))

        @pl.when(step == self.PB_0 - 1)
        def _():
            for copy in self.piece_stores(0, pieces - 1):
                copy.wait()
            for copy in self.input_loads(0) + self.weight_loads(0, 0):
                copy.start()
        pl.when(between(step, self.PB_0, blocks))(lambda: self.input_block(0, step - self.PB_0))

        @pl.when(step == self.PB_0 + blocks)
        def _():
            self.store(self.big.at[3], "dx_0", 0).wait()


def finish_kernel(groups, chunks, in_names, out_names, remote, *refs):
    names = [*in_names, *out_names]
    at, scratch = dict(zip(names, refs[:len(names)])), refs[len(names):]
    (big, total_buf, w_buf, p_buf, item_sem, drain_sem), scratch = scratch[:6], scratch[6:]
    backward = Backward(at, big, total_buf, w_buf, p_buf, item_sem, drain_sem)
    if not remote:
        backward.begin()

        def alone(step, carry):
            backward.item(step)
            return carry
        lax.fori_loop(0, chunks + WRITE_AT + 1, alone, 0)
        return
    (lhs_buf, rhs_buf, own, part, part_in, gath), scratch = scratch[:6], scratch[6:]
    land_keys = [key for key, st in enumerate(STAGES) if st[1].startswith("rs")]
    landing = dict(zip(land_keys, scratch[:len(land_keys)]))
    load_sem, send_sem, recv_sem, pair_send, pair_recv, out_sem, out_send, out_recv, credit = scratch[len(land_keys):]

    me = lax.axis_index("data")
    core = lax.rem(me, 2)
    coord = {"x": lax.rem(lax.div(me, 2), 2), "y": lax.rem(lax.div(me, 4), 2)}
    z = lax.div(me, 8)
    partner = me + 1 - 2 * core
    near = {"x": me + 2 - 4 * coord["x"], "y": me + 4 - 8 * coord["y"]}
    up_ok, down_ok = z < 3, z > 0
    peers = [(partner, 0, None), (near["x"], 1, None), (near["y"], 2, None), (me + 8, 3, up_ok), (me - 8, 4, down_ok)]

    def guarded(cond, fn):
        if cond is None:
            fn()
        else:
            pl.when(cond)(fn)

    barrier = pltpu.get_barrier_semaphore()
    for dev, _, cond in peers:
        guarded(cond, lambda dev=dev: pl.semaphore_signal(barrier, inc=1, device_id=(dev,), device_id_type=MESH))
    inner = jnp.logical_and(up_ok, down_ok)
    guarded(inner, lambda: pl.semaphore_wait(barrier, 5))
    guarded(jnp.logical_not(inner), lambda: pl.semaphore_wait(barrier, 4))

    def region(name, kind, which):
        _, row, rows, order = TYPES[name]
        if order[2] == "z":
            h1, h2 = coord[order[0]], coord[order[1]]
            if kind == "1":
                return pl.ds(row, rows), pl.ds(pl.multiple_of(512 * which, 128), 512)
            if kind == "2":
                return pl.ds(row, rows), pl.ds(pl.multiple_of(512 * h1 + 256 * which, 128), 256)
            first = pl.multiple_of(row + (rows // 2) * lax.div(which, 2), 8)
            lane = pl.multiple_of(512 * h1 + 256 * h2 + 128 * lax.rem(which, 2), 128)
            return pl.ds(first, rows // 2), pl.ds(lane, 128)
        h1 = coord[order[1]]
        if kind == "z":
            first = pl.multiple_of(row + (rows // 2) * lax.div(which, 2), 8)
            return pl.ds(first, rows // 2), pl.ds(pl.multiple_of(512 * lax.rem(which, 2), 128), 512)
        first = pl.multiple_of(row + (rows // 2) * lax.div(z, 2), 8)
        if kind == "1":
            return pl.ds(first, rows // 2), pl.ds(pl.multiple_of(512 * lax.rem(z, 2) + 256 * which, 128), 256)
        lane = pl.multiple_of(512 * lax.rem(z, 2) + 256 * h1 + 128 * which, 128)
        return pl.ds(first, rows // 2), pl.ds(lane, 128)

    def exchange_axis(name, kind):
        order = TYPES[name][3]
        dims = order[:2] if order[2] == "z" else order[1:]
        return dims[int(kind) - 1]

    def plan(key, chunk, parity):
        name, kind, step, way, _ = STAGES[key]
        mine, slot = lax.rem(chunk, OWN_SLOTS), lax.rem(chunk, AG_SLOTS)
        if kind in ("rs1", "rs2"):
            axis = exchange_axis(name, kind[2])
            src, keep = region(name, kind[2], 1 - coord[axis]), region(name, kind[2], coord[axis])
            dev, send_ok, recv_ok = near[axis], None, None
            sent = own.at[mine, src[0], src[1]]
        elif kind in ("ag1", "ag2"):
            axis = exchange_axis(name, kind[2])
            src = keep = region(name, kind[2], coord[axis])
            dev, send_ok, recv_ok = near[axis], None, None
            sent = gath.at[slot, src[0], src[1]]
        elif kind == "rsz":
            if way:
                dev, k_send, k_keep = me + 8, z + 3 - step, z + 2 - step
                send_ok, recv_ok = k_send <= 3, jnp.logical_and(k_keep <= 3, down_ok)
            else:
                dev, k_send, k_keep = me - 8, z - 3 + step, z - 2 + step
                send_ok, recv_ok = k_send >= 0, jnp.logical_and(k_keep >= 0, up_ok)
            src, keep = region(name, "z", k_send), region(name, "z", k_keep)
            sent = own.at[mine, src[0], src[1]]
        else:
            if way:
                dev, k_send, k_keep = me + 8, z - step, z - 1 - step
                send_ok, recv_ok = jnp.logical_and(k_send >= 0, up_ok), k_keep >= 0
            else:
                dev, k_send, k_keep = me - 8, z + step, z + 1 + step
                send_ok, recv_ok = jnp.logical_and(k_send <= 3, down_ok), k_keep <= 3
            src, keep = region(name, "z", k_send), region(name, "z", k_keep)
            sent = gath.at[slot, src[0], src[1]]
        sems = dict(send_sem=send_sem.at[key, parity], recv_sem=recv_sem.at[key, parity], device_id=(dev,), device_id_type=MESH)
        if kind.startswith("rs"):
            target = landing[key].at[parity]
            send = lambda: pltpu.make_async_remote_copy(src_ref=sent, dst_ref=target, **sems)
            recv = lambda: pltpu.make_async_remote_copy(
                src_ref=own.at[mine, keep[0], keep[1]], dst_ref=target, **sems)

            def arrive():
                own[mine, keep[0], keep[1]] += landing[key][parity]
        else:
            send = lambda: pltpu.make_async_remote_copy(src_ref=sent, dst_ref=sent, **sems)
            recv = lambda: pltpu.make_async_remote_copy(
                src_ref=gath.at[slot, keep[0], keep[1]], dst_ref=gath.at[slot, keep[0], keep[1]], **sems)
            arrive = None
        return send, recv, send_ok, recv_ok, arrive

    def finish(name, chunk):
        order = TYPES[name][3]
        reg = region(name, "z", z) if order[2] == "z" else region(name, "2", coord[order[2]])
        gath[lax.rem(chunk, AG_SLOTS), reg[0], reg[1]] = own[lax.rem(chunk, OWN_SLOTS), reg[0], reg[1]]

    def valid(chunk):
        return jnp.logical_and(chunk >= 0, chunk < chunks)

    def set_rows(half):
        return pl.ds(half * SET_ROWS, SET_ROWS)

    def pair_copy(half, parity):
        return pltpu.make_async_remote_copy(
            src_ref=part.at[parity, set_rows(half)], dst_ref=part_in.at[parity, set_rows(half)],
            send_sem=pair_send.at[half], recv_sem=pair_recv.at[half, parity], device_id=(partner,), device_id_type=MESH)

    half_lanes = LANES // 2

    def outlets(half, group, local, whose):
        out, layer = group["out"]
        ref = at[out] if layer is None else at[out].at[layer]
        rows, cols = group["place"](local)
        if not group["narrow"]:
            first = pl.multiple_of(rows + CORE_ROWS * whose + half * SET_ROWS, SET_ROWS)
            return [(pl.ds(0, LANES), ref.at[pl.ds(first, SET_ROWS), pl.ds(pl.multiple_of(cols, 128), LANES)])]
        places = []
        for sub in (0, 1):
            first = pl.multiple_of(2 * CORE_ROWS * whose + CORE_ROWS * sub + half * SET_ROWS, SET_ROWS)
            places.append((pl.ds(half_lanes * sub, half_lanes), ref.at[pl.ds(first, SET_ROWS), pl.ds(cols, half_lanes)]))
        return places

    def write_copies(half, chunk, lanes, dest):
        slot = lax.rem(chunk, AG_SLOTS)
        src = gath.at[slot, set_rows(half), lanes]
        here = pltpu.make_async_copy(src, dest, out_sem.at[half])
        there = pltpu.make_async_remote_copy(
            src_ref=src, dst_ref=dest, send_sem=out_send.at[half], recv_sem=out_recv.at[half, lax.rem(chunk, 2)],
            device_id=(partner,), device_id_type=MESH)
        return here, there

    def load_copies(group, local, slot):
        rows, cols = group["place"](local)
        narrow = group["narrow"]
        lhs, rhs = [], []
        for sub in range(2 if narrow else len(group["lhs"])):
            for whose in (0, 1):
                owner = core if whose == 0 else 1 - core
                first = 2 * CORE_ROWS * owner + CORE_ROWS * sub if narrow else rows + CORE_ROWS * owner
                source = at[group["lhs"][0 if narrow else sub]]
                lhs.append(pltpu.make_async_copy(
                    source.at[:, pl.ds(pl.multiple_of(first, CORE_ROWS), CORE_ROWS)],
                    lhs_buf.at[slot, sub, whose], load_sem.at[slot, sub, whose]))
        for app, name in enumerate(group["rhs"]):
            size = half_lanes if narrow else LANES
            rhs.append(pltpu.make_async_copy(
                at[name].at[:, pl.ds(0 if narrow else pl.multiple_of(cols, 128), size)], rhs_buf.at[slot, app, :, pl.ds(0, size)],
                load_sem.at[slot, app, 2]))
        return lhs, rhs

    def for_group(chunk, fn):
        for group in groups:
            inside = jnp.logical_and(chunk >= group["start"], chunk < group["start"] + group["count"])
            pl.when(inside)(functools.partial(fn, group, chunk - group["start"]))

    def among(chunk, chosen):
        flags = [jnp.logical_and(chunk >= g["start"], chunk < g["start"] + g["count"]) for g in groups if chosen(g)]
        return functools.reduce(jnp.logical_or, flags)

    def is_two(group):
        return len(group["lhs"]) == 2

    def is_narrow(group):
        return group["narrow"]

    def start_load(chunk):
        def go(group, local):
            for copy in sum(load_copies(group, local, lax.rem(chunk, 2)), []):
                copy.start()
        for_group(chunk, go)

    def wait_load(chunk):
        slot = lax.rem(chunk, 2)
        two_lhs, two_rhs = load_copies(next(filter(is_two, groups)), 0, slot)
        slim_lhs, slim_rhs = load_copies(next(filter(is_narrow, groups)), 0, slot)
        for copy in two_lhs[:2]:
            copy.wait()

        @pl.when(jnp.logical_not(among(chunk, is_narrow)))
        def _():
            two_rhs[0].wait()

        @pl.when(among(chunk, is_narrow))
        def _():
            for copy in slim_rhs + slim_lhs[2:]:
                copy.wait()

        @pl.when(among(chunk, is_two))
        def _():
            for copy in two_lhs[2:] + two_rhs[1:]:
                copy.wait()

    def tile(chunk):
        slot, mine, parity = lax.rem(chunk, 2), lax.rem(chunk, OWN_SLOTS), lax.rem(chunk, 2)

        def product(sub, whose, rhs):
            return dot(lhs_buf[slot, sub, whose], rhs, 0, 0)

        @pl.when(among(chunk, is_narrow))
        def _():
            for sub in (0, 1):
                lanes, rhs = pl.ds(half_lanes * sub, half_lanes), rhs_buf[slot, 0, :, pl.ds(0, half_lanes)]
                own[mine, :, lanes] = product(sub, 0, rhs)
                part[parity, :, lanes] = product(sub, 1, rhs)

        @pl.when(jnp.logical_not(among(chunk, is_narrow)))
        def _():
            own[mine] = product(0, 0, rhs_buf[slot, 0])
            part[parity] = product(0, 1, rhs_buf[slot, 0])

        @pl.when(among(chunk, is_two))
        def _():
            own[mine] += product(1, 0, rhs_buf[slot, 1])
            part[parity] += product(1, 1, rhs_buf[slot, 1])

    last = chunks + WRITE_AT

    def section(half, step):
        before = lax.rem(step + 1, 2)
        now = lax.rem(step, 2)
        names = [name for name in TYPES if TYPES[name][0] == half]
        at_stage = {}
        for key, (name, _, _, _, at) in enumerate(STAGES):
            if name in names:
                at_stage.setdefault((at, name), []).append(key)
        finals = {name: max(st[4] for st in STAGES if st[0] == name and st[1].startswith("rs")) for name in names}

        def start(at, name):
            chunk = step - at

            @pl.when(valid(chunk))
            def _():
                for key in at_stage[at, name]:
                    send, _, send_ok, _, _ = plan(key, chunk, now)
                    guarded(send_ok, lambda send=send: send().start())

        def finish_stage(at, name):
            chunk = step - 1 - at

            @pl.when(valid(chunk))
            def _():
                for key in at_stage[at, name]:
                    send, recv, send_ok, recv_ok, arrive = plan(key, chunk, before)

                    def arrived(recv=recv, arrive=arrive):
                        recv().wait_recv()
                        if arrive is not None:
                            arrive()
                    guarded(recv_ok, arrived)
                    guarded(send_ok, lambda send=send: send().wait_send())
                if at == finals[name]:
                    finish(name, chunk)

        @pl.when(step > 0)
        def _():
            for dev, way, cond in peers:
                guarded(cond, lambda way=way: pl.semaphore_wait(credit.at[half, way], 1))

        @pl.when(valid(step - 1))
        def _():
            copy = pair_copy(half, before)
            copy.wait_send()
            copy.wait_recv()
            mine = lax.rem(step - 1, OWN_SLOTS)
            own[mine, set_rows(half)] += part_in[before, set_rows(half)]

        done = step - 1 - WRITE_AT

        @pl.when(valid(done))
        def _():
            (lanes, dest), = outlets(half, next(filter(is_two, groups)), 0, 0)
            here, there = write_copies(half, done, lanes, dest)
            here.wait()
            there.wait_send()
            there.wait_recv()

        held = []
        for name in names:
            start(1, name)
        for at in range(1, WRITE_AT):
            for name in names:
                finish_stage(at, name)
                if held:
                    start(*held.pop(0))
                if at + 1 < WRITE_AT:
                    held.append((at + 1, name))
        assert not held
        out_chunk = step - WRITE_AT

        @pl.when(step < last)
        def _():
            for dev, way, cond in peers:
                to = way if way < 3 else 7 - way
                guarded(cond, lambda dev=dev, to=to: pl.semaphore_signal(
                    credit.at[half, to], inc=1, device_id=(dev,), device_id_type=MESH))

        @pl.when(valid(out_chunk))
        def _():
            def go(group, local):
                for lanes, dest in outlets(half, group, local, core):
                    for copy in write_copies(half, out_chunk, lanes, dest):
                        copy.start()
            for_group(out_chunk, go)

    backward.begin()
    start_load(jnp.int32(0))

    def round_(step, carry):
        section(0, step)

        @pl.when(valid(step))
        def _():
            pl.when(step + 1 < chunks)(lambda: start_load(step + 1))
            wait_load(step)
            tile(step)
            pair_copy(0, lax.rem(step, 2)).start()

        section(1, step)

        @pl.when(valid(step))
        def _():
            pair_copy(1, lax.rem(step, 2)).start()

        backward.item(step)
        return carry

    lax.fori_loop(0, last + 1, round_, 0)


def finish_backward(inputs, groups, chunks, weights, tokens, seq, collective_id=0, remote=True):
    width, ff = inputs["w_up"].shape
    landing = [pltpu.VMEM((2,) + piece_shape(st[0], st[1]), jnp.float32) for st in STAGES if st[1].startswith("rs")]
    apps = 2
    outs = {name: jax.ShapeDtypeStruct(shape, jnp.float32) for name, shape in weights.items()}
    for name in ("dx_0", "dx_1", "dh_0", "dq_0", "dk_0", "dv_0"):
        outs[name] = bf16(tokens, width)
    for name in ("dqb_1", "dkb_1", "dvb_1"):
        outs[name] = bf16(tokens, width // 2)
    outs["dpre_0"] = bf16(tokens, ff)
    heads = width // HEAD_DIM
    scratch = [
        pltpu.VMEM((6, tokens, width), jnp.bfloat16),
        pltpu.VMEM((tokens, width), jnp.float32),
        pltpu.VMEM((2, 3, OUT_BLOCK, width), jnp.bfloat16),
        pltpu.VMEM((2, heads // 2, seq, seq), jnp.bfloat16),
        pltpu.SemaphoreType.DMA((14,)),
        pltpu.SemaphoreType.DMA((6,)),
    ]
    if remote:
        scratch += [
            pltpu.VMEM((2, apps, 2, tokens, CORE_ROWS), jnp.bfloat16),
            pltpu.VMEM((2, apps, tokens, LANES), jnp.bfloat16),
            pltpu.VMEM((OWN_SLOTS, CORE_ROWS, LANES), jnp.float32),
            pltpu.VMEM((2, CORE_ROWS, LANES), jnp.float32),
            pltpu.VMEM((2, CORE_ROWS, LANES), jnp.float32),
            pltpu.VMEM((AG_SLOTS, CORE_ROWS, LANES), jnp.float32),
            *landing,
            pltpu.SemaphoreType.DMA((2, apps, 3)),
            pltpu.SemaphoreType.DMA((len(STAGES), 2)),
            pltpu.SemaphoreType.DMA((len(STAGES), 2)),
            pltpu.SemaphoreType.DMA((2,)),
            pltpu.SemaphoreType.DMA((2, 2)),
            pltpu.SemaphoreType.DMA((2,)),
            pltpu.SemaphoreType.DMA((2,)),
            pltpu.SemaphoreType.DMA((2, 2)),
            pltpu.SemaphoreType.REGULAR((2, 5)),
        ]
    params = dict(collective_id=collective_id, has_side_effects=True) if remote else {}
    results = pl.pallas_call(
        functools.partial(finish_kernel, groups, chunks, list(inputs), list(outs), remote),
        out_shape=list(outs.values()),
        in_specs=[pl.BlockSpec(memory_space=pl.ANY)] * len(inputs),
        out_specs=[pl.BlockSpec(memory_space=pl.ANY)] * len(outs),
        scratch_shapes=scratch,
        compiler_params=pltpu.CompilerParams(vmem_limit_bytes=67_043_328, **params),
        cost_estimate=pl.CostEstimate(flops=20 * tokens * width * ff, bytes_accessed=256 * MIB, transcendentals=0),
        name="finish_backward",
    )(*inputs.values())
    return dict(zip(outs, results))


DELIVER_ROWS = 256
DELIVER_SLOTS = 40
DELIVER_AHEAD = 20


def deliver(arrays, small):
    def blocks_of(array):
        lead = [(i,) for i in range(array.shape[0])] if len(array.shape) == 3 else [()]
        rows, cols = array.shape[-2:]
        return [(*index, pl.ds(row, DELIVER_ROWS), pl.ds(col, LANES))
                for index in lead for row in range(0, rows, DELIVER_ROWS) for col in range(0, cols, LANES)]

    work = [(i, index) for i, array in enumerate(arrays) for index in blocks_of(array)]
    count = len(arrays) + 1

    def kernel(*refs):
        ins, outs, buf, whole_buf, in_sem, out_sem, whole_sem = refs[:count], refs[count:2 * count], *refs[2 * count:]
        whole_in = pltpu.make_async_copy(ins[-1], whole_buf, whole_sem.at[0])
        whole_out = pltpu.make_async_copy(whole_buf, outs[-1], whole_sem.at[1])

        def fetch(t):
            i, index = work[t]
            return pltpu.make_async_copy(ins[i].at[index], buf.at[t % DELIVER_SLOTS], in_sem.at[t % DELIVER_SLOTS])

        def put(t):
            i, index = work[t]
            return pltpu.make_async_copy(buf.at[t % DELIVER_SLOTS], outs[i].at[index], out_sem.at[t % DELIVER_SLOTS])

        whole_in.start()
        for t in range(min(DELIVER_AHEAD, len(work))):
            fetch(t).start()
        whole_in.wait()
        whole_out.start()
        for t in range(len(work)):
            if t + DELIVER_AHEAD < len(work):
                if t + DELIVER_AHEAD >= DELIVER_SLOTS:
                    put(t + DELIVER_AHEAD - DELIVER_SLOTS).wait()
                fetch(t + DELIVER_AHEAD).start()
            fetch(t).wait()
            put(t).start()
        for t in range(max(0, len(work) - DELIVER_SLOTS), len(work)):
            put(t).wait()
        whole_out.wait()

    return pl.pallas_call(
        kernel,
        out_shape=[jax.ShapeDtypeStruct(array.shape, array.dtype) for array in (*arrays, small)],
        in_specs=[pl.BlockSpec(memory_space=pl.ANY)] * count,
        out_specs=[pl.BlockSpec(memory_space=pl.ANY)] * count,
        scratch_shapes=[pltpu.VMEM((DELIVER_SLOTS, DELIVER_ROWS, LANES), jnp.float32), pltpu.VMEM(small.shape, small.dtype),
                        pltpu.SemaphoreType.DMA((DELIVER_SLOTS,)), pltpu.SemaphoreType.DMA((DELIVER_SLOTS,)),
                        pltpu.SemaphoreType.DMA((2,))],
        compiler_params=pltpu.CompilerParams(vmem_limit_bytes=67_043_328),
        cost_estimate=pl.CostEstimate(flops=0, bytes_accessed=2 * sum(a.size for a in arrays) * 4, transcendentals=0),
        name="deliver",
    )(*arrays, small)


def gradient_groups(width, ff):
    groups = []

    def add(count, lhs, rhs, out, place, narrow=False):
        start = groups[-1]["start"] + groups[-1]["count"] if groups else 0
        groups.append(dict(start=start, count=count, lhs=lhs, rhs=rhs, out=out, place=place, narrow=narrow))

    def tall(local):
        return TILE_ROWS * local, 0

    def wide(local):
        return TILE_ROWS * lax.rem(local, width // TILE_ROWS), LANES * lax.div(local, width // TILE_ROWS)

    for half in (0, 1):
        for kind in "qkv":
            add(1, ["u_1"], [f"d{kind}{'ab'[half]}_1"], (f"g_{kind}", 1), lambda local, half=half: (0, width // 2 * half), narrow=True)
        if half == 0:
            add(width // TILE_ROWS, ["mixed_1"], ["dh_1"], ("g_o", 1), tall)
    add(ff // TILE_ROWS, ["act_0", "act_1"], ["dx_1", "cot"], ("g_down", None), tall)
    add(ff // TILE_ROWS, ["n_0", "n_1"], ["dpre_0", "dpre_1"], ("g_up", None), wide)
    for kind in "qkv":
        add(width // TILE_ROWS, ["u_0"], [f"d{kind}_0"], (f"g_{kind}", 0), tall)
    add(width // TILE_ROWS, ["mixed_0"], ["dh_0"], ("g_o", 0), tall)
    return groups, sum(group["count"] for group in groups)


def local_operands(x_init, cot_out, w_query, w_key, w_value, w_proj, w_up, w_down):
    batch, seq, width = x_init.shape
    tokens = batch * seq
    at = {"x_0": x_init.reshape(tokens, width), "cot": cot_out.reshape(tokens, width)}
    at.update(wq=w_query, wk=w_key, wv=w_value, wo=w_proj, w_up=w_up, w_down=w_down)
    at.update(front(at, batch, seq))
    return at


def solution(mesh):
    def local_step(x_init, cot_out, w_query, w_key, w_value, w_proj, w_up, w_down):
        batch, seq, width = x_init.shape
        inputs = local_operands(x_init, cot_out, w_query, w_key, w_value, w_proj, w_up, w_down)
        groups, chunks = gradient_groups(width, w_up.shape[1])
        weights = dict(g_q=w_query.shape, g_k=w_key.shape, g_v=w_value.shape, g_o=w_proj.shape, g_up=w_up.shape, g_down=w_down.shape)
        res = finish_backward(inputs, groups, chunks, weights, batch * seq, seq)
        *grads, d_init = deliver([res[name] for name in weights], res["dx_0"])
        return (*grads, d_init.reshape(x_init.shape))

    data_spec = P("data")
    full_spec = P()
    in_specs = (data_spec, data_spec, full_spec, full_spec, full_spec, full_spec, full_spec, full_spec)
    out_specs = (full_spec, full_spec, full_spec, full_spec, full_spec, full_spec, data_spec)
    return jax.shard_map(local_step, mesh=mesh, in_specs=in_specs, out_specs=out_specs, check_vma=False)
```
